32 devices in a mesh: data: 1 (over z), tensor: 32 (over y, x, core).
Axes of the slice: x: 4, y: 4, z: 1, core: 2. Of those that a mesh axis runs over, the one named last changes fastest.
The devices are a block of a 4x4x8 slice.
Arguments:
- x_in: bfloat16 [32, 128, 4096], P('data')
- adapter_ids: int32 [32], P('data')
- gain_attn: float32 [4096], replicated
- gain_mlp: float32 [4096], replicated
- w_q: bfloat16 [4096, 32, 128], P(None, 'tensor')
- w_k: bfloat16 [4096, 32, 128], P(None, 'tensor')
- w_v: bfloat16 [4096, 32, 128], P(None, 'tensor')
- w_o: bfloat16 [32, 128, 4096], P('tensor')
- w_gate: bfloat16 [4096, 11008], P(None, 'tensor')
- w_up: bfloat16 [4096, 11008], P(None, 'tensor')
- w_down: bfloat16 [11008, 4096], P('tensor')
- a_q: bfloat16 [2, 4096, 128], P(None, None, 'tensor')
- b_q: bfloat16 [2, 128, 32, 128], P(None, None, 'tensor')
- a_k: bfloat16 [2, 4096, 128], P(None, None, 'tensor')
- b_k: bfloat16 [2, 128, 32, 128], P(None, None, 'tensor')
- a_v: bfloat16 [2, 4096, 128], P(None, None, 'tensor')
- b_v: bfloat16 [2, 128, 32, 128], P(None, None, 'tensor')
- a_o: bfloat16 [2, 32, 128, 128], P(None, 'tensor')
- b_o: bfloat16 [2, 128, 4096], P(None, None, 'tensor')
- a_gate: bfloat16 [2, 4096, 128], P(None, None, 'tensor')
- b_gate: bfloat16 [2, 128, 11008], P(None, None, 'tensor')
- a_up: bfloat16 [2, 4096, 128], P(None, None, 'tensor')
- b_up: bfloat16 [2, 128, 11008], P(None, None, 'tensor')
- a_down: bfloat16 [2, 11008, 128], P(None, 'tensor')
- b_down: bfloat16 [2, 128, 4096], P(None, None, 'tensor')
Outputs:
- output: bfloat16 [32, 128, 4096], P('data')
All inputs are finite; a program needn't handle non-finite values.
Results may differ from the reference program's by a relative error of at most 0.02.
Values are sent between devices in bfloat16 or wider.
A program may use at most 768 MiB of HBM per device.

```python
import jax
import jax.numpy as jnp
from jax import lax

MODEL_DIM = 4096
FFN_DIM = 11008
NUM_HEADS = 32
KV_HEADS = 32
HEAD_DIM = 128
BATCH = 32
SEQ_LEN = 128
RANK = 128
ADAPTERS = 2
ALPHA = 16
ROPE_BASE = 10000

Q_WIDTH = NUM_HEADS * HEAD_DIM
KV_WIDTH = KV_HEADS * HEAD_DIM
GROUP_SIZE = NUM_HEADS // KV_HEADS
LORA_SCALE = ALPHA / RANK
EPSILON = 1e-5


def draw_ids(key_in):
    key_first, key_second, key_perm = jax.random.split(key_in, 3)
    first_draw = jax.random.randint(key_first, (BATCH,), 0, ADAPTERS)
    second_draw = jax.random.randint(key_second, (BATCH,), 0, ADAPTERS)
    slot_index = jnp.arange(BATCH)
    chosen = jnp.where(slot_index < ADAPTERS, slot_index, jnp.minimum(first_draw, second_draw))
    return jax.random.permutation(key_perm, chosen).astype(jnp.int32)


def setup_inputs(seed: int = 0, part: int = 0) -> dict:
    root_key = jax.random.key(seed)
    key_x, key_ids = jax.random.split(jax.random.fold_in(root_key, part), 2)
    key_list = jax.random.split(root_key, 23)
    b_scale = 0.2 * RANK ** 0.5 / ALPHA

    def normal_bf16(key_in, arr_shape, scale_val):
        return (jax.random.normal(key_in, arr_shape, jnp.float32) * scale_val).astype(jnp.bfloat16)

    return {
        'x_in': normal_bf16(key_x, (BATCH, SEQ_LEN, MODEL_DIM), 1.0),
        'adapter_ids': draw_ids(key_ids),
        'gain_attn': 1.0 + 0.25 * jax.random.normal(key_list[0], (MODEL_DIM,), jnp.float32),
        'gain_mlp': 1.0 + 0.25 * jax.random.normal(key_list[1], (MODEL_DIM,), jnp.float32),
        'w_q': normal_bf16(key_list[2], (MODEL_DIM, NUM_HEADS, HEAD_DIM), 1.6 * MODEL_DIM ** -0.5),
        'w_k': normal_bf16(key_list[3], (MODEL_DIM, KV_HEADS, HEAD_DIM), 1.6 * MODEL_DIM ** -0.5),
        'w_v': normal_bf16(key_list[4], (MODEL_DIM, KV_HEADS, HEAD_DIM), MODEL_DIM ** -0.5),
        'w_o': normal_bf16(key_list[5], (NUM_HEADS, HEAD_DIM, MODEL_DIM), 1.4 * Q_WIDTH ** -0.5),
        'w_gate': normal_bf16(key_list[6], (MODEL_DIM, FFN_DIM), MODEL_DIM ** -0.5),
        'w_up': normal_bf16(key_list[7], (MODEL_DIM, FFN_DIM), MODEL_DIM ** -0.5),
        'w_down': normal_bf16(key_list[8], (FFN_DIM, MODEL_DIM), 1.4 * FFN_DIM ** -0.5),
        'a_q': normal_bf16(key_list[9], (ADAPTERS, MODEL_DIM, RANK), MODEL_DIM ** -0.5),
        'b_q': normal_bf16(key_list[10], (ADAPTERS, RANK, NUM_HEADS, HEAD_DIM), 1.6 * b_scale),
        'a_k': normal_bf16(key_list[11], (ADAPTERS, MODEL_DIM, RANK), MODEL_DIM ** -0.5),
        'b_k': normal_bf16(key_list[12], (ADAPTERS, RANK, KV_HEADS, HEAD_DIM), 1.6 * b_scale),
        'a_v': normal_bf16(key_list[13], (ADAPTERS, MODEL_DIM, RANK), MODEL_DIM ** -0.5),
        'b_v': normal_bf16(key_list[14], (ADAPTERS, RANK, KV_HEADS, HEAD_DIM), b_scale),
        'a_o': normal_bf16(key_list[15], (ADAPTERS, NUM_HEADS, HEAD_DIM, RANK), Q_WIDTH ** -0.5),
        'b_o': normal_bf16(key_list[16], (ADAPTERS, RANK, MODEL_DIM), 1.4 * b_scale),
        'a_gate': normal_bf16(key_list[17], (ADAPTERS, MODEL_DIM, RANK), MODEL_DIM ** -0.5),
        'b_gate': normal_bf16(key_list[18], (ADAPTERS, RANK, FFN_DIM), b_scale),
        'a_up': normal_bf16(key_list[19], (ADAPTERS, MODEL_DIM, RANK), MODEL_DIM ** -0.5),
        'b_up': normal_bf16(key_list[20], (ADAPTERS, RANK, FFN_DIM), b_scale),
        'a_down': normal_bf16(key_list[21], (ADAPTERS, FFN_DIM, RANK), FFN_DIM ** -0.5),
        'b_down': normal_bf16(key_list[22], (ADAPTERS, RANK, MODEL_DIM), 1.4 * b_scale),
    }


def rms_gain(act_in, gain_vec):
    act_f32 = act_in.astype(jnp.float32)
    inv_rms = lax.rsqrt(jnp.mean(act_f32 * act_f32, axis=-1, keepdims=True) + EPSILON)
    return (act_f32 * inv_rms * gain_vec).astype(jnp.bfloat16)


def rope_rotate(head_vals):
    half_dim = HEAD_DIM // 2
    inv_freq = ROPE_BASE ** (-2.0 * jnp.arange(half_dim, dtype=jnp.float32) / HEAD_DIM)
    angle_tab = jnp.arange(SEQ_LEN, dtype=jnp.float32)[:, None] * inv_freq[None, :]
    cos_tab = jnp.cos(angle_tab)[:, None, :]
    sin_tab = jnp.sin(angle_tab)[:, None, :]
    first_half = head_vals[..., :half_dim]
    second_half = head_vals[..., half_dim:]
    return jnp.concatenate([first_half * cos_tab - second_half * sin_tab, second_half * cos_tab + first_half * sin_tab], axis=-1)


def reference(x_in, adapter_ids, gain_attn, gain_mlp, w_q, w_k, w_v, w_o, w_gate, w_up, w_down, a_q, b_q, a_k, b_k, a_v, b_v, a_o, b_o, a_gate, b_gate, a_up, b_up, a_down, b_down):
    flat_q = w_q.reshape(MODEL_DIM, Q_WIDTH)
    flat_k = w_k.reshape(MODEL_DIM, KV_WIDTH)
    flat_v = w_v.reshape(MODEL_DIM, KV_WIDTH)
    flat_o = w_o.reshape(Q_WIDTH, MODEL_DIM)
    causal = jnp.arange(SEQ_LEN)[:, None] >= jnp.arange(SEQ_LEN)[None, :]

    def project(act_in, weight, a_mat, b_mat):
        base_out = jnp.dot(act_in, weight, preferred_element_type=jnp.float32)
        low_rank = jnp.dot(act_in, a_mat, preferred_element_type=jnp.float32).astype(jnp.bfloat16)
        return base_out + LORA_SCALE * jnp.dot(low_rank, b_mat, preferred_element_type=jnp.float32)

    def one_sequence(seq_pair):
        x_seq, adapter = seq_pair
        h_attn = rms_gain(x_seq, gain_attn)
        z_q = project(h_attn, flat_q, a_q[adapter], b_q[adapter].reshape(RANK, Q_WIDTH))
        z_k = project(h_attn, flat_k, a_k[adapter], b_k[adapter].reshape(RANK, KV_WIDTH))
        z_v = project(h_attn, flat_v, a_v[adapter], b_v[adapter].reshape(RANK, KV_WIDTH))
        q_heads = rope_rotate(z_q.reshape(SEQ_LEN, NUM_HEADS, HEAD_DIM)).astype(jnp.bfloat16)
        k_heads = rope_rotate(z_k.reshape(SEQ_LEN, KV_HEADS, HEAD_DIM)).astype(jnp.bfloat16)
        v_heads = z_v.reshape(SEQ_LEN, KV_HEADS, HEAD_DIM).astype(jnp.bfloat16)
        q_group = q_heads.reshape(SEQ_LEN, KV_HEADS, GROUP_SIZE, HEAD_DIM)
        scores = jnp.einsum('skgd,tkd->kgst', q_group.astype(jnp.float32), k_heads.astype(jnp.float32)) * HEAD_DIM ** -0.5
        attn_prob = jax.nn.softmax(jnp.where(causal, scores, -1e30), axis=-1).astype(jnp.bfloat16)
        mixed_out = jnp.einsum('kgst,tkd->skgd', attn_prob.astype(jnp.float32), v_heads.astype(jnp.float32))
        attn_out = mixed_out.astype(jnp.bfloat16).reshape(SEQ_LEN, Q_WIDTH)
        z_o = project(attn_out, flat_o, a_o[adapter].reshape(Q_WIDTH, RANK), b_o[adapter])
        x_mid = (x_seq.astype(jnp.float32) + z_o).astype(jnp.bfloat16)
        h_mlp = rms_gain(x_mid, gain_mlp)
        z_gate = project(h_mlp, w_gate, a_gate[adapter], b_gate[adapter])
        z_up = project(h_mlp, w_up, a_up[adapter], b_up[adapter])
        hidden = (jax.nn.silu(z_gate) * z_up).astype(jnp.bfloat16)
        z_down = project(hidden, w_down, a_down[adapter], b_down[adapter])
        return (x_mid.astype(jnp.float32) + z_down).astype(jnp.bfloat16)

    return lax.map(one_sequence, (x_in, adapter_ids))
```

```python
import functools
import math

import jax
import jax.numpy as jnp
from jax import lax
from jax.experimental import pallas as pl
from jax.experimental.pallas import tpu as pltpu
from jax.sharding import PartitionSpec as P

ALPHA = 16.0
ROPE_BASE = 10000.0
EPSILON = 1e-5
BF = jnp.bfloat16
F32 = jnp.float32
LANE = 128
VMEM_MOST = 67043328
MESH = pl.DeviceIdType.MESH
HBM = pl.BlockSpec(memory_space=pltpu.HBM)
SMEM = pl.BlockSpec(memory_space=pltpu.SMEM)


def round_up(size, unit):
    return (size + unit - 1) // unit * unit


def fit(size, most):
    return max(c for c in range(LANE, most + 1, LANE) if size % c == 0)


class Place:
    def __init__(self, side):
        index = lax.axis_index('tensor')
        self.side = side
        self.core = lax.rem(index, 2)
        chip = index // 2
        self.y, self.x = chip // side, lax.rem(chip, side)

    def device(self, y, x):
        return (lax.rem(y + self.side, self.side) * self.side + lax.rem(x + self.side, self.side)) * 2 + self.core

    def fast(self, part, step):
        return self.device(self.y, self.x + step) if part == 0 else self.device(self.y + step, self.x)

    def slow(self, part, step):
        return self.fast(1 - part, step)

    def sequence(self, part, slow_step, fast_step):
        fast_is_x = part == 0
        dy = jnp.where(fast_is_x, slow_step, fast_step)
        dx = jnp.where(fast_is_x, fast_step, slow_step)
        return self.device(self.y + dy, self.x + dx)

    def barrier(self):
        sem = pltpu.get_barrier_semaphore()
        for part in (0, 1):
            for step in (1, -1):
                pl.semaphore_signal(sem, inc=1, device_id={'tensor': self.fast(part, step)}, device_id_type=MESH)
        pl.semaphore_wait(sem, 4)


def remote(src, dst, send_sem, recv_sem, to):
    return pltpu.make_async_remote_copy(src_ref=src, dst_ref=dst, send_sem=send_sem, recv_sem=recv_sem, device_id={'tensor': to}, device_id_type=MESH)


def gather_messages(place, gbuf, send_sem, recv_sem):
    def message(part, slot):
        sems = (send_sem.at[part, slot], recv_sem.at[part, slot])
        if slot < 4:
            src = (gbuf.at[part, 0, 0], gbuf.at[part, 0, 0], gbuf.at[part, 0, 3, 0], gbuf.at[part, 0, 1, 1])[slot]
            dst = (gbuf.at[part, 0, 3], gbuf.at[part, 0, 1], gbuf.at[part, 0, 2, 0], gbuf.at[part, 0, 2, 1])[slot]
            to = place.fast(part, (1, -1, 1, -1)[slot])
        else:
            j, kind = divmod(slot - 4, 4)
            src = (gbuf.at[part, 0, j], gbuf.at[part, 0, j], gbuf.at[part, 3, j, 0], gbuf.at[part, 1, j, 1])[kind]
            dst = (gbuf.at[part, 3, j], gbuf.at[part, 1, j], gbuf.at[part, 2, j, 0], gbuf.at[part, 2, j, 1])[kind]
            to = place.slow(part, (1, -1, 1, -1)[kind])
        return remote(src, dst, *sems, to)

    return message


GATHER_SLOTS = 20


def gather(message, on_near, on_sides, on_far):
    def start(*slots):
        for slot in slots:
            for part in (0, 1):
                message(part, slot).start()

    def then(part, slot, *nexts):
        message(part, slot).wait_recv()
        for n in nexts:
            message(part, n).start()

    start(0, 1)
    start(4, 5)
    for part in (0, 1):
        then(part, 0, 2, 16, 17)
        then(part, 1, 3, 8, 9)
    for part in (0, 1):
        then(part, 2)
        then(part, 3, 12, 13)
    for part in (0, 1):
        then(part, 4, 6)
        then(part, 5, 7)
    on_near()
    for j in (3, 1, 2):
        for part in (0, 1):
            then(part, 4 + 4 * j, 6 + 4 * j)
            then(part, 5 + 4 * j, 7 + 4 * j)
    on_sides()
    for j in (0, 3, 1, 2):
        for part in (0, 1):
            then(part, 6 + 4 * j)
            then(part, 7 + 4 * j)
    on_far()
    for part in (0, 1):
        for slot in range(GATHER_SLOTS):
            message(part, slot).wait_send()


def gather_scratch(rows, cols):
    return [
        pltpu.VMEM((2, 4, 4, 2, rows, cols), BF),
        pltpu.SemaphoreType.DMA((2, GATHER_SLOTS)),
        pltpu.SemaphoreType.DMA((2, GATHER_SLOTS)),
    ]


def small_gather_kernel(side, own_ref, out_ref, gbuf, send_sem, recv_sem, copy_sem):
    place = Place(side)
    load = pltpu.make_async_copy(own_ref, gbuf.at[:, 0, 0], copy_sem.at[0])
    load.start()
    place.barrier()
    load.wait()
    nothing = lambda: None
    gather(gather_messages(place, gbuf, send_sem, recv_sem), nothing, nothing, nothing)
    stores = []
    for part in (0, 1):
        mine = (place.y, place.x) if part == 0 else (place.x, place.y)
        for ds in range(4):
            for df in range(4):
                slow, fast = lax.rem(mine[0] + ds, side), lax.rem(mine[1] + df, side)
                stores.append(pltpu.make_async_copy(gbuf.at[part, ds, df], out_ref.at[part, slow, fast], copy_sem.at[1]))
    for s in stores:
        s.start()
    for s in stores:
        s.wait()


def small_gather(own, side, collective_id):
    _, _, rows, cols = own.shape
    return pl.pallas_call(
        functools.partial(small_gather_kernel, side),
        out_shape=jax.ShapeDtypeStruct((2, 4, 4, 2, rows, cols), BF),
        in_specs=[HBM],
        out_specs=HBM,
        scratch_shapes=gather_scratch(rows, cols) + [pltpu.SemaphoreType.DMA((2,))],
        compiler_params=pltpu.CompilerParams(collective_id=collective_id, has_side_effects=True, vmem_limit_bytes=VMEM_MOST),
        name='small_gather',
    )(own)


def adapter_of_rows(place, ids_ref, part, ds, shape):
    block = lax.broadcasted_iota(jnp.int32, shape, 0) // (shape[0] // 4)
    chosen = jnp.zeros(shape, jnp.int32)
    for df in range(4):
        chosen = jnp.where(block == df, ids_ref[place.sequence(part, ds, df)], chosen)
    return chosen


def gate_up_kernel(side, adapters, rank, scale, ids_ref, own_ref, wg_own, wg_par, wu_own, wu_par, bg_own, bg_par, bu_own, bu_par, hid_ref,
                   gbuf, send_sem, recv_sem, wg, wu, bg, bu, hid, load_sem, store_sem):
    place = Place(side)
    half = wg_own.shape[1]
    width = gbuf.shape[-1] - 2 * rank
    own_load = pltpu.make_async_copy(own_ref, gbuf.at[:, 0, 0], load_sem.at[0])
    own_load.start()
    loads = []
    for dst, own, par in ((wg, wg_own, wg_par), (wu, wu_own, wu_par), (bg, bg_own, bg_par), (bu, bu_own, bu_par)):
        loads.append(pltpu.make_async_copy(own, dst.at[:, pl.ds(0, half)], load_sem.at[1]))
        loads.append(pltpu.make_async_copy(par, dst.at[:, pl.ds(half, half)], load_sem.at[1]))
    for load in loads:
        load.start()
    place.barrier()
    own_load.wait()
    chunk = fit(2 * half, 256)
    rows = 8 * gbuf.shape[4]

    def unit(part, ds):
        low = gbuf[part, ds, :, :, :, width:].reshape(rows, 2 * rank).astype(F32)
        chosen = adapter_of_rows(place, ids_ref, part, ds, (rows, rank))
        low_g, low_u = (jnp.concatenate([jnp.where(chosen == a, v, 0.0) for a in range(adapters)], axis=1).astype(BF) for v in (low[:, :rank], low[:, rank:]))

        def columns(n, carry):
            at = pl.ds(pl.multiple_of(n * chunk, chunk), chunk)
            act = gbuf[part, ds, :, :, :, :width].reshape(rows, width)
            z_g = jnp.dot(act, wg[:, at], preferred_element_type=F32) + scale * jnp.dot(low_g, bg[:, at], preferred_element_type=F32)
            z_u = jnp.dot(act, wu[:, at], preferred_element_type=F32) + scale * jnp.dot(low_u, bu[:, at], preferred_element_type=F32)
            hid[part, ds, :, at] = (z_g * jax.nn.sigmoid(z_g) * z_u).astype(BF)
            return carry

        lax.fori_loop(0, 2 * half // chunk, columns, 0)
        pltpu.make_async_copy(hid.at[part, ds], hid_ref.at[part, ds], store_sem).start()

    def on_near():
        for load in loads:
            load.wait()
        lax.fori_loop(0, 2, lambda part, c: (unit(part, 0), c)[1], 0)

    def on_sides():
        lax.fori_loop(0, 4, lambda i, c: (unit(lax.rem(i, 2), 1 + 2 * (i // 2)), c)[1], 0)

    def on_far():
        lax.fori_loop(0, 2, lambda part, c: (unit(part, 2), c)[1], 0)

    gather(gather_messages(place, gbuf, send_sem, recv_sem), on_near, on_sides, on_far)
    pltpu.make_async_copy(hid, hid_ref, store_sem).wait()


def gate_up(ids, own, w, side, adapters, rank, scale, collective_id):
    _, _, rows, cols = own.shape
    half = w[0].shape[1]
    depth = w[0].shape[0]
    hidden = jax.ShapeDtypeStruct((2, 4, 8 * rows, 2 * half), BF)
    return pl.pallas_call(
        functools.partial(gate_up_kernel, side, adapters, rank, scale),
        out_shape=hidden,
        in_specs=[SMEM] + [HBM] * 9,
        out_specs=HBM,
        scratch_shapes=gather_scratch(rows, cols) + [
            pltpu.VMEM((depth, 2 * half), BF),
            pltpu.VMEM((depth, 2 * half), BF),
            pltpu.VMEM((adapters * rank, 2 * half), BF),
            pltpu.VMEM((adapters * rank, 2 * half), BF),
            pltpu.VMEM(hidden.shape, BF),
            pltpu.SemaphoreType.DMA((2,)),
            pltpu.SemaphoreType.DMA,
        ],
        compiler_params=pltpu.CompilerParams(collective_id=collective_id, has_side_effects=True, vmem_limit_bytes=VMEM_MOST),
        name='gate_up',
    )(ids, own, *w)


SCATTER_SLOTS = 18


def row_proj_kernel(side, adapters, ids_ref, act_ref, w_own, w_par, a_own, a_par, out_ref,
                    act, w, stage, near, landed, fast_near, fast_landed, send_sem, recv_sem, load_sem):
    place = Place(side)
    half, width = w_own.shape
    rank = a_own.shape[2]
    rows = stage.shape[3]
    quarter = rows // 2
    loads = [pltpu.make_async_copy(act_ref, act, load_sem)]
    for at, w_part, a_part in ((0, w_own, a_own), (half, w_par, a_par)):
        loads.append(pltpu.make_async_copy(w_part, w.at[pl.ds(at, half), pl.ds(0, width)], load_sem))
        for a in range(adapters):
            loads.append(pltpu.make_async_copy(a_part.at[a], w.at[pl.ds(at, half), pl.ds(width + a * rank, rank)], load_sem))
    for load in loads:
        load.start()
    place.barrier()
    for load in loads:
        load.wait()
    chunk = fit(width, 512)

    def unit(part, ds):
        def columns(n, carry):
            at = pl.ds(pl.multiple_of(n * chunk, chunk), chunk)
            sums = jnp.dot(act[part, ds], w[:, at], preferred_element_type=F32)
            stage[part, ds, :, :, at] = sums.reshape(4, rows, chunk).astype(BF)
            return carry

        lax.fori_loop(0, width // chunk, columns, 0)
        low = jnp.dot(act[part, ds], w[:, width:], preferred_element_type=F32)
        chosen = adapter_of_rows(place, ids_ref, part, ds, (4 * rows, rank))
        kept = low[:, :rank]
        for a in range(1, adapters):
            kept = jnp.where(chosen == a, low[:, a * rank:(a + 1) * rank], kept)
        stage[part, ds, :, :, width:] = kept.reshape(4, rows, rank).astype(BF)

    def message(part, slot):
        sems = (send_sem.at[part, slot], recv_sem.at[part, slot])
        lo, hi = pl.ds(0, quarter), pl.ds(quarter, quarter)
        table = (
            (stage.at[part, 2, 2], near.at[part, 0], 's', 1),
            (stage.at[part, 2, 3], near.at[part, 1], 's', 1),
            (stage.at[part, 2, 0], near.at[part, 2], 's', -1),
            (stage.at[part, 2, 1], near.at[part, 3], 's', -1),
            (stage.at[part, 1, 0], landed.at[part, 0, 0], 's', 1),
            (stage.at[part, 1, 1], landed.at[part, 0, 1], 's', 1),
            (stage.at[part, 3, 2], landed.at[part, 1, 2], 's', -1),
            (stage.at[part, 3, 3], landed.at[part, 1, 3], 's', -1),
            (stage.at[part, 1, 2], landed.at[part, 0, 2], 's', 1),
            (stage.at[part, 1, 3], landed.at[part, 0, 3], 's', 1),
            (stage.at[part, 3, 0], landed.at[part, 1, 0], 's', -1),
            (stage.at[part, 3, 1], landed.at[part, 1, 1], 's', -1),
            (stage.at[part, 0, 2, lo], fast_near.at[part, 0], 'f', 1),
            (stage.at[part, 0, 2, hi], fast_near.at[part, 1], 'f', -1),
            (stage.at[part, 0, 1, hi], fast_landed.at[part, 0, hi], 'f', 1),
            (stage.at[part, 0, 3, lo], fast_landed.at[part, 1, lo], 'f', -1),
            (stage.at[part, 0, 1, lo], fast_landed.at[part, 0, lo], 'f', 1),
            (stage.at[part, 0, 3, hi], fast_landed.at[part, 1, hi], 'f', -1),
        )
        src, dst, ring, step = table[slot]
        return remote(src, dst, *sems, place.slow(part, step) if ring == 's' else place.fast(part, step))

    def add(into, *others):
        def some(i, carry):
            at = pl.ds(pl.multiple_of(i * 16, 16), 16)
            total = into[at, :].astype(F32)
            for other in others:
                total += other[at, :].astype(F32)
            into[at, :] = total.astype(BF)
            return carry

        lax.fori_loop(0, into.shape[0] // 16, some, 0)

    def start(slot, parts=(0, 1)):
        for part in parts:
            message(part, slot).start()

    def arrived(slot, parts=(0, 1)):
        for part in parts:
            message(part, slot).wait_recv()

    for part in (0, 1):
        unit(part, 2)
        for slot in (0, 2, 1, 3):
            start(slot, (part,))
    lax.fori_loop(0, 4, lambda i, c: (unit(lax.rem(i, 2), 1 + 2 * (i // 2)), c)[1], 0)
    for slot in (4, 6, 5, 7):
        start(slot)
    lax.fori_loop(0, 2, lambda part, c: (unit(part, 0), c)[1], 0)
    for near_slot, ds, df, slot in ((0, 1, 2, 8), (2, 3, 0, 10), (1, 1, 3, 9), (3, 3, 1, 11)):
        for part in (0, 1):
            arrived(near_slot, (part,))
            add(stage.at[part, ds, df], near.at[part, near_slot])
            start(slot, (part,))
    for df, slots, nexts in ((2, (6, 8), (12, 13)), (0, (4, 10), ()), (3, (7, 9), (15,)), (1, (5, 11), (14,))):
        for part in (0, 1):
            for slot in slots:
                arrived(slot, (part,))
            add(stage.at[part, 0, df], landed.at[part, 0, df], landed.at[part, 1, df])
            for slot in nexts:
                start(slot, (part,))
    for part in (0, 1):
        arrived(12, (part,))
        add(stage.at[part, 0, 1, pl.ds(0, quarter)], fast_near.at[part, 0])
        start(16, (part,))
        arrived(13, (part,))
        add(stage.at[part, 0, 3, pl.ds(quarter, quarter)], fast_near.at[part, 1])
        start(17, (part,))
    for part in (0, 1):
        for slot in (14, 15, 16, 17):
            arrived(slot, (part,))
        add(stage.at[part, 0, 0], fast_landed.at[part, 0], fast_landed.at[part, 1])
    out = [pltpu.make_async_copy(stage.at[part, 0, 0], out_ref.at[pl.ds(part * rows, rows)], load_sem) for part in (0, 1)]
    for copy in out:
        copy.start()
    for copy in out:
        copy.wait()
    for part in (0, 1):
        for slot in range(SCATTER_SLOTS):
            message(part, slot).wait_send()


def row_proj(ids, act, w_own, w_par, a_own, a_par, side, collective_id):
    adapters, _, rank = a_own.shape
    half, width = w_own.shape
    rows = act.shape[2] // 4
    cols = width + rank
    return pl.pallas_call(
        functools.partial(row_proj_kernel, side, adapters),
        out_shape=jax.ShapeDtypeStruct((2 * rows, cols), BF),
        in_specs=[SMEM] + [HBM] * 5,
        out_specs=HBM,
        scratch_shapes=[
            pltpu.VMEM(act.shape, BF),
            pltpu.VMEM((2 * half, width + adapters * rank), BF),
            pltpu.VMEM((2, 4, 4, rows, cols), BF),
            pltpu.VMEM((2, 4, rows, cols), BF),
            pltpu.VMEM((2, 2, 4, rows, cols), BF),
            pltpu.VMEM((2, 2, rows // 2, cols), BF),
            pltpu.VMEM((2, 2, rows, cols), BF),
            pltpu.SemaphoreType.DMA((2, SCATTER_SLOTS)),
            pltpu.SemaphoreType.DMA((2, SCATTER_SLOTS)),
            pltpu.SemaphoreType.DMA,
        ],
        compiler_params=pltpu.CompilerParams(collective_id=collective_id, has_side_effects=True, vmem_limit_bytes=VMEM_MOST),
        name='row_proj',
    )(ids, act, w_own, w_par, a_own, a_par)


def qkv_kernel(where_ref, ids_ref, xa_ref, xb_ref, gain_ref, at_ref, *rest):
    weights, (z_ref, low_ref, w, h, sem) = rest[:6], rest[6:]
    step = pl.program_id(0)
    head = weights[0].shape[1]
    seq_len = xa_ref.shape[1]

    @pl.when(step == 0)
    def _():
        copies = [pltpu.make_async_copy(weights[i], w.at[:, pl.ds(i * head, head)], sem) for i in range(6)]
        for c in copies:
            c.start()
        for c in copies:
            c.wait()

    for i, x_ref in enumerate((xa_ref, xb_ref)):
        act = x_ref[0].astype(F32)
        inv_rms = lax.rsqrt(jnp.mean(act * act, axis=-1, keepdims=True) + EPSILON)
        h[i * seq_len:(i + 1) * seq_len, :] = (act * inv_rms * gain_ref[...]).astype(BF)
    chunk = fit(6 * head, 256)
    for n in range(6 * head // chunk):
        z_ref[:, n * chunk:(n + 1) * chunk] = jnp.dot(h[...], w[:, n * chunk:(n + 1) * chunk], preferred_element_type=F32)
    low = lax.dot_general(at_ref[...], h[...], (((1,), (1,)), ((), ())), preferred_element_type=F32)
    adapters = at_ref.shape[0] // 32
    pieces = []
    for i in range(2):
        chosen = ids_ref[2 * step + i]
        piece = low[:32, i * seq_len:(i + 1) * seq_len]
        for a in range(1, adapters):
            piece = jnp.where(chosen == a, low[32 * a:32 * (a + 1), i * seq_len:(i + 1) * seq_len], piece)
        pieces.append(piece)
    low_sel = jnp.concatenate(pieces, axis=1).astype(BF)
    low_ref[0, 0] = low_sel[:16]
    low_ref[1, 0] = low_sel[16:]


def qkv(where, plane_ids, x_in, gain, a_rows, weights):
    depth = x_in.shape[2]
    seq_len = x_in.shape[1]
    head = weights[0].shape[1]
    seqs = x_in.shape[0] // 2
    steps = seqs // 2
    grid_spec = pltpu.PrefetchScalarGridSpec(
        num_scalar_prefetch=2,
        grid=(steps,),
        in_specs=[
            pl.BlockSpec((1, seq_len, depth), lambda i, where, ids: (4 * i + where[0], 0, 0)),
            pl.BlockSpec((1, seq_len, depth), lambda i, where, ids: (4 * i + 2 + where[0], 0, 0)),
            pl.BlockSpec((1, depth), lambda i, where, ids: (0, 0)),
            pl.BlockSpec(a_rows.shape, lambda i, where, ids: (0, 0)),
        ] + [HBM] * 6,
        out_specs=[
            pl.BlockSpec((2 * seq_len, 6 * head), lambda i, where, ids: (i, 0)),
            pl.BlockSpec((2, 1, 16, 2 * seq_len), lambda i, where, ids: (0, i // (steps // 2), 0, lax.rem(i, steps // 2))),
        ],
        scratch_shapes=[pltpu.VMEM((depth, 6 * head), BF), pltpu.VMEM((2 * seq_len, depth), BF), pltpu.SemaphoreType.DMA],
    )
    tokens = seqs * seq_len
    return pl.pallas_call(
        qkv_kernel,
        grid_spec=grid_spec,
        out_shape=[jax.ShapeDtypeStruct((tokens, 6 * head), F32), jax.ShapeDtypeStruct((2, 2, 16, tokens // 2), BF)],
        compiler_params=pltpu.CompilerParams(dimension_semantics=('arbitrary',), vmem_limit_bytes=VMEM_MOST),
        cost_estimate=pl.CostEstimate(flops=2 * tokens * depth * 7 * head, bytes_accessed=2 * tokens * depth * 2, transcendentals=0),
        name='qkv',
    )(where, plane_ids, x_in, x_in, gain.reshape(1, depth), a_rows, *weights)


def attention_kernel(scale, where_ref, ids_ref, z_ref, low_ref, bqk_ref, bv_ref, cos_ref, sin_ref, out_a_ref, out_b_ref):
    head = cos_ref.shape[1]
    seq_len = z_ref.shape[0]
    c = where_ref[1 + pl.program_id(0)]
    adapter = ids_ref[c]
    parts = [low_ref[p, :, 0].reshape(-1, seq_len) for p in (0, 1)]
    across = (((0,), (0,)), ((), ()))
    z_qk = z_ref[:, :4 * head] + scale * lax.dot_general(parts[0], bqk_ref[adapter], across, preferred_element_type=F32)
    z_v = z_ref[:, 4 * head:] + scale * lax.dot_general(parts[1], bv_ref[adapter], across, preferred_element_type=F32)
    cos, sin = cos_ref[...], sin_ref[...]
    rotated = []
    for i in range(4):
        z = z_qk[:, i * head:(i + 1) * head]
        rotated.append((z * cos + pltpu.roll(z, head // 2, axis=1) * sin).astype(BF))
    values = z_v.astype(BF)
    causal = lax.broadcasted_iota(jnp.int32, (seq_len, seq_len), 0) >= lax.broadcasted_iota(jnp.int32, (seq_len, seq_len), 1)
    for i in range(2):
        scores = lax.dot_general(rotated[i], rotated[2 + i], (((1,), (1,)), ((), ())), preferred_element_type=F32) * head ** -0.5
        scores = jnp.where(causal, scores, -1e30)
        e = jnp.exp(scores - jnp.max(scores, axis=-1, keepdims=True))
        prob = (e / jnp.sum(e, axis=-1, keepdims=True)).astype(BF)
        mixed = jnp.dot(prob, values[:, i * head:(i + 1) * head], preferred_element_type=F32).astype(BF)
        out_a_ref[0, :, i * head:(i + 1) * head] = mixed[:seq_len // 2]
        out_b_ref[0, :, i * head:(i + 1) * head] = mixed[seq_len // 2:]


def attention(where, plane_ids, z, low, b_qk, b_v, scale):
    tokens, cols = z.shape
    head = cols // 6
    chips = 16
    seq_len = tokens // chips
    half_dim = head // 2
    inv_freq = ROPE_BASE ** (-2.0 * jnp.arange(half_dim, dtype=F32) / head)
    angle = jnp.arange(seq_len, dtype=F32)[:, None] * inv_freq[None, :]
    cos = jnp.concatenate([jnp.cos(angle)] * 2, axis=1)
    sin = jnp.concatenate([-jnp.sin(angle), jnp.sin(angle)], axis=1)
    whole = lambda a: pl.BlockSpec(a.shape, lambda i, where, ids: (0,) * a.ndim)
    chip_of = lambda i, where: where[1 + i]
    grid_spec = pltpu.PrefetchScalarGridSpec(
        num_scalar_prefetch=2,
        grid=(chips,),
        in_specs=[
            pl.BlockSpec((seq_len, cols), lambda i, where, ids: (chip_of(i, where), 0)),
            pl.BlockSpec((2, chips, 1, 16, seq_len), lambda i, where, ids: (0, 0, chip_of(i, where) // (chips // 2), 0, lax.rem(chip_of(i, where), chips // 2))),
            whole(b_qk), whole(b_v), whole(cos), whole(sin),
        ],
        out_specs=[
            pl.BlockSpec((1, seq_len // 2, 2 * head), lambda i, where, ids: (i, 0, 0)),
            pl.BlockSpec((1, seq_len // 2, 2 * head), lambda i, where, ids: (lax.rem(i, 4) * 4 + i // 4, 0, 0)),
        ],
    )
    one = jax.ShapeDtypeStruct((chips, seq_len // 2, 2 * head), BF)
    return pl.pallas_call(
        functools.partial(attention_kernel, scale),
        grid_spec=grid_spec,
        out_shape=[one, one],
        compiler_params=pltpu.CompilerParams(dimension_semantics=('arbitrary',), vmem_limit_bytes=VMEM_MOST),
        cost_estimate=pl.CostEstimate(flops=16 * tokens * head * head, bytes_accessed=tokens * cols * 4, transcendentals=tokens * seq_len * 2),
        name='attention',
    )(where, plane_ids, z, low.reshape(2, chips, 2, 16, tokens // 2), b_qk, b_v, cos, sin)


def solution(mesh):
    tp_size = mesh.shape['tensor']
    side = math.isqrt(tp_size // 2)
    partner = [(i, i ^ 1) for i in range(tp_size)]
    head_split = P(None, 'tensor', None)
    last_split = P(None, None, 'tensor')
    b_head_split = P(None, None, 'tensor', None)
    in_specs = (P('data', None, None), P('data'), P(None), P(None),
                head_split, head_split, head_split, P('tensor', None, None),
                P(None, 'tensor'), P(None, 'tensor'), P('tensor', None),
                last_split, b_head_split, last_split, b_head_split, last_split, b_head_split,
                P(None, 'tensor', None, None), last_split,
                last_split, last_split, last_split, last_split,
                P(None, 'tensor', None), last_split)

    def local_layer(x_in, adapter_ids, gain_attn, gain_mlp, w_q, w_k, w_v, w_o, w_gate, w_up, w_down, a_q, b_q, a_k, b_k, a_v, b_v, a_o, b_o, a_gate, b_gate, a_up, b_up, a_down, b_down):
        depth = x_in.shape[2]
        seq_len = x_in.shape[1]
        adapters, rank = b_q.shape[0], b_q.shape[1]
        scale = ALPHA / rank
        index = lax.axis_index('tensor')
        core = lax.rem(index, 2)
        my_y, my_x = index // 2 // side, lax.rem(index // 2, side)

        def other(a):
            return lax.ppermute(a, 'tensor', partner)

        plane_ids = lax.dynamic_index_in_dim(adapter_ids.reshape(-1, 2), core, axis=1, keepdims=False)
        steps = jnp.arange(side)
        chips = (lax.rem(my_y + steps, side)[:, None] * side + lax.rem(my_x + steps, side)[None, :]).reshape(-1)
        where = jnp.concatenate([core[None], chips]).astype(jnp.int32)

        own_qkv = [w_q[:, 0], w_k[:, 0], w_v[:, 0]]
        par_qkv = [other(w) for w in own_qkv]
        own_a = jnp.stack([a.swapaxes(1, 2) for a in (a_q, a_k, a_v)], axis=1)
        par_a = other(own_a)
        first = jnp.where(core == 0, own_a, par_a)
        second = jnp.where(core == 0, par_a, own_a)
        a_rows = jnp.concatenate([first, second], axis=2)
        a_rows = jnp.pad(a_rows, ((0, 0), (0, 1), (0, 0), (0, 0))).reshape(adapters * 32, depth)
        z, low = qkv(where, plane_ids, x_in, gain_attn, a_rows, [w for pair in zip(own_qkv, par_qkv) for w in pair])

        def both_heads(b):
            return jnp.concatenate([b[:, :, 0], other(b)[:, :, 0]], axis=-1).reshape(adapters, side * side, 8, -1)

        bq2, bk2, bv2 = both_heads(b_q), both_heads(b_k), both_heads(b_v)
        blank = jnp.zeros_like(bq2)
        b_qk = jnp.concatenate([jnp.concatenate([bq2, blank], axis=-1), jnp.concatenate([blank, bk2], axis=-1)], axis=2).reshape(adapters, 2 * rank, -1)
        bv2 = bv2.reshape(adapters, side, side, 8, -1).swapaxes(1, 2).reshape(bv2.shape)
        b_v2 = jnp.concatenate([bv2, blank], axis=2).reshape(adapters, 2 * rank, -1)
        low_all = small_gather(low, side, 0)
        attn_a, attn_b = attention(where, plane_ids, z, low_all, b_qk, b_v2, scale)
        attn = jnp.stack([attn_a, attn_b]).reshape(2, 4, 4 * (seq_len // 2), -1)

        my_id = adapter_ids[index]

        def pick(a):
            return lax.dynamic_index_in_dim(a, my_id, axis=0, keepdims=False)

        full_b = lax.all_gather(jnp.stack([b_o, b_down], axis=1), 'tensor', axis=0)
        full_a = lax.all_gather(jnp.stack([a_gate.swapaxes(1, 2), a_up.swapaxes(1, 2)], axis=1), 'tensor', axis=0)
        my_b = lax.dynamic_index_in_dim(full_b, my_id, axis=1, keepdims=False)
        my_a = lax.dynamic_index_in_dim(full_a, my_id, axis=1, keepdims=False)

        def finish(sums, b_mine, resid):
            base, low_rank = sums[:, :depth].astype(F32), sums[:, depth:]
            delta = jnp.einsum('sr,jrc->sjc', low_rank, b_mine, preferred_element_type=F32).reshape(seq_len, depth)
            return (resid.astype(F32) + (base + scale * delta)).astype(BF)

        x_own = lax.dynamic_index_in_dim(x_in, index, axis=0, keepdims=False)
        a_o2 = a_o[:, 0]
        sums = row_proj(adapter_ids, attn, w_o[0], other(w_o[0]), a_o2, other(a_o2), side, 1)
        x_mid = finish(sums, my_b[:, 0], x_own)
        mid_f32 = x_mid.astype(F32)
        h_mlp = (mid_f32 * lax.rsqrt(jnp.mean(mid_f32 * mid_f32, axis=-1, keepdims=True) + EPSILON) * gain_mlp).astype(BF)
        low_gu = jnp.einsum('sd,jprd->spjr', h_mlp, my_a, preferred_element_type=F32).astype(BF).reshape(seq_len, 2 * rank)
        payload = jnp.concatenate([h_mlp, low_gu], axis=1).reshape(2, 2, seq_len // 4, depth + 2 * rank)

        ffn = w_gate.shape[1]
        half = round_up(ffn, LANE)
        pad_cols = lambda w: jnp.pad(w, ((0, 0),) * (w.ndim - 1) + ((0, half - ffn),))
        gate_up_w = []
        for w in (w_gate, w_up, b_gate.reshape(adapters * rank, ffn), b_up.reshape(adapters * rank, ffn)):
            w = pad_cols(w)
            gate_up_w += [w, other(w)]
        hidden = gate_up(adapter_ids, payload, gate_up_w, side, adapters, rank, scale, 2)
        w_d = jnp.pad(w_down, ((0, half - ffn), (0, 0)))
        a_d = jnp.pad(a_down, ((0, 0), (0, half - ffn), (0, 0)))
        sums = row_proj(adapter_ids, hidden, w_d, other(w_d), a_d, other(a_d), side, 3)
        y_own = finish(sums, my_b[:, 1], x_mid)
        return lax.all_gather(y_own, 'tensor', axis=0)

    return jax.shard_map(local_layer, mesh=mesh, in_specs=in_specs, out_specs=P('data', None, None), check_vma=False)
```

```python
import functools
import math

import jax
import jax.numpy as jnp
import numpy as np
from jax import lax
from jax.experimental import pallas as pl
from jax.experimental.pallas import tpu as pltpu
from jax.sharding import PartitionSpec as P

ALPHA = 16.0
ROPE_BASE = 10000.0
EPSILON = 1e-5
BF = jnp.bfloat16
F32 = jnp.float32
LANE = 128
TILE = 16
VMEM_MOST = 67043328
MESH = pl.DeviceIdType.MESH
HBM = pl.BlockSpec(memory_space=pltpu.HBM)
VMEM = pl.BlockSpec(memory_space=pltpu.VMEM)
SMEM = pl.BlockSpec(memory_space=pltpu.SMEM)
DMA = pltpu.SemaphoreType.DMA

OWN, NEXT, FAR, LAST = RING = range(4)
UP, DOWN = BOTH = range(2)
STEP = (NEXT, -NEXT)
FROM = (LAST, NEXT)
TOWARD = (NEXT, LAST)
FAST, SLOW = BOTH


def fit(size, most):
    return max(c for c in range(LANE, most + 1, LANE) if size % c == 0)


def first(size):
    return pl.ds(0, size)


def dot(a, b):
    return jnp.dot(a, b, preferred_element_type=F32)


def dot_rows(a, b):
    return lax.dot_general(a, b, (((1,), (1,)), ((), ())), preferred_element_type=F32)


def dot_columns(a, b):
    return lax.dot_general(a, b, (((0,), (0,)), ((), ())), preferred_element_type=F32)


def normed(act, gain):
    return (act * lax.rsqrt(jnp.mean(act * act, axis=-1, keepdims=True) + EPSILON) * gain).astype(BF)


def ends(copies):
    for copy in copies:
        copy.start()
    return copies


def wait(copies):
    for copy in copies:
        copy.wait()


def loop(count, body):
    lax.fori_loop(0, count, lambda i, carry: (body(i), carry)[1], 0)


class Place:
    def __init__(self, side):
        index = lax.axis_index('tensor')
        self.side = side
        self.core = lax.rem(index, 2)
        chip = index // 2
        self.y, self.x = chip // side, lax.rem(chip, side)
        self.partner = index + 1 - 2 * self.core

    def turn(self, at, steps):
        return lax.rem(at + steps + self.side, self.side)

    def device(self, dy, dx):
        return (self.turn(self.y, dy) * self.side + self.turn(self.x, dx)) * 2 + self.core

    def neighbour(self, part, ring, step):
        return self.device(0, step) if part == ring else self.device(step, 0)

    def sequence(self, part, ds, df):
        return self.device(jnp.where(part == 0, ds, df), jnp.where(part == 0, df, ds))

    def barrier(self, *more):
        sem = pltpu.get_barrier_semaphore()
        to = [self.neighbour(0, ring, step) for ring in BOTH for step in STEP] + list(more)
        for device in to:
            pl.semaphore_signal(sem, inc=1, device_id={'tensor': device}, device_id_type=MESH)
        pl.semaphore_wait(sem, len(to))


def remote(src, dst, send_sem, recv_sem, to):
    return pltpu.make_async_remote_copy(src_ref=src, dst_ref=dst, send_sem=send_sem, recv_sem=recv_sem, device_id={'tensor': to}, device_id_type=MESH)


GATHER_SEMS = [DMA((2, 2, 2, 2, 4))] * 2


def gather(place, block, send_sem, recv_sem, absolute=False, seen=None, on_near=None, on_sides=None, on_far=None):
    def message(part, ring, passed, d, j=OWN):
        spot = (lambda s: (s, j)) if ring == SLOW else (lambda s: (OWN, s))
        src, dst = (FROM[d], FAR) if passed else (OWN, FROM[d])
        a, b = block(part, *spot(src)), block(part, *spot(src if absolute else dst))
        if passed:
            a, b = a.at[d], b.at[d]
        sems = (part, ring, passed, d, j)
        return remote(a, b, send_sem.at[sems], recv_sem.at[sems], place.neighbour(part, ring, STEP[d]))

    def start(*which):
        for d in BOTH:
            for part in BOTH:
                message(part, *which[:2], d, *which[2:]).start()

    def arrived(part, ring, passed, d, j=OWN):
        message(part, ring, passed, d, j).wait_recv()
        if seen:
            at = FAR if passed else FROM[d]
            seen(part, *((at, j) if ring == SLOW else (OWN, at)), d if passed else None)

    start(FAST, 0)
    start(SLOW, 0, OWN)
    for d in BOTH:
        for part in BOTH:
            arrived(part, FAST, 0, d)
            message(part, FAST, 1, d).start()
            for e in BOTH:
                message(part, SLOW, 0, e, FROM[d]).start()
    for part in BOTH:
        for d in BOTH:
            arrived(part, FAST, 1, d)
        for e in BOTH:
            message(part, SLOW, 0, e, FAR).start()

    def pass_on(j):
        for part in BOTH:
            for d in BOTH:
                arrived(part, SLOW, 0, d, j)
                message(part, SLOW, 1, d, j).start()

    order = (OWN,) + FROM + (FAR,)
    pass_on(OWN)
    if on_near:
        on_near()
    for j in order[1:]:
        pass_on(j)
    if on_sides:
        on_sides()
    for j in order:
        for part in BOTH:
            for d in BOTH:
                arrived(part, SLOW, 1, d, j)
    if on_far:
        on_far()
    for part in BOTH:
        for d in BOTH:
            for passed in BOTH:
                message(part, FAST, passed, d).wait_send()
                for j in RING:
                    message(part, SLOW, passed, d, j).wait_send()


def rows_of_adapter(place, ids_ref, part, ds, shape):
    block = lax.broadcasted_iota(jnp.int32, shape, 0) // (shape[0] // len(RING))
    chosen = jnp.zeros(shape, jnp.int32)
    for df in RING:
        chosen = jnp.where(block == df, ids_ref[place.sequence(part, ds, df)], chosen)
    return chosen


def spread(low, chosen, adapters):
    return jnp.concatenate([jnp.where(chosen == a, low, 0.0) for a in range(adapters)], axis=1).astype(BF)


def comm_params(collective_id):
    return pltpu.CompilerParams(collective_id=collective_id, has_side_effects=True, vmem_limit_bytes=VMEM_MOST)


def attend_kernel(side, adapters, scale, n_keep, ids_ref, x_ref, gain_ref, cos_ref, sin_ref, *rest):
    heads, rest = rest[:5], rest[5:]
    given, rest = rest[:n_keep], rest[n_keep:]
    att_ref, rest = rest[0], rest[1:]
    kept, rest = rest[:n_keep], rest[n_keep:]
    w, a_rows, bx, xbuf, h, z, lows, att, pair_send, pair_recv, load_sem, x_sem, send_sem, recv_sem = rest
    place = Place(side)
    head, seq_len, depth = cos_ref.shape[1], x_ref.shape[1], x_ref.shape[2]
    cols = heads[4].shape[-1]
    chips = side * side
    a_own = a_rows.at[pl.ds(pl.multiple_of(place.core * 2 * TILE, TILE), 2 * TILE)]
    spots = [[w.at[:, pl.ds(at + i * head, head)] for i in range(3)] + [a_own, bx.at[:, :, :, pl.ds(at, cols)]] for at in (0, cols)]
    loads = [pltpu.make_async_copy(src, dst, load_sem) for src, dst in zip(heads, spots[0])]
    ends(loads)

    def x_loads(step):
        slot = lax.rem(step, 2)
        return [pltpu.make_async_copy(x_ref.at[4 * step + 2 * i + place.core], xbuf.at[slot, i], x_sem.at[slot]) for i in BOTH]

    ends(x_loads(0))
    place.barrier(place.partner)
    moves = list(zip(heads, spots[1][:3] + [a_own] + spots[1][4:])) + list(zip(given, kept))
    pair = [remote(src, dst, pair_send.at[i], pair_recv.at[i], place.partner) for i, (src, dst) in enumerate(moves)]
    ends(pair)
    wait(loads)
    for copy in pair[:len(heads)]:
        copy.wait_recv()
    mine = [(place.y, place.x), (place.x, place.y)]
    steps = chips // 2

    def block(part, ds, df):
        return lows.at[part, place.turn(mine[part][0], ds), place.turn(mine[part][1], df)]

    def project(step):
        slot = lax.rem(step, 2)

        @pl.when(step + 1 < steps)
        def _():
            ends(x_loads(step + 1))

        wait(x_loads(step))
        for i in BOTH:
            h[i * seq_len:(i + 1) * seq_len, :] = normed(xbuf[slot, i].astype(F32), gain_ref[...])
        rows = pl.ds(pl.multiple_of(step * 2 * seq_len, LANE), 2 * seq_len)
        chunk = fit(2 * cols, 256)
        for n in range(2 * cols // chunk):
            z[rows, n * chunk:(n + 1) * chunk] = dot(h[...], w[:, n * chunk:(n + 1) * chunk])
        low = dot_rows(a_rows[...], h[...])
        half, at = step // (steps // 2), lax.rem(step, steps // 2) * 2 * seq_len
        for part in BOTH:
            pieces = []
            for i in BOTH:
                options = [low[TILE * (2 * part + a):TILE * (2 * part + a + 1), i * seq_len:(i + 1) * seq_len] for a in range(adapters)]
                piece = options[0]
                for a in range(1, adapters):
                    piece = jnp.where(ids_ref[4 * step + 2 * i + place.core] == a, options[a], piece)
                pieces.append(piece)
            lows[part, mine[part][0], mine[part][1], half, :, pl.ds(pl.multiple_of(at, LANE), 2 * seq_len)] = jnp.concatenate(pieces, axis=1).astype(BF)

    loop(steps, project)
    gather(place, block, send_sem, recv_sem, absolute=True)
    causal = lax.broadcasted_iota(jnp.int32, (seq_len, seq_len), 0) >= lax.broadcasted_iota(jnp.int32, (seq_len, seq_len), 1)

    def attention(i):
        dy, dx = i // side, lax.rem(i, side)
        chip = place.turn(place.y, dy) * side + place.turn(place.x, dx)
        adapter = ids_ref[2 * chip + place.core]
        half, at = chip // steps, pl.ds(pl.multiple_of(lax.rem(chip, steps) * seq_len, LANE), seq_len)
        zs = z[pl.ds(pl.multiple_of(chip * seq_len, LANE), seq_len), :]
        for part in BOTH:
            zs += scale * dot_columns(lows[part, :, :, half, :, at].reshape(-1, seq_len), bx[adapter, part])
        for i_head in BOTH:
            q, k, v = (zs[:, i_head * cols + i * head:i_head * cols + (i + 1) * head] for i in range(3))
            q, k = ((r * cos_ref[...] + pltpu.roll(r, head // 2, axis=1) * sin_ref[...]).astype(BF) for r in (q, k))
            scores = jnp.where(causal, dot_rows(q, k) * head ** -0.5, -1e30)
            e = jnp.exp(scores - jnp.max(scores, axis=-1, keepdims=True))
            prob = (e / jnp.sum(e, axis=-1, keepdims=True)).astype(BF)
            mixed = dot(prob, v.astype(BF)).astype(BF)
            for part, spot in enumerate((i, dx * side + dy)):
                att[part, spot, :, i_head * head:(i_head + 1) * head] = mixed[part * seq_len // 2:(part + 1) * seq_len // 2]

    loop(chips, attention)
    wait(ends([pltpu.make_async_copy(att, att_ref, load_sem)]))
    for copy in pair[len(heads):]:
        copy.wait_recv()
    for copy in pair:
        copy.wait_send()


def attend(ids, x_in, gain, heads, given, side, adapters, scale, collective_id):
    _, seq_len, depth = x_in.shape
    head, cols = heads[0].shape[1], heads[4].shape[-1]
    chips = side * side
    half_dim = head // 2
    inv_freq = ROPE_BASE ** (-2.0 * np.arange(half_dim) / head)
    angle = np.arange(seq_len)[:, None] * inv_freq[None, :]
    cos, sin = np.cos(angle), np.sin(angle)
    tables = [jnp.asarray(np.concatenate(pair, axis=1), F32) for pair in ((cos, cos), (-sin, sin))]
    att = jax.ShapeDtypeStruct((2, chips, seq_len // 2, 2 * head), BF)
    n_moves = len(heads) + len(given)
    return pl.pallas_call(
        functools.partial(attend_kernel, side, adapters, scale, len(given)),
        out_shape=[att] + [jax.ShapeDtypeStruct(g.shape, g.dtype) for g in given],
        in_specs=[SMEM, HBM, VMEM, VMEM, VMEM] + [HBM] * n_moves,
        out_specs=[HBM] * (1 + len(given)),
        scratch_shapes=[
            pltpu.VMEM((depth, 2 * cols), BF),
            pltpu.VMEM((2 * 2 * TILE, depth), BF),
            pltpu.VMEM(heads[4].shape[:3] + (2 * cols,), BF),
            pltpu.VMEM((2, 2, seq_len, depth), BF),
            pltpu.VMEM((2 * seq_len, depth), BF),
            pltpu.VMEM((chips * seq_len, 2 * cols), F32),
            pltpu.VMEM((2, side, side, 2, TILE, chips * seq_len // 2), BF),
            pltpu.VMEM(att.shape, BF),
            DMA((n_moves,)), DMA((n_moves,)), DMA, DMA((2,)),
        ] + GATHER_SEMS,
        compiler_params=comm_params(collective_id),
        name='attend',
    )(ids, x_in, gain.reshape(1, depth), *tables, *heads, *given)


def row_proj_kernel(side, adapters, ids_ref, act_ref, w_own, w_par, a_own, a_par, out_ref,
                    act, w, stage, near, landed, fast_near, fast_landed, slow_send, slow_recv, fast_send, fast_recv, load_sem):
    place = Place(side)
    share, width = w_own.shape
    half = w.shape[0] // 2
    rank = a_own.shape[2]
    rows = stage.shape[3]
    quarter = rows // 2
    if share < half:
        for at in (0, half):
            w[at + share // TILE * TILE:at + half, :] = jnp.zeros((half - share // TILE * TILE, w.shape[1]), BF)
    loads = [pltpu.make_async_copy(act_ref, act, load_sem)]
    for at, w_part, a_part in ((0, w_own, a_own), (half, w_par, a_par)):
        loads.append(pltpu.make_async_copy(w_part, w.at[pl.ds(at, share), first(width)], load_sem))
        for a in range(adapters):
            loads.append(pltpu.make_async_copy(a_part.at[a], w.at[pl.ds(at, share), pl.ds(width + a * rank, rank)], load_sem))
    ends(loads)
    place.barrier()
    wait(loads)
    chunk = fit(width, 512)

    def unit(part, ds):
        def columns(n):
            at = pl.ds(pl.multiple_of(n * chunk, chunk), chunk)
            stage[part, ds, :, :, at] = dot(act[part, ds], w[:, at]).reshape(len(RING), rows, chunk).astype(BF)

        loop(width // chunk, columns)
        low = dot(act[part, ds], w[:, width:])
        chosen = rows_of_adapter(place, ids_ref, part, ds, (len(RING) * rows, rank))
        kept = low[:, :rank]
        for a in range(1, adapters):
            kept = jnp.where(chosen == a, low[:, a * rank:(a + 1) * rank], kept)
        stage[part, ds, :, :, width:] = kept.reshape(len(RING), rows, rank).astype(BF)

    blocks = ((FAR, LAST), (OWN, NEXT))
    halves = (first(quarter), pl.ds(quarter, quarter))
    PASS, FREE, SUM = range(3)

    def slow(part, kind, d, i):
        df = blocks[1 - d][i] if kind == FREE else blocks[d][i]
        sems = (part, kind, d, i)
        src = stage.at[part, FAR if kind == PASS else TOWARD[d], df]
        dst = near.at[part, d, i] if kind == PASS else landed.at[part, d, df]
        return remote(src, dst, slow_send.at[sems], slow_recv.at[sems], place.neighbour(part, SLOW, STEP[d]))

    def fast(part, kind, d):
        at = halves[1 - d] if kind == FREE else halves[d]
        sems = (part, kind, d)
        src = stage.at[part, OWN, FAR if kind == PASS else TOWARD[d], at]
        dst = fast_near.at[part, d] if kind == PASS else fast_landed.at[part, d, at]
        return remote(src, dst, fast_send.at[sems], fast_recv.at[sems], place.neighbour(part, FAST, STEP[d]))

    def add(into, *others):
        def some(i):
            at = pl.ds(pl.multiple_of(i * TILE, TILE), TILE)
            total = into[at, :].astype(F32)
            for other in others:
                total += other[at, :].astype(F32)
            into[at, :] = total.astype(BF)

        loop(into.shape[0] // TILE, some)

    for part in BOTH:
        unit(part, FAR)
        for i in BOTH:
            for d in BOTH:
                slow(part, PASS, d, i).start()
    loop(len(RING), lambda i: unit(lax.rem(i, 2), NEXT + 2 * (i // 2)))
    for i in BOTH:
        for d in BOTH:
            for part in BOTH:
                slow(part, FREE, d, i).start()
    loop(2, lambda part: unit(part, OWN))
    for i in BOTH:
        for d in BOTH:
            for part in BOTH:
                slow(part, PASS, d, i).wait_recv()
                add(stage.at[part, TOWARD[d], blocks[d][i]], near.at[part, d, i])
                slow(part, SUM, d, i).start()
    for i in BOTH:
        for d in BOTH:
            df = blocks[d][i]
            for part in BOTH:
                slow(part, SUM, d, i).wait_recv()
                slow(part, FREE, 1 - d, i).wait_recv()
                add(stage.at[part, OWN, df], landed.at[part, UP, df], landed.at[part, DOWN, df])
                for e in BOTH:
                    if df == FAR:
                        fast(part, PASS, e).start()
                    elif df == TOWARD[e]:
                        fast(part, FREE, e).start()
    for d in BOTH:
        for part in BOTH:
            fast(part, PASS, d).wait_recv()
            add(stage.at[part, OWN, TOWARD[d], halves[d]], fast_near.at[part, d])
            fast(part, SUM, d).start()
    for part in BOTH:
        for d in BOTH:
            fast(part, FREE, d).wait_recv()
            fast(part, SUM, d).wait_recv()
        add(stage.at[part, OWN, OWN], fast_landed.at[part, UP], fast_landed.at[part, DOWN])
    wait(ends([pltpu.make_async_copy(stage.at[part, OWN, OWN], out_ref.at[pl.ds(part * rows, rows)], load_sem) for part in BOTH]))
    for part in BOTH:
        for kind in range(3):
            for d in BOTH:
                fast(part, kind, d).wait_send()
                for i in BOTH:
                    slow(part, kind, d, i).wait_send()


def row_proj(ids, act, w_own, w_par, a_own, a_par, side, collective_id):
    adapters, _, rank = a_own.shape
    width = w_own.shape[1]
    rows = act.shape[2] // side
    cols = width + rank
    blocks = (rows, cols)
    return pl.pallas_call(
        functools.partial(row_proj_kernel, side, adapters),
        out_shape=jax.ShapeDtypeStruct((2 * rows, cols), BF),
        in_specs=[SMEM] + [HBM] * 5,
        out_specs=HBM,
        scratch_shapes=[
            pltpu.VMEM(act.shape, BF),
            pltpu.VMEM((act.shape[3], width + adapters * rank), BF),
            pltpu.VMEM((2, side, side) + blocks, BF),
            pltpu.VMEM((2, 2, 2) + blocks, BF),
            pltpu.VMEM((2, 2, side) + blocks, BF),
            pltpu.VMEM((2, 2, rows // 2, cols), BF),
            pltpu.VMEM((2, 2) + blocks, BF),
            DMA((2, 3, 2, 2)), DMA((2, 3, 2, 2)), DMA((2, 3, 2)), DMA((2, 3, 2)), DMA,
        ],
        compiler_params=comm_params(collective_id),
        name='row_proj',
    )(ids, act, w_own, w_par, a_own, a_par)


def finish(sums_ref, resid, b_ref, chosen, scale, adapters):
    devices, _, rank, part = b_ref.shape
    width = devices * part
    low = spread(sums_ref[:, width:].astype(F32), chosen, adapters)
    delta = [dot(low, b_ref[j].reshape(adapters * rank, part)) for j in range(devices)]
    return resid.astype(F32) + (sums_ref[:, :width].astype(F32) + scale * jnp.concatenate(delta, axis=1))


def gate_up_kernel(side, adapters, scale, ids_ref, sums_ref, x_ref, gain_ref, a_ref, b_all, wg_own, wg_par, wu_own, wu_par, bg_own, bg_par, bu_own, bu_par,
                   hid_ref, mid_ref, gbuf, w, b, b_ref, hid, load_sem, b_sem, store_sem, send_sem, recv_sem):
    place = Place(side)
    b_load = ends([pltpu.make_async_copy(b_all.at[0], b_ref, b_sem)])
    share, width = wg_own.shape
    half = w.shape[1] // 2
    rank = bg_own.shape[2]
    seq_len = sums_ref.shape[0]
    edge = share // TILE * TILE
    for at in (0, half):
        for kind in BOTH:
            w[kind, at + edge:at + half, :] = jnp.zeros((half - edge, width), BF)
            b[kind, at + edge:at + half, :] = jnp.zeros((half - edge, adapters * rank), BF)
    loads = []
    for kind, pieces in enumerate(((wg_own, wg_par, bg_own, bg_par), (wu_own, wu_par, bu_own, bu_par))):
        for i, at in enumerate((0, half)):
            loads.append(pltpu.make_async_copy(pieces[i], w.at[kind, pl.ds(at, share)], load_sem))
            for a in range(adapters):
                loads.append(pltpu.make_async_copy(pieces[2 + i].at[a], b.at[kind, pl.ds(at, share), pl.ds(a * rank, rank)], load_sem))
    ends(loads)
    rows = seq_len // 4
    chosen = jnp.full((seq_len, rank), ids_ref[place.device(0, 0)], jnp.int32)
    wait(b_load)
    mid = finish(sums_ref, x_ref[...], b_ref, chosen, scale, adapters).astype(BF)
    mid_ref[...] = mid
    h2 = normed(mid.astype(F32), gain_ref[...])
    low = dot_rows(h2, a_ref[...]).astype(BF)
    n_low = low.shape[1]
    per = rank // (2 * side * side)
    to = lax.broadcasted_iota(jnp.int32, (n_low, 2 * rank), 1)
    frm = lax.broadcasted_iota(jnp.int32, (n_low, 2 * rank), 0)
    kind, rank_at = to // rank, lax.rem(to, rank)
    pick = (rank_at // per) * (2 * adapters * per) + ids_ref[place.device(0, 0)] * (2 * per) + kind * per + lax.rem(rank_at, per)
    low = dot(low, jnp.where(frm == pick, 1.0, 0.0).astype(BF)).astype(BF)
    for part in BOTH:
        for piece in BOTH:
            at = (2 * part + piece) * rows
            gbuf[part, OWN, OWN, piece, :, :width] = h2[at:at + rows]
            gbuf[part, OWN, OWN, piece, :, width:] = low[at:at + rows]
    place.barrier()
    chunk = fit(2 * half, 256)

    def unit(part, ds):
        unit_rows = len(RING) * 2 * rows
        low = gbuf[part, ds, :, :, :, width:].reshape(unit_rows, 2 * rank).astype(F32)
        chosen = rows_of_adapter(place, ids_ref, part, ds, (unit_rows, rank))
        lows = [spread(low[:, kind * rank:(kind + 1) * rank], chosen, adapters) for kind in BOTH]

        def columns(n):
            at = pl.ds(pl.multiple_of(n * chunk, chunk), chunk)
            act = gbuf[part, ds, :, :, :, :width].reshape(unit_rows, width)
            gate, up = (dot_rows(act, w[kind, at]) + scale * dot_rows(lows[kind], b[kind, at]) for kind in BOTH)
            hid[part, ds, :, at] = (gate * jax.nn.sigmoid(gate) * up).astype(BF)

        loop(2 * half // chunk, columns)
        pltpu.make_async_copy(hid.at[part, ds], hid_ref.at[part, ds], store_sem).start()

    def on_near():
        wait(loads)
        loop(2, lambda part: unit(part, OWN))

    gather(place, lambda part, ds, df: gbuf.at[part, ds, df], send_sem, recv_sem, on_near=on_near,
           on_sides=lambda: loop(len(RING), lambda i: unit(lax.rem(i, 2), NEXT + 2 * (i // 2))),
           on_far=lambda: loop(2, lambda part: unit(part, FAR)))
    pltpu.make_async_copy(hid, hid_ref, store_sem).wait()


def gate_up(ids, sums, x_own, gain, b_all, a_all, w, side, scale, collective_id):
    seq_len, depth = x_own.shape
    share = w[0].shape[0]
    adapters, _, rank = w[4].shape
    half = (share + LANE - 1) // LANE * LANE
    hidden = jax.ShapeDtypeStruct((2, side, side * seq_len // 2, 2 * half), BF)
    return pl.pallas_call(
        functools.partial(gate_up_kernel, side, adapters, scale),
        out_shape=[hidden, jax.ShapeDtypeStruct(x_own.shape, BF)],
        in_specs=[SMEM] + [VMEM] * 4 + [HBM] * (1 + len(w)),
        out_specs=[HBM, VMEM],
        scratch_shapes=[
            pltpu.VMEM((2, side, side, 2, seq_len // 4, depth + 2 * rank), BF),
            pltpu.VMEM((2, 2 * half, depth), BF),
            pltpu.VMEM((2, 2 * half, adapters * rank), BF),
            pltpu.VMEM(b_all.shape[1:], BF),
            pltpu.VMEM(hidden.shape, BF),
            DMA, DMA, DMA,
        ] + GATHER_SEMS,
        compiler_params=comm_params(collective_id),
        name='gate_up',
    )(ids, sums, x_own, gain.reshape(1, depth), a_all, b_all, *w)


def deliver_kernel(side, adapters, scale, ids_ref, sums_ref, x_ref, b_all, out_ref, gbuf, b_ref, b_sem, pair_send, pair_recv, store_sem, send_sem, recv_sem):
    place = Place(side)
    b_load = ends([pltpu.make_async_copy(b_all.at[1], b_ref, b_sem)])
    seq_len = sums_ref.shape[0]
    rows = seq_len // 4
    rank = b_ref.shape[2]
    chosen = jnp.full((seq_len, rank), ids_ref[place.device(0, 0)], jnp.int32)
    wait(b_load)
    y = finish(sums_ref, x_ref[...], b_ref, chosen, scale, adapters).astype(BF)
    for part in BOTH:
        for piece in BOTH:
            at = (2 * part + piece) * rows
            gbuf[part, OWN, OWN, piece] = y[at:at + rows]
    place.barrier(place.partner)

    def block(part, ds, df):
        return gbuf.at[part, ds, df]

    def seen(part, ds, df, half):
        src, dst = block(part, ds, df), out_ref.at[place.sequence(part, ds, df), part]
        if half is not None:
            src, dst = src.at[half], dst.at[half]
        remote(src, dst, pair_send, pair_recv, place.partner).start()
        pltpu.make_async_copy(src, dst, store_sem).start()

    for part in BOTH:
        seen(part, OWN, OWN, None)
    gather(place, block, send_sem, recv_sem, seen=seen)
    every = out_ref.at[first(side * side)]
    for sem in (store_sem, pair_send, pair_recv):
        pltpu.make_async_copy(every, every, sem).wait()


def deliver(ids, sums, x_mid, b_all, side, scale, collective_id):
    seq_len, depth = x_mid.shape
    rows = seq_len // 4
    return pl.pallas_call(
        functools.partial(deliver_kernel, side, b_all.shape[2], scale),
        out_shape=jax.ShapeDtypeStruct((2 * side * side, 2, 2, rows, depth), BF),
        in_specs=[SMEM] + [VMEM] * 2 + [HBM],
        out_specs=HBM,
        scratch_shapes=[pltpu.VMEM((2, side, side, 2, rows, depth), BF), pltpu.VMEM(b_all.shape[1:], BF), DMA, DMA, DMA, DMA] + GATHER_SEMS,
        compiler_params=comm_params(collective_id),
        name='deliver',
    )(ids, sums, x_mid, b_all)


def solution(mesh):
    tp_size = mesh.shape['tensor']
    side = math.isqrt(tp_size // 2)
    rows_only = P('tensor', None)
    head_split = P(None, 'tensor', None)
    last_split = P(None, None, 'tensor')
    b_head_split = P(None, None, 'tensor', None)
    in_specs = (P('data', None, None), P('data'), P(None), P(None),
                head_split, head_split, head_split, P('tensor', None, None),
                P(None, 'tensor'), P(None, 'tensor'), rows_only,
                last_split, b_head_split, last_split, b_head_split, last_split, b_head_split,
                P(None, 'tensor', None, None), last_split,
                last_split, last_split, last_split, last_split,
                head_split, last_split)

    def local_layer(x_in, adapter_ids, gain_attn, gain_mlp, w_q, w_k, w_v, w_o, w_gate, w_up, w_down, a_q, b_q, a_k, b_k, a_v, b_v, a_o, b_o, a_gate, b_gate, a_up, b_up, a_down, b_down):
        depth = x_in.shape[2]
        adapters, rank = b_q.shape[:2]
        scale = ALPHA / rank
        index = lax.axis_index('tensor')

        def across(a):
            return a.swapaxes(-1, -2)

        per = a_q.shape[2]
        own_a = jnp.stack([across(a) for a in (a_q, a_k, a_v)] + [jnp.zeros((adapters, per, depth), BF)], axis=1).reshape(-1, depth)
        spread_b = jnp.stack([jnp.pad(b[:, :, 0].reshape(adapters, side, side, 2, 1, per, -1), ((0, 0),) * 4 + ((i, 3 - i),) + ((0, 0),) * 2)
                              for i, b in enumerate((b_q, b_k, b_v))], axis=-2)
        own_b = jnp.stack([spread_b[:, :, :, 0], spread_b[:, :, :, 1].swapaxes(1, 2)], axis=1).reshape(adapters, 2, 2 * rank, -1)
        heads = [w_q[:, 0], w_k[:, 0], w_v[:, 0], own_a, own_b]
        given = [w_o[0], a_o[:, 0], across(w_gate), across(w_up), w_down, across(b_gate), across(b_up), a_down]
        att, *kept = attend(adapter_ids, x_in, gain_attn, heads, given, side, adapters, scale, 0)

        all_b = lax.all_gather(jnp.stack([b_o, b_down]), 'tensor', axis=1)
        all_a = lax.all_gather(jnp.stack([across(a_gate), across(a_up)], axis=1).reshape(-1, depth), 'tensor', axis=0, tiled=True)
        x_own = lax.dynamic_index_in_dim(x_in, index, axis=0, keepdims=False)
        att = att.reshape(2, side, -1, att.shape[-1])
        sums = row_proj(adapter_ids, att, given[0], kept[0], given[1], kept[1], side, 1)
        w = [piece for i in (2, 3, 5, 6) for piece in (given[i], kept[i])]
        hidden, x_mid = gate_up(adapter_ids, sums, x_own, gain_mlp, all_b, all_a, w, side, scale, 2)
        sums = row_proj(adapter_ids, hidden, given[4], kept[4], given[7], kept[7], side, 3)
        y = deliver(adapter_ids, sums, x_mid, all_b, side, scale, 4)
        return y.reshape(x_in.shape)

    return jax.shard_map(local_layer, mesh=mesh, in_specs=in_specs, out_specs=P('data', None, None), check_vma=False)
```

```python
import functools
import math

import jax
import jax.numpy as jnp
import numpy as np
from jax import lax
from jax.experimental import pallas as pl
from jax.experimental.pallas import tpu as pltpu
from jax.sharding import PartitionSpec as P

ALPHA = 16.0
ROPE_BASE = 10000.0
EPSILON = 1e-5
BF = jnp.bfloat16
F32 = jnp.float32
LANE = 128
TILE = 16
VMEM_MOST = 67043328
MESH = pl.DeviceIdType.MESH
HBM = pl.BlockSpec(memory_space=pltpu.HBM)
VMEM = pl.BlockSpec(memory_space=pltpu.VMEM)
SMEM = pl.BlockSpec(memory_space=pltpu.SMEM)
DMA = pltpu.SemaphoreType.DMA

OWN, NEXT, FAR, LAST = RING = range(4)
UP, DOWN = BOTH = range(2)
STEP = (NEXT, -NEXT)
FROM = (LAST, NEXT)
TOWARD = (NEXT, LAST)
FAST, SLOW = BOTH


def fit(size, most):
    return max(c for c in range(LANE, most + 1, LANE) if size % c == 0)


def first(size):
    return pl.ds(0, size)


def dot(a, b):
    return jnp.dot(a, b, preferred_element_type=F32)


def dot_rows(a, b):
    return lax.dot_general(a, b, (((1,), (1,)), ((), ())), preferred_element_type=F32)


def dot_columns(a, b):
    return lax.dot_general(a, b, (((0,), (0,)), ((), ())), preferred_element_type=F32)


def normed(act, gain):
    return (act * lax.rsqrt(jnp.mean(act * act, axis=-1, keepdims=True) + EPSILON) * gain).astype(BF)


def ends(copies):
    for copy in copies:
        copy.start()
    return copies


def wait(copies):
    for copy in copies:
        copy.wait()


def loop(count, body):
    lax.fori_loop(0, count, lambda i, carry: (body(i), carry)[1], 0)


class Place:
    def __init__(self, side):
        index = lax.axis_index('tensor')
        self.side = side
        self.core = lax.rem(index, 2)
        chip = index // 2
        self.y, self.x = chip // side, lax.rem(chip, side)
        self.partner = index + 1 - 2 * self.core

    def turn(self, at, steps):
        return lax.rem(at + steps + self.side, self.side)

    def device(self, dy, dx):
        return (self.turn(self.y, dy) * self.side + self.turn(self.x, dx)) * 2 + self.core

    def neighbour(self, part, ring, step):
        return self.device(0, step) if part == ring else self.device(step, 0)

    def sequence(self, part, ds, df):
        return self.device(jnp.where(part == 0, ds, df), jnp.where(part == 0, df, ds))

    def barrier(self, *more):
        sem = pltpu.get_barrier_semaphore()
        to = [self.neighbour(0, ring, step) for ring in BOTH for step in STEP] + list(more)
        for device in to:
            pl.semaphore_signal(sem, inc=1, device_id={'tensor': device}, device_id_type=MESH)
        pl.semaphore_wait(sem, len(to))


def remote(src, dst, send_sem, recv_sem, to):
    return pltpu.make_async_remote_copy(src_ref=src, dst_ref=dst, send_sem=send_sem, recv_sem=recv_sem, device_id={'tensor': to}, device_id_type=MESH)


GATHER_SEMS = [DMA((2, 2, 2, 2, 4))] * 2


def gather(place, block, send_sem, recv_sem, absolute=False, seen=None, on_near=None, on_sides=None, on_far=None):
    def message(part, ring, passed, d, j=OWN):
        spot = (lambda s: (s, j)) if ring == SLOW else (lambda s: (OWN, s))
        src, dst = (FROM[d], FAR) if passed else (OWN, FROM[d])
        a, b = block(part, *spot(src)), block(part, *spot(src if absolute else dst))
        if passed:
            a, b = a.at[d], b.at[d]
        sems = (part, ring, passed, d, j)
        return remote(a, b, send_sem.at[sems], recv_sem.at[sems], place.neighbour(part, ring, STEP[d]))

    def start(*which):
        for d in BOTH:
            for part in BOTH:
                message(part, *which[:2], d, *which[2:]).start()

    def arrived(part, ring, passed, d, j=OWN):
        message(part, ring, passed, d, j).wait_recv()
        if seen:
            at = FAR if passed else FROM[d]
            seen(part, *((at, j) if ring == SLOW else (OWN, at)), d if passed else None)

    start(FAST, 0)
    start(SLOW, 0, OWN)
    for d in BOTH:
        for part in BOTH:
            arrived(part, FAST, 0, d)
            message(part, FAST, 1, d).start()
            for e in BOTH:
                message(part, SLOW, 0, e, FROM[d]).start()
    for part in BOTH:
        for d in BOTH:
            arrived(part, FAST, 1, d)
        for e in BOTH:
            message(part, SLOW, 0, e, FAR).start()

    def pass_on(j):
        for part in BOTH:
            for d in BOTH:
                arrived(part, SLOW, 0, d, j)
                message(part, SLOW, 1, d, j).start()

    order = (OWN,) + FROM + (FAR,)
    pass_on(OWN)
    if on_near:
        on_near()
    for j in order[1:]:
        pass_on(j)
    if on_sides:
        on_sides()
    for j in order:
        for part in BOTH:
            for d in BOTH:
                arrived(part, SLOW, 1, d, j)
    if on_far:
        on_far()
    for part in BOTH:
        for d in BOTH:
            for passed in BOTH:
                message(part, FAST, passed, d).wait_send()
                for j in RING:
                    message(part, SLOW, passed, d, j).wait_send()


def rows_of_adapter(place, ids_ref, part, ds, shape):
    block = lax.broadcasted_iota(jnp.int32, shape, 0) // (shape[0] // len(RING))
    chosen = jnp.zeros(shape, jnp.int32)
    for df in RING:
        chosen = jnp.where(block == df, ids_ref[place.sequence(part, ds, df)], chosen)
    return chosen


def pick_columns(low, chosen):
    rank = chosen.shape[1]
    kept = low[:, :rank]
    for a in range(1, low.shape[1] // rank):
        kept = jnp.where(chosen == a, low[:, a * rank:(a + 1) * rank], kept)
    return kept


def spread(low, chosen, adapters):
    return jnp.concatenate([jnp.where(chosen == a, low, 0.0) for a in range(adapters)], axis=1).astype(BF)


PASS, FREE, SUM = range(3)
FAST_SEMS = [DMA((2, 3, 2))] * 2


def add(into, *others):
    def some(i):
        at = pl.ds(pl.multiple_of(i * TILE, TILE), TILE)
        total = into[at, :].astype(F32)
        for other in others:
            total += other[at, :].astype(F32)
        into[at, :] = total.astype(BF)

    loop(into.shape[0] // TILE, some)


class FastScatter:
    def __init__(self, place, stage, near, landed, send_sem, recv_sem):
        self.place, self.stage, self.near, self.landed, self.sems = place, stage, near, landed, (send_sem, recv_sem)
        quarter = near.shape[2]
        self.halves = (first(quarter), pl.ds(quarter, quarter))

    def message(self, part, kind, d):
        at = self.halves[1 - d] if kind == FREE else self.halves[d]
        src = self.stage(part, FAR if kind == PASS else TOWARD[d]).at[at]
        dst = self.near.at[part, d] if kind == PASS else self.landed.at[part, d, at]
        sems = [sem.at[part, kind, d] for sem in self.sems]
        return remote(src, dst, *sems, self.place.neighbour(part, FAST, STEP[d]))

    def ready(self, part, df):
        for d in BOTH:
            if df == FAR:
                self.message(part, PASS, d).start()
            elif df == TOWARD[d]:
                self.message(part, FREE, d).start()

    def finish(self):
        for d in BOTH:
            for part in BOTH:
                self.message(part, PASS, d).wait_recv()
                add(self.stage(part, TOWARD[d]).at[self.halves[d]], self.near.at[part, d])
                self.message(part, SUM, d).start()
        for part in BOTH:
            for d in BOTH:
                self.message(part, FREE, d).wait_recv()
                self.message(part, SUM, d).wait_recv()
            add(self.stage(part, OWN), self.landed.at[part, UP], self.landed.at[part, DOWN])

    def store(self, out_ref, sem):
        rows = self.landed.shape[2]
        wait(ends([pltpu.make_async_copy(self.stage(part, OWN), out_ref.at[pl.ds(part * rows, rows)], sem) for part in BOTH]))
        for part in BOTH:
            for kind in range(3):
                for d in BOTH:
                    self.message(part, kind, d).wait_send()


def fast_scratch(rows, cols):
    return [pltpu.VMEM((2, 2, rows // 2, cols), BF), pltpu.VMEM((2, 2, rows, cols), BF)]


def comm_params(collective_id):
    return pltpu.CompilerParams(collective_id=collective_id, has_side_effects=True, vmem_limit_bytes=VMEM_MOST)


def attend_kernel(side, adapters, scale, n_keep, ids_ref, x_ref, gain_ref, cos_ref, sin_ref, wo_ref, ao_ref, *rest):
    heads, rest = rest[:5], rest[5:]
    given, rest = rest[:n_keep], rest[n_keep:]
    out_ref, rest = rest[0], rest[1:]
    kept, rest = rest[:n_keep], rest[n_keep:]
    (w, a_rows, bx, xbuf, h, z, lows, att, act, wo, stage, near, landed, pair_send, pair_recv, load_sem, x_sem, wo_load, wo_send, wo_recv,
     wo_pair_send, wo_pair_recv, swap_send, swap_recv, send_sem, recv_sem, fast_send, fast_recv) = rest
    place = Place(side)
    head, seq_len, depth = cos_ref.shape[1], x_ref.shape[1], x_ref.shape[2]
    cols = heads[4].shape[-1]
    chips = side * side
    a_own = a_rows.at[pl.ds(pl.multiple_of(place.core * 2 * TILE, TILE), 2 * TILE)]
    spots = [[w.at[:, pl.ds(at + i * head, head)] for i in range(3)] + [a_own, bx.at[:, :, :, pl.ds(at, cols)]] for at in (0, cols)]
    loads = [pltpu.make_async_copy(src, dst, load_sem) for src, dst in zip(heads, spots[0])]
    ends(loads)

    def x_loads(step):
        slot = lax.rem(step, 2)
        return [pltpu.make_async_copy(x_ref.at[4 * step + 2 * i + place.core], xbuf.at[slot, i], x_sem.at[slot]) for i in BOTH]

    ends(x_loads(0))
    width = wo_ref.shape[1]
    rank = ao_ref.shape[2]
    wo_loads = []
    for part in BOTH:
        wo_loads.append(pltpu.make_async_copy(wo_ref, wo.at[part, OWN, 0, :, first(width)], wo_load))
        for a in range(adapters):
            wo_loads.append(pltpu.make_async_copy(ao_ref.at[a], wo.at[part, OWN, 0, :, pl.ds(width + a * rank, rank)], wo_load))
    ends(wo_loads)
    place.barrier(place.partner, place.device(0, FAR), place.device(FAR, 0))
    moves = list(zip(heads, spots[1][:3] + [a_own] + spots[1][4:])) + list(zip(given, kept))
    pair = [remote(src, dst, pair_send.at[i], pair_recv.at[i], place.partner) for i, (src, dst) in enumerate(moves)]
    ends(pair)

    def wo_message(part, passed, d):
        src, dst = (wo.at[part, s, 0] for s in ((FROM[d], FAR) if passed else (OWN, FROM[d])))
        if passed:
            at = pl.ds(d * head // 2, head // 2)
            src, dst = src.at[at], dst.at[at]
        return remote(src, dst, wo_send.at[part, passed, d], wo_recv.at[part, passed, d], place.neighbour(part, SLOW, STEP[d]))

    def wo_to_partner(part, s):
        remote(wo.at[part, s, 0], wo.at[part, s, 1], wo_pair_send, wo_pair_recv, place.partner).start()

    wait(wo_loads)
    for d in BOTH:
        for part in BOTH:
            wo_message(part, 0, d).start()
    for part in BOTH:
        wo_to_partner(part, OWN)

    def wo_pass():
        for d in BOTH:
            for part in BOTH:
                wo_message(part, 0, d).wait_recv()
                wo_message(part, 1, d).start()
                wo_to_partner(part, FROM[d])

    def wo_last():
        for part in BOTH:
            for d in BOTH:
                wo_message(part, 1, d).wait_recv()
            wo_to_partner(part, FAR)

    wait(loads)
    for copy in pair[:len(heads)]:
        copy.wait_recv()
    mine = [(place.y, place.x), (place.x, place.y)]
    steps = chips // 2

    def block(part, ds, df):
        return lows.at[part, place.turn(mine[part][0], ds), place.turn(mine[part][1], df)]

    def project(step):
        slot = lax.rem(step, 2)

        @pl.when(step + 1 < steps)
        def _():
            ends(x_loads(step + 1))

        wait(x_loads(step))
        for i in BOTH:
            h[i * seq_len:(i + 1) * seq_len, :] = normed(xbuf[slot, i].astype(F32), gain_ref[...])
        rows = pl.ds(pl.multiple_of(step * 2 * seq_len, LANE), 2 * seq_len)
        chunk = fit(2 * cols, 256)
        for n in range(2 * cols // chunk):
            z[rows, n * chunk:(n + 1) * chunk] = dot(h[...], w[:, n * chunk:(n + 1) * chunk])
        low = dot_rows(a_rows[...], h[...])
        half, at = step // (steps // 2), lax.rem(step, steps // 2) * 2 * seq_len
        for part in BOTH:
            pieces = []
            for i in BOTH:
                options = [low[TILE * (2 * part + a):TILE * (2 * part + a + 1), i * seq_len:(i + 1) * seq_len] for a in range(adapters)]
                piece = options[0]
                for a in range(1, adapters):
                    piece = jnp.where(ids_ref[4 * step + 2 * i + place.core] == a, options[a], piece)
                pieces.append(piece)
            lows[part, mine[part][0], mine[part][1], half, :, pl.ds(pl.multiple_of(at, LANE), 2 * seq_len)] = jnp.concatenate(pieces, axis=1).astype(BF)

        pl.when(step == steps - 3)(wo_pass)

    loop(steps, project)
    gather(place, block, send_sem, recv_sem, absolute=True)
    causal = lax.broadcasted_iota(jnp.int32, (seq_len, seq_len), 0) >= lax.broadcasted_iota(jnp.int32, (seq_len, seq_len), 1)

    def swap(part, ds, df):
        sems = (part, ds, df)
        to = place.neighbour(part, SLOW, ds)
        return remote(att.at[sems], act.at[part, lax.rem(len(RING) - ds, len(RING)), df], swap_send.at[sems], swap_recv.at[sems], to)

    def attention(i):
        dy, dx = side - 1 - i // side, side - 1 - lax.rem(i, side)
        chip = place.turn(place.y, dy) * side + place.turn(place.x, dx)
        adapter = ids_ref[2 * chip + place.core]
        half, at = chip // steps, pl.ds(pl.multiple_of(lax.rem(chip, steps) * seq_len, LANE), seq_len)
        zs = z[pl.ds(pl.multiple_of(chip * seq_len, LANE), seq_len), :]
        for part in BOTH:
            zs += scale * dot_columns(lows[part, :, :, half, :, at].reshape(-1, seq_len), bx[adapter, part])
        for i_head in BOTH:
            q, k, v = (zs[:, i_head * cols + i * head:i_head * cols + (i + 1) * head] for i in range(3))
            q, k = ((r * cos_ref[...] + pltpu.roll(r, head // 2, axis=1) * sin_ref[...]).astype(BF) for r in (q, k))
            scores = jnp.where(causal, dot_rows(q, k) * head ** -0.5, -1e30)
            e = jnp.exp(scores - jnp.max(scores, axis=-1, keepdims=True))
            prob = (e / jnp.sum(e, axis=-1, keepdims=True)).astype(BF)
            mixed = dot(prob, v.astype(BF)).astype(BF)
            for part, (ds, df) in enumerate(((dy, dx), (dx, dy))):
                att[part, ds, df, :, i_head * head:(i_head + 1) * head] = mixed[part * seq_len // 2:(part + 1) * seq_len // 2]

    def attention_pair(k):
        for i in BOTH:
            attention(2 * k + i)
        for i in BOTH:
            dy, dx = side - 1 - (2 * k + i) // side, side - 1 - lax.rem(2 * k + i, side)
            for part, (ds, df) in enumerate(((dy, dx), (dx, dy))):
                pl.when(ds != OWN)(swap(part, ds, df).start)
        pl.when(k == 2)(wo_last)

    loop(chips // 2, attention_pair)
    for part in BOTH:
        act[part, OWN] = att[part, OWN]
    pltpu.make_async_copy(wo.at[:, :, 1], wo.at[:, :, 1], wo_pair_recv).wait()
    chunk = fit(width, 512)
    rows = seq_len // 2
    blocks = (len(RING), rows)
    fast = FastScatter(place, lambda part, df: stage.at[part, df], near, landed, fast_send, fast_recv)

    def sum_heads(part, at):
        return sum(dot(act[part, s].reshape(-1, 2 * head), wo[part, s, :, :, at].reshape(2 * head, -1)) for s in RING)

    for part in BOTH:
        for ds in RING[1:]:
            for df in RING:
                swap(part, ds, df).wait_recv()

        def columns(n):
            at = pl.ds(pl.multiple_of(n * chunk, chunk), chunk)
            stage[part, :, :, at] = sum_heads(part, at).reshape(blocks + (chunk,)).astype(BF)

        loop(width // chunk, columns)
        chosen = rows_of_adapter(place, ids_ref, part, OWN, (len(RING) * rows, rank))
        stage[part, :, :, width:] = pick_columns(sum_heads(part, pl.ds(width, adapters * rank)), chosen).reshape(blocks + (rank,)).astype(BF)
        for df in RING[1:]:
            fast.ready(part, df)
    fast.finish()
    fast.store(out_ref, load_sem)
    for copy in pair[len(heads):]:
        copy.wait_recv()
    for copy in pair:
        copy.wait_send()
    pltpu.make_async_copy(wo.at[:, :, 1], wo.at[:, :, 1], wo_pair_send).wait()
    for part in BOTH:
        for d in BOTH:
            for passed in BOTH:
                wo_message(part, passed, d).wait_send()
        for ds in RING[1:]:
            for df in RING:
                swap(part, ds, df).wait_send()


def attend(ids, x_in, gain, w_o, a_o, heads, given, side, scale, collective_id):
    _, seq_len, depth = x_in.shape
    head, cols = heads[0].shape[1], heads[4].shape[-1]
    adapters, _, rank = a_o.shape
    chips = side * side
    half_dim = head // 2
    inv_freq = ROPE_BASE ** (-2.0 * np.arange(half_dim) / head)
    angle = np.arange(seq_len)[:, None] * inv_freq[None, :]
    cos, sin = np.cos(angle), np.sin(angle)
    tables = [jnp.asarray(np.concatenate(pair, axis=1), F32) for pair in ((cos, cos), (-sin, sin))]
    n_moves = len(heads) + len(given)
    rows, out_cols = seq_len // 2, depth + rank
    return pl.pallas_call(
        functools.partial(attend_kernel, side, adapters, scale, len(given)),
        out_shape=[jax.ShapeDtypeStruct((seq_len, out_cols), BF)] + [jax.ShapeDtypeStruct(g.shape, g.dtype) for g in given],
        in_specs=[SMEM, HBM, VMEM, VMEM, VMEM] + [HBM] * (2 + n_moves),
        out_specs=[HBM] * (1 + len(given)),
        scratch_shapes=[
            pltpu.VMEM((depth, 2 * cols), BF),
            pltpu.VMEM((2 * 2 * TILE, depth), BF),
            pltpu.VMEM(heads[4].shape[:3] + (2 * cols,), BF),
            pltpu.VMEM((2, 2, seq_len, depth), BF),
            pltpu.VMEM((2 * seq_len, depth), BF),
            pltpu.VMEM((chips * seq_len, 2 * cols), F32),
            pltpu.VMEM((2, side, side, 2, TILE, chips * seq_len // 2), BF),
            pltpu.VMEM((2, side, side, rows, 2 * head), BF),
            pltpu.VMEM((2, side, side, rows, 2 * head), BF),
            pltpu.VMEM((2, side, 2, head, depth + adapters * rank), BF),
            pltpu.VMEM((2, side, rows, out_cols), BF),
        ] + fast_scratch(rows, out_cols) + [
            DMA((n_moves,)), DMA((n_moves,)), DMA, DMA((2,)), DMA, DMA((2, 2, 2)), DMA((2, 2, 2)), DMA, DMA, DMA((2, 4, 4)), DMA((2, 4, 4)),
        ] + GATHER_SEMS + FAST_SEMS,
        compiler_params=comm_params(collective_id),
        name='attend',
    )(ids, x_in, gain.reshape(1, depth), *tables, w_o, a_o, *heads, *given)


def row_proj_kernel(side, adapters, ids_ref, act_ref, w_own, w_par, a_own, a_par, out_ref,
                    act, w, stage, near, landed, fast_near, fast_landed, slow_send, slow_recv, fast_send, fast_recv, load_sem):
    place = Place(side)
    share, width = w_own.shape
    half = w.shape[0] // 2
    rank = a_own.shape[2]
    rows = stage.shape[3]
    quarter = rows // 2
    if share < half:
        for at in (0, half):
            w[at + share // TILE * TILE:at + half, :] = jnp.zeros((half - share // TILE * TILE, w.shape[1]), BF)
    loads = [pltpu.make_async_copy(act_ref, act, load_sem)]
    for at, w_part, a_part in ((0, w_own, a_own), (half, w_par, a_par)):
        loads.append(pltpu.make_async_copy(w_part, w.at[pl.ds(at, share), first(width)], load_sem))
        for a in range(adapters):
            loads.append(pltpu.make_async_copy(a_part.at[a], w.at[pl.ds(at, share), pl.ds(width + a * rank, rank)], load_sem))
    ends(loads)
    place.barrier()
    wait(loads)
    chunk = fit(width, 512)

    def unit(part, ds):
        def columns(n):
            at = pl.ds(pl.multiple_of(n * chunk, chunk), chunk)
            stage[part, ds, :, :, at] = dot(act[part, ds], w[:, at]).reshape(len(RING), rows, chunk).astype(BF)

        loop(width // chunk, columns)
        chosen = rows_of_adapter(place, ids_ref, part, ds, (len(RING) * rows, rank))
        stage[part, ds, :, :, width:] = pick_columns(dot(act[part, ds], w[:, width:]), chosen).reshape(len(RING), rows, rank).astype(BF)

    blocks = ((FAR, LAST), (OWN, NEXT))

    def slow(part, kind, d, i):
        df = blocks[1 - d][i] if kind == FREE else blocks[d][i]
        sems = (part, kind, d, i)
        src = stage.at[part, FAR if kind == PASS else TOWARD[d], df]
        dst = near.at[part, d, i] if kind == PASS else landed.at[part, d, df]
        return remote(src, dst, slow_send.at[sems], slow_recv.at[sems], place.neighbour(part, SLOW, STEP[d]))

    fast = FastScatter(place, lambda part, df: stage.at[part, OWN, df], fast_near, fast_landed, fast_send, fast_recv)
    for part in BOTH:
        unit(part, FAR)
        for i in BOTH:
            for d in BOTH:
                slow(part, PASS, d, i).start()
    loop(len(RING), lambda i: unit(lax.rem(i, 2), NEXT + 2 * (i // 2)))
    for i in BOTH:
        for d in BOTH:
            for part in BOTH:
                slow(part, FREE, d, i).start()
    loop(2, lambda part: unit(part, OWN))
    for i in BOTH:
        for d in BOTH:
            for part in BOTH:
                slow(part, PASS, d, i).wait_recv()
                add(stage.at[part, TOWARD[d], blocks[d][i]], near.at[part, d, i])
                slow(part, SUM, d, i).start()
    for i in BOTH:
        for d in BOTH:
            df = blocks[d][i]
            for part in BOTH:
                slow(part, SUM, d, i).wait_recv()
                slow(part, FREE, 1 - d, i).wait_recv()
                add(stage.at[part, OWN, df], landed.at[part, UP, df], landed.at[part, DOWN, df])
                fast.ready(part, df)
    fast.finish()
    fast.store(out_ref, load_sem)
    for part in BOTH:
        for kind in range(3):
            for d in BOTH:
                for i in BOTH:
                    slow(part, kind, d, i).wait_send()


def row_proj(ids, act, w_own, w_par, a_own, a_par, side, collective_id):
    adapters, _, rank = a_own.shape
    width = w_own.shape[1]
    rows = act.shape[2] // side
    cols = width + rank
    blocks = (rows, cols)
    return pl.pallas_call(
        functools.partial(row_proj_kernel, side, adapters),
        out_shape=jax.ShapeDtypeStruct((2 * rows, cols), BF),
        in_specs=[SMEM] + [HBM] * 5,
        out_specs=HBM,
        scratch_shapes=[
            pltpu.VMEM(act.shape, BF),
            pltpu.VMEM((act.shape[3], width + adapters * rank), BF),
            pltpu.VMEM((2, side, side) + blocks, BF),
            pltpu.VMEM((2, 2, 2) + blocks, BF),
            pltpu.VMEM((2, 2, side) + blocks, BF),
        ] + fast_scratch(rows, cols) + [DMA((2, 3, 2, 2))] * 2 + FAST_SEMS + [DMA],
        compiler_params=comm_params(collective_id),
        name='row_proj',
    )(ids, act, w_own, w_par, a_own, a_par)


def finish(sums_ref, resid, b_ref, chosen, scale, adapters):
    devices, _, rank, part = b_ref.shape
    width = devices * part
    low = spread(sums_ref[:, width:].astype(F32), chosen, adapters)
    delta = [dot(low, b_ref[j].reshape(adapters * rank, part)) for j in range(devices)]
    return resid.astype(F32) + (sums_ref[:, :width].astype(F32) + scale * jnp.concatenate(delta, axis=1))


def gate_up_kernel(side, adapters, scale, ids_ref, sums_ref, x_ref, gain_ref, a_ref, b_all, wg_own, wg_par, wu_own, wu_par, bg_own, bg_par, bu_own, bu_par,
                   hid_ref, mid_ref, gbuf, w, b, b_ref, hid, load_sem, b_sem, store_sem, send_sem, recv_sem):
    place = Place(side)
    b_load = ends([pltpu.make_async_copy(b_all.at[0], b_ref, b_sem)])
    share, width = wg_own.shape
    half = w.shape[1] // 2
    rank = bg_own.shape[2]
    seq_len = sums_ref.shape[0]
    edge = share // TILE * TILE
    for at in (0, half):
        for kind in BOTH:
            w[kind, at + edge:at + half, :] = jnp.zeros((half - edge, width), BF)
            b[kind, at + edge:at + half, :] = jnp.zeros((half - edge, adapters * rank), BF)
    loads = []
    for kind, pieces in enumerate(((wg_own, wg_par, bg_own, bg_par), (wu_own, wu_par, bu_own, bu_par))):
        for i, at in enumerate((0, half)):
            loads.append(pltpu.make_async_copy(pieces[i], w.at[kind, pl.ds(at, share)], load_sem))
            for a in range(adapters):
                loads.append(pltpu.make_async_copy(pieces[2 + i].at[a], b.at[kind, pl.ds(at, share), pl.ds(a * rank, rank)], load_sem))
    ends(loads)
    rows = seq_len // 4
    chosen = jnp.full((seq_len, rank), ids_ref[place.device(0, 0)], jnp.int32)
    wait(b_load)
    mid = finish(sums_ref, x_ref[...], b_ref, chosen, scale, adapters).astype(BF)
    mid_ref[...] = mid
    h2 = normed(mid.astype(F32), gain_ref[...])
    low = dot_rows(h2, a_ref[...]).astype(BF)
    n_low = low.shape[1]
    per = rank // (2 * side * side)
    to = lax.broadcasted_iota(jnp.int32, (n_low, 2 * rank), 1)
    frm = lax.broadcasted_iota(jnp.int32, (n_low, 2 * rank), 0)
    kind, rank_at = to // rank, lax.rem(to, rank)
    pick = (rank_at // per) * (2 * adapters * per) + ids_ref[place.device(0, 0)] * (2 * per) + kind * per + lax.rem(rank_at, per)
    low = dot(low, jnp.where(frm == pick, 1.0, 0.0).astype(BF)).astype(BF)
    for part in BOTH:
        for piece in BOTH:
            at = (2 * part + piece) * rows
            gbuf[part, OWN, OWN, piece, :, :width] = h2[at:at + rows]
            gbuf[part, OWN, OWN, piece, :, width:] = low[at:at + rows]
    place.barrier()
    chunk = fit(2 * half, 256)

    def unit(part, ds):
        unit_rows = len(RING) * 2 * rows
        low = gbuf[part, ds, :, :, :, width:].reshape(unit_rows, 2 * rank).astype(F32)
        chosen = rows_of_adapter(place, ids_ref, part, ds, (unit_rows, rank))
        lows = [spread(low[:, kind * rank:(kind + 1) * rank], chosen, adapters) for kind in BOTH]

        def columns(n):
            at = pl.ds(pl.multiple_of(n * chunk, chunk), chunk)
            act = gbuf[part, ds, :, :, :, :width].reshape(unit_rows, width)
            gate, up = (dot_rows(act, w[kind, at]) + scale * dot_rows(lows[kind], b[kind, at]) for kind in BOTH)
            hid[part, ds, :, at] = (gate * jax.nn.sigmoid(gate) * up).astype(BF)

        loop(2 * half // chunk, columns)
        pltpu.make_async_copy(hid.at[part, ds], hid_ref.at[part, ds], store_sem).start()

    def on_near():
        wait(loads)
        loop(2, lambda part: unit(part, OWN))

    gather(place, lambda part, ds, df: gbuf.at[part, ds, df], send_sem, recv_sem, on_near=on_near,
           on_sides=lambda: loop(len(RING), lambda i: unit(lax.rem(i, 2), NEXT + 2 * (i // 2))),
           on_far=lambda: loop(2, lambda part: unit(part, FAR)))
    pltpu.make_async_copy(hid, hid_ref, store_sem).wait()


def gate_up(ids, sums, x_own, gain, b_all, a_all, w, side, scale, collective_id):
    seq_len, depth = x_own.shape
    share = w[0].shape[0]
    adapters, _, rank = w[4].shape
    half = (share + LANE - 1) // LANE * LANE
    hidden = jax.ShapeDtypeStruct((2, side, side * seq_len // 2, 2 * half), BF)
    return pl.pallas_call(
        functools.partial(gate_up_kernel, side, adapters, scale),
        out_shape=[hidden, jax.ShapeDtypeStruct(x_own.shape, BF)],
        in_specs=[SMEM] + [VMEM] * 4 + [HBM] * (1 + len(w)),
        out_specs=[HBM, VMEM],
        scratch_shapes=[
            pltpu.VMEM((2, side, side, 2, seq_len // 4, depth + 2 * rank), BF),
            pltpu.VMEM((2, 2 * half, depth), BF),
            pltpu.VMEM((2, 2 * half, adapters * rank), BF),
            pltpu.VMEM(b_all.shape[1:], BF),
            pltpu.VMEM(hidden.shape, BF),
            DMA, DMA, DMA,
        ] + GATHER_SEMS,
        compiler_params=comm_params(collective_id),
        name='gate_up',
    )(ids, sums, x_own, gain.reshape(1, depth), a_all, b_all, *w)


def deliver_kernel(side, adapters, scale, ids_ref, sums_ref, x_ref, b_all, out_ref, gbuf, b_ref, b_sem, pair_send, pair_recv, store_sem, send_sem, recv_sem):
    place = Place(side)
    b_load = ends([pltpu.make_async_copy(b_all.at[1], b_ref, b_sem)])
    seq_len = sums_ref.shape[0]
    rows = seq_len // 4
    rank = b_ref.shape[2]
    chosen = jnp.full((seq_len, rank), ids_ref[place.device(0, 0)], jnp.int32)
    wait(b_load)
    y = finish(sums_ref, x_ref[...], b_ref, chosen, scale, adapters).astype(BF)
    for part in BOTH:
        for piece in BOTH:
            at = (2 * part + piece) * rows
            gbuf[part, OWN, OWN, piece] = y[at:at + rows]
    place.barrier(place.partner)

    def block(part, ds, df):
        return gbuf.at[part, ds, df]

    def seen(part, ds, df, half):
        src, dst = block(part, ds, df), out_ref.at[place.sequence(part, ds, df), part]
        if half is not None:
            src, dst = src.at[half], dst.at[half]
        remote(src, dst, pair_send, pair_recv, place.partner).start()
        pltpu.make_async_copy(src, dst, store_sem).start()

    for part in BOTH:
        seen(part, OWN, OWN, None)
    gather(place, block, send_sem, recv_sem, seen=seen)
    every = out_ref.at[first(side * side)]
    for sem in (store_sem, pair_send, pair_recv):
        pltpu.make_async_copy(every, every, sem).wait()


def deliver(ids, sums, x_mid, b_all, side, scale, collective_id):
    seq_len, depth = x_mid.shape
    rows = seq_len // 4
    return pl.pallas_call(
        functools.partial(deliver_kernel, side, b_all.shape[2], scale),
        out_shape=jax.ShapeDtypeStruct((2 * side * side, 2, 2, rows, depth), BF),
        in_specs=[SMEM] + [VMEM] * 2 + [HBM],
        out_specs=HBM,
        scratch_shapes=[pltpu.VMEM((2, side, side, 2, rows, depth), BF), pltpu.VMEM(b_all.shape[1:], BF), DMA, DMA, DMA, DMA] + GATHER_SEMS,
        compiler_params=comm_params(collective_id),
        name='deliver',
    )(ids, sums, x_mid, b_all)


def solution(mesh):
    tp_size = mesh.shape['tensor']
    side = math.isqrt(tp_size // 2)
    rows_only = P('tensor', None)
    head_split = P(None, 'tensor', None)
    last_split = P(None, None, 'tensor')
    b_head_split = P(None, None, 'tensor', None)
    in_specs = (P('data', None, None), P('data'), P(None), P(None),
                head_split, head_split, head_split, P('tensor', None, None),
                P(None, 'tensor'), P(None, 'tensor'), rows_only,
                last_split, b_head_split, last_split, b_head_split, last_split, b_head_split,
                P(None, 'tensor', None, None), last_split,
                last_split, last_split, last_split, last_split,
                head_split, last_split)

    def local_layer(x_in, adapter_ids, gain_attn, gain_mlp, w_q, w_k, w_v, w_o, w_gate, w_up, w_down, a_q, b_q, a_k, b_k, a_v, b_v, a_o, b_o, a_gate, b_gate, a_up, b_up, a_down, b_down):
        depth = x_in.shape[2]
        adapters, rank = b_q.shape[:2]
        scale = ALPHA / rank
        index = lax.axis_index('tensor')

        def across(a):
            return a.swapaxes(-1, -2)

        per = a_q.shape[2]
        own_a = jnp.stack([across(a) for a in (a_q, a_k, a_v)] + [jnp.zeros((adapters, per, depth), BF)], axis=1).reshape(-1, depth)
        spread_b = jnp.stack([jnp.pad(b[:, :, 0].reshape(adapters, side, side, 2, 1, per, -1), ((0, 0),) * 4 + ((i, 3 - i),) + ((0, 0),) * 2)
                              for i, b in enumerate((b_q, b_k, b_v))], axis=-2)
        own_b = jnp.stack([spread_b[:, :, :, 0], spread_b[:, :, :, 1].swapaxes(1, 2)], axis=1).reshape(adapters, 2, 2 * rank, -1)
        heads = [w_q[:, 0], w_k[:, 0], w_v[:, 0], own_a, own_b]
        given = [across(w_gate), across(w_up), across(b_gate), across(b_up), w_down, a_down]
        sums, *kept = attend(adapter_ids, x_in, gain_attn, w_o[0], a_o[:, 0], heads, given, side, scale, 0)

        all_b = lax.all_gather(jnp.stack([b_o, b_down]), 'tensor', axis=1)
        all_a = lax.all_gather(jnp.stack([across(a_gate), across(a_up)], axis=1).reshape(-1, depth), 'tensor', axis=0, tiled=True)
        x_own = lax.dynamic_index_in_dim(x_in, index, axis=0, keepdims=False)
        w = [piece for pair in zip(given[:4], kept[:4]) for piece in pair]
        hidden, x_mid = gate_up(adapter_ids, sums, x_own, gain_mlp, all_b, all_a, w, side, scale, 1)
        sums = row_proj(adapter_ids, hidden, given[4], kept[4], given[5], kept[5], side, 2)
        y = deliver(adapter_ids, sums, x_mid, all_b, side, scale, 3)
        return y.reshape(x_in.shape)

    return jax.shard_map(local_layer, mesh=mesh, in_specs=in_specs, out_specs=P('data', None, None), check_vma=False)
```

```python
import functools
import math

import jax
import jax.numpy as jnp
import numpy as np
from jax import lax
from jax.experimental import pallas as pl
from jax.experimental.pallas import tpu as pltpu
from jax.sharding import PartitionSpec as P

ALPHA = 16.0
ROPE_BASE = 10000.0
EPSILON = 1e-5
BF = jnp.bfloat16
F32 = jnp.float32
LANE = 128
TILE = 16
VMEM_MOST = 67043328
VMEM_SMALL = VMEM_MOST * 3 // 8
VMEM_LEAST = VMEM_MOST // 32
MESH = pl.DeviceIdType.MESH
HBM = pl.BlockSpec(memory_space=pltpu.HBM)
VMEM = pl.BlockSpec(memory_space=pltpu.VMEM)
SMEM = pl.BlockSpec(memory_space=pltpu.SMEM)
DMA = pltpu.SemaphoreType.DMA

OWN, NEXT, FAR, LAST = RING = range(4)
UP, DOWN = BOTH = range(2)
STEP = (NEXT, -NEXT)
FROM = (LAST, NEXT)
TOWARD = (NEXT, LAST)
FAST, SLOW = BOTH


def fit(size, most):
    return max(c for c in range(LANE, most + 1, LANE) if size % c == 0)


def first(size):
    return pl.ds(0, size)


def dot(a, b):
    return jnp.dot(a, b, preferred_element_type=F32)


def dot_rows(a, b):
    return lax.dot_general(a, b, (((1,), (1,)), ((), ())), preferred_element_type=F32)


def dot_columns(a, b):
    return lax.dot_general(a, b, (((0,), (0,)), ((), ())), preferred_element_type=F32)


def normed(act, gain):
    return (act * lax.rsqrt(jnp.mean(act * act, axis=-1, keepdims=True) + EPSILON) * gain).astype(BF)


def ends(copies):
    for copy in copies:
        copy.start()
    return copies


def wait(copies):
    for copy in copies:
        copy.wait()


def loop(count, body):
    lax.fori_loop(0, count, lambda i, carry: (body(i), carry)[1], 0)


class Place:
    def __init__(self, side):
        index = lax.axis_index('tensor')
        self.side = side
        self.core = lax.rem(index, 2)
        chip = index // 2
        self.y, self.x = chip // side, lax.rem(chip, side)
        self.partner = index + 1 - 2 * self.core

    def turn(self, at, steps):
        return lax.rem(at + steps + self.side, self.side)

    def device(self, dy, dx):
        return (self.turn(self.y, dy) * self.side + self.turn(self.x, dx)) * 2 + self.core

    def neighbour(self, part, ring, step):
        return self.device(0, step) if part == ring else self.device(step, 0)

    def sequence(self, part, ds, df):
        return self.device(jnp.where(part == 0, ds, df), jnp.where(part == 0, df, ds))

    def barrier(self, *more):
        sem = pltpu.get_barrier_semaphore()
        to = [self.neighbour(0, ring, step) for ring in BOTH for step in STEP] + list(more)
        for device in to:
            pl.semaphore_signal(sem, inc=1, device_id={'tensor': device}, device_id_type=MESH)
        pl.semaphore_wait(sem, len(to))


def remote(src, dst, send_sem, recv_sem, to):
    return pltpu.make_async_remote_copy(src_ref=src, dst_ref=dst, send_sem=send_sem, recv_sem=recv_sem, device_id={'tensor': to}, device_id_type=MESH)


GATHER_SEMS = [DMA((2, 2, 2, 2, 4))] * 2


class Gather:
    def __init__(self, place, block, send_sem, recv_sem, absolute=False, seen=None):
        self.place, self.block, self.sems, self.absolute, self.seen = place, block, (send_sem, recv_sem), absolute, seen

    def message(self, part, ring, passed, d, j=OWN):
        spot = (lambda s: (s, j)) if ring == SLOW else (lambda s: (OWN, s))
        src, dst = (FROM[d], FAR) if passed else (OWN, FROM[d])
        a, b = self.block(part, *spot(src)), self.block(part, *spot(src if self.absolute else dst))
        if passed:
            a, b = a.at[d], b.at[d]
        return remote(a, b, *(sem.at[part, ring, passed, d, j] for sem in self.sems), self.place.neighbour(part, ring, STEP[d]))

    def arrived(self, part, ring, passed, d, j=OWN):
        self.message(part, ring, passed, d, j).wait_recv()
        if self.seen:
            at = FAR if passed else FROM[d]
            self.seen(part, *((at, j) if ring == SLOW else (OWN, at)), d if passed else None)

    def own(self):
        for ring in BOTH:
            for d in BOTH:
                for part in BOTH:
                    self.message(part, ring, 0, d).start()

    def near(self):
        for d in BOTH:
            for part in BOTH:
                self.arrived(part, FAST, 0, d)
                self.message(part, FAST, 1, d).start()
                for e in BOTH:
                    self.message(part, SLOW, 0, e, FROM[d]).start()

    def row(self):
        for part in BOTH:
            for d in BOTH:
                self.arrived(part, FAST, 1, d)
            for e in BOTH:
                self.message(part, SLOW, 0, e, FAR).start()
        self.sides(OWN)

    def sides(self, *blocks):
        for j in blocks:
            for part in BOTH:
                for d in BOTH:
                    self.arrived(part, SLOW, 0, d, j)
                    self.message(part, SLOW, 1, d, j).start()

    def far(self):
        for j in (OWN,) + FROM + (FAR,):
            for part in BOTH:
                for d in BOTH:
                    self.arrived(part, SLOW, 1, d, j)

    def sent(self):
        for part in BOTH:
            for d in BOTH:
                for passed in BOTH:
                    self.message(part, FAST, passed, d).wait_send()
                    for j in RING:
                        self.message(part, SLOW, passed, d, j).wait_send()

    def run(self, on_row=None, on_sides=None, on_far=None):
        self.own()
        self.near()
        self.row()
        if on_row:
            on_row()
        self.sides(*FROM, FAR)
        if on_sides:
            on_sides()
        self.far()
        if on_far:
            on_far()
        self.sent()


def rows_of_adapter(place, ids_ref, part, ds, shape):
    block = lax.broadcasted_iota(jnp.int32, shape, 0) // (shape[0] // len(RING))
    chosen = jnp.zeros(shape, jnp.int32)
    for df in RING:
        chosen = jnp.where(block == df, ids_ref[place.sequence(part, ds, df)], chosen)
    return chosen


def pick_columns(low, chosen):
    rank = chosen.shape[1]
    kept = low[:, :rank]
    for a in range(1, low.shape[1] // rank):
        kept = jnp.where(chosen == a, low[:, a * rank:(a + 1) * rank], kept)
    return kept


def spread(low, chosen, adapters):
    return jnp.concatenate([jnp.where(chosen == a, low, 0.0) for a in range(adapters)], axis=1).astype(BF)


PASS, FREE, SUM = range(3)
FAST_SEMS = [DMA((2, 3, 2))] * 2


def add(into, *others):
    def some(i):
        at = pl.ds(pl.multiple_of(i * TILE, TILE), TILE)
        total = into[at, :].astype(F32)
        for other in others:
            total += other[at, :].astype(F32)
        into[at, :] = total.astype(BF)

    loop(into.shape[0] // TILE, some)


class FastScatter:
    def __init__(self, place, stage, near, landed, send_sem, recv_sem):
        self.place, self.stage, self.near, self.landed, self.sems = place, stage, near, landed, (send_sem, recv_sem)
        quarter = near.shape[2]
        self.halves = (first(quarter), pl.ds(quarter, quarter))

    def message(self, part, kind, d):
        at = self.halves[1 - d] if kind == FREE else self.halves[d]
        src = self.stage(part, FAR if kind == PASS else TOWARD[d]).at[at]
        dst = self.near.at[part, d] if kind == PASS else self.landed.at[part, d, at]
        sems = [sem.at[part, kind, d] for sem in self.sems]
        return remote(src, dst, *sems, self.place.neighbour(part, FAST, STEP[d]))

    def ready(self, part, df):
        for d in BOTH:
            if df == FAR:
                self.message(part, PASS, d).start()
            elif df == TOWARD[d]:
                self.message(part, FREE, d).start()

    def finish(self):
        for d in BOTH:
            for part in BOTH:
                self.message(part, PASS, d).wait_recv()
                add(self.stage(part, TOWARD[d]).at[self.halves[d]], self.near.at[part, d])
                self.message(part, SUM, d).start()
        for part in BOTH:
            for d in BOTH:
                self.message(part, FREE, d).wait_recv()
                self.message(part, SUM, d).wait_recv()
            add(self.stage(part, OWN), self.landed.at[part, UP], self.landed.at[part, DOWN])

    def store(self, out_ref, sem):
        rows = self.landed.shape[2]
        wait(ends([pltpu.make_async_copy(self.stage(part, OWN), out_ref.at[pl.ds(part * rows, rows)], sem) for part in BOTH]))
        for part in BOTH:
            for kind in range(3):
                for d in BOTH:
                    self.message(part, kind, d).wait_send()


def fast_scratch(rows, cols):
    return [pltpu.VMEM((2, 2, rows // 2, cols), BF), pltpu.VMEM((2, 2, rows, cols), BF)]


def comm_params(collective_id, limit=VMEM_MOST):
    return pltpu.CompilerParams(collective_id=collective_id, has_side_effects=True, vmem_limit_bytes=limit)


WO_CHUNKS = 4


def attend_kernel(side, adapters, scale, n_keep, ids_ref, x_ref, gain_ref, cos_ref, sin_ref, *rest):
    w_heads, a_heads, b_heads, (wo_ref, ao_ref), a_mlp, b_rows, rest = rest[:3], rest[3:6], rest[6:9], rest[9:11], rest[11:13], rest[13:15], rest[15:]
    given, rest = rest[:n_keep], rest[n_keep:]
    (out_ref, a_all, b_all), rest = rest[:3], rest[3:]
    kept, rest = rest[:n_keep], rest[n_keep:]
    (w, a_raw, b_raw, a_rows, bx, xbuf, h, z, lows, att, act, wo, stage, near, landed, am_raw, am_rows, pair_send, pair_recv, load_sem, x_sem, own_sem,
     wo_load, wo_send, wo_recv, bulk_send, bulk_recv, swap_send, swap_recv,
     send_sem, recv_sem, a_send, a_recv, b_send, b_recv, fast_send, fast_recv) = rest
    place = Place(side)
    head, seq_len, depth = cos_ref.shape[1], x_ref.shape[1], x_ref.shape[2]
    cols = len(w_heads) * head
    chips = side * side
    per = a_raw.shape[3]
    half_depth = depth // 4
    heads = w_heads + a_heads + b_heads
    spots = [[w.at[:, pl.ds(at * cols + i * head, head)] for i in range(3)] + [a_raw.at[place.core, i] for i in range(3)] + [b_raw.at[at, i] for i in range(3)]
             for at in BOTH]
    loads = ends([pltpu.make_async_copy(src, dst, load_sem) for src, dst in zip(heads, spots[0])])

    def x_loads(step):
        slot = lax.rem(step, 2)
        return [pltpu.make_async_copy(x_ref.at[4 * step + 2 * i + place.core], xbuf.at[slot, i], x_sem.at[slot]) for i in BOTH]

    ends(x_loads(0))

    def every(ref):
        return lambda part, ds, df: ref.at[place.core, part, place.turn(place.y, df if part else ds), place.turn(place.x, ds if part else df)]

    every_a, every_b = every(a_all), every(b_all)
    own_loads = ends([pltpu.make_async_copy(a_mlp[i], am_raw.at[i], own_sem) for i in BOTH])
    own_b = [pltpu.make_async_copy(b_rows[half].at[part], every_b(part, OWN, OWN).at[half], load_sem) for part in BOTH for half in BOTH]
    ends(own_b)
    width = wo_ref.shape[1]
    rank = ao_ref.shape[2]
    wo_loads = []
    for part in BOTH:
        wo_loads.append(pltpu.make_async_copy(wo_ref, wo.at[part, OWN, 0, :, first(width)], wo_load))
        for a in range(adapters):
            wo_loads.append(pltpu.make_async_copy(ao_ref.at[a], wo.at[part, OWN, 0, :, pl.ds(width + a * rank, rank)], wo_load))
    ends(wo_loads)
    wait(own_loads)
    am_rows[...] = jnp.concatenate([am_raw[i, a] for i in BOTH for a in range(adapters)], axis=0)
    place.barrier(place.partner, place.device(0, FAR), place.device(FAR, 0))
    pair = [remote(src, dst, pair_send.at[i], pair_recv.at[i], place.partner) for i, (src, dst) in
            enumerate(list(zip(heads, spots[1])) + list(zip(given, kept)))]
    ends(pair[:len(heads)])
    a_own = ends([pltpu.make_async_copy(am_rows.at[:, pl.ds((2 * part + half) * half_depth, half_depth)], every_a(part, OWN, OWN).at[half], own_sem)
                  for part in BOTH for half in BOTH])

    piece = head // WO_CHUNKS

    def wo_message(part, passed, d, i):
        src, dst = (wo.at[part, s, 0, pl.ds(i * piece, piece)] for s in ((FROM[d], FAR) if passed else (OWN, FROM[d])))
        sems = (part, passed, d, i)
        return remote(src, dst, wo_send.at[sems], wo_recv.at[sems], place.neighbour(part, SLOW, STEP[d]))

    def wo_to_partner(part, s):
        remote(wo.at[part, s, 0], wo.at[part, s, 1], bulk_send, bulk_recv, place.partner).start()

    passes = [range(d * WO_CHUNKS // 2, (d + 1) * WO_CHUNKS // 2) for d in BOTH]

    def wo_start(i):
        for d in BOTH:
            for part in BOTH:
                wo_message(part, 0, d, i).start()

    def wo_pass(k):
        for d in BOTH:
            for part in BOTH:
                wo_message(part, 0, d, passes[d][k]).wait_recv()
                wo_message(part, 1, d, passes[d][k]).start()

    def wo_arrived():
        for d in BOTH:
            for part in BOTH:
                for i in passes[1 - d]:
                    wo_message(part, 0, d, i).wait_recv()
                wo_to_partner(part, FROM[d])

    def wo_last():
        for part in BOTH:
            for d in BOTH:
                for i in passes[d]:
                    wo_message(part, 1, d, i).wait_recv()
            wo_to_partner(part, FAR)

    wait(wo_loads)
    wo_start(0)
    wait(a_own)
    wait(loads)
    wait(own_b)
    gathers = [Gather(place, every_a, a_send, a_recv, absolute=True), Gather(place, every_b, b_send, b_recv, absolute=True)]

    def both(stage_of, *more):
        return lambda: [getattr(g, stage_of)(*more) for g in gathers]

    both('own')()
    for part in BOTH:
        wo_to_partner(part, OWN)
    for copy in pair[:len(heads)]:
        copy.wait_recv()
    for core in BOTH:
        pieces = [a_raw[core, i, a] if i < len(w_heads) else jnp.zeros((per, depth), BF) for a in range(adapters) for i in RING]
        a_rows[core * 2 * TILE:(core + 1) * 2 * TILE, :] = jnp.concatenate(pieces, axis=0)
    mine = [(place.y, place.x), (place.x, place.y)]
    steps = chips // 2

    def block(part, ds, df):
        return lows.at[part, place.turn(mine[part][0], ds), place.turn(mine[part][1], df)]

    background = {1: lambda: (wo_start(1), ends(pair[len(heads):])), 2: both('near'), 3: lambda: wo_start(2), 4: both('row'), 5: lambda: wo_start(3),
                  7: both('sides', *FROM, FAR)}

    def project(step):
        slot = lax.rem(step, 2)

        @pl.when(step + 1 < steps)
        def _():
            ends(x_loads(step + 1))

        for at, what in background.items():
            pl.when(step == at)(lambda what=what: (what(), None)[1])
        wait(x_loads(step))
        for i in BOTH:
            h[i * seq_len:(i + 1) * seq_len, :] = normed(xbuf[slot, i].astype(F32), gain_ref[...])
        rows = pl.ds(pl.multiple_of(step * 2 * seq_len, LANE), 2 * seq_len)
        chunk = fit(2 * cols, 256)
        for n in range(2 * cols // chunk):
            z[rows, n * chunk:(n + 1) * chunk] = dot(h[...], w[:, n * chunk:(n + 1) * chunk])
        low = dot_rows(a_rows[...], h[...])
        half, at = step // (steps // 2), lax.rem(step, steps // 2) * 2 * seq_len
        for part in BOTH:
            pieces = []
            for i in BOTH:
                options = [low[TILE * (2 * part + a):TILE * (2 * part + a + 1), i * seq_len:(i + 1) * seq_len] for a in range(adapters)]
                chosen = options[0]
                for a in range(1, adapters):
                    chosen = jnp.where(ids_ref[4 * step + 2 * i + place.core] == a, options[a], chosen)
                pieces.append(chosen)
            lows[part, mine[part][0], mine[part][1], half, :, pl.ds(pl.multiple_of(at, LANE), 2 * seq_len)] = jnp.concatenate(pieces, axis=1).astype(BF)

    loop(steps, project)
    low_gather = Gather(place, block, send_sem, recv_sem, absolute=True)
    low_gather.own()
    row, col = (lax.broadcasted_iota(jnp.int32, (2 * rank, rank), axis) for axis in BOTH)
    spot, kind = row // TILE, lax.rem(row, TILE) // per
    for part in BOTH:
        chip_of = spot if part == 0 else lax.rem(spot, side) * side + spot // side
        to = chip_of * 2 * per + part * per + lax.rem(row, per)
        for i in range(3):
            spread_rows = jnp.where((kind == i) & (col == to), 1.0, 0.0).astype(BF)
            for a in range(adapters):
                for o in BOTH:
                    bx[a, part, :, o * cols + i * head:o * cols + (i + 1) * head] = dot(spread_rows, b_raw[o, i, a]).astype(BF)
    low_gather.near()
    wo_pass(0)
    low_gather.row()
    wo_pass(1)
    low_gather.sides(*FROM, FAR)
    wo_arrived()
    low_gather.far()
    causal = lax.broadcasted_iota(jnp.int32, (seq_len, seq_len), 0) >= lax.broadcasted_iota(jnp.int32, (seq_len, seq_len), 1)

    def swap(part, ds, df):
        sems = (part, ds, df)
        to = place.neighbour(part, SLOW, ds)
        return remote(att.at[sems], act.at[part, lax.rem(len(RING) - ds, len(RING)), df], swap_send.at[sems], swap_recv.at[sems], to)

    def attention(i):
        dy, dx = side - 1 - i // side, side - 1 - lax.rem(i, side)
        chip = place.turn(place.y, dy) * side + place.turn(place.x, dx)
        adapter = ids_ref[2 * chip + place.core]
        half, at = chip // steps, pl.ds(pl.multiple_of(lax.rem(chip, steps) * seq_len, LANE), seq_len)
        zs = z[pl.ds(pl.multiple_of(chip * seq_len, LANE), seq_len), :]
        for part in BOTH:
            zs += scale * dot_columns(lows[part, :, :, half, :, at].reshape(-1, seq_len), bx[adapter, part])
        for i_head in BOTH:
            q, k, v = (zs[:, i_head * cols + i * head:i_head * cols + (i + 1) * head] for i in range(3))
            q, k = ((r * cos_ref[...] + pltpu.roll(r, head // 2, axis=1) * sin_ref[...]).astype(BF) for r in (q, k))
            scores = jnp.where(causal, dot_rows(q, k) * head ** -0.5, -1e30)
            e = jnp.exp(scores - jnp.max(scores, axis=-1, keepdims=True))
            prob = (e / jnp.sum(e, axis=-1, keepdims=True)).astype(BF)
            mixed = dot(prob, v.astype(BF)).astype(BF)
            for part, (ds, df) in enumerate(((dy, dx), (dx, dy))):
                att[part, ds, df, :, i_head * head:(i_head + 1) * head] = mixed[part * seq_len // 2:(part + 1) * seq_len // 2]

    def attention_pair(k):
        for i in BOTH:
            attention(2 * k + i)
        for i in BOTH:
            dy, dx = side - 1 - (2 * k + i) // side, side - 1 - lax.rem(2 * k + i, side)
            for part, (ds, df) in enumerate(((dy, dx), (dx, dy))):
                pl.when(ds != OWN)(swap(part, ds, df).start)
        pl.when(k == 2)(wo_last)

    loop(chips // 2, attention_pair)
    for part in BOTH:
        act[part, OWN] = att[part, OWN]
    both('far')()
    bulk = [remote(ref.at[place.core], ref.at[place.core], pair_send.at[len(pair) + i], pair_recv.at[len(pair) + i], place.partner) for i, ref in enumerate((a_all, b_all))]
    ends(bulk)
    pltpu.make_async_copy(wo.at[:, :, 1], wo.at[:, :, 1], bulk_recv).wait()
    chunk = fit(width, 512)
    rows = seq_len // 2
    blocks = (len(RING), rows)
    fast = FastScatter(place, lambda part, df: stage.at[part, df], near, landed, fast_send, fast_recv)

    def sum_heads(part, at):
        return sum(dot(act[part, s].reshape(-1, 2 * head), wo[part, s, :, :, at].reshape(2 * head, -1)) for s in RING)

    for part in BOTH:
        for ds in RING[1:]:
            for df in RING:
                swap(part, ds, df).wait_recv()

        def columns(n):
            at = pl.ds(pl.multiple_of(n * chunk, chunk), chunk)
            stage[part, :, :, at] = sum_heads(part, at).reshape(blocks + (chunk,)).astype(BF)

        loop(width // chunk, columns)
        chosen = rows_of_adapter(place, ids_ref, part, OWN, (len(RING) * rows, rank))
        stage[part, :, :, width:] = pick_columns(sum_heads(part, pl.ds(width, adapters * rank)), chosen).reshape(blocks + (rank,)).astype(BF)
        for df in RING[1:]:
            fast.ready(part, df)
    fast.finish()
    fast.store(out_ref, load_sem)
    for copy in pair[len(heads):] + bulk:
        copy.wait_recv()
    for copy in pair + bulk:
        copy.wait_send()
    for g in gathers + [low_gather]:
        g.sent()
    pltpu.make_async_copy(wo.at[:, :, 1], wo.at[:, :, 1], bulk_send).wait()
    for part in BOTH:
        for d in BOTH:
            for i in range(WO_CHUNKS):
                wo_message(part, 0, d, i).wait_send()
            for i in passes[d]:
                wo_message(part, 1, d, i).wait_send()
        for ds in RING[1:]:
            for df in RING:
                swap(part, ds, df).wait_send()


def attend(ids, x_in, gain, heads, w_o, a_o, a_mlp, b_rows, given, side, scale, collective_id):
    _, seq_len, depth = x_in.shape
    head = heads[0].shape[1]
    cols = 3 * head
    adapters, _, rank = a_o.shape
    per = a_mlp[0].shape[1]
    chips = side * side
    half_dim = head // 2
    inv_freq = ROPE_BASE ** (-2.0 * np.arange(half_dim) / head)
    angle = np.arange(seq_len)[:, None] * inv_freq[None, :]
    cos, sin = np.cos(angle), np.sin(angle)
    tables = [jnp.asarray(np.concatenate(pair, axis=1), F32) for pair in ((cos, cos), (-sin, sin))]
    n_pair = len(heads) + len(given) + 2
    rows, out_cols = seq_len // 2, depth + rank
    every = (2, 2, side, side, 2)
    return pl.pallas_call(
        functools.partial(attend_kernel, side, adapters, scale, len(given)),
        out_shape=[jax.ShapeDtypeStruct((seq_len, out_cols), BF), jax.ShapeDtypeStruct(every + (2 * adapters * per, depth // 4), BF),
                   jax.ShapeDtypeStruct(every + b_rows[0].shape[1:], BF)] + [jax.ShapeDtypeStruct(g.shape, g.dtype) for g in given],
        in_specs=[SMEM, HBM, VMEM, VMEM, VMEM] + [HBM] * (len(heads) + 6 + len(given)),
        out_specs=[HBM] * (3 + len(given)),
        scratch_shapes=[
            pltpu.VMEM((depth, 2 * cols), BF),
            pltpu.VMEM((2, 3, adapters, per, depth), BF),
            pltpu.VMEM((2, 3, adapters, rank, head), BF),
            pltpu.VMEM((2 * 2 * TILE, depth), BF),
            pltpu.VMEM((adapters, 2, 2 * rank, 2 * cols), BF),
            pltpu.VMEM((2, 2, seq_len, depth), BF),
            pltpu.VMEM((2 * seq_len, depth), BF),
            pltpu.VMEM((chips * seq_len, 2 * cols), F32),
            pltpu.VMEM((2, side, side, 2, TILE, chips * seq_len // 2), BF),
            pltpu.VMEM((2, side, side, rows, 2 * head), BF),
            pltpu.VMEM((2, side, side, rows, 2 * head), BF),
            pltpu.VMEM((2, side, 2, head, depth + adapters * rank), BF),
            pltpu.VMEM((2, side, rows, out_cols), BF),
        ] + fast_scratch(rows, out_cols) + [
            pltpu.VMEM((2, adapters, per, depth), BF),
            pltpu.VMEM((2 * adapters * per, depth), BF),
            DMA((n_pair,)), DMA((n_pair,)), DMA, DMA((2,)), DMA, DMA, DMA((2, 2, 2, WO_CHUNKS)), DMA((2, 2, 2, WO_CHUNKS)), DMA, DMA, DMA((2, 4, 4)), DMA((2, 4, 4)),
        ] + GATHER_SEMS * 3 + FAST_SEMS,
        compiler_params=comm_params(collective_id),
        name='attend',
    )(ids, x_in, gain.reshape(1, depth), *tables, *heads, w_o, a_o, *a_mlp, *b_rows, *given)


def row_proj_kernel(side, adapters, ids_ref, act_ref, w_own, w_par, a_own, a_par, out_ref,
                    act, w, stage, near, landed, fast_near, fast_landed, slow_send, slow_recv, fast_send, fast_recv, load_sem):
    place = Place(side)
    share, width = w_own.shape
    half = w.shape[0] // 2
    rank = a_own.shape[2]
    rows = stage.shape[3]
    quarter = rows // 2
    if share < half:
        for at in (0, half):
            w[at + share // TILE * TILE:at + half, :] = jnp.zeros((half - share // TILE * TILE, w.shape[1]), BF)
    loads = [pltpu.make_async_copy(act_ref, act, load_sem)]
    for at, w_part, a_part in ((0, w_own, a_own), (half, w_par, a_par)):
        loads.append(pltpu.make_async_copy(w_part, w.at[pl.ds(at, share), first(width)], load_sem))
        for a in range(adapters):
            loads.append(pltpu.make_async_copy(a_part.at[a], w.at[pl.ds(at, share), pl.ds(width + a * rank, rank)], load_sem))
    ends(loads)
    place.barrier()
    wait(loads)
    chunk = fit(width, 512)

    def unit(part, ds):
        def columns(n):
            at = pl.ds(pl.multiple_of(n * chunk, chunk), chunk)
            stage[part, ds, :, :, at] = dot(act[part, ds], w[:, at]).reshape(len(RING), rows, chunk).astype(BF)

        loop(width // chunk, columns)
        chosen = rows_of_adapter(place, ids_ref, part, ds, (len(RING) * rows, rank))
        stage[part, ds, :, :, width:] = pick_columns(dot(act[part, ds], w[:, width:]), chosen).reshape(len(RING), rows, rank).astype(BF)

    blocks = ((FAR, LAST), (OWN, NEXT))

    def slow(part, kind, d, i):
        df = blocks[1 - d][i] if kind == FREE else blocks[d][i]
        sems = (part, kind, d, i)
        src = stage.at[part, FAR if kind == PASS else TOWARD[d], df]
        dst = near.at[part, d, i] if kind == PASS else landed.at[part, d, df]
        return remote(src, dst, slow_send.at[sems], slow_recv.at[sems], place.neighbour(part, SLOW, STEP[d]))

    fast = FastScatter(place, lambda part, df: stage.at[part, OWN, df], fast_near, fast_landed, fast_send, fast_recv)
    for part in BOTH:
        unit(part, FAR)
        for i in BOTH:
            for d in BOTH:
                slow(part, PASS, d, i).start()
    loop(len(RING), lambda i: unit(lax.rem(i, 2), NEXT + 2 * (i // 2)))
    for i in BOTH:
        for d in BOTH:
            for part in BOTH:
                slow(part, FREE, d, i).start()
    loop(2, lambda part: unit(part, OWN))
    for i in BOTH:
        for d in BOTH:
            for part in BOTH:
                slow(part, PASS, d, i).wait_recv()
                add(stage.at[part, TOWARD[d], blocks[d][i]], near.at[part, d, i])
                slow(part, SUM, d, i).start()
    for i in BOTH:
        for d in BOTH:
            df = blocks[d][i]
            for part in BOTH:
                slow(part, SUM, d, i).wait_recv()
                slow(part, FREE, 1 - d, i).wait_recv()
                add(stage.at[part, OWN, df], landed.at[part, UP, df], landed.at[part, DOWN, df])
                fast.ready(part, df)
    fast.finish()
    fast.store(out_ref, load_sem)
    for part in BOTH:
        for kind in range(3):
            for d in BOTH:
                for i in BOTH:
                    slow(part, kind, d, i).wait_send()


def row_proj(ids, act, w_own, w_par, a_own, a_par, side, collective_id):
    adapters, _, rank = a_own.shape
    width = w_own.shape[1]
    rows = act.shape[2] // side
    cols = width + rank
    blocks = (rows, cols)
    return pl.pallas_call(
        functools.partial(row_proj_kernel, side, adapters),
        out_shape=jax.ShapeDtypeStruct((2 * rows, cols), BF),
        in_specs=[SMEM] + [HBM] * 5,
        out_specs=HBM,
        scratch_shapes=[
            pltpu.VMEM(act.shape, BF),
            pltpu.VMEM((act.shape[3], width + adapters * rank), BF),
            pltpu.VMEM((2, side, side) + blocks, BF),
            pltpu.VMEM((2, 2, 2) + blocks, BF),
            pltpu.VMEM((2, 2, side) + blocks, BF),
        ] + fast_scratch(rows, cols) + [DMA((2, 3, 2, 2))] * 2 + FAST_SEMS + [DMA],
        compiler_params=comm_params(collective_id),
        name='row_proj',
    )(ids, act, w_own, w_par, a_own, a_par)


def finish(sums_ref, resid, b_ref, chosen, scale, adapters):
    _, _, side, _, rank, part = b_ref.shape
    width = sums_ref.shape[1] - rank
    low = spread(sums_ref[:, width:].astype(F32), chosen, adapters)
    delta = [dot(low, b_ref[core, :, y, x].reshape(adapters * rank, part)) for y in range(side) for x in range(side) for core in BOTH]
    return resid.astype(F32) + (sums_ref[:, :width].astype(F32) + scale * jnp.concatenate(delta, axis=1))


def own_rows(place, ids_ref, shape):
    return jnp.full(shape, ids_ref[place.device(0, 0)], jnp.int32)


def gate_up_kernel(side, adapters, scale, ids_ref, sums_ref, x_ref, gain_ref, a_all, b_all, wg_own, wg_par, wu_own, wu_par, bg_own, bg_par, bu_own, bu_par,
                   hid_ref, mid_ref, gbuf, w, b, a_ref, b_ref, hid, load_sem, b_sem, store_sem, send_sem, recv_sem):
    place = Place(side)
    b_load = ends([pltpu.make_async_copy(b_all.at[:, :, :, :, 0], b_ref, b_sem), pltpu.make_async_copy(a_all, a_ref, b_sem)])
    share, width = wg_own.shape
    half = w.shape[1] // 2
    rank = bg_own.shape[2]
    seq_len = sums_ref.shape[0]
    edge = share // TILE * TILE
    for at in (0, half):
        for kind in BOTH:
            w[kind, at + edge:at + half, :] = jnp.zeros((half - edge, width), BF)
            b[kind, at + edge:at + half, :] = jnp.zeros((half - edge, adapters * rank), BF)
    loads = []
    for kind, pieces in enumerate(((wg_own, wg_par, bg_own, bg_par), (wu_own, wu_par, bu_own, bu_par))):
        for i, at in enumerate((0, half)):
            loads.append(pltpu.make_async_copy(pieces[i], w.at[kind, pl.ds(at, share)], load_sem))
            for a in range(adapters):
                loads.append(pltpu.make_async_copy(pieces[2 + i].at[a], b.at[kind, pl.ds(at, share), pl.ds(a * rank, rank)], load_sem))
    ends(loads)
    rows = seq_len // 4
    chosen = own_rows(place, ids_ref, (seq_len, rank))
    wait(b_load)
    mid = finish(sums_ref, x_ref[...], b_ref, chosen, scale, adapters).astype(BF)
    mid_ref[...] = mid
    h2 = normed(mid.astype(F32), gain_ref[...])
    lows = []
    for core in BOTH:
        pieces = [dot_rows(h2[:, i * width // 4:(i + 1) * width // 4], a_ref[core, i // 2, :, :, i % 2].reshape(-1, width // 4)) for i in RING]
        lows.append(sum(pieces).astype(BF))
    low = jnp.concatenate(lows, axis=1)
    per = rank // (2 * side * side)
    row, col = (lax.broadcasted_iota(jnp.int32, (low.shape[1], 2 * rank), axis) for axis in BOTH)
    kind, rank_at = col // rank, lax.rem(col, rank)
    chip, core = rank_at // (2 * per), lax.rem(rank_at // per, 2)
    pick = ((core * side * side + chip) * 2 + kind) * adapters * per + ids_ref[place.device(0, 0)] * per + lax.rem(rank_at, per)
    low = dot(low, jnp.where(row == pick, 1.0, 0.0).astype(BF)).astype(BF)
    for part in BOTH:
        for piece in BOTH:
            at = (2 * part + piece) * rows
            gbuf[part, OWN, OWN, piece, :, :width] = h2[at:at + rows]
            gbuf[part, OWN, OWN, piece, :, width:] = low[at:at + rows]
    place.barrier()
    chunk = fit(2 * half, 256)

    def unit(part, ds):
        unit_rows = len(RING) * 2 * rows
        low = gbuf[part, ds, :, :, :, width:].reshape(unit_rows, 2 * rank).astype(F32)
        chosen = rows_of_adapter(place, ids_ref, part, ds, (unit_rows, rank))
        lows = [spread(low[:, kind * rank:(kind + 1) * rank], chosen, adapters) for kind in BOTH]

        def columns(n):
            at = pl.ds(pl.multiple_of(n * chunk, chunk), chunk)
            act = gbuf[part, ds, :, :, :, :width].reshape(unit_rows, width)
            gate, up = (dot_rows(act, w[kind, at]) + scale * dot_rows(lows[kind], b[kind, at]) for kind in BOTH)
            hid[part, ds, :, at] = (gate * jax.nn.sigmoid(gate) * up).astype(BF)

        loop(2 * half // chunk, columns)
        pltpu.make_async_copy(hid.at[part, ds], hid_ref.at[part, ds], store_sem).start()

    def on_row():
        wait(loads)
        loop(2, lambda part: unit(part, OWN))

    Gather(place, lambda part, ds, df: gbuf.at[part, ds, df], send_sem, recv_sem).run(
        on_row, lambda: loop(len(RING), lambda i: unit(lax.rem(i, 2), NEXT + 2 * (i // 2))), lambda: loop(2, lambda part: unit(part, FAR)))
    pltpu.make_async_copy(hid, hid_ref, store_sem).wait()


def gate_up(ids, sums, x_own, gain, a_all, b_all, w, side, scale, collective_id):
    seq_len, depth = x_own.shape
    share = w[0].shape[0]
    adapters, _, rank = w[4].shape
    half = (share + LANE - 1) // LANE * LANE
    hidden = jax.ShapeDtypeStruct((2, side, side * seq_len // 2, 2 * half), BF)
    return pl.pallas_call(
        functools.partial(gate_up_kernel, side, adapters, scale),
        out_shape=[hidden, jax.ShapeDtypeStruct(x_own.shape, BF)],
        in_specs=[SMEM] + [VMEM] * 3 + [HBM] * (2 + len(w)),
        out_specs=[HBM, VMEM],
        scratch_shapes=[
            pltpu.VMEM((2, side, side, 2, seq_len // 4, depth + 2 * rank), BF),
            pltpu.VMEM((2, 2 * half, depth), BF),
            pltpu.VMEM((2, 2 * half, adapters * rank), BF),
            pltpu.VMEM(a_all.shape, BF),
            pltpu.VMEM(b_all.shape[:4] + b_all.shape[5:], BF),
            pltpu.VMEM(hidden.shape, BF),
            DMA, DMA, DMA,
        ] + GATHER_SEMS,
        compiler_params=comm_params(collective_id),
        name='gate_up',
    )(ids, sums, x_own, gain.reshape(1, depth), a_all, b_all, *w)


def deliver_kernel(side, adapters, scale, ids_ref, sums_ref, x_ref, b_all, out_ref, b_ref, b_sem, pair_send, pair_recv, send_sem, recv_sem):
    place = Place(side)
    b_load = ends([pltpu.make_async_copy(b_all.at[:, :, :, :, 1], b_ref, b_sem)])
    seq_len = sums_ref.shape[0]
    rows = seq_len // 4
    chosen = own_rows(place, ids_ref, (seq_len, b_ref.shape[4]))
    wait(b_load)
    y = finish(sums_ref, x_ref[...], b_ref, chosen, scale, adapters).astype(BF)
    for part in BOTH:
        for piece in BOTH:
            at = (2 * part + piece) * rows
            out_ref[place.device(0, 0), part, piece] = y[at:at + rows]
    place.barrier(place.partner)

    def block(part, ds, df):
        return out_ref.at[place.sequence(part, ds, df), part]

    def seen(part, ds, df, half):
        ref = block(part, ds, df) if half is None else block(part, ds, df).at[half]
        remote(ref, ref, pair_send, pair_recv, place.partner).start()

    for part in BOTH:
        seen(part, OWN, OWN, None)
    Gather(place, block, send_sem, recv_sem, absolute=True, seen=seen).run()
    every = out_ref.at[first(side * side)]
    for sem in (pair_send, pair_recv):
        pltpu.make_async_copy(every, every, sem).wait()


def put_kernel(y_ref, out_ref, sem):
    wait(ends([pltpu.make_async_copy(y_ref.at[i], out_ref.at[i], sem) for i in range(y_ref.shape[0])]))


def deliver(ids, sums, x_mid, b_all, side, scale, collective_id):
    seq_len, depth = x_mid.shape
    rows = seq_len // 4
    y = pl.pallas_call(
        functools.partial(deliver_kernel, side, b_all.shape[1], scale),
        out_shape=pltpu.VMEM((2 * side * side, 2, 2, rows, depth), BF),
        in_specs=[SMEM] + [VMEM] * 2 + [HBM],
        scratch_shapes=[pltpu.VMEM(b_all.shape[:4] + b_all.shape[5:], BF), DMA, DMA, DMA] + GATHER_SEMS,
        compiler_params=comm_params(collective_id, VMEM_SMALL),
        name='deliver',
    )(ids, sums, x_mid, b_all)
    return pl.pallas_call(
        put_kernel,
        out_shape=jax.ShapeDtypeStruct(y.shape, BF),
        in_specs=[pl.BlockSpec(memory_space=pl.ANY)],
        out_specs=HBM,
        scratch_shapes=[DMA],
        compiler_params=pltpu.CompilerParams(vmem_limit_bytes=VMEM_LEAST),
        name='put',
    )(y)


def solution(mesh):
    tp_size = mesh.shape['tensor']
    side = math.isqrt(tp_size // 2)
    rows_only = P('tensor', None)
    head_split = P(None, 'tensor', None)
    last_split = P(None, None, 'tensor')
    b_head_split = P(None, None, 'tensor', None)
    in_specs = (P('data', None, None), P('data'), P(None), P(None),
                head_split, head_split, head_split, P('tensor', None, None),
                P(None, 'tensor'), P(None, 'tensor'), rows_only,
                last_split, b_head_split, last_split, b_head_split, last_split, b_head_split,
                P(None, 'tensor', None, None), last_split,
                last_split, last_split, last_split, last_split,
                head_split, last_split)

    def local_layer(x_in, adapter_ids, gain_attn, gain_mlp, w_q, w_k, w_v, w_o, w_gate, w_up, w_down, a_q, b_q, a_k, b_k, a_v, b_v, a_o, b_o, a_gate, b_gate, a_up, b_up, a_down, b_down):
        scale = ALPHA / b_q.shape[1]
        index = lax.axis_index('tensor')

        def across(a):
            return a.swapaxes(-1, -2)

        heads = [w[:, 0] for w in (w_q, w_k, w_v)] + [across(a) for a in (a_q, a_k, a_v)] + [b[:, :, 0] for b in (b_q, b_k, b_v)]
        given = [across(w_gate), across(w_up), across(b_gate), across(b_up), w_down, a_down]
        sums, all_a, all_b, *kept = attend(adapter_ids, x_in, gain_attn, heads, w_o[0], a_o[:, 0], (across(a_gate), across(a_up)), (b_o, b_down), given, side, scale, 0)
        x_own = lax.dynamic_index_in_dim(x_in, index, axis=0, keepdims=False)
        w = [piece for pair in zip(given[:4], kept[:4]) for piece in pair]
        hidden, x_mid = gate_up(adapter_ids, sums, x_own, gain_mlp, all_a, all_b, w, side, scale, 1)
        sums = row_proj(adapter_ids, hidden, given[4], kept[4], given[5], kept[5], side, 2)
        y = deliver(adapter_ids, sums, x_mid, all_b, side, scale, 3)
        return y.reshape(x_in.shape)

    return jax.shard_map(local_layer, mesh=mesh, in_specs=in_specs, out_specs=P('data', None, None), check_vma=False)
```

```python
import functools
import math

import jax
import jax.numpy as jnp
import numpy as np
from jax import lax
from jax.experimental import pallas as pl
from jax.experimental.pallas import tpu as pltpu
from jax.sharding import PartitionSpec as P

ALPHA = 16.0
ROPE_BASE = 10000.0
EPSILON = 1e-5
BF = jnp.bfloat16
F32 = jnp.float32
LANE = 128
TILE = 16
VMEM_MOST = 67043328
VMEM_SMALL = VMEM_MOST * 3 // 8
VMEM_LEAST = VMEM_MOST // 32
MESH = pl.DeviceIdType.MESH
HBM = pl.BlockSpec(memory_space=pltpu.HBM)
VMEM = pl.BlockSpec(memory_space=pltpu.VMEM)
SMEM = pl.BlockSpec(memory_space=pltpu.SMEM)
DMA = pltpu.SemaphoreType.DMA

OWN, NEXT, FAR, LAST = RING = range(4)
UP, DOWN = BOTH = range(2)
STEP = (NEXT, -NEXT)
FROM = (LAST, NEXT)
AWAY = (NEXT, LAST, FAR)
TOWARD = (NEXT, LAST)
FAST, SLOW = BOTH


def fit(size, most):
    return max(c for c in range(LANE, most + 1, LANE) if size % c == 0)


def first(size):
    return pl.ds(0, size)


def dot(a, b):
    return jnp.dot(a, b, preferred_element_type=F32)


def dot_rows(a, b):
    return lax.dot_general(a, b, (((1,), (1,)), ((), ())), preferred_element_type=F32)


def dot_columns(a, b):
    return lax.dot_general(a, b, (((0,), (0,)), ((), ())), preferred_element_type=F32)


def normed(act, gain):
    return (act * lax.rsqrt(jnp.mean(act * act, axis=-1, keepdims=True) + EPSILON) * gain).astype(BF)


def ends(copies):
    for copy in copies:
        copy.start()
    return copies


def wait(copies):
    for copy in copies:
        copy.wait()


def loop(count, body):
    lax.fori_loop(0, count, lambda i, carry: (body(i), carry)[1], 0)


class Place:
    def __init__(self, side):
        index = lax.axis_index('tensor')
        self.side = side
        self.core = lax.rem(index, 2)
        chip = index // 2
        self.y, self.x = chip // side, lax.rem(chip, side)
        self.partner = index + 1 - 2 * self.core

    def turn(self, at, steps):
        return lax.rem(at + steps + self.side, self.side)

    def device(self, dy, dx):
        return (self.turn(self.y, dy) * self.side + self.turn(self.x, dx)) * 2 + self.core

    def neighbour(self, part, ring, step):
        return self.device(0, step) if part == ring else self.device(step, 0)

    def sequence(self, part, ds, df):
        return self.device(jnp.where(part == 0, ds, df), jnp.where(part == 0, df, ds))

    def announce(self, *more):
        to = [self.neighbour(0, ring, step) for ring in BOTH for step in STEP] + list(more)
        for device in to:
            pl.semaphore_signal(pltpu.get_barrier_semaphore(), inc=1, device_id={'tensor': device}, device_id_type=MESH)
        self.announced = len(to)

    def meet(self):
        pl.semaphore_wait(pltpu.get_barrier_semaphore(), self.announced)


def remote(src, dst, send_sem, recv_sem, to):
    return pltpu.make_async_remote_copy(src_ref=src, dst_ref=dst, send_sem=send_sem, recv_sem=recv_sem, device_id={'tensor': to}, device_id_type=MESH)


GATHER_SEMS = [DMA((2, 2, 2, 2, 4))] * 2


class Gather:
    def __init__(self, place, block, send_sem, recv_sem, absolute=False, seen=None):
        self.place, self.block, self.sems, self.absolute, self.seen = place, block, (send_sem, recv_sem), absolute, seen

    def message(self, part, ring, passed, d, j=OWN):
        spot = (lambda s: (s, j)) if ring == SLOW else (lambda s: (OWN, s))
        src, dst = (FROM[d], FAR) if passed else (OWN, FROM[d])
        a, b = self.block(part, *spot(src)), self.block(part, *spot(src if self.absolute else dst))
        if passed:
            a, b = a.at[d], b.at[d]
        return remote(a, b, *(sem.at[part, ring, passed, d, j] for sem in self.sems), self.place.neighbour(part, ring, STEP[d]))

    def arrived(self, part, ring, passed, d, j=OWN):
        self.message(part, ring, passed, d, j).wait_recv()
        if self.seen:
            at = FAR if passed else FROM[d]
            self.seen(part, *((at, j) if ring == SLOW else (OWN, at)), d if passed else None)

    def own(self):
        for ring in BOTH:
            for d in BOTH:
                for part in BOTH:
                    self.message(part, ring, 0, d).start()

    def near(self):
        for d in BOTH:
            for part in BOTH:
                self.arrived(part, FAST, 0, d)
                self.message(part, FAST, 1, d).start()
                for e in BOTH:
                    self.message(part, SLOW, 0, e, FROM[d]).start()

    def row(self):
        for part in BOTH:
            for d in BOTH:
                self.arrived(part, FAST, 1, d)
            for e in BOTH:
                self.message(part, SLOW, 0, e, FAR).start()
        self.sides(OWN)

    def sides(self, *blocks):
        for j in blocks:
            for part in BOTH:
                for d in BOTH:
                    self.arrived(part, SLOW, 0, d, j)
                    self.message(part, SLOW, 1, d, j).start()

    def far(self):
        for j in (OWN,) + AWAY:
            for part in BOTH:
                for d in BOTH:
                    self.arrived(part, SLOW, 1, d, j)

    def sent(self):
        for part in BOTH:
            for d in BOTH:
                for passed in BOTH:
                    self.message(part, FAST, passed, d).wait_send()
                    for j in RING:
                        self.message(part, SLOW, passed, d, j).wait_send()

    def run(self, on_row=None, on_sides=None, on_far=None):
        self.own()
        self.near()
        self.row()
        if on_row:
            on_row()
        self.sides(*AWAY)
        if on_sides:
            on_sides()
        self.far()
        if on_far:
            on_far()
        self.sent()


def rows_of_adapter(place, ids_ref, part, ds, shape):
    block = lax.broadcasted_iota(jnp.int32, shape, 0) // (shape[0] // len(RING))
    chosen = jnp.zeros(shape, jnp.int32)
    for df in RING:
        chosen = jnp.where(block == df, ids_ref[place.sequence(part, ds, df)], chosen)
    return chosen


def pick_columns(low, chosen):
    rank = chosen.shape[1]
    kept = low[:, :rank]
    for a in range(1, low.shape[1] // rank):
        kept = jnp.where(chosen == a, low[:, a * rank:(a + 1) * rank], kept)
    return kept


def spread(low, chosen, adapters):
    return jnp.concatenate([jnp.where(chosen == a, low, 0.0) for a in range(adapters)], axis=1).astype(BF)


PASS, FREE, SUM = range(3)
FAST_SEMS = [DMA((2, 3, 2))] * 2


def add(into, *others):
    def some(i):
        at = pl.ds(pl.multiple_of(i * TILE, TILE), TILE)
        total = into[at, :].astype(F32)
        for other in others:
            total += other[at, :].astype(F32)
        into[at, :] = total.astype(BF)

    loop(into.shape[0] // TILE, some)


class FastScatter:
    def __init__(self, place, stage, near, landed, send_sem, recv_sem):
        self.place, self.stage, self.near, self.landed, self.sems = place, stage, near, landed, (send_sem, recv_sem)
        quarter = near.shape[2]
        self.halves = (first(quarter), pl.ds(quarter, quarter))

    def message(self, part, kind, d):
        at = self.halves[1 - d] if kind == FREE else self.halves[d]
        src = self.stage(part, FAR if kind == PASS else TOWARD[d]).at[at]
        dst = self.near.at[part, d] if kind == PASS else self.landed.at[part, d, at]
        sems = [sem.at[part, kind, d] for sem in self.sems]
        return remote(src, dst, *sems, self.place.neighbour(part, FAST, STEP[d]))

    def ready(self, part, df):
        for d in BOTH:
            if df == FAR:
                self.message(part, PASS, d).start()
            elif df == TOWARD[d]:
                self.message(part, FREE, d).start()

    def finish(self):
        for d in BOTH:
            for part in BOTH:
                self.message(part, PASS, d).wait_recv()
                add(self.stage(part, TOWARD[d]).at[self.halves[d]], self.near.at[part, d])
                self.message(part, SUM, d).start()
        for part in BOTH:
            for d in BOTH:
                self.message(part, FREE, d).wait_recv()
                self.message(part, SUM, d).wait_recv()
            add(self.stage(part, OWN), self.landed.at[part, UP], self.landed.at[part, DOWN])

    def store(self, out_ref, sem):
        rows = self.landed.shape[2]
        wait(ends([pltpu.make_async_copy(self.stage(part, OWN), out_ref.at[pl.ds(part * rows, rows)], sem) for part in BOTH]))
        for part in BOTH:
            for kind in range(3):
                for d in BOTH:
                    self.message(part, kind, d).wait_send()


def fast_scratch(rows, cols):
    return [pltpu.VMEM((2, 2, rows // 2, cols), BF), pltpu.VMEM((2, 2, rows, cols), BF)]


def comm_params(collective_id, limit=VMEM_MOST):
    return pltpu.CompilerParams(collective_id=collective_id, has_side_effects=True, vmem_limit_bytes=limit)


WO_CHUNKS = 8


def attend_kernel(side, adapters, scale, n_keep, ids_ref, x_ref, gain_ref, cos_ref, sin_ref, *rest):
    w_heads, a_heads, b_heads, (wo_ref, ao_ref), a_mlp, b_rows, rest = rest[:3], rest[3:6], rest[6:9], rest[9:11], rest[11:13], rest[13:15], rest[15:]
    given, rest = rest[:n_keep], rest[n_keep:]
    (out_ref, a_all, b_all), rest = rest[:3], rest[3:]
    kept, rest = rest[:n_keep], rest[n_keep:]
    (w, a_raw, b_raw, a_rows, bx, xbuf, h, z, lows, att, act, wo, stage, near, landed, am_raw, am_rows, pair_send, pair_recv, load_sem, x_sem, own_sem,
     wo_load, wo_send, wo_recv, bulk_send, bulk_recv, swap_send, swap_recv,
     send_sem, recv_sem, a_send, a_recv, b_send, b_recv, fast_send, fast_recv) = rest
    place = Place(side)
    place.announce(place.partner, place.device(0, FAR), place.device(FAR, 0))
    head, seq_len, depth = cos_ref.shape[1], x_ref.shape[1], x_ref.shape[2]
    cols = len(w_heads) * head
    chips = side * side
    per = a_raw.shape[3]
    half_depth = depth // 4
    heads = w_heads + a_heads + b_heads
    spots = [[w.at[:, pl.ds(at * cols + i * head, head)] for i in range(3)] + [a_raw.at[place.core, i] for i in range(3)] + [b_raw.at[at, i] for i in range(3)]
             for at in BOTH]
    loads = ends([pltpu.make_async_copy(src, dst, load_sem) for src, dst in zip(heads, spots[0])])

    def x_loads(step):
        slot = lax.rem(step, 2)
        return [pltpu.make_async_copy(x_ref.at[4 * step + 2 * i + place.core], xbuf.at[slot, i], x_sem.at[slot]) for i in BOTH]

    ends(x_loads(0))

    def every(ref):
        return lambda part, ds, df: ref.at[place.core, part, place.turn(place.y, df if part else ds), place.turn(place.x, ds if part else df)]

    every_a, every_b = every(a_all), every(b_all)
    own_loads = ends([pltpu.make_async_copy(a_mlp[i], am_raw.at[i], own_sem) for i in BOTH])
    own_b = [pltpu.make_async_copy(b_rows[half].at[part], every_b(part, OWN, OWN).at[half], load_sem) for part in BOTH for half in BOTH]
    ends(own_b)
    width = wo_ref.shape[1]
    rank = ao_ref.shape[2]
    wo_loads = []
    for part in BOTH:
        wo_loads.append(pltpu.make_async_copy(wo_ref, wo.at[part, OWN, 0, :, first(width)], wo_load))
        for a in range(adapters):
            wo_loads.append(pltpu.make_async_copy(ao_ref.at[a], wo.at[part, OWN, 0, :, pl.ds(width + a * rank, rank)], wo_load))
    ends(wo_loads)
    wait(own_loads)
    am_rows[...] = jnp.concatenate([am_raw[i, a] for i in BOTH for a in range(adapters)], axis=0)
    place.meet()
    pair = [remote(src, dst, pair_send.at[i], pair_recv.at[i], place.partner) for i, (src, dst) in
            enumerate(list(zip(heads, spots[1])) + list(zip(given, kept)))]
    ends(pair[:len(heads)])
    a_own = ends([pltpu.make_async_copy(am_rows.at[:, pl.ds((2 * part + half) * half_depth, half_depth)], every_a(part, OWN, OWN).at[half], own_sem)
                  for part in BOTH for half in BOTH])

    piece = head // WO_CHUNKS

    def wo_message(part, passed, d, i):
        src, dst = (wo.at[part, s, 0, pl.ds(i * piece, piece)] for s in ((FROM[d], FAR) if passed else (OWN, FROM[d])))
        sems = (part, passed, d, i)
        return remote(src, dst, wo_send.at[sems], wo_recv.at[sems], place.neighbour(part, SLOW, STEP[d]))

    def wo_to_partner(part, s):
        remote(wo.at[part, s, 0], wo.at[part, s, 1], bulk_send, bulk_recv, place.partner).start()

    passes = [range(d * WO_CHUNKS // 2, (d + 1) * WO_CHUNKS // 2) for d in BOTH]

    def wo_start(i):
        for d in BOTH:
            for part in BOTH:
                wo_message(part, 0, d, i).start()

    def wo_pass(k):
        for d in BOTH:
            for part in BOTH:
                wo_message(part, 0, d, passes[d][k]).wait_recv()
                wo_message(part, 1, d, passes[d][k]).start()

    def wo_arrived():
        for d in BOTH:
            for part in BOTH:
                for i in passes[1 - d]:
                    wo_message(part, 0, d, i).wait_recv()
                wo_to_partner(part, FROM[d])

    def wo_last():
        for part in BOTH:
            for d in BOTH:
                for i in passes[d]:
                    wo_message(part, 1, d, i).wait_recv()
            wo_to_partner(part, FAR)

    wait(wo_loads)
    for i in range(WO_CHUNKS // 2):
        wo_start(i)
    wait(a_own)
    wait(loads)
    wait(own_b)
    gathers = [Gather(place, every_a, a_send, a_recv, absolute=True), Gather(place, every_b, b_send, b_recv, absolute=True)]

    def both(stage_of, *more):
        for g in gathers:
            getattr(g, stage_of)(*more)

    both('own')
    for i in range(WO_CHUNKS // 2, WO_CHUNKS):
        wo_start(i)
    for part in BOTH:
        wo_to_partner(part, OWN)
    for copy in pair[:len(heads)]:
        copy.wait_recv()
    for core in BOTH:
        pieces = [a_raw[core, i, a] if i < len(w_heads) else jnp.zeros((per, depth), BF) for a in range(adapters) for i in RING]
        a_rows[core * 2 * TILE:(core + 1) * 2 * TILE, :] = jnp.concatenate(pieces, axis=0)
    mine = [(place.y, place.x), (place.x, place.y)]
    steps = chips // 2

    def block(part, ds, df):
        return lows.at[part, place.turn(mine[part][0], ds), place.turn(mine[part][1], df)]

    def project(step):
        slot = lax.rem(step, 2)

        @pl.when(step + 1 < steps)
        def _():
            ends(x_loads(step + 1))

        @pl.when(step == 2)
        def _():
            ends(pair[len(heads):])

        wait(x_loads(step))
        for i in BOTH:
            h[i * seq_len:(i + 1) * seq_len, :] = normed(xbuf[slot, i].astype(F32), gain_ref[...])
        rows = pl.ds(pl.multiple_of(step * 2 * seq_len, LANE), 2 * seq_len)
        chunk = fit(2 * cols, 256)
        for n in range(2 * cols // chunk):
            z[rows, n * chunk:(n + 1) * chunk] = dot(h[...], w[:, n * chunk:(n + 1) * chunk])
        low = dot_rows(a_rows[...], h[...])
        half, at = step // (steps // 2), lax.rem(step, steps // 2) * 2 * seq_len
        for part in BOTH:
            pieces = []
            for i in BOTH:
                options = [low[TILE * (2 * part + a):TILE * (2 * part + a + 1), i * seq_len:(i + 1) * seq_len] for a in range(adapters)]
                chosen = options[0]
                for a in range(1, adapters):
                    chosen = jnp.where(ids_ref[4 * step + 2 * i + place.core] == a, options[a], chosen)
                pieces.append(chosen)
            lows[part, mine[part][0], mine[part][1], half, :, pl.ds(pl.multiple_of(at, LANE), 2 * seq_len)] = jnp.concatenate(pieces, axis=1).astype(BF)

    loop(steps, project)
    low_gather = Gather(place, block, send_sem, recv_sem, absolute=True)
    low_gather.own()
    row, col = (lax.broadcasted_iota(jnp.int32, (2 * rank, rank), axis) for axis in BOTH)
    spot, kind = row // TILE, lax.rem(row, TILE) // per
    for part in BOTH:
        chip_of = spot if part == 0 else lax.rem(spot, side) * side + spot // side
        to = chip_of * 2 * per + part * per + lax.rem(row, per)
        for i in range(3):
            spread_rows = jnp.where((kind == i) & (col == to), 1.0, 0.0).astype(BF)
            for a in range(adapters):
                for o in BOTH:
                    bx[a, part, :, o * cols + i * head:o * cols + (i + 1) * head] = dot(spread_rows, b_raw[o, i, a]).astype(BF)
    low_gather.near()
    wo_pass(0)
    low_gather.row()
    wo_pass(1)
    low_gather.sides(*AWAY)
    wo_pass(2)
    low_gather.far()
    wo_pass(3)
    wo_arrived()
    both('near')
    causal = lax.broadcasted_iota(jnp.int32, (seq_len, seq_len), 0) >= lax.broadcasted_iota(jnp.int32, (seq_len, seq_len), 1)

    def swap(part, ds, df):
        sems = (part, ds, df)
        to = place.neighbour(part, SLOW, ds)
        return remote(att.at[sems], act.at[part, lax.rem(len(RING) - ds, len(RING)), df], swap_send.at[sems], swap_recv.at[sems], to)

    def attention(i):
        dy, dx = side - 1 - i // side, side - 1 - lax.rem(i, side)
        chip = place.turn(place.y, dy) * side + place.turn(place.x, dx)
        adapter = ids_ref[2 * chip + place.core]
        half, at = chip // steps, pl.ds(pl.multiple_of(lax.rem(chip, steps) * seq_len, LANE), seq_len)
        zs = z[pl.ds(pl.multiple_of(chip * seq_len, LANE), seq_len), :]
        for part in BOTH:
            zs += scale * dot_columns(lows[part, :, :, half, :, at].reshape(-1, seq_len), bx[adapter, part])
        for i_head in BOTH:
            q, k, v = (zs[:, i_head * cols + i * head:i_head * cols + (i + 1) * head] for i in range(3))
            q, k = ((r * cos_ref[...] + pltpu.roll(r, head // 2, axis=1) * sin_ref[...]).astype(BF) for r in (q, k))
            scores = jnp.where(causal, dot_rows(q, k) * head ** -0.5, -1e30)
            e = jnp.exp(scores - jnp.max(scores, axis=-1, keepdims=True))
            prob = (e / jnp.sum(e, axis=-1, keepdims=True)).astype(BF)
            mixed = dot(prob, v.astype(BF)).astype(BF)
            for part, (ds, df) in enumerate(((dy, dx), (dx, dy))):
                att[part, ds, df, :, i_head * head:(i_head + 1) * head] = mixed[part * seq_len // 2:(part + 1) * seq_len // 2]

    def attention_pair(k):
        for i in BOTH:
            attention(2 * k + i)
        for i in BOTH:
            dy, dx = side - 1 - (2 * k + i) // side, side - 1 - lax.rem(2 * k + i, side)
            for part, (ds, df) in enumerate(((dy, dx), (dx, dy))):
                pl.when(ds != OWN)(swap(part, ds, df).start)
        pl.when(k == chips // 4)(lambda: both('row'))

    loop(chips // 2, attention_pair)
    wo_last()
    for part in BOTH:
        act[part, OWN] = att[part, OWN]
    both('sides', *AWAY)
    bulk = [remote(ref.at[place.core], ref.at[place.core], pair_send.at[len(pair) + i], pair_recv.at[len(pair) + i], place.partner) for i, ref in enumerate((a_all, b_all))]
    pltpu.make_async_copy(wo.at[:, :, 1], wo.at[:, :, 1], bulk_recv).wait()
    chunk = fit(width, 512)
    rows = seq_len // 2
    blocks = (len(RING), rows)
    fast = FastScatter(place, lambda part, df: stage.at[part, df], near, landed, fast_send, fast_recv)

    def sum_heads(part, at):
        return sum(dot(act[part, s].reshape(-1, 2 * head), wo[part, s, :, :, at].reshape(2 * head, -1)) for s in RING)

    for part in BOTH:
        for ds in RING[1:]:
            for df in RING:
                swap(part, ds, df).wait_recv()

        def columns(n):
            at = pl.ds(pl.multiple_of(n * chunk, chunk), chunk)
            stage[part, :, :, at] = sum_heads(part, at).reshape(blocks + (chunk,)).astype(BF)

        loop(width // chunk, columns)
        chosen = rows_of_adapter(place, ids_ref, part, OWN, (len(RING) * rows, rank))
        stage[part, :, :, width:] = pick_columns(sum_heads(part, pl.ds(width, adapters * rank)), chosen).reshape(blocks + (rank,)).astype(BF)
        for df in RING[1:]:
            fast.ready(part, df)
    both('far')
    ends(bulk)
    fast.finish()
    fast.store(out_ref, load_sem)
    for copy in pair[len(heads):] + bulk:
        copy.wait_recv()
    for copy in pair + bulk:
        copy.wait_send()
    for g in gathers + [low_gather]:
        g.sent()
    pltpu.make_async_copy(wo.at[:, :, 1], wo.at[:, :, 1], bulk_send).wait()
    for part in BOTH:
        for d in BOTH:
            for i in range(WO_CHUNKS):
                wo_message(part, 0, d, i).wait_send()
            for i in passes[d]:
                wo_message(part, 1, d, i).wait_send()
        for ds in RING[1:]:
            for df in RING:
                swap(part, ds, df).wait_send()


def attend(ids, x_in, gain, heads, w_o, a_o, a_mlp, b_rows, given, side, scale, collective_id):
    _, seq_len, depth = x_in.shape
    head = heads[0].shape[1]
    cols = 3 * head
    adapters, _, rank = a_o.shape
    per = a_mlp[0].shape[1]
    chips = side * side
    half_dim = head // 2
    inv_freq = ROPE_BASE ** (-2.0 * np.arange(half_dim) / head)
    angle = np.arange(seq_len)[:, None] * inv_freq[None, :]
    cos, sin = np.cos(angle), np.sin(angle)
    tables = [jnp.asarray(np.concatenate(pair, axis=1), F32) for pair in ((cos, cos), (-sin, sin))]
    n_pair = len(heads) + len(given) + 2
    rows, out_cols = seq_len // 2, depth + rank
    every = (2, 2, side, side, 2)
    return pl.pallas_call(
        functools.partial(attend_kernel, side, adapters, scale, len(given)),
        out_shape=[jax.ShapeDtypeStruct((seq_len, out_cols), BF), jax.ShapeDtypeStruct(every + (2 * adapters * per, depth // 4), BF),
                   jax.ShapeDtypeStruct(every + b_rows[0].shape[1:], BF)] + [jax.ShapeDtypeStruct(g.shape, g.dtype) for g in given],
        in_specs=[SMEM, HBM, VMEM, VMEM, VMEM] + [HBM] * (len(heads) + 6 + len(given)),
        out_specs=[HBM] * (3 + len(given)),
        scratch_shapes=[
            pltpu.VMEM((depth, 2 * cols), BF),
            pltpu.VMEM((2, 3, adapters, per, depth), BF),
            pltpu.VMEM((2, 3, adapters, rank, head), BF),
            pltpu.VMEM((2 * 2 * TILE, depth), BF),
            pltpu.VMEM((adapters, 2, 2 * rank, 2 * cols), BF),
            pltpu.VMEM((2, 2, seq_len, depth), BF),
            pltpu.VMEM((2 * seq_len, depth), BF),
            pltpu.VMEM((chips * seq_len, 2 * cols), F32),
            pltpu.VMEM((2, side, side, 2, TILE, chips * seq_len // 2), BF),
            pltpu.VMEM((2, side, side, rows, 2 * head), BF),
            pltpu.VMEM((2, side, side, rows, 2 * head), BF),
            pltpu.VMEM((2, side, 2, head, depth + adapters * rank), BF),
            pltpu.VMEM((2, side, rows, out_cols), BF),
        ] + fast_scratch(rows, out_cols) + [
            pltpu.VMEM((2, adapters, per, depth), BF),
            pltpu.VMEM((2 * adapters * per, depth), BF),
            DMA((n_pair,)), DMA((n_pair,)), DMA, DMA((2,)), DMA, DMA, DMA((2, 2, 2, WO_CHUNKS)), DMA((2, 2, 2, WO_CHUNKS)), DMA, DMA, DMA((2, 4, 4)), DMA((2, 4, 4)),
        ] + GATHER_SEMS * 3 + FAST_SEMS,
        compiler_params=comm_params(collective_id),
        name='attend',
    )(ids, x_in, gain.reshape(1, depth), *tables, *heads, w_o, a_o, *a_mlp, *b_rows, *given)


def row_proj_kernel(side, adapters, ids_ref, act_ref, w_own, w_par, a_own, a_par, out_ref,
                    act, w, stage, near, landed, fast_near, fast_landed, slow_send, slow_recv, fast_send, fast_recv, load_sem):
    place = Place(side)
    place.announce()
    share, width = w_own.shape
    half = w.shape[0] // 2
    rank = a_own.shape[2]
    rows = stage.shape[3]
    quarter = rows // 2
    if share < half:
        for at in (0, half):
            w[at + share // TILE * TILE:at + half, :] = jnp.zeros((half - share // TILE * TILE, w.shape[1]), BF)
    loads = [pltpu.make_async_copy(act_ref, act, load_sem)]
    for at, w_part, a_part in ((0, w_own, a_own), (half, w_par, a_par)):
        loads.append(pltpu.make_async_copy(w_part, w.at[pl.ds(at, share), first(width)], load_sem))
        for a in range(adapters):
            loads.append(pltpu.make_async_copy(a_part.at[a], w.at[pl.ds(at, share), pl.ds(width + a * rank, rank)], load_sem))
    ends(loads)
    wait(loads)
    chunk = fit(width, 512)

    def unit(part, ds):
        def columns(n):
            at = pl.ds(pl.multiple_of(n * chunk, chunk), chunk)
            stage[part, ds, :, :, at] = dot(act[part, ds], w[:, at]).reshape(len(RING), rows, chunk).astype(BF)

        loop(width // chunk, columns)
        chosen = rows_of_adapter(place, ids_ref, part, ds, (len(RING) * rows, rank))
        stage[part, ds, :, :, width:] = pick_columns(dot(act[part, ds], w[:, width:]), chosen).reshape(len(RING), rows, rank).astype(BF)

    blocks = ((FAR, LAST), (OWN, NEXT))

    def slow(part, kind, d, i):
        df = blocks[1 - d][i] if kind == FREE else blocks[d][i]
        sems = (part, kind, d, i)
        src = stage.at[part, FAR if kind == PASS else TOWARD[d], df]
        dst = near.at[part, d, i] if kind == PASS else landed.at[part, d, df]
        return remote(src, dst, slow_send.at[sems], slow_recv.at[sems], place.neighbour(part, SLOW, STEP[d]))

    fast = FastScatter(place, lambda part, df: stage.at[part, OWN, df], fast_near, fast_landed, fast_send, fast_recv)
    for part in BOTH:
        unit(part, FAR)
        if part == 0:
            place.meet()
        for i in BOTH:
            for d in BOTH:
                slow(part, PASS, d, i).start()
    loop(len(RING), lambda i: unit(lax.rem(i, 2), NEXT + 2 * (i // 2)))
    for i in BOTH:
        for d in BOTH:
            for part in BOTH:
                slow(part, FREE, d, i).start()
    loop(2, lambda part: unit(part, OWN))
    for i in BOTH:
        for d in BOTH:
            for part in BOTH:
                slow(part, PASS, d, i).wait_recv()
                add(stage.at[part, TOWARD[d], blocks[d][i]], near.at[part, d, i])
                slow(part, SUM, d, i).start()
    for i in BOTH:
        for d in BOTH:
            df = blocks[d][i]
            for part in BOTH:
                slow(part, SUM, d, i).wait_recv()
                slow(part, FREE, 1 - d, i).wait_recv()
                add(stage.at[part, OWN, df], landed.at[part, UP, df], landed.at[part, DOWN, df])
                fast.ready(part, df)
    fast.finish()
    fast.store(out_ref, load_sem)
    for part in BOTH:
        for kind in range(3):
            for d in BOTH:
                for i in BOTH:
                    slow(part, kind, d, i).wait_send()


def row_proj(ids, act, w_own, w_par, a_own, a_par, side, collective_id):
    adapters, _, rank = a_own.shape
    width = w_own.shape[1]
    rows = act.shape[2] // side
    cols = width + rank
    blocks = (rows, cols)
    return pl.pallas_call(
        functools.partial(row_proj_kernel, side, adapters),
        out_shape=jax.ShapeDtypeStruct((2 * rows, cols), BF),
        in_specs=[SMEM] + [HBM] * 5,
        out_specs=HBM,
        scratch_shapes=[
            pltpu.VMEM(act.shape, BF),
            pltpu.VMEM((act.shape[3], width + adapters * rank), BF),
            pltpu.VMEM((2, side, side) + blocks, BF),
            pltpu.VMEM((2, 2, 2) + blocks, BF),
            pltpu.VMEM((2, 2, side) + blocks, BF),
        ] + fast_scratch(rows, cols) + [DMA((2, 3, 2, 2))] * 2 + FAST_SEMS + [DMA],
        compiler_params=comm_params(collective_id),
        name='row_proj',
    )(ids, act, w_own, w_par, a_own, a_par)


def finish(sums_ref, resid, b_ref, chosen, scale, adapters):
    _, _, side, _, rank, part = b_ref.shape
    width = sums_ref.shape[1] - rank
    low = spread(sums_ref[:, width:].astype(F32), chosen, adapters)
    delta = [dot(low, b_ref[core, :, y, x].reshape(adapters * rank, part)) for y in range(side) for x in range(side) for core in BOTH]
    return resid.astype(F32) + (sums_ref[:, :width].astype(F32) + scale * jnp.concatenate(delta, axis=1))


def own_rows(place, ids_ref, shape):
    return jnp.full(shape, ids_ref[place.device(0, 0)], jnp.int32)


def gate_up_kernel(side, adapters, scale, ids_ref, sums_ref, gain_ref, x_all, a_all, b_all, wg_own, wg_par, wu_own, wu_par, bg_own, bg_par, bu_own, bu_par,
                   hid_ref, mid_ref, gbuf, w, b, x_ref, a_ref, b_ref, hid, load_sem, a_sem, b_sem, store_sem, send_sem, recv_sem):
    place = Place(side)
    place.announce()
    b_load = ends([pltpu.make_async_copy(b_all.at[:, :, :, :, 0], b_ref, b_sem), pltpu.make_async_copy(x_all.at[place.device(0, 0)], x_ref, b_sem)])
    a_load = ends([pltpu.make_async_copy(a_all, a_ref, a_sem)])
    share, width = wg_own.shape
    half = w.shape[1] // 2
    rank = bg_own.shape[2]
    seq_len = sums_ref.shape[0]
    edge = share // TILE * TILE
    for at in (0, half):
        for kind in BOTH:
            w[kind, at + edge:at + half, :] = jnp.zeros((half - edge, width), BF)
            b[kind, at + edge:at + half, :] = jnp.zeros((half - edge, adapters * rank), BF)
    loads = []
    for kind, pieces in enumerate(((wg_own, wg_par, bg_own, bg_par), (wu_own, wu_par, bu_own, bu_par))):
        for i, at in enumerate((0, half)):
            loads.append(pltpu.make_async_copy(pieces[i], w.at[kind, pl.ds(at, share)], load_sem))
            for a in range(adapters):
                loads.append(pltpu.make_async_copy(pieces[2 + i].at[a], b.at[kind, pl.ds(at, share), pl.ds(a * rank, rank)], load_sem))
    ends(loads)
    rows = seq_len // 4
    chosen = own_rows(place, ids_ref, (seq_len, rank))
    wait(b_load)
    mid = finish(sums_ref, x_ref[...], b_ref, chosen, scale, adapters).astype(BF)
    mid_ref[...] = mid
    h2 = normed(mid.astype(F32), gain_ref[...])
    lows = []
    wait(a_load)
    for core in BOTH:
        pieces = [dot_rows(h2[:, i * width // 4:(i + 1) * width // 4], a_ref[core, i // 2, :, :, i % 2].reshape(-1, width // 4)) for i in RING]
        lows.append(sum(pieces).astype(BF))
    low = jnp.concatenate(lows, axis=1)
    per = rank // (2 * side * side)
    row, col = (lax.broadcasted_iota(jnp.int32, (low.shape[1], 2 * rank), axis) for axis in BOTH)
    kind, rank_at = col // rank, lax.rem(col, rank)
    chip, core = rank_at // (2 * per), lax.rem(rank_at // per, 2)
    pick = ((core * side * side + chip) * 2 + kind) * adapters * per + ids_ref[place.device(0, 0)] * per + lax.rem(rank_at, per)
    low = dot(low, jnp.where(row == pick, 1.0, 0.0).astype(BF)).astype(BF)
    for part in BOTH:
        for piece in BOTH:
            at = (2 * part + piece) * rows
            gbuf[part, OWN, OWN, piece, :, :width] = h2[at:at + rows]
            gbuf[part, OWN, OWN, piece, :, width:] = low[at:at + rows]
    place.meet()
    chunk = fit(2 * half, 256)

    def unit(ds):
        unit_rows = 2 * len(RING) * 2 * rows
        low = gbuf[:, ds, :, :, :, width:].reshape(unit_rows, 2 * rank).astype(F32)
        chosen = jnp.concatenate([rows_of_adapter(place, ids_ref, part, ds, (unit_rows // 2, rank)) for part in BOTH], axis=0)
        lows = [spread(low[:, kind * rank:(kind + 1) * rank], chosen, adapters) for kind in BOTH]

        def columns(n):
            at = pl.ds(pl.multiple_of(n * chunk, chunk), chunk)
            act = gbuf[:, ds, :, :, :, :width].reshape(unit_rows, width)
            gate, up = (dot_rows(act, w[kind, at]) + scale * dot_rows(lows[kind], b[kind, at]) for kind in BOTH)
            hid[:, ds, :, at] = (gate * jax.nn.sigmoid(gate) * up).astype(BF).reshape(2, unit_rows // 2, chunk)

        loop(2 * half // chunk, columns)
        ends([pltpu.make_async_copy(hid.at[part, ds], hid_ref.at[part, ds], store_sem) for part in BOTH])

    def on_row():
        wait(loads)
        unit(OWN)

    Gather(place, lambda part, ds, df: gbuf.at[part, ds, df], send_sem, recv_sem).run(
        on_row, lambda: loop(2, lambda i: unit(NEXT + 2 * i)), lambda: unit(FAR))
    pltpu.make_async_copy(hid, hid_ref, store_sem).wait()


def gate_up(ids, sums, gain, x_in, a_all, b_all, w, side, scale, collective_id):
    _, seq_len, depth = x_in.shape
    share = w[0].shape[0]
    adapters, _, rank = w[4].shape
    half = (share + LANE - 1) // LANE * LANE
    hidden = jax.ShapeDtypeStruct((2, side, side * seq_len // 2, 2 * half), BF)
    return pl.pallas_call(
        functools.partial(gate_up_kernel, side, adapters, scale),
        out_shape=[hidden, jax.ShapeDtypeStruct((seq_len, depth), BF)],
        in_specs=[SMEM] + [VMEM] * 2 + [HBM] * (3 + len(w)),
        out_specs=[HBM, VMEM],
        scratch_shapes=[
            pltpu.VMEM((2, side, side, 2, seq_len // 4, depth + 2 * rank), BF),
            pltpu.VMEM((2, 2 * half, depth), BF),
            pltpu.VMEM((2, 2 * half, adapters * rank), BF),
            pltpu.VMEM((seq_len, depth), BF),
            pltpu.VMEM(a_all.shape, BF),
            pltpu.VMEM(b_all.shape[:4] + b_all.shape[5:], BF),
            pltpu.VMEM(hidden.shape, BF),
            DMA, DMA, DMA, DMA,
        ] + GATHER_SEMS,
        compiler_params=comm_params(collective_id),
        name='gate_up',
    )(ids, sums, gain.reshape(1, depth), x_in, a_all, b_all, *w)


def deliver_kernel(side, adapters, scale, ids_ref, sums_ref, x_ref, b_all, out_ref, b_ref, b_sem, pair_send, pair_recv, send_sem, recv_sem):
    place = Place(side)
    place.announce(place.partner)
    b_load = ends([pltpu.make_async_copy(b_all.at[:, :, :, :, 1], b_ref, b_sem)])
    seq_len = sums_ref.shape[0]
    rows = seq_len // 4
    chosen = own_rows(place, ids_ref, (seq_len, b_ref.shape[4]))
    wait(b_load)
    y = finish(sums_ref, x_ref[...], b_ref, chosen, scale, adapters).astype(BF)
    for part in BOTH:
        for piece in BOTH:
            at = (2 * part + piece) * rows
            out_ref[place.device(0, 0), part, piece] = y[at:at + rows]
    place.meet()

    def block(part, ds, df):
        return out_ref.at[place.sequence(part, ds, df), part]

    def seen(part, ds, df, half):
        ref = block(part, ds, df) if half is None else block(part, ds, df).at[half]
        remote(ref, ref, pair_send, pair_recv, place.partner).start()

    for part in BOTH:
        seen(part, OWN, OWN, None)
    Gather(place, block, send_sem, recv_sem, absolute=True, seen=seen).run()
    every = out_ref.at[first(side * side)]
    for sem in (pair_send, pair_recv):
        pltpu.make_async_copy(every, every, sem).wait()


def put_kernel(y_ref, out_ref, sem):
    wait(ends([pltpu.make_async_copy(y_ref.at[i], out_ref.at[i], sem) for i in range(y_ref.shape[0])]))


def deliver(ids, sums, x_mid, b_all, side, scale, collective_id):
    seq_len, depth = x_mid.shape
    rows = seq_len // 4
    y = pl.pallas_call(
        functools.partial(deliver_kernel, side, b_all.shape[1], scale),
        out_shape=pltpu.VMEM((2 * side * side, 2, 2, rows, depth), BF),
        in_specs=[SMEM] + [VMEM] * 2 + [HBM],
        scratch_shapes=[pltpu.VMEM(b_all.shape[:4] + b_all.shape[5:], BF), DMA, DMA, DMA] + GATHER_SEMS,
        compiler_params=comm_params(collective_id, VMEM_SMALL),
        name='deliver',
    )(ids, sums, x_mid, b_all)
    return pl.pallas_call(
        put_kernel,
        out_shape=jax.ShapeDtypeStruct(y.shape, BF),
        in_specs=[pl.BlockSpec(memory_space=pl.ANY)],
        out_specs=HBM,
        scratch_shapes=[DMA],
        compiler_params=pltpu.CompilerParams(vmem_limit_bytes=VMEM_LEAST),
        name='put',
    )(y)


def solution(mesh):
    tp_size = mesh.shape['tensor']
    side = math.isqrt(tp_size // 2)
    rows_only = P('tensor', None)
    head_split = P(None, 'tensor', None)
    last_split = P(None, None, 'tensor')
    b_head_split = P(None, None, 'tensor', None)
    in_specs = (P('data', None, None), P('data'), P(None), P(None),
                head_split, head_split, head_split, P('tensor', None, None),
                P(None, 'tensor'), P(None, 'tensor'), rows_only,
                last_split, b_head_split, last_split, b_head_split, last_split, b_head_split,
                P(None, 'tensor', None, None), last_split,
                last_split, last_split, last_split, last_split,
                head_split, last_split)

    def local_layer(x_in, adapter_ids, gain_attn, gain_mlp, w_q, w_k, w_v, w_o, w_gate, w_up, w_down, a_q, b_q, a_k, b_k, a_v, b_v, a_o, b_o, a_gate, b_gate, a_up, b_up, a_down, b_down):
        scale = ALPHA / b_q.shape[1]

        def across(a):
            return a.swapaxes(-1, -2)

        heads = [w[:, 0] for w in (w_q, w_k, w_v)] + [across(a) for a in (a_q, a_k, a_v)] + [b[:, :, 0] for b in (b_q, b_k, b_v)]
        given = [across(w_gate), across(w_up), across(b_gate), across(b_up), w_down, a_down]
        sums, all_a, all_b, *kept = attend(adapter_ids, x_in, gain_attn, heads, w_o[0], a_o[:, 0], (across(a_gate), across(a_up)), (b_o, b_down), given, side, scale, 0)
        w = [piece for pair in zip(given[:4], kept[:4]) for piece in pair]
        hidden, x_mid = gate_up(adapter_ids, sums, gain_mlp, x_in, all_a, all_b, w, side, scale, 1)
        sums = row_proj(adapter_ids, hidden, given[4], kept[4], given[5], kept[5], side, 2)
        y = deliver(adapter_ids, sums, x_mid, all_b, side, scale, 3)
        return y.reshape(x_in.shape)

    return jax.shard_map(local_layer, mesh=mesh, in_specs=in_specs, out_specs=P('data', None, None), check_vma=False)
```

```python
import functools
import math

import jax
import jax.numpy as jnp
import numpy as np
from jax import lax
from jax.experimental import pallas as pl
from jax.experimental.pallas import tpu as pltpu
from jax.sharding import PartitionSpec as P

ALPHA = 16.0
ROPE_BASE = 10000.0
EPSILON = 1e-5
BF = jnp.bfloat16
F32 = jnp.float32
LANE = 128
TILE = 16
VMEM_MOST = 67043328
VMEM_SMALL = VMEM_MOST // 6
VMEM_LEAST = VMEM_MOST // 32
MESH = pl.DeviceIdType.MESH
HBM = pl.BlockSpec(memory_space=pltpu.HBM)
VMEM = pl.BlockSpec(memory_space=pltpu.VMEM)
SMEM = pl.BlockSpec(memory_space=pltpu.SMEM)
DMA = pltpu.SemaphoreType.DMA

OWN, NEXT, FAR, LAST = RING = range(4)
UP, DOWN = BOTH = range(2)
STEP = (NEXT, -NEXT)
FROM = (LAST, NEXT)
AWAY = (NEXT, LAST, FAR)
PAIRS = ((OWN, NEXT), (LAST, FAR))
TOWARD = (NEXT, LAST)
FAST, SLOW = BOTH


def fit(size, most):
    return max(c for c in range(LANE, most + 1, LANE) if size % c == 0)


def first(size):
    return pl.ds(0, size)


def dot(a, b):
    return jnp.dot(a, b, preferred_element_type=F32)


def dot_rows(a, b):
    return lax.dot_general(a, b, (((1,), (1,)), ((), ())), preferred_element_type=F32)


def dot_columns(a, b):
    return lax.dot_general(a, b, (((0,), (0,)), ((), ())), preferred_element_type=F32)


def normed(act, gain):
    return (act * lax.rsqrt(jnp.mean(act * act, axis=-1, keepdims=True) + EPSILON) * gain).astype(BF)


def ends(copies):
    for copy in copies:
        copy.start()
    return copies


def wait(copies):
    for copy in copies:
        copy.wait()


def loop(count, body):
    lax.fori_loop(0, count, lambda i, carry: (body(i), carry)[1], 0)


class Place:
    def __init__(self, side):
        index = lax.axis_index('tensor')
        self.side = side
        self.core = lax.rem(index, 2)
        chip = index // 2
        self.y, self.x = chip // side, lax.rem(chip, side)
        self.partner = index + 1 - 2 * self.core

    def turn(self, at, steps):
        return lax.rem(at + steps + self.side, self.side)

    def device(self, dy, dx):
        return (self.turn(self.y, dy) * self.side + self.turn(self.x, dx)) * 2 + self.core

    def neighbour(self, part, ring, step):
        return self.device(0, step) if part == ring else self.device(step, 0)

    def sequence(self, part, ds, df):
        return self.device(jnp.where(part == 0, ds, df), jnp.where(part == 0, df, ds))

    def announce(self, *more):
        to = [self.neighbour(0, ring, step) for ring in BOTH for step in STEP] + list(more)
        for device in to:
            pl.semaphore_signal(pltpu.get_barrier_semaphore(), inc=1, device_id={'tensor': device}, device_id_type=MESH)
        self.announced = len(to)

    def meet(self):
        pl.semaphore_wait(pltpu.get_barrier_semaphore(), self.announced)


def remote(src, dst, send_sem, recv_sem, to):
    return pltpu.make_async_remote_copy(src_ref=src, dst_ref=dst, send_sem=send_sem, recv_sem=recv_sem, device_id={'tensor': to}, device_id_type=MESH)


GATHER_SEMS = [DMA((2, 2, 2, 2, 4))] * 2


class Gather:
    def __init__(self, place, block, send_sem, recv_sem, absolute=False, seen=None):
        self.place, self.block, self.sems, self.absolute, self.seen = place, block, (send_sem, recv_sem), absolute, seen

    def message(self, part, ring, passed, d, j=OWN):
        spot = (lambda s: (s, j)) if ring == SLOW else (lambda s: (OWN, s))
        src, dst = (FROM[d], FAR) if passed else (OWN, FROM[d])
        a, b = self.block(part, *spot(src)), self.block(part, *spot(src if self.absolute else dst))
        if passed:
            a, b = a.at[d], b.at[d]
        return remote(a, b, *(sem.at[part, ring, passed, d, j] for sem in self.sems), self.place.neighbour(part, ring, STEP[d]))

    def arrived(self, part, ring, passed, d, j=OWN):
        self.message(part, ring, passed, d, j).wait_recv()
        if self.seen:
            at = FAR if passed else FROM[d]
            self.seen(part, *((at, j) if ring == SLOW else (OWN, at)), d if passed else None)

    def own(self):
        for ring in BOTH:
            for d in BOTH:
                for part in BOTH:
                    self.message(part, ring, 0, d).start()

    def near(self):
        for d in BOTH:
            for part in BOTH:
                self.arrived(part, FAST, 0, d)
                self.message(part, FAST, 1, d).start()
                for e in BOTH:
                    self.message(part, SLOW, 0, e, FROM[d]).start()

    def row(self):
        for part in BOTH:
            for d in BOTH:
                self.arrived(part, FAST, 1, d)
            for e in BOTH:
                self.message(part, SLOW, 0, e, FAR).start()
        self.sides(OWN)

    def sides(self, *blocks):
        for j in blocks:
            for part in BOTH:
                for d in BOTH:
                    self.arrived(part, SLOW, 0, d, j)
                    self.message(part, SLOW, 1, d, j).start()

    def far(self, *blocks):
        for j in blocks:
            for part in BOTH:
                for d in BOTH:
                    self.arrived(part, SLOW, 1, d, j)

    def sent(self):
        for part in BOTH:
            for d in BOTH:
                for passed in BOTH:
                    self.message(part, FAST, passed, d).wait_send()
                    for j in RING:
                        self.message(part, SLOW, passed, d, j).wait_send()


def rows_of_adapter(place, ids_ref, part, ds, shape):
    block = lax.broadcasted_iota(jnp.int32, shape, 0) // (shape[0] // len(RING))
    chosen = jnp.zeros(shape, jnp.int32)
    for df in RING:
        chosen = jnp.where(block == df, ids_ref[place.sequence(part, ds, df)], chosen)
    return chosen


def pick_columns(low, chosen):
    rank = chosen.shape[1]
    kept = low[:, :rank]
    for a in range(1, low.shape[1] // rank):
        kept = jnp.where(chosen == a, low[:, a * rank:(a + 1) * rank], kept)
    return kept


def spread(low, chosen, adapters):
    return jnp.concatenate([jnp.where(chosen == a, low, 0.0) for a in range(adapters)], axis=1).astype(BF)


PASS, FREE, SUM = range(3)
FAST_SEMS = [DMA((2, 3, 2))] * 2


def add(into, *others):
    def some(i):
        at = pl.ds(pl.multiple_of(i * TILE, TILE), TILE)
        total = into[at, :].astype(F32)
        for other in others:
            total += other[at, :].astype(F32)
        into[at, :] = total.astype(BF)

    loop(into.shape[0] // TILE, some)


class FastScatter:
    def __init__(self, place, stage, near, landed, send_sem, recv_sem):
        self.place, self.stage, self.near, self.landed, self.sems = place, stage, near, landed, (send_sem, recv_sem)
        quarter = near.shape[2]
        self.halves = (first(quarter), pl.ds(quarter, quarter))

    def message(self, part, kind, d):
        at = self.halves[1 - d] if kind == FREE else self.halves[d]
        src = self.stage(part, FAR if kind == PASS else TOWARD[d]).at[at]
        dst = self.near.at[part, d] if kind == PASS else self.landed.at[part, d, at]
        sems = [sem.at[part, kind, d] for sem in self.sems]
        return remote(src, dst, *sems, self.place.neighbour(part, FAST, STEP[d]))

    def ready(self, part, df):
        for d in BOTH:
            if df == FAR:
                self.message(part, PASS, d).start()
            elif df == TOWARD[d]:
                self.message(part, FREE, d).start()

    def finish(self):
        for d in BOTH:
            for part in BOTH:
                self.message(part, PASS, d).wait_recv()
                add(self.stage(part, TOWARD[d]).at[self.halves[d]], self.near.at[part, d])
                self.message(part, SUM, d).start()
        for part in BOTH:
            for d in BOTH:
                self.message(part, FREE, d).wait_recv()
                self.message(part, SUM, d).wait_recv()
            add(self.stage(part, OWN), self.landed.at[part, UP], self.landed.at[part, DOWN])

    def store(self, out_ref):
        rows = self.landed.shape[2]
        for part in BOTH:
            out_ref[part * rows:(part + 1) * rows] = self.stage(part, OWN)[...]
        for part in BOTH:
            for kind in range(3):
                for d in BOTH:
                    self.message(part, kind, d).wait_send()


def fast_scratch(rows, cols):
    return [pltpu.VMEM((2, 2, rows // 2, cols), BF), pltpu.VMEM((2, 2, rows, cols), BF)]


def comm_params(collective_id, limit=VMEM_MOST):
    return pltpu.CompilerParams(collective_id=collective_id, has_side_effects=True, vmem_limit_bytes=limit)


WO_CHUNKS = 8


def attend_kernel(side, adapters, scale, n_keep, ids_ref, x_ref, gain_ref, cos_ref, sin_ref, *rest):
    w_heads, a_heads, b_heads, (wo_ref, ao_ref), a_mlp, b_rows, rest = rest[:3], rest[3:6], rest[6:9], rest[9:11], rest[11:13], rest[13:15], rest[15:]
    given, rest = rest[:n_keep], rest[n_keep:]
    (out_ref, a_all, b_all), rest = rest[:3], rest[3:]
    kept, rest = rest[:n_keep], rest[n_keep:]
    (w, a_raw, b_raw, a_rows, bx, xbuf, h, z, lows, att, act, wo, stage, near, landed, am_raw, am_rows, pair_send, pair_recv, load_sem, x_sem, own_sem,
     wo_load, wo_send, wo_recv, bulk_send, bulk_recv, swap_send, swap_recv,
     send_sem, recv_sem, a_send, a_recv, b_send, b_recv, fast_send, fast_recv) = rest
    place = Place(side)
    place.announce(place.partner, place.device(0, FAR), place.device(FAR, 0))
    head, seq_len, depth = cos_ref.shape[1], x_ref.shape[1], x_ref.shape[2]
    cols = len(w_heads) * head
    chips = side * side
    per = a_raw.shape[3]
    half_depth = depth // 4
    heads = w_heads + a_heads + b_heads
    spots = [[w.at[:, pl.ds(at * cols + i * head, head)] for i in range(3)] + [a_raw.at[place.core, i] for i in range(3)] + [b_raw.at[at, i] for i in range(3)]
             for at in BOTH]
    loads = ends([pltpu.make_async_copy(src, dst, load_sem) for src, dst in zip(heads, spots[0])])

    def x_loads(step):
        slot = lax.rem(step, 2)
        return [pltpu.make_async_copy(x_ref.at[4 * step + 2 * i + place.core], xbuf.at[slot, i], x_sem.at[slot]) for i in BOTH]

    ends(x_loads(0))

    def every(ref):
        return lambda part, ds, df: ref.at[place.core, part, place.turn(place.y, df if part else ds), place.turn(place.x, ds if part else df)]

    every_a, every_b = every(a_all), every(b_all)
    own_loads = ends([pltpu.make_async_copy(a_mlp[i], am_raw.at[i], own_sem) for i in BOTH])
    own_b = [pltpu.make_async_copy(b_rows[half].at[part], every_b(part, OWN, OWN).at[half], load_sem) for part in BOTH for half in BOTH]
    ends(own_b)
    width = wo_ref.shape[1]
    rank = ao_ref.shape[2]
    wo_loads = []
    for part in BOTH:
        wo_loads.append(pltpu.make_async_copy(wo_ref, wo.at[part, OWN, 0, :, first(width)], wo_load))
        for a in range(adapters):
            wo_loads.append(pltpu.make_async_copy(ao_ref.at[a], wo.at[part, OWN, 0, :, pl.ds(width + a * rank, rank)], wo_load))
    ends(wo_loads)
    wait(own_loads)
    am_rows[...] = jnp.concatenate([am_raw[i, a] for i in BOTH for a in range(adapters)], axis=0)
    place.meet()
    pair = [remote(src, dst, pair_send.at[i], pair_recv.at[i], place.partner) for i, (src, dst) in
            enumerate(list(zip(heads, spots[1])) + list(zip(given, kept)))]
    ends(pair[:len(heads)])
    a_own = ends([pltpu.make_async_copy(am_rows.at[:, pl.ds((2 * part + half) * half_depth, half_depth)], every_a(part, OWN, OWN).at[half], own_sem)
                  for part in BOTH for half in BOTH])

    piece = head // WO_CHUNKS

    def wo_message(part, passed, d, i):
        src, dst = (wo.at[part, s, 0, pl.ds(i * piece, piece)] for s in ((FROM[d], FAR) if passed else (OWN, FROM[d])))
        sems = (part, passed, d, i)
        return remote(src, dst, wo_send.at[sems], wo_recv.at[sems], place.neighbour(part, SLOW, STEP[d]))

    def wo_to_partner(part, s):
        remote(wo.at[part, s, 0], wo.at[part, s, 1], bulk_send, bulk_recv, place.partner).start()

    passes = [range(d * WO_CHUNKS // 2, (d + 1) * WO_CHUNKS // 2) for d in BOTH]

    def wo_start(i):
        for d in BOTH:
            for part in BOTH:
                wo_message(part, 0, d, i).start()

    def wo_pass(k):
        for d in BOTH:
            for part in BOTH:
                wo_message(part, 0, d, passes[d][k]).wait_recv()
                wo_message(part, 1, d, passes[d][k]).start()

    def wo_arrived():
        for d in BOTH:
            for part in BOTH:
                for i in passes[1 - d]:
                    wo_message(part, 0, d, i).wait_recv()
                wo_to_partner(part, FROM[d])

    def wo_last():
        for part in BOTH:
            for d in BOTH:
                for i in passes[d]:
                    wo_message(part, 1, d, i).wait_recv()
            wo_to_partner(part, FAR)

    wait(wo_loads)
    for i in range(WO_CHUNKS // 2):
        wo_start(i)
    wait(a_own)
    wait(loads)
    wait(own_b)
    gathers = [Gather(place, every_a, a_send, a_recv, absolute=True), Gather(place, every_b, b_send, b_recv, absolute=True)]

    def both(stage_of, *more):
        for g in gathers:
            getattr(g, stage_of)(*more)

    both('own')
    for i in range(WO_CHUNKS // 2, WO_CHUNKS):
        wo_start(i)
    for part in BOTH:
        wo_to_partner(part, OWN)
    for copy in pair[:len(heads)]:
        copy.wait_recv()
    for core in BOTH:
        pieces = [a_raw[core, i, a] if i < len(w_heads) else jnp.zeros((per, depth), BF) for a in range(adapters) for i in RING]
        a_rows[core * 2 * TILE:(core + 1) * 2 * TILE, :] = jnp.concatenate(pieces, axis=0)
    mine = [(place.y, place.x), (place.x, place.y)]
    steps = chips // 2

    def block(part, ds, df):
        return lows.at[part, place.turn(mine[part][0], ds), place.turn(mine[part][1], df)]

    def project(step):
        slot = lax.rem(step, 2)

        @pl.when(step + 1 < steps)
        def _():
            ends(x_loads(step + 1))

        @pl.when(step == 2)
        def _():
            ends(pair[len(heads):])

        wait(x_loads(step))
        for i in BOTH:
            h[i * seq_len:(i + 1) * seq_len, :] = normed(xbuf[slot, i].astype(F32), gain_ref[...])
        rows = pl.ds(pl.multiple_of(step * 2 * seq_len, LANE), 2 * seq_len)
        chunk = fit(2 * cols, 256)
        for n in range(2 * cols // chunk):
            z[rows, n * chunk:(n + 1) * chunk] = dot(h[...], w[:, n * chunk:(n + 1) * chunk])
        low = dot_rows(a_rows[...], h[...])
        half, at = step // (steps // 2), lax.rem(step, steps // 2) * 2 * seq_len
        for part in BOTH:
            pieces = []
            for i in BOTH:
                options = [low[TILE * (2 * part + a):TILE * (2 * part + a + 1), i * seq_len:(i + 1) * seq_len] for a in range(adapters)]
                chosen = options[0]
                for a in range(1, adapters):
                    chosen = jnp.where(ids_ref[4 * step + 2 * i + place.core] == a, options[a], chosen)
                pieces.append(chosen)
            lows[part, mine[part][0], mine[part][1], half, :, pl.ds(pl.multiple_of(at, LANE), 2 * seq_len)] = jnp.concatenate(pieces, axis=1).astype(BF)

    loop(steps, project)
    low_gather = Gather(place, block, send_sem, recv_sem, absolute=True)
    low_gather.own()
    row, col = (lax.broadcasted_iota(jnp.int32, (2 * rank, rank), axis) for axis in BOTH)
    spot, kind = row // TILE, lax.rem(row, TILE) // per
    for part in BOTH:
        chip_of = spot if part == 0 else lax.rem(spot, side) * side + spot // side
        to = chip_of * 2 * per + part * per + lax.rem(row, per)
        for i in range(3):
            spread_rows = jnp.where((kind == i) & (col == to), 1.0, 0.0).astype(BF)
            for a in range(adapters):
                for o in BOTH:
                    bx[a, part, :, o * cols + i * head:o * cols + (i + 1) * head] = dot(spread_rows, b_raw[o, i, a]).astype(BF)
    low_gather.near()
    wo_pass(0)
    low_gather.row()
    wo_pass(1)
    low_gather.sides(*AWAY)
    wo_pass(2)
    low_gather.far(*RING)
    wo_pass(3)
    wo_arrived()
    causal = lax.broadcasted_iota(jnp.int32, (seq_len, seq_len), 0) >= lax.broadcasted_iota(jnp.int32, (seq_len, seq_len), 1)

    def swap(part, ds, df):
        sems = (part, ds, df)
        to = place.neighbour(part, SLOW, ds)
        return remote(att.at[sems], act.at[part, lax.rem(len(RING) - ds, len(RING)), df], swap_send.at[sems], swap_recv.at[sems], to)

    def attention(i):
        dy, dx = side - 1 - i // side, side - 1 - lax.rem(i, side)
        chip = place.turn(place.y, dy) * side + place.turn(place.x, dx)
        adapter = ids_ref[2 * chip + place.core]
        half, at = chip // steps, pl.ds(pl.multiple_of(lax.rem(chip, steps) * seq_len, LANE), seq_len)
        zs = z[pl.ds(pl.multiple_of(chip * seq_len, LANE), seq_len), :]
        for part in BOTH:
            zs += scale * dot_columns(lows[part, :, :, half, :, at].reshape(-1, seq_len), bx[adapter, part])
        for i_head in BOTH:
            q, k, v = (zs[:, i_head * cols + i * head:i_head * cols + (i + 1) * head] for i in range(3))
            q, k = ((r * cos_ref[...] + pltpu.roll(r, head // 2, axis=1) * sin_ref[...]).astype(BF) for r in (q, k))
            scores = jnp.where(causal, dot_rows(q, k) * head ** -0.5, -1e30)
            e = jnp.exp(scores - jnp.max(scores, axis=-1, keepdims=True))
            prob = (e / jnp.sum(e, axis=-1, keepdims=True)).astype(BF)
            mixed = dot(prob, v.astype(BF)).astype(BF)
            for part, (ds, df) in enumerate(((dy, dx), (dx, dy))):
                att[part, ds, df, :, i_head * head:(i_head + 1) * head] = mixed[part * seq_len // 2:(part + 1) * seq_len // 2]

    def attention_pair(k):
        for i in BOTH:
            attention(2 * k + i)
        for i in BOTH:
            dy, dx = side - 1 - (2 * k + i) // side, side - 1 - lax.rem(2 * k + i, side)
            for part, (ds, df) in enumerate(((dy, dx), (dx, dy))):
                pl.when(ds != OWN)(swap(part, ds, df).start)

    loop(chips // 2, attention_pair)
    both('near')
    wo_last()
    for part in BOTH:
        act[part, OWN] = att[part, OWN]
    bulk = [remote(ref.at[place.core], ref.at[place.core], pair_send.at[len(pair) + i], pair_recv.at[len(pair) + i], place.partner) for i, ref in enumerate((a_all, b_all))]
    pltpu.make_async_copy(wo.at[:, :, 1], wo.at[:, :, 1], bulk_recv).wait()
    chunk = fit(width, 512)
    rows = seq_len // 2
    blocks = (len(RING), rows)
    fast = FastScatter(place, lambda part, df: stage.at[part, df], near, landed, fast_send, fast_recv)

    def sum_heads(part, at):
        return sum(dot(act[part, s].reshape(-1, 2 * head), wo[part, s, :, :, at].reshape(2 * head, -1)) for s in RING)

    for part in BOTH:
        for ds in RING[1:]:
            for df in RING:
                swap(part, ds, df).wait_recv()

        def columns(n):
            at = pl.ds(pl.multiple_of(n * chunk, chunk), chunk)
            stage[part, :, :, at] = sum_heads(part, at).reshape(blocks + (chunk,)).astype(BF)

        loop(width // chunk, columns)
        chosen = rows_of_adapter(place, ids_ref, part, OWN, (len(RING) * rows, rank))
        stage[part, :, :, width:] = pick_columns(sum_heads(part, pl.ds(width, adapters * rank)), chosen).reshape(blocks + (rank,)).astype(BF)
        for df in RING[1:]:
            fast.ready(part, df)
        if part == 0:
            both('row')
    both('sides', *AWAY)
    fast.finish()
    both('far', *RING)
    ends(bulk)
    fast.store(out_ref)
    for copy in pair[len(heads):] + bulk:
        copy.wait_recv()
    for copy in pair + bulk:
        copy.wait_send()
    for g in gathers + [low_gather]:
        g.sent()
    pltpu.make_async_copy(wo.at[:, :, 1], wo.at[:, :, 1], bulk_send).wait()
    for part in BOTH:
        for d in BOTH:
            for i in range(WO_CHUNKS):
                wo_message(part, 0, d, i).wait_send()
            for i in passes[d]:
                wo_message(part, 1, d, i).wait_send()
        for ds in RING[1:]:
            for df in RING:
                swap(part, ds, df).wait_send()


def attend(ids, x_in, gain, heads, w_o, a_o, a_mlp, b_rows, given, side, scale, collective_id):
    _, seq_len, depth = x_in.shape
    head = heads[0].shape[1]
    cols = 3 * head
    adapters, _, rank = a_o.shape
    per = a_mlp[0].shape[1]
    chips = side * side
    half_dim = head // 2
    inv_freq = ROPE_BASE ** (-2.0 * np.arange(half_dim) / head)
    angle = np.arange(seq_len)[:, None] * inv_freq[None, :]
    cos, sin = np.cos(angle), np.sin(angle)
    tables = [jnp.asarray(np.concatenate(pair, axis=1), F32) for pair in ((cos, cos), (-sin, sin))]
    n_pair = len(heads) + len(given) + 2
    rows, out_cols = seq_len // 2, depth + rank
    every = (2, 2, side, side, 2)
    return pl.pallas_call(
        functools.partial(attend_kernel, side, adapters, scale, len(given)),
        out_shape=[jax.ShapeDtypeStruct((seq_len, out_cols), BF), jax.ShapeDtypeStruct(every + (2 * adapters * per, depth // 4), BF),
                   jax.ShapeDtypeStruct(every + b_rows[0].shape[1:], BF)] + [jax.ShapeDtypeStruct(g.shape, g.dtype) for g in given],
        in_specs=[SMEM, HBM, VMEM, VMEM, VMEM] + [HBM] * (len(heads) + 6 + len(given)),
        out_specs=[VMEM] + [HBM] * (2 + len(given)),
        scratch_shapes=[
            pltpu.VMEM((depth, 2 * cols), BF),
            pltpu.VMEM((2, 3, adapters, per, depth), BF),
            pltpu.VMEM((2, 3, adapters, rank, head), BF),
            pltpu.VMEM((2 * 2 * TILE, depth), BF),
            pltpu.VMEM((adapters, 2, 2 * rank, 2 * cols), BF),
            pltpu.VMEM((2, 2, seq_len, depth), BF),
            pltpu.VMEM((2 * seq_len, depth), BF),
            pltpu.VMEM((chips * seq_len, 2 * cols), F32),
            pltpu.VMEM((2, side, side, 2, TILE, chips * seq_len // 2), BF),
            pltpu.VMEM((2, side, side, rows, 2 * head), BF),
            pltpu.VMEM((2, side, side, rows, 2 * head), BF),
            pltpu.VMEM((2, side, 2, head, depth + adapters * rank), BF),
            pltpu.VMEM((2, side, rows, out_cols), BF),
        ] + fast_scratch(rows, out_cols) + [
            pltpu.VMEM((2, adapters, per, depth), BF),
            pltpu.VMEM((2 * adapters * per, depth), BF),
            DMA((n_pair,)), DMA((n_pair,)), DMA, DMA((2,)), DMA, DMA, DMA((2, 2, 2, WO_CHUNKS)), DMA((2, 2, 2, WO_CHUNKS)), DMA, DMA, DMA((2, 4, 4)), DMA((2, 4, 4)),
        ] + GATHER_SEMS * 3 + FAST_SEMS,
        compiler_params=comm_params(collective_id),
        name='attend',
    )(ids, x_in, gain.reshape(1, depth), *tables, *heads, w_o, a_o, *a_mlp, *b_rows, *given)


def row_proj_kernel(side, adapters, rank, ids_ref, act, w, out_ref, stage, near, landed, fast_near, fast_landed, slow_send, slow_recv, fast_send, fast_recv):
    place = Place(side)
    place.announce()
    rows, cols = stage.shape[3:]
    quarter = rows // 2
    width = cols - rank
    chunk = fit(width, 512)

    def unit(part, ds):
        def columns(n):
            at = pl.ds(pl.multiple_of(n * chunk, chunk), chunk)
            stage[part, ds, :, :, at] = dot(act[part, ds], w[:, at]).reshape(len(RING), rows, chunk).astype(BF)

        loop(width // chunk, columns)
        chosen = rows_of_adapter(place, ids_ref, part, ds, (len(RING) * rows, rank))
        stage[part, ds, :, :, width:] = pick_columns(dot(act[part, ds], w[:, width:]), chosen).reshape(len(RING), rows, rank).astype(BF)

    blocks = ((FAR, LAST), (OWN, NEXT))

    def slow(part, kind, d, i):
        df = blocks[1 - d][i] if kind == FREE else blocks[d][i]
        sems = (part, kind, d, i)
        src = stage.at[part, FAR if kind == PASS else TOWARD[d], df]
        dst = near.at[part, d, i] if kind == PASS else landed.at[part, d, df]
        return remote(src, dst, slow_send.at[sems], slow_recv.at[sems], place.neighbour(part, SLOW, STEP[d]))

    fast = FastScatter(place, lambda part, df: stage.at[part, OWN, df], fast_near, fast_landed, fast_send, fast_recv)
    for part in BOTH:
        unit(part, FAR)
        if part == 0:
            place.meet()
        for i in BOTH:
            for d in BOTH:
                slow(part, PASS, d, i).start()
    loop(len(RING), lambda i: unit(lax.rem(i, 2), NEXT + 2 * (i // 2)))
    for i in BOTH:
        for d in BOTH:
            for part in BOTH:
                slow(part, FREE, d, i).start()
    loop(2, lambda part: unit(part, OWN))
    for i in BOTH:
        for d in BOTH:
            for part in BOTH:
                slow(part, PASS, d, i).wait_recv()
                add(stage.at[part, TOWARD[d], blocks[d][i]], near.at[part, d, i])
                slow(part, SUM, d, i).start()
    for i in BOTH:
        for d in BOTH:
            df = blocks[d][i]
            for part in BOTH:
                slow(part, SUM, d, i).wait_recv()
                slow(part, FREE, 1 - d, i).wait_recv()
                add(stage.at[part, OWN, df], landed.at[part, UP, df], landed.at[part, DOWN, df])
                fast.ready(part, df)
    fast.finish()
    fast.store(out_ref)
    for part in BOTH:
        for kind in range(3):
            for d in BOTH:
                for i in BOTH:
                    slow(part, kind, d, i).wait_send()


def row_proj(ids, act, w, adapters, rank, side, collective_id):
    rows = act.shape[2] // side
    cols = w.shape[1] - (adapters - 1) * rank
    blocks = (rows, cols)
    return pl.pallas_call(
        functools.partial(row_proj_kernel, side, adapters, rank),
        out_shape=pltpu.VMEM((2 * rows, cols), BF),
        in_specs=[SMEM, VMEM, VMEM],
        out_specs=VMEM,
        scratch_shapes=[
            pltpu.VMEM((2, side, side) + blocks, BF),
            pltpu.VMEM((2, 2, 2) + blocks, BF),
            pltpu.VMEM((2, 2, side) + blocks, BF),
        ] + fast_scratch(rows, cols) + [DMA((2, 3, 2, 2))] * 2 + FAST_SEMS,
        compiler_params=comm_params(collective_id, VMEM_MOST * 5 // 8),
        name='row_proj',
    )(ids, act, w)


def finish(sums_ref, resid, b_ref, chosen, scale, adapters):
    _, _, side, _, rank, part = b_ref.shape
    width = sums_ref.shape[1] - rank
    low = spread(sums_ref[:, width:].astype(F32), chosen, adapters)
    delta = [dot(low, b_ref[core, :, y, x].reshape(adapters * rank, part)) for y in range(side) for x in range(side) for core in BOTH]
    return resid.astype(F32) + (sums_ref[:, :width].astype(F32) + scale * jnp.concatenate(delta, axis=1))


def own_rows(place, ids_ref, shape):
    return jnp.full(shape, ids_ref[place.device(0, 0)], jnp.int32)


def gate_up_kernel(side, adapters, scale, ids_ref, sums_ref, gain_ref, x_all, a_all, b_all, wg_own, wg_par, wu_own, wu_par, bg_own, bg_par, bu_own, bu_par,
                   wd_own, wd_par, ad_own, ad_par, hid, mid_ref, wd, gbuf, raw, w, b, x_ref, a_ref, b_ref, raw_sem, load_sem, a_sem, b_sem, wd_sem, send_sem, recv_sem):
    place = Place(side)
    place.announce()
    b_load = ends([pltpu.make_async_copy(b_all.at[:, :, :, :, 0], b_ref, b_sem), pltpu.make_async_copy(x_all.at[place.device(0, 0)], x_ref, b_sem)])
    a_load = ends([pltpu.make_async_copy(a_all, a_ref, a_sem)])
    share, width = wg_own.shape
    half = raw.shape[1]
    rank = bg_own.shape[2]
    seq_len = sums_ref.shape[0]
    edge = share // TILE * TILE
    shares = (wg_own, wg_par, wu_own, wu_par)

    def raw_load(i):
        return pltpu.make_async_copy(shares[i], raw.at[i % 2, first(share)], raw_sem.at[i % 2])

    for i in BOTH:
        raw[i, edge:] = jnp.zeros((half - edge, width), BF)
        raw_load(i).start()
        for kind in BOTH:
            b[kind, i * half + edge:(i + 1) * half] = jnp.zeros((half - edge, adapters * rank), BF)
        wd[i * half + edge:(i + 1) * half] = jnp.zeros((half - edge, wd.shape[1]), BF)
    loads, wd_loads = [], []
    for i, at in enumerate((0, half)):
        wd_loads.append(pltpu.make_async_copy((wd_own, wd_par)[i], wd.at[pl.ds(at, share), first(width)], wd_sem))
        for a in range(adapters):
            wd_loads.append(pltpu.make_async_copy((ad_own, ad_par)[i].at[a], wd.at[pl.ds(at, share), pl.ds(width + a * rank, rank)], wd_sem))
            for kind, pair in enumerate(((bg_own, bg_par), (bu_own, bu_par))):
                loads.append(pltpu.make_async_copy(pair[i].at[a], b.at[kind, pl.ds(at, share), pl.ds(a * rank, rank)], load_sem))
    ends(loads)
    rows = seq_len // 4
    chosen = own_rows(place, ids_ref, (seq_len, rank))
    wait(b_load)
    mid = finish(sums_ref, x_ref[...], b_ref, chosen, scale, adapters).astype(BF)
    mid_ref[...] = mid
    h2 = normed(mid.astype(F32), gain_ref[...])
    lows = []
    wait(a_load)
    for core in BOTH:
        pieces = [dot_rows(h2[:, i * width // 4:(i + 1) * width // 4], a_ref[core, i // 2, :, :, i % 2].reshape(-1, width // 4)) for i in RING]
        lows.append(sum(pieces).astype(BF))
    low = jnp.concatenate(lows, axis=1)
    per = rank // (2 * side * side)
    row, col = (lax.broadcasted_iota(jnp.int32, (low.shape[1], 2 * rank), axis) for axis in BOTH)
    kind, rank_at = col // rank, lax.rem(col, rank)
    chip, core = rank_at // (2 * per), lax.rem(rank_at // per, 2)
    pick = ((core * side * side + chip) * 2 + kind) * adapters * per + ids_ref[place.device(0, 0)] * per + lax.rem(rank_at, per)
    low = dot(low, jnp.where(row == pick, 1.0, 0.0).astype(BF)).astype(BF)
    for part in BOTH:
        for piece in BOTH:
            at = (2 * part + piece) * rows
            gbuf[part, OWN, OWN, piece, :, :width] = h2[at:at + rows]
            gbuf[part, OWN, OWN, piece, :, width:] = low[at:at + rows]
    place.meet()
    chunk = fit(2 * half, 256)

    def unit(ds, blocks=RING):
        lo, hi = min(blocks), max(blocks) + 1
        unit_rows = (hi - lo) * 2 * rows
        low = gbuf[:, ds, lo:hi, :, :, width:].reshape(2 * unit_rows, 2 * rank).astype(F32)
        chosen = jnp.concatenate([rows_of_adapter(place, ids_ref, part, ds, (len(RING) * 2 * rows, rank))[lo * 2 * rows:hi * 2 * rows] for part in BOTH], axis=0)
        lows = [spread(low[:, kind * rank:(kind + 1) * rank], chosen, adapters) for kind in BOTH]

        def columns(n):
            at = pl.ds(pl.multiple_of(n * chunk, chunk), chunk)
            act = gbuf[:, ds, lo:hi, :, :, :width].reshape(2 * unit_rows, width)
            gate, up = (dot(act, w[kind, :, at]) + scale * dot_rows(lows[kind], b[kind, at]) for kind in BOTH)
            hid[:, ds, lo * 2 * rows:hi * 2 * rows, at] = (gate * jax.nn.sigmoid(gate) * up).astype(BF).reshape(2, unit_rows, chunk)

        loop(2 * half // chunk, columns)

    gather = Gather(place, lambda part, ds, df: gbuf.at[part, ds, df], send_sem, recv_sem)
    gather.own()
    for i in range(len(shares)):
        raw_load(i).wait()

        def turn(n):
            at = pl.ds(pl.multiple_of(n * LANE, LANE), LANE)
            w[i // 2, at, i % 2 * half:(i % 2 + 1) * half] = raw[i % 2, :, at].T

        loop(width // LANE, turn)
        if i + 2 < len(shares):
            raw_load(i + 2).start()
    gather.near()
    gather.row()
    ends(wd_loads)
    wait(loads)
    unit(OWN)
    gather.sides(*AWAY)
    loop(2, lambda i: unit(NEXT + 2 * i))
    wait(wd_loads)
    for pair in PAIRS:
        gather.far(*pair)
        unit(FAR, pair)
    gather.sent()


def gate_up(ids, sums, gain, x_in, a_all, b_all, w, side, scale, collective_id):
    _, seq_len, depth = x_in.shape
    share = w[0].shape[0]
    adapters, _, rank = w[4].shape
    half = (share + LANE - 1) // LANE * LANE
    hidden = (2, side, side * seq_len // 2, 2 * half)
    return pl.pallas_call(
        functools.partial(gate_up_kernel, side, adapters, scale),
        out_shape=[pltpu.VMEM(hidden, BF), pltpu.VMEM((seq_len, depth), BF), pltpu.VMEM((2 * half, depth + adapters * rank), BF)],
        in_specs=[SMEM] + [VMEM] * 2 + [HBM] * (3 + len(w)),
        out_specs=[VMEM] * 3,
        scratch_shapes=[
            pltpu.VMEM((2, side, side, 2, seq_len // 4, depth + 2 * rank), BF),
            pltpu.VMEM((2, half, depth), BF),
            pltpu.VMEM((2, depth, 2 * half), BF),
            pltpu.VMEM((2, 2 * half, adapters * rank), BF),
            pltpu.VMEM((seq_len, depth), BF),
            pltpu.VMEM(a_all.shape, BF),
            pltpu.VMEM(b_all.shape[:4] + b_all.shape[5:], BF),
            DMA((2,)), DMA, DMA, DMA, DMA,
        ] + GATHER_SEMS,
        compiler_params=comm_params(collective_id, VMEM_MOST * 51 // 64),
        name='gate_up',
    )(ids, sums, gain.reshape(1, depth), x_in, a_all, b_all, *w)


def deliver_kernel(side, adapters, scale, ids_ref, sums_ref, x_ref, b_all, out_ref, b_ref, b_sem, pair_send, pair_recv, send_sem, recv_sem):
    place = Place(side)
    place.announce(place.partner)
    b_load = ends([pltpu.make_async_copy(b_all.at[:, :, :, :, 1], b_ref, b_sem)])
    seq_len = sums_ref.shape[0]
    rows = seq_len // 4
    chosen = own_rows(place, ids_ref, (seq_len, b_ref.shape[4]))
    wait(b_load)
    y = finish(sums_ref, x_ref[...], b_ref, chosen, scale, adapters).astype(BF)
    for part in BOTH:
        for piece in BOTH:
            at = (2 * part + piece) * rows
            out_ref[place.device(0, 0), part, piece] = y[at:at + rows]
    place.meet()

    def block(part, ds, df):
        return out_ref.at[place.sequence(part, ds, df), part]

    def seen(part, ds, df, half):
        ref = block(part, ds, df) if half is None else block(part, ds, df).at[half]
        remote(ref, ref, pair_send, pair_recv, place.partner).start()

    for part in BOTH:
        seen(part, OWN, OWN, None)
    gather = Gather(place, block, send_sem, recv_sem, absolute=True, seen=seen)
    gather.own()
    gather.near()
    gather.row()
    gather.sides(*AWAY)
    gather.far(*RING)
    gather.sent()
    every = out_ref.at[first(side * side)]
    for sem in (pair_send, pair_recv):
        pltpu.make_async_copy(every, every, sem).wait()


def put_kernel(y_ref, out_ref, sem):
    wait(ends([pltpu.make_async_copy(y_ref.at[i], out_ref.at[i], sem) for i in range(y_ref.shape[0])]))


def deliver(ids, sums, x_mid, b_all, side, scale, collective_id):
    seq_len, depth = x_mid.shape
    rows = seq_len // 4
    y = pl.pallas_call(
        functools.partial(deliver_kernel, side, b_all.shape[1], scale),
        out_shape=pltpu.VMEM((2 * side * side, 2, 2, rows, depth), BF),
        in_specs=[SMEM] + [VMEM] * 2 + [HBM],
        scratch_shapes=[pltpu.VMEM(b_all.shape[:4] + b_all.shape[5:], BF), DMA, DMA, DMA] + GATHER_SEMS,
        compiler_params=comm_params(collective_id, VMEM_SMALL),
        name='deliver',
    )(ids, sums, x_mid, b_all)
    return pl.pallas_call(
        put_kernel,
        out_shape=jax.ShapeDtypeStruct(y.shape, BF),
        in_specs=[pl.BlockSpec(memory_space=pl.ANY)],
        out_specs=HBM,
        scratch_shapes=[DMA],
        compiler_params=pltpu.CompilerParams(vmem_limit_bytes=VMEM_LEAST),
        name='put',
    )(y)


def solution(mesh):
    tp_size = mesh.shape['tensor']
    side = math.isqrt(tp_size // 2)
    rows_only = P('tensor', None)
    head_split = P(None, 'tensor', None)
    last_split = P(None, None, 'tensor')
    b_head_split = P(None, None, 'tensor', None)
    in_specs = (P('data', None, None), P('data'), P(None), P(None),
                head_split, head_split, head_split, P('tensor', None, None),
                P(None, 'tensor'), P(None, 'tensor'), rows_only,
                last_split, b_head_split, last_split, b_head_split, last_split, b_head_split,
                P(None, 'tensor', None, None), last_split,
                last_split, last_split, last_split, last_split,
                head_split, last_split)

    def local_layer(x_in, adapter_ids, gain_attn, gain_mlp, w_q, w_k, w_v, w_o, w_gate, w_up, w_down, a_q, b_q, a_k, b_k, a_v, b_v, a_o, b_o, a_gate, b_gate, a_up, b_up, a_down, b_down):
        scale = ALPHA / b_q.shape[1]

        def across(a):
            return a.swapaxes(-1, -2)

        heads = [w[:, 0] for w in (w_q, w_k, w_v)] + [across(a) for a in (a_q, a_k, a_v)] + [b[:, :, 0] for b in (b_q, b_k, b_v)]
        given = [across(w_gate), across(w_up), across(b_gate), across(b_up), w_down, a_down]
        sums, all_a, all_b, *kept = attend(adapter_ids, x_in, gain_attn, heads, w_o[0], a_o[:, 0], (across(a_gate), across(a_up)), (b_o, b_down), given, side, scale, 0)
        w = [piece for pair in zip(given, kept) for piece in pair]
        hidden, x_mid, w_d = gate_up(adapter_ids, sums, gain_mlp, x_in, all_a, all_b, w, side, scale, 1)
        sums = row_proj(adapter_ids, hidden, w_d, *a_o.shape[::3], side, 2)
        y = deliver(adapter_ids, sums, x_mid, pltpu.with_memory_space_constraint(all_b, pltpu.HBM), side, scale, 3)
        return y.reshape(x_in.shape)

    return jax.shard_map(local_layer, mesh=mesh, in_specs=in_specs, out_specs=P('data', None, None), check_vma=False)
```

```python
import functools
import math

import jax
import jax.numpy as jnp
import numpy as np
from jax import lax
from jax.experimental import pallas as pl
from jax.experimental.pallas import tpu as pltpu
from jax.sharding import PartitionSpec as P

ALPHA = 16.0
ROPE_BASE = 10000.0
EPSILON = 1e-5
BF = jnp.bfloat16
F32 = jnp.float32
LANE = 128
TILE = 16
VMEM_MOST = 67043328
VMEM_SMALL = VMEM_MOST // 6
VMEM_LEAST = VMEM_MOST // 32
MESH = pl.DeviceIdType.MESH
HBM = pl.BlockSpec(memory_space=pltpu.HBM)
VMEM = pl.BlockSpec(memory_space=pltpu.VMEM)
SMEM = pl.BlockSpec(memory_space=pltpu.SMEM)
DMA = pltpu.SemaphoreType.DMA

OWN, NEXT, FAR, LAST = RING = range(4)
UP, DOWN = BOTH = range(2)
STEP = (NEXT, -NEXT)
FROM = (LAST, NEXT)
AWAY = (NEXT, LAST, FAR)
PAIRS = ((OWN, NEXT), (LAST, FAR))
TOWARD = (NEXT, LAST)
FAST, SLOW = BOTH


def fit(size, most):
    return max(c for c in range(LANE, most + 1, LANE) if size % c == 0)


def first(size):
    return pl.ds(0, size)


def dot(a, b):
    return jnp.dot(a, b, preferred_element_type=F32)


def dot_rows(a, b):
    return lax.dot_general(a, b, (((1,), (1,)), ((), ())), preferred_element_type=F32)


def dot_columns(a, b):
    return lax.dot_general(a, b, (((0,), (0,)), ((), ())), preferred_element_type=F32)


def normed(act, gain):
    return (act * lax.rsqrt(jnp.mean(act * act, axis=-1, keepdims=True) + EPSILON) * gain).astype(BF)


def ends(copies):
    for copy in copies:
        copy.start()
    return copies


def wait(copies):
    for copy in copies:
        copy.wait()


def loop(count, body):
    lax.fori_loop(0, count, lambda i, carry: (body(i), carry)[1], 0)


class Place:
    def __init__(self, side):
        index = lax.axis_index('tensor')
        self.side = side
        self.core = lax.rem(index, 2)
        chip = index // 2
        self.y, self.x = chip // side, lax.rem(chip, side)
        self.partner = index + 1 - 2 * self.core

    def turn(self, at, steps):
        return lax.rem(at + steps + self.side, self.side)

    def device(self, dy, dx):
        return (self.turn(self.y, dy) * self.side + self.turn(self.x, dx)) * 2 + self.core

    def neighbour(self, part, ring, step):
        return self.device(0, step) if part == ring else self.device(step, 0)

    def sequence(self, part, ds, df):
        return self.device(jnp.where(part == 0, ds, df), jnp.where(part == 0, df, ds))

    def announce(self, *more):
        to = [self.neighbour(0, ring, step) for ring in BOTH for step in STEP] + list(more)
        for device in to:
            pl.semaphore_signal(pltpu.get_barrier_semaphore(), inc=1, device_id={'tensor': device}, device_id_type=MESH)
        self.announced = len(to)

    def meet(self):
        pl.semaphore_wait(pltpu.get_barrier_semaphore(), self.announced)


def remote(src, dst, send_sem, recv_sem, to):
    return pltpu.make_async_remote_copy(src_ref=src, dst_ref=dst, send_sem=send_sem, recv_sem=recv_sem, device_id={'tensor': to}, device_id_type=MESH)


GATHER_SEMS = [DMA((2, 2, 2, 2, 4))] * 2


class Gather:
    def __init__(self, place, block, send_sem, recv_sem, absolute=False, seen=None):
        self.place, self.block, self.sems, self.absolute, self.seen = place, block, (send_sem, recv_sem), absolute, seen

    def message(self, part, ring, passed, d, j=OWN):
        spot = (lambda s: (s, j)) if ring == SLOW else (lambda s: (OWN, s))
        src, dst = (FROM[d], FAR) if passed else (OWN, FROM[d])
        a, b = self.block(part, *spot(src)), self.block(part, *spot(src if self.absolute else dst))
        if passed:
            a, b = a.at[d], b.at[d]
        return remote(a, b, *(sem.at[part, ring, passed, d, j] for sem in self.sems), self.place.neighbour(part, ring, STEP[d]))

    def arrived(self, part, ring, passed, d, j=OWN):
        self.message(part, ring, passed, d, j).wait_recv()
        if self.seen:
            at = FAR if passed else FROM[d]
            self.seen(part, *((at, j) if ring == SLOW else (OWN, at)), d if passed else None)

    def own(self):
        for ring in BOTH:
            for d in BOTH:
                for part in BOTH:
                    self.message(part, ring, 0, d).start()

    def near(self):
        for d in BOTH:
            for part in BOTH:
                self.arrived(part, FAST, 0, d)
                self.message(part, FAST, 1, d).start()
                for e in BOTH:
                    self.message(part, SLOW, 0, e, FROM[d]).start()

    def row(self):
        for part in BOTH:
            for d in BOTH:
                self.arrived(part, FAST, 1, d)
            for e in BOTH:
                self.message(part, SLOW, 0, e, FAR).start()
        self.sides(OWN)

    def sides(self, *blocks):
        for j in blocks:
            for part in BOTH:
                for d in BOTH:
                    self.arrived(part, SLOW, 0, d, j)
                    self.message(part, SLOW, 1, d, j).start()

    def far(self, *blocks):
        for j in blocks:
            for part in BOTH:
                for d in BOTH:
                    self.arrived(part, SLOW, 1, d, j)

    def sent(self):
        for part in BOTH:
            for d in BOTH:
                for passed in BOTH:
                    self.message(part, FAST, passed, d).wait_send()
                    for j in RING:
                        self.message(part, SLOW, passed, d, j).wait_send()


def rows_of_adapter(place, ids_ref, part, ds, shape):
    block = lax.broadcasted_iota(jnp.int32, shape, 0) // (shape[0] // len(RING))
    chosen = jnp.zeros(shape, jnp.int32)
    for df in RING:
        chosen = jnp.where(block == df, ids_ref[place.sequence(part, ds, df)], chosen)
    return chosen


def pick_columns(low, chosen):
    rank = chosen.shape[1]
    kept = low[:, :rank]
    for a in range(1, low.shape[1] // rank):
        kept = jnp.where(chosen == a, low[:, a * rank:(a + 1) * rank], kept)
    return kept


def spread(low, chosen, adapters):
    return jnp.concatenate([jnp.where(chosen == a, low, 0.0) for a in range(adapters)], axis=1).astype(BF)


PASS, FREE, SUM = range(3)
FAST_SEMS = [DMA((2, 3, 2))] * 2


def add(into, *others):
    def some(i):
        at = pl.ds(pl.multiple_of(i * TILE, TILE), TILE)
        total = into[at, :].astype(F32)
        for other in others:
            total += other[at, :].astype(F32)
        into[at, :] = total.astype(BF)

    loop(into.shape[0] // TILE, some)


class FastScatter:
    def __init__(self, place, stage, near, landed, send_sem, recv_sem):
        self.place, self.stage, self.near, self.landed, self.sems = place, stage, near, landed, (send_sem, recv_sem)
        quarter = near.shape[2]
        self.halves = (first(quarter), pl.ds(quarter, quarter))

    def message(self, part, kind, d):
        at = self.halves[1 - d] if kind == FREE else self.halves[d]
        src = self.stage(part, FAR if kind == PASS else TOWARD[d]).at[at]
        dst = self.near.at[part, d] if kind == PASS else self.landed.at[part, d, at]
        sems = [sem.at[part, kind, d] for sem in self.sems]
        return remote(src, dst, *sems, self.place.neighbour(part, FAST, STEP[d]))

    def ready(self, part, df):
        for d in BOTH:
            if df == FAR:
                self.message(part, PASS, d).start()
            elif df == TOWARD[d]:
                self.message(part, FREE, d).start()

    def finish(self):
        for d in BOTH:
            for part in BOTH:
                self.message(part, PASS, d).wait_recv()
                add(self.stage(part, TOWARD[d]).at[self.halves[d]], self.near.at[part, d])
                self.message(part, SUM, d).start()
        for part in BOTH:
            for d in BOTH:
                self.message(part, FREE, d).wait_recv()
                self.message(part, SUM, d).wait_recv()
            add(self.stage(part, OWN), self.landed.at[part, UP], self.landed.at[part, DOWN])

    def store(self, out_ref):
        rows = self.landed.shape[2]
        for part in BOTH:
            out_ref[part * rows:(part + 1) * rows] = self.stage(part, OWN)[...]
        for part in BOTH:
            for kind in range(3):
                for d in BOTH:
                    self.message(part, kind, d).wait_send()


def fast_scratch(rows, cols):
    return [pltpu.VMEM((2, 2, rows // 2, cols), BF), pltpu.VMEM((2, 2, rows, cols), BF)]


def comm_params(collective_id, limit=VMEM_MOST):
    return pltpu.CompilerParams(collective_id=collective_id, has_side_effects=True, vmem_limit_bytes=limit)


WO_CHUNKS = 8


def attend_kernel(side, adapters, scale, n_keep, ids_ref, x_ref, gain_ref, cos_ref, sin_ref, *rest):
    w_heads, a_heads, b_heads, (wo_ref, ao_ref), a_mlp, b_rows, rest = rest[:3], rest[3:6], rest[6:9], rest[9:11], rest[11:13], rest[13:15], rest[15:]
    given, rest = rest[:n_keep], rest[n_keep:]
    (out_ref, a_all, b_all), rest = rest[:3], rest[3:]
    kept, rest = rest[:n_keep], rest[n_keep:]
    (w, a_raw, b_raw, a_rows, bx, xbuf, h, z, lows, att, act, wo, stage, near, landed, am_raw, am_rows, pair_send, pair_recv, load_sem, x_sem, own_sem,
     wo_load, wo_send, wo_recv, bulk_send, bulk_recv, swap_send, swap_recv,
     send_sem, recv_sem, a_send, a_recv, b_send, b_recv, fast_send, fast_recv) = rest
    place = Place(side)
    place.announce(place.partner, place.device(0, FAR), place.device(FAR, 0))
    head, seq_len, depth = cos_ref.shape[1], x_ref.shape[1], x_ref.shape[2]
    cols = len(w_heads) * head
    chips = side * side
    per = a_raw.shape[3]
    half_depth = depth // 4
    heads = a_heads + b_heads + w_heads
    spots = [[a_raw.at[place.core, i] for i in range(3)] + [b_raw.at[at, i] for i in range(3)] + [w.at[:, pl.ds(at * cols + i * head, head)] for i in range(3)]
             for at in BOTH]
    few = len(a_heads) + len(b_heads)
    steps = chips // 2
    loads = ends([pltpu.make_async_copy(src, dst, load_sem) for src, dst in zip(heads, spots[0])])

    def x_loads(step):
        slot = lax.rem(step, 2)
        return [pltpu.make_async_copy(x_ref.at[4 * lax.rem(step, steps) + 2 * i + place.core], xbuf.at[slot, i], x_sem.at[slot]) for i in BOTH]

    ends(x_loads(0))

    def every(ref):
        return lambda part, ds, df: ref.at[place.core, part, place.turn(place.y, df if part else ds), place.turn(place.x, ds if part else df)]

    every_a, every_b = every(a_all), every(b_all)
    own_loads = ends([pltpu.make_async_copy(a_mlp[i], am_raw.at[i], own_sem) for i in BOTH])
    own_b = [pltpu.make_async_copy(b_rows[half].at[part], every_b(part, OWN, OWN).at[half], load_sem) for part in BOTH for half in BOTH]
    ends(own_b)
    width = wo_ref.shape[1]
    rank = ao_ref.shape[2]
    wo_loads = []
    for part in BOTH:
        wo_loads.append(pltpu.make_async_copy(wo_ref, wo.at[part, OWN, 0, :, first(width)], wo_load))
        for a in range(adapters):
            wo_loads.append(pltpu.make_async_copy(ao_ref.at[a], wo.at[part, OWN, 0, :, pl.ds(width + a * rank, rank)], wo_load))
    ends(wo_loads)
    wait(own_loads)
    am_rows[...] = jnp.concatenate([am_raw[i, a] for i in BOTH for a in range(adapters)], axis=0)
    place.meet()
    pair = [remote(src, dst, pair_send.at[i], pair_recv.at[i], place.partner) for i, (src, dst) in
            enumerate(list(zip(heads, spots[1])) + list(zip(given, kept)))]
    ends(pair[:len(heads)])
    a_own = ends([pltpu.make_async_copy(am_rows.at[:, pl.ds((2 * part + half) * half_depth, half_depth)], every_a(part, OWN, OWN).at[half], own_sem)
                  for part in BOTH for half in BOTH])

    piece = head // WO_CHUNKS

    def wo_message(part, passed, d, i):
        src, dst = (wo.at[part, s, 0, pl.ds(i * piece, piece)] for s in ((FROM[d], FAR) if passed else (OWN, FROM[d])))
        sems = (part, passed, d, i)
        return remote(src, dst, wo_send.at[sems], wo_recv.at[sems], place.neighbour(part, SLOW, STEP[d]))

    def wo_to_partner(part, s):
        remote(wo.at[part, s, 0], wo.at[part, s, 1], bulk_send, bulk_recv, place.partner).start()

    passes = [range(d * WO_CHUNKS // 2, (d + 1) * WO_CHUNKS // 2) for d in BOTH]

    def wo_start(i):
        for d in BOTH:
            for part in BOTH:
                wo_message(part, 0, d, i).start()

    def wo_pass(k):
        for d in BOTH:
            for part in BOTH:
                wo_message(part, 0, d, passes[d][k]).wait_recv()
                wo_message(part, 1, d, passes[d][k]).start()

    def wo_arrived():
        for d in BOTH:
            for part in BOTH:
                for i in passes[1 - d]:
                    wo_message(part, 0, d, i).wait_recv()
                wo_to_partner(part, FROM[d])

    def wo_last():
        for k in range(WO_CHUNKS // 2):
            for part in BOTH:
                for d in BOTH:
                    wo_message(part, 1, d, passes[d][k]).wait_recv()
                    at = pl.ds(passes[d][k] * piece, piece)
                    remote(wo.at[part, FAR, 0, at], wo.at[part, FAR, 1, at], bulk_send, bulk_recv, place.partner).start()

    wait(wo_loads)
    early = WO_CHUNKS // 2 + 1
    for i in range(early):
        wo_start(i)
    wait(a_own)
    wait(loads)
    wait(own_b)
    gathers = [Gather(place, every_a, a_send, a_recv, absolute=True), Gather(place, every_b, b_send, b_recv, absolute=True)]

    def both(stage_of, *more):
        for g in gathers:
            getattr(g, stage_of)(*more)

    for copy in pair[:few]:
        copy.wait_recv()
    for core in BOTH:
        pieces = [a_raw[core, i, a] if i < len(w_heads) else jnp.zeros((per, depth), BF) for a in range(adapters) for i in RING]
        a_rows[core * 2 * TILE:(core + 1) * 2 * TILE, :] = jnp.concatenate(pieces, axis=0)
    mine = [(place.y, place.x), (place.x, place.y)]

    def block(part, ds, df):
        return lows.at[part, place.turn(mine[part][0], ds), place.turn(mine[part][1], df)]

    low_gather = Gather(place, block, send_sem, recv_sem, absolute=True)

    def norm(step, last):
        slot = lax.rem(step, 2)

        @pl.when(step + 1 < last)
        def _():
            ends(x_loads(step + 1))

        wait(x_loads(step))
        for i in BOTH:
            h[i * seq_len:(i + 1) * seq_len, :] = normed(xbuf[slot, i].astype(F32), gain_ref[...])

    def products(step):
        norm(step, 2 * steps)
        low = dot_rows(a_rows[...], h[...])
        half, at = step // (steps // 2), lax.rem(step, steps // 2) * 2 * seq_len
        for part in BOTH:
            pieces = []
            for i in BOTH:
                options = [low[TILE * (2 * part + a):TILE * (2 * part + a + 1), i * seq_len:(i + 1) * seq_len] for a in range(adapters)]
                chosen = options[0]
                for a in range(1, adapters):
                    chosen = jnp.where(ids_ref[4 * step + 2 * i + place.core] == a, options[a], chosen)
                pieces.append(chosen)
            lows[part, mine[part][0], mine[part][1], half, :, pl.ds(pl.multiple_of(at, LANE), 2 * seq_len)] = jnp.concatenate(pieces, axis=1).astype(BF)

    loop(steps, products)
    low_gather.own()
    for copy in pair[few:len(heads)]:
        copy.wait_recv()
    for part in BOTH:
        wo_to_partner(part, OWN)
    events = [lambda: ends(pair[len(heads):]), lambda: wo_start(early), low_gather.near, lambda: wo_start(early + 1), low_gather.row, lambda: wo_start(early + 2),
              lambda: low_gather.sides(*AWAY), lambda: wo_pass(0)]

    def project(step):
        for at, what in enumerate(events):
            pl.when(step == at)(lambda what=what: (what(), None)[1])
        norm(step + steps, 2 * steps)
        rows = pl.ds(pl.multiple_of(step * 2 * seq_len, LANE), 2 * seq_len)
        chunk = fit(2 * cols, 256)
        for n in range(2 * cols // chunk):
            z[rows, n * chunk:(n + 1) * chunk] = dot(h[...], w[:, n * chunk:(n + 1) * chunk])

    loop(steps, project)
    row, col = (lax.broadcasted_iota(jnp.int32, (2 * rank, rank), axis) for axis in BOTH)
    spot, kind = row // TILE, lax.rem(row, TILE) // per
    for part in BOTH:
        chip_of = spot if part == 0 else lax.rem(spot, side) * side + spot // side
        to = chip_of * 2 * per + part * per + lax.rem(row, per)
        for i in range(3):
            spread_rows = jnp.where((kind == i) & (col == to), 1.0, 0.0).astype(BF)
            for a in range(adapters):
                for o in BOTH:
                    bx[a, part, :, o * cols + i * head:o * cols + (i + 1) * head] = dot(spread_rows, b_raw[o, i, a]).astype(BF)
    low_gather.far(*RING)
    causal = lax.broadcasted_iota(jnp.int32, (seq_len, seq_len), 0) >= lax.broadcasted_iota(jnp.int32, (seq_len, seq_len), 1)

    def swap(part, ds, df):
        sems = (part, ds, df)
        to = place.neighbour(part, SLOW, ds)
        return remote(att.at[sems], act.at[part, lax.rem(len(RING) - ds, len(RING)), df], swap_send.at[sems], swap_recv.at[sems], to)

    def attention(i):
        dy, dx = side - 1 - i // side, side - 1 - lax.rem(i, side)
        chip = place.turn(place.y, dy) * side + place.turn(place.x, dx)
        adapter = ids_ref[2 * chip + place.core]
        half, at = chip // steps, pl.ds(pl.multiple_of(lax.rem(chip, steps) * seq_len, LANE), seq_len)
        zs = z[pl.ds(pl.multiple_of(chip * seq_len, LANE), seq_len), :]
        for part in BOTH:
            zs += scale * dot_columns(lows[part, :, :, half, :, at].reshape(-1, seq_len), bx[adapter, part])
        for i_head in BOTH:
            q, k, v = (zs[:, i_head * cols + i * head:i_head * cols + (i + 1) * head] for i in range(3))
            q, k = ((r * cos_ref[...] + pltpu.roll(r, head // 2, axis=1) * sin_ref[...]).astype(BF) for r in (q, k))
            scores = jnp.where(causal, dot_rows(q, k) * head ** -0.5, -1e30)
            e = jnp.exp(scores - jnp.max(scores, axis=-1, keepdims=True))
            prob = (e / jnp.sum(e, axis=-1, keepdims=True)).astype(BF)
            mixed = dot(prob, v.astype(BF)).astype(BF)
            for part, (ds, df) in enumerate(((dy, dx), (dx, dy))):
                att[part, ds, df, :, i_head * head:(i_head + 1) * head] = mixed[part * seq_len // 2:(part + 1) * seq_len // 2]

    def attention_pair(k):
        for i in BOTH:
            attention(2 * k + i)
        for i in BOTH:
            dy, dx = side - 1 - (2 * k + i) // side, side - 1 - lax.rem(2 * k + i, side)
            for part, (ds, df) in enumerate(((dy, dx), (dx, dy))):
                pl.when(ds != OWN)(swap(part, ds, df).start)
        for i in range(1, WO_CHUNKS // 2):
            pl.when(k == 2 * i)(lambda i=i: wo_pass(i))

    loop(chips // 2, attention_pair)
    wo_arrived()
    both('own')
    wo_last()
    for part in BOTH:
        act[part, OWN] = att[part, OWN]
    bulk = [remote(ref.at[place.core], ref.at[place.core], pair_send.at[len(pair) + i], pair_recv.at[len(pair) + i], place.partner) for i, ref in enumerate((a_all, b_all))]
    pltpu.make_async_copy(wo.at[:, :, 1], wo.at[:, :, 1], bulk_recv).wait()
    chunk = fit(width, 512)
    rows = seq_len // 2
    blocks = (len(RING), rows)
    fast = FastScatter(place, lambda part, df: stage.at[part, df], near, landed, fast_send, fast_recv)

    def sum_heads(part, at):
        return sum(dot(act[part, s].reshape(-1, 2 * head), wo[part, s, :, :, at].reshape(2 * head, -1)) for s in RING)

    for part in BOTH:
        for ds in RING[1:]:
            for df in RING:
                swap(part, ds, df).wait_recv()

        def columns(n):
            at = pl.ds(pl.multiple_of(n * chunk, chunk), chunk)
            stage[part, :, :, at] = sum_heads(part, at).reshape(blocks + (chunk,)).astype(BF)

        loop(width // chunk, columns)
        chosen = rows_of_adapter(place, ids_ref, part, OWN, (len(RING) * rows, rank))
        stage[part, :, :, width:] = pick_columns(sum_heads(part, pl.ds(width, adapters * rank)), chosen).reshape(blocks + (rank,)).astype(BF)
        for df in RING[1:]:
            fast.ready(part, df)
        both(('near', 'row')[part])
    both('sides', *AWAY)
    fast.finish()
    both('far', *RING)
    ends(bulk)
    fast.store(out_ref)
    for copy in pair[len(heads):] + bulk:
        copy.wait_recv()
    for copy in pair + bulk:
        copy.wait_send()
    for g in gathers + [low_gather]:
        g.sent()
    pltpu.make_async_copy(wo.at[:, :, 1], wo.at[:, :, 1], bulk_send).wait()
    for part in BOTH:
        for d in BOTH:
            for i in range(WO_CHUNKS):
                wo_message(part, 0, d, i).wait_send()
            for i in passes[d]:
                wo_message(part, 1, d, i).wait_send()
        for ds in RING[1:]:
            for df in RING:
                swap(part, ds, df).wait_send()


def attend(ids, x_in, gain, heads, w_o, a_o, a_mlp, b_rows, given, side, scale, collective_id):
    _, seq_len, depth = x_in.shape
    head = heads[0].shape[1]
    cols = 3 * head
    adapters, _, rank = a_o.shape
    per = a_mlp[0].shape[1]
    chips = side * side
    half_dim = head // 2
    inv_freq = ROPE_BASE ** (-2.0 * np.arange(half_dim) / head)
    angle = np.arange(seq_len)[:, None] * inv_freq[None, :]
    cos, sin = np.cos(angle), np.sin(angle)
    tables = [jnp.asarray(np.concatenate(pair, axis=1), F32) for pair in ((cos, cos), (-sin, sin))]
    n_pair = len(heads) + len(given) + 2
    rows, out_cols = seq_len // 2, depth + rank
    every = (2, 2, side, side, 2)
    return pl.pallas_call(
        functools.partial(attend_kernel, side, adapters, scale, len(given)),
        out_shape=[jax.ShapeDtypeStruct((seq_len, out_cols), BF), jax.ShapeDtypeStruct(every + (2 * adapters * per, depth // 4), BF),
                   jax.ShapeDtypeStruct(every + b_rows[0].shape[1:], BF)] + [jax.ShapeDtypeStruct(g.shape, g.dtype) for g in given],
        in_specs=[SMEM, HBM, VMEM, VMEM, VMEM] + [HBM] * (len(heads) + 6 + len(given)),
        out_specs=[VMEM] + [HBM] * (2 + len(given)),
        scratch_shapes=[
            pltpu.VMEM((depth, 2 * cols), BF),
            pltpu.VMEM((2, 3, adapters, per, depth), BF),
            pltpu.VMEM((2, 3, adapters, rank, head), BF),
            pltpu.VMEM((2 * 2 * TILE, depth), BF),
            pltpu.VMEM((adapters, 2, 2 * rank, 2 * cols), BF),
            pltpu.VMEM((2, 2, seq_len, depth), BF),
            pltpu.VMEM((2 * seq_len, depth), BF),
            pltpu.VMEM((chips * seq_len, 2 * cols), F32),
            pltpu.VMEM((2, side, side, 2, TILE, chips * seq_len // 2), BF),
            pltpu.VMEM((2, side, side, rows, 2 * head), BF),
            pltpu.VMEM((2, side, side, rows, 2 * head), BF),
            pltpu.VMEM((2, side, 2, head, depth + adapters * rank), BF),
            pltpu.VMEM((2, side, rows, out_cols), BF),
        ] + fast_scratch(rows, out_cols) + [
            pltpu.VMEM((2, adapters, per, depth), BF),
            pltpu.VMEM((2 * adapters * per, depth), BF),
            DMA((n_pair,)), DMA((n_pair,)), DMA, DMA((2,)), DMA, DMA, DMA((2, 2, 2, WO_CHUNKS)), DMA((2, 2, 2, WO_CHUNKS)), DMA, DMA, DMA((2, 4, 4)), DMA((2, 4, 4)),
        ] + GATHER_SEMS * 3 + FAST_SEMS,
        compiler_params=comm_params(collective_id),
        name='attend',
    )(ids, x_in, gain.reshape(1, depth), *tables, *heads, w_o, a_o, *a_mlp, *b_rows, *given)


def row_proj_kernel(side, adapters, rank, ids_ref, act, w, out_ref, stage, near, landed, fast_near, fast_landed, slow_send, slow_recv, fast_send, fast_recv):
    place = Place(side)
    place.announce()
    rows, cols = stage.shape[3:]
    quarter = rows // 2
    width = cols - rank
    chunk = fit(width, 512)

    def unit(part, ds):
        def columns(n):
            at = pl.ds(pl.multiple_of(n * chunk, chunk), chunk)
            stage[part, ds, :, :, at] = dot(act[part, ds], w[:, at]).reshape(len(RING), rows, chunk).astype(BF)

        loop(width // chunk, columns)
        chosen = rows_of_adapter(place, ids_ref, part, ds, (len(RING) * rows, rank))
        stage[part, ds, :, :, width:] = pick_columns(dot(act[part, ds], w[:, width:]), chosen).reshape(len(RING), rows, rank).astype(BF)

    blocks = ((FAR, LAST), (OWN, NEXT))

    def slow(part, kind, d, i):
        df = blocks[1 - d][i] if kind == FREE else blocks[d][i]
        sems = (part, kind, d, i)
        src = stage.at[part, FAR if kind == PASS else TOWARD[d], df]
        dst = near.at[part, d, i] if kind == PASS else landed.at[part, d, df]
        return remote(src, dst, slow_send.at[sems], slow_recv.at[sems], place.neighbour(part, SLOW, STEP[d]))

    fast = FastScatter(place, lambda part, df: stage.at[part, OWN, df], fast_near, fast_landed, fast_send, fast_recv)
    for part in BOTH:
        unit(part, FAR)
        if part == 0:
            place.meet()
        for i in BOTH:
            for d in BOTH:
                slow(part, PASS, d, i).start()
    loop(len(RING), lambda i: unit(lax.rem(i, 2), NEXT + 2 * (i // 2)))
    for i in BOTH:
        for d in BOTH:
            for part in BOTH:
                slow(part, FREE, d, i).start()
    loop(2, lambda part: unit(part, OWN))
    for i in BOTH:
        for d in BOTH:
            for part in BOTH:
                slow(part, PASS, d, i).wait_recv()
                add(stage.at[part, TOWARD[d], blocks[d][i]], near.at[part, d, i])
                slow(part, SUM, d, i).start()
    for i in BOTH:
        for d in BOTH:
            df = blocks[d][i]
            for part in BOTH:
                slow(part, SUM, d, i).wait_recv()
                slow(part, FREE, 1 - d, i).wait_recv()
                add(stage.at[part, OWN, df], landed.at[part, UP, df], landed.at[part, DOWN, df])
                fast.ready(part, df)
    fast.finish()
    fast.store(out_ref)
    for part in BOTH:
        for kind in range(3):
            for d in BOTH:
                for i in BOTH:
                    slow(part, kind, d, i).wait_send()


def row_proj(ids, act, w, adapters, rank, side, collective_id):
    rows = act.shape[2] // side
    cols = w.shape[1] - (adapters - 1) * rank
    blocks = (rows, cols)
    return pl.pallas_call(
        functools.partial(row_proj_kernel, side, adapters, rank),
        out_shape=pltpu.VMEM((2 * rows, cols), BF),
        in_specs=[SMEM, VMEM, VMEM],
        out_specs=VMEM,
        scratch_shapes=[
            pltpu.VMEM((2, side, side) + blocks, BF),
            pltpu.VMEM((2, 2, 2) + blocks, BF),
            pltpu.VMEM((2, 2, side) + blocks, BF),
        ] + fast_scratch(rows, cols) + [DMA((2, 3, 2, 2))] * 2 + FAST_SEMS,
        compiler_params=comm_params(collective_id, VMEM_MOST * 5 // 8),
        name='row_proj',
    )(ids, act, w)


def finish(sums_ref, resid, b_ref, chosen, scale, adapters):
    _, _, side, _, rank, part = b_ref.shape
    width = sums_ref.shape[1] - rank
    low = spread(sums_ref[:, width:].astype(F32), chosen, adapters)
    delta = [dot(low, b_ref[core, :, y, x].reshape(adapters * rank, part)) for y in range(side) for x in range(side) for core in BOTH]
    return resid.astype(F32) + (sums_ref[:, :width].astype(F32) + scale * jnp.concatenate(delta, axis=1))


def own_rows(place, ids_ref, shape):
    return jnp.full(shape, ids_ref[place.device(0, 0)], jnp.int32)


def gate_up_kernel(side, adapters, scale, ids_ref, sums_ref, gain_ref, x_all, a_all, b_all, wg_own, wg_par, wu_own, wu_par, bg_own, bg_par, bu_own, bu_par,
                   wd_own, wd_par, ad_own, ad_par, hid, mid_ref, wd, gbuf, raw, w, b, x_ref, a_ref, b_ref, raw_sem, load_sem, a_sem, b_sem, wd_sem, send_sem, recv_sem):
    place = Place(side)
    place.announce()
    b_load = ends([pltpu.make_async_copy(b_all.at[:, :, :, :, 0], b_ref, b_sem), pltpu.make_async_copy(x_all.at[place.device(0, 0)], x_ref, b_sem)])
    a_load = ends([pltpu.make_async_copy(a_all, a_ref, a_sem)])
    share, width = wg_own.shape
    half = raw.shape[1]
    rank = bg_own.shape[2]
    seq_len = sums_ref.shape[0]
    edge = share // TILE * TILE
    shares = (wg_own, wg_par, wu_own, wu_par)

    def raw_load(i):
        return pltpu.make_async_copy(shares[i], raw.at[i % 2, first(share)], raw_sem.at[i % 2])

    for i in BOTH:
        raw[i, edge:] = jnp.zeros((half - edge, width), BF)
        raw_load(i).start()
        for kind in BOTH:
            b[kind, i * half + edge:(i + 1) * half] = jnp.zeros((half - edge, adapters * rank), BF)
        wd[i * half + edge:(i + 1) * half] = jnp.zeros((half - edge, wd.shape[1]), BF)
    loads, wd_loads = [], []
    for i, at in enumerate((0, half)):
        wd_loads.append(pltpu.make_async_copy((wd_own, wd_par)[i], wd.at[pl.ds(at, share), first(width)], wd_sem))
        for a in range(adapters):
            wd_loads.append(pltpu.make_async_copy((ad_own, ad_par)[i].at[a], wd.at[pl.ds(at, share), pl.ds(width + a * rank, rank)], wd_sem))
            for kind, pair in enumerate(((bg_own, bg_par), (bu_own, bu_par))):
                loads.append(pltpu.make_async_copy(pair[i].at[a], b.at[kind, pl.ds(at, share), pl.ds(a * rank, rank)], load_sem))
    ends(loads)
    rows = seq_len // 4
    chosen = own_rows(place, ids_ref, (seq_len, rank))
    wait(b_load)
    mid = finish(sums_ref, x_ref[...], b_ref, chosen, scale, adapters).astype(BF)
    mid_ref[...] = mid
    h2 = normed(mid.astype(F32), gain_ref[...])
    lows = []
    wait(a_load)
    for core in BOTH:
        pieces = [dot_rows(h2[:, i * width // 4:(i + 1) * width // 4], a_ref[core, i // 2, :, :, i % 2].reshape(-1, width // 4)) for i in RING]
        lows.append(sum(pieces).astype(BF))
    low = jnp.concatenate(lows, axis=1)
    per = rank // (2 * side * side)
    row, col = (lax.broadcasted_iota(jnp.int32, (low.shape[1], 2 * rank), axis) for axis in BOTH)
    kind, rank_at = col // rank, lax.rem(col, rank)
    chip, core = rank_at // (2 * per), lax.rem(rank_at // per, 2)
    pick = ((core * side * side + chip) * 2 + kind) * adapters * per + ids_ref[place.device(0, 0)] * per + lax.rem(rank_at, per)
    low = dot(low, jnp.where(row == pick, 1.0, 0.0).astype(BF)).astype(BF)
    for part in BOTH:
        for piece in BOTH:
            at = (2 * part + piece) * rows
            gbuf[part, OWN, OWN, piece, :, :width] = h2[at:at + rows]
            gbuf[part, OWN, OWN, piece, :, width:] = low[at:at + rows]
    place.meet()
    chunk = fit(2 * half, 256)

    def unit(ds, blocks=RING):
        lo, hi = min(blocks), max(blocks) + 1
        unit_rows = (hi - lo) * 2 * rows
        low = gbuf[:, ds, lo:hi, :, :, width:].reshape(2 * unit_rows, 2 * rank).astype(F32)
        chosen = jnp.concatenate([rows_of_adapter(place, ids_ref, part, ds, (len(RING) * 2 * rows, rank))[lo * 2 * rows:hi * 2 * rows] for part in BOTH], axis=0)
        lows = [spread(low[:, kind * rank:(kind + 1) * rank], chosen, adapters) for kind in BOTH]

        def columns(n):
            at = pl.ds(pl.multiple_of(n * chunk, chunk), chunk)
            act = gbuf[:, ds, lo:hi, :, :, :width].reshape(2 * unit_rows, width)
            gate, up = (dot(act, w[kind, :, at]) + scale * dot_rows(lows[kind], b[kind, at]) for kind in BOTH)
            hid[:, ds, lo * 2 * rows:hi * 2 * rows, at] = (gate * jax.nn.sigmoid(gate) * up).astype(BF).reshape(2, unit_rows, chunk)

        loop(2 * half // chunk, columns)

    gather = Gather(place, lambda part, ds, df: gbuf.at[part, ds, df], send_sem, recv_sem)
    gather.own()
    for i in range(len(shares)):
        raw_load(i).wait()

        def turn(n):
            at = pl.ds(pl.multiple_of(n * LANE, LANE), LANE)
            w[i // 2, at, i % 2 * half:(i % 2 + 1) * half] = raw[i % 2, :, at].T

        loop(width // LANE, turn)
        if i + 2 < len(shares):
            raw_load(i + 2).start()
    gather.near()
    gather.row()
    ends(wd_loads)
    wait(loads)
    unit(OWN)
    gather.sides(*AWAY)
    loop(2, lambda i: unit(NEXT + 2 * i))
    wait(wd_loads)
    for pair in PAIRS:
        gather.far(*pair)
        unit(FAR, pair)
    gather.sent()


def gate_up(ids, sums, gain, x_in, a_all, b_all, w, side, scale, collective_id):
    _, seq_len, depth = x_in.shape
    share = w[0].shape[0]
    adapters, _, rank = w[4].shape
    half = (share + LANE - 1) // LANE * LANE
    hidden = (2, side, side * seq_len // 2, 2 * half)
    return pl.pallas_call(
        functools.partial(gate_up_kernel, side, adapters, scale),
        out_shape=[pltpu.VMEM(hidden, BF), pltpu.VMEM((seq_len, depth), BF), pltpu.VMEM((2 * half, depth + adapters * rank), BF)],
        in_specs=[SMEM] + [VMEM] * 2 + [HBM] * (3 + len(w)),
        out_specs=[VMEM] * 3,
        scratch_shapes=[
            pltpu.VMEM((2, side, side, 2, seq_len // 4, depth + 2 * rank), BF),
            pltpu.VMEM((2, half, depth), BF),
            pltpu.VMEM((2, depth, 2 * half), BF),
            pltpu.VMEM((2, 2 * half, adapters * rank), BF),
            pltpu.VMEM((seq_len, depth), BF),
            pltpu.VMEM(a_all.shape, BF),
            pltpu.VMEM(b_all.shape[:4] + b_all.shape[5:], BF),
            DMA((2,)), DMA, DMA, DMA, DMA,
        ] + GATHER_SEMS,
        compiler_params=comm_params(collective_id, VMEM_MOST * 51 // 64),
        name='gate_up',
    )(ids, sums, gain.reshape(1, depth), x_in, a_all, b_all, *w)


def deliver_kernel(side, adapters, scale, ids_ref, sums_ref, x_ref, b_all, out_ref, b_ref, b_sem, pair_send, pair_recv, send_sem, recv_sem):
    place = Place(side)
    place.announce(place.partner)
    b_load = ends([pltpu.make_async_copy(b_all.at[:, :, :, :, 1], b_ref, b_sem)])
    seq_len = sums_ref.shape[0]
    rows = seq_len // 4
    chosen = own_rows(place, ids_ref, (seq_len, b_ref.shape[4]))
    wait(b_load)
    y = finish(sums_ref, x_ref[...], b_ref, chosen, scale, adapters).astype(BF)
    for part in BOTH:
        for piece in BOTH:
            at = (2 * part + piece) * rows
            out_ref[place.device(0, 0), part, piece] = y[at:at + rows]
    place.meet()

    def block(part, ds, df):
        return out_ref.at[place.sequence(part, ds, df), part]

    def seen(part, ds, df, half):
        ref = block(part, ds, df) if half is None else block(part, ds, df).at[half]
        remote(ref, ref, pair_send, pair_recv, place.partner).start()

    for part in BOTH:
        seen(part, OWN, OWN, None)
    gather = Gather(place, block, send_sem, recv_sem, absolute=True, seen=seen)
    gather.own()
    gather.near()
    gather.row()
    gather.sides(*AWAY)
    gather.far(*RING)
    gather.sent()
    every = out_ref.at[first(side * side)]
    for sem in (pair_send, pair_recv):
        pltpu.make_async_copy(every, every, sem).wait()


def put_kernel(y_ref, out_ref, sem):
    wait(ends([pltpu.make_async_copy(y_ref.at[i], out_ref.at[i], sem) for i in range(y_ref.shape[0])]))


def deliver(ids, sums, x_mid, b_all, side, scale, collective_id):
    seq_len, depth = x_mid.shape
    rows = seq_len // 4
    y = pl.pallas_call(
        functools.partial(deliver_kernel, side, b_all.shape[1], scale),
        out_shape=pltpu.VMEM((2 * side * side, 2, 2, rows, depth), BF),
        in_specs=[SMEM] + [VMEM] * 2 + [HBM],
        scratch_shapes=[pltpu.VMEM(b_all.shape[:4] + b_all.shape[5:], BF), DMA, DMA, DMA] + GATHER_SEMS,
        compiler_params=comm_params(collective_id, VMEM_SMALL),
        name='deliver',
    )(ids, sums, x_mid, b_all)
    return pl.pallas_call(
        put_kernel,
        out_shape=jax.ShapeDtypeStruct(y.shape, BF),
        in_specs=[pl.BlockSpec(memory_space=pl.ANY)],
        out_specs=HBM,
        scratch_shapes=[DMA],
        compiler_params=pltpu.CompilerParams(vmem_limit_bytes=VMEM_LEAST),
        name='put',
    )(y)


def solution(mesh):
    tp_size = mesh.shape['tensor']
    side = math.isqrt(tp_size // 2)
    rows_only = P('tensor', None)
    head_split = P(None, 'tensor', None)
    last_split = P(None, None, 'tensor')
    b_head_split = P(None, None, 'tensor', None)
    in_specs = (P('data', None, None), P('data'), P(None), P(None),
                head_split, head_split, head_split, P('tensor', None, None),
                P(None, 'tensor'), P(None, 'tensor'), rows_only,
                last_split, b_head_split, last_split, b_head_split, last_split, b_head_split,
                P(None, 'tensor', None, None), last_split,
                last_split, last_split, last_split, last_split,
                head_split, last_split)

    def local_layer(x_in, adapter_ids, gain_attn, gain_mlp, w_q, w_k, w_v, w_o, w_gate, w_up, w_down, a_q, b_q, a_k, b_k, a_v, b_v, a_o, b_o, a_gate, b_gate, a_up, b_up, a_down, b_down):
        scale = ALPHA / b_q.shape[1]

        def across(a):
            return a.swapaxes(-1, -2)

        heads = [w[:, 0] for w in (w_q, w_k, w_v)] + [across(a) for a in (a_q, a_k, a_v)] + [b[:, :, 0] for b in (b_q, b_k, b_v)]
        given = [across(w_gate), across(w_up), across(b_gate), across(b_up), w_down, a_down]
        sums, all_a, all_b, *kept = attend(adapter_ids, x_in, gain_attn, heads, w_o[0], a_o[:, 0], (across(a_gate), across(a_up)), (b_o, b_down), given, side, scale, 0)
        w = [piece for pair in zip(given, kept) for piece in pair]
        hidden, x_mid, w_d = gate_up(adapter_ids, sums, gain_mlp, x_in, all_a, all_b, w, side, scale, 1)
        sums = row_proj(adapter_ids, hidden, w_d, *a_o.shape[::3], side, 2)
        y = deliver(adapter_ids, sums, x_mid, pltpu.with_memory_space_constraint(all_b, pltpu.HBM), side, scale, 3)
        return y.reshape(x_in.shape)

    return jax.shard_map(local_layer, mesh=mesh, in_specs=in_specs, out_specs=P('data', None, None), check_vma=False)
```

```python
import functools
import math

import jax
import jax.numpy as jnp
import numpy as np
from jax import lax
from jax.experimental import pallas as pl
from jax.experimental.pallas import tpu as pltpu
from jax.sharding import PartitionSpec as P

ALPHA = 16.0
ROPE_BASE = 10000.0
EPSILON = 1e-5
BF = jnp.bfloat16
F32 = jnp.float32
LANE = 128
TILE = 16
VMEM_MOST = 67043328
VMEM_SMALL = VMEM_MOST // 6
VMEM_LEAST = VMEM_MOST // 32
MESH = pl.DeviceIdType.MESH
HBM = pl.BlockSpec(memory_space=pltpu.HBM)
VMEM = pl.BlockSpec(memory_space=pltpu.VMEM)
SMEM = pl.BlockSpec(memory_space=pltpu.SMEM)
DMA = pltpu.SemaphoreType.DMA

OWN, NEXT, FAR, LAST = RING = range(4)
UP, DOWN = BOTH = range(2)
STEP = (NEXT, -NEXT)
FROM = (LAST, NEXT)
AWAY = (NEXT, LAST, FAR)
PAIRS = ((OWN, NEXT), (LAST, FAR))
TOWARD = (NEXT, LAST)
FAST, SLOW = BOTH


def fit(size, most):
    return max(c for c in range(LANE, most + 1, LANE) if size % c == 0)


def first(size):
    return pl.ds(0, size)


def dot(a, b):
    return jnp.dot(a, b, preferred_element_type=F32)


def dot_rows(a, b):
    return lax.dot_general(a, b, (((1,), (1,)), ((), ())), preferred_element_type=F32)


def dot_columns(a, b):
    return lax.dot_general(a, b, (((0,), (0,)), ((), ())), preferred_element_type=F32)


def normed(act, gain):
    return (act * lax.rsqrt(jnp.mean(act * act, axis=-1, keepdims=True) + EPSILON) * gain).astype(BF)


def ends(copies):
    for copy in copies:
        copy.start()
    return copies


def wait(copies):
    for copy in copies:
        copy.wait()


def loop(count, body):
    lax.fori_loop(0, count, lambda i, carry: (body(i), carry)[1], 0)


class Place:
    def __init__(self, side):
        index = lax.axis_index('tensor')
        self.side = side
        self.core = lax.rem(index, 2)
        chip = index // 2
        self.y, self.x = chip // side, lax.rem(chip, side)
        self.partner = index + 1 - 2 * self.core

    def turn(self, at, steps):
        return lax.rem(at + steps + self.side, self.side)

    def device(self, dy, dx):
        return (self.turn(self.y, dy) * self.side + self.turn(self.x, dx)) * 2 + self.core

    def neighbour(self, part, ring, step):
        return self.device(0, step) if part == ring else self.device(step, 0)

    def sequence(self, part, ds, df):
        return self.device(jnp.where(part == 0, ds, df), jnp.where(part == 0, df, ds))

    def announce(self, *more):
        to = [self.neighbour(0, ring, step) for ring in BOTH for step in STEP] + list(more)
        for device in to:
            pl.semaphore_signal(pltpu.get_barrier_semaphore(), inc=1, device_id={'tensor': device}, device_id_type=MESH)
        self.announced = len(to)

    def meet(self):
        pl.semaphore_wait(pltpu.get_barrier_semaphore(), self.announced)


def remote(src, dst, send_sem, recv_sem, to):
    return pltpu.make_async_remote_copy(src_ref=src, dst_ref=dst, send_sem=send_sem, recv_sem=recv_sem, device_id={'tensor': to}, device_id_type=MESH)


GATHER_SEMS = [DMA((2, 2, 2, 2, 4))] * 2


class Gather:
    def __init__(self, place, block, send_sem, recv_sem, absolute=False, seen=None):
        self.place, self.block, self.sems, self.absolute, self.seen = place, block, (send_sem, recv_sem), absolute, seen

    def message(self, part, ring, passed, d, j=OWN):
        spot = (lambda s: (s, j)) if ring == SLOW else (lambda s: (OWN, s))
        src, dst = (FROM[d], FAR) if passed else (OWN, FROM[d])
        a, b = self.block(part, *spot(src)), self.block(part, *spot(src if self.absolute else dst))
        if passed:
            a, b = a.at[d], b.at[d]
        return remote(a, b, *(sem.at[part, ring, passed, d, j] for sem in self.sems), self.place.neighbour(part, ring, STEP[d]))

    def arrived(self, part, ring, passed, d, j=OWN):
        self.message(part, ring, passed, d, j).wait_recv()
        if self.seen:
            at = FAR if passed else FROM[d]
            self.seen(part, *((at, j) if ring == SLOW else (OWN, at)), d if passed else None)

    def own(self):
        for ring in BOTH:
            for d in BOTH:
                for part in BOTH:
                    self.message(part, ring, 0, d).start()

    def near(self):
        for d in BOTH:
            for part in BOTH:
                self.arrived(part, FAST, 0, d)
                self.message(part, FAST, 1, d).start()
                for e in BOTH:
                    self.message(part, SLOW, 0, e, FROM[d]).start()

    def row(self):
        for part in BOTH:
            for d in BOTH:
                self.arrived(part, FAST, 1, d)
            for e in BOTH:
                self.message(part, SLOW, 0, e, FAR).start()
        self.sides(OWN)

    def sides(self, *blocks):
        for j in blocks:
            for part in BOTH:
                for d in BOTH:
                    self.arrived(part, SLOW, 0, d, j)
                    self.message(part, SLOW, 1, d, j).start()

    def far(self, *blocks):
        for j in blocks:
            for part in BOTH:
                for d in BOTH:
                    self.arrived(part, SLOW, 1, d, j)

    def sent(self):
        for part in BOTH:
            for d in BOTH:
                for passed in BOTH:
                    self.message(part, FAST, passed, d).wait_send()
                    for j in RING:
                        self.message(part, SLOW, passed, d, j).wait_send()


ROW_SEMS = [DMA((2, 2, 2, 2))] * 2


class RowGather:
    def __init__(self, place, row, mine, send_sem, recv_sem):
        self.place, self.row_at, self.mine, self.sems = place, row, mine, (send_sem, recv_sem)

    def message(self, part, ring, passed, d):
        if ring == SLOW:
            ref = self.row_at(part, FROM[d] if passed else OWN)
            ref = ref.at[:, d] if passed else ref
        else:
            ref = self.row_at(part, OWN).at[self.place.turn(self.mine(part), FROM[d] if passed else OWN)]
            ref = ref.at[d] if passed else ref
        return remote(ref, ref, *(sem.at[part, ring, passed, d] for sem in self.sems), self.place.neighbour(part, ring, STEP[d]))

    def pass_on(self, ring, passed):
        for part in BOTH:
            for d in BOTH:
                self.landing(part, ring, passed, d).wait_recv()
                if not passed:
                    self.message(part, ring, 1, d).start()
            if passed and ring == FAST:
                for d in BOTH:
                    self.message(part, SLOW, 0, d).start()

    def landing(self, part, ring, passed, d):
        at = FAR if passed else FROM[d]
        ref = self.row_at(part, at) if ring == SLOW else self.row_at(part, OWN).at[self.place.turn(self.mine(part), at)]
        if passed:
            ref = ref.at[:, d] if ring == SLOW else ref.at[d]
        return remote(ref, ref, *(sem.at[part, ring, passed, d] for sem in self.sems), self.place.neighbour(part, ring, STEP[d]))

    def own(self):
        for d in BOTH:
            for part in BOTH:
                self.message(part, FAST, 0, d).start()

    def near(self):
        self.pass_on(FAST, 0)

    def row(self):
        self.pass_on(FAST, 1)

    def sides(self):
        self.pass_on(SLOW, 0)

    def far(self):
        self.pass_on(SLOW, 1)

    def sent(self):
        for part in BOTH:
            for ring in BOTH:
                for passed in BOTH:
                    for d in BOTH:
                        self.message(part, ring, passed, d).wait_send()


def rows_of_adapter(place, ids_ref, part, ds, shape):
    block = lax.broadcasted_iota(jnp.int32, shape, 0) // (shape[0] // len(RING))
    chosen = jnp.zeros(shape, jnp.int32)
    for df in RING:
        chosen = jnp.where(block == df, ids_ref[place.sequence(part, ds, df)], chosen)
    return chosen


def pick_columns(low, chosen):
    rank = chosen.shape[1]
    kept = low[:, :rank]
    for a in range(1, low.shape[1] // rank):
        kept = jnp.where(chosen == a, low[:, a * rank:(a + 1) * rank], kept)
    return kept


def spread(low, chosen, adapters):
    return jnp.concatenate([jnp.where(chosen == a, low, 0.0) for a in range(adapters)], axis=1).astype(BF)


PASS, FREE, SUM = range(3)
FAST_SEMS = [DMA((2, 3, 2))] * 2


def add(into, *others):
    def some(i):
        at = pl.ds(pl.multiple_of(i * TILE, TILE), TILE)
        total = into[at, :].astype(F32)
        for other in others:
            total += other[at, :].astype(F32)
        into[at, :] = total.astype(BF)

    loop(into.shape[0] // TILE, some)


class FastScatter:
    def __init__(self, place, stage, near, landed, send_sem, recv_sem):
        self.place, self.stage, self.near, self.landed, self.sems = place, stage, near, landed, (send_sem, recv_sem)
        quarter = near.shape[2]
        self.halves = (first(quarter), pl.ds(quarter, quarter))

    def message(self, part, kind, d):
        at = self.halves[1 - d] if kind == FREE else self.halves[d]
        src = self.stage(part, FAR if kind == PASS else TOWARD[d]).at[at]
        dst = self.near.at[part, d] if kind == PASS else self.landed.at[part, d, at]
        sems = [sem.at[part, kind, d] for sem in self.sems]
        return remote(src, dst, *sems, self.place.neighbour(part, FAST, STEP[d]))

    def ready(self, part, df):
        for d in BOTH:
            if df == FAR:
                self.message(part, PASS, d).start()
            elif df == TOWARD[d]:
                self.message(part, FREE, d).start()

    def sum(self):
        for d in BOTH:
            for part in BOTH:
                self.message(part, PASS, d).wait_recv()
                add(self.stage(part, TOWARD[d]).at[self.halves[d]], self.near.at[part, d])
                self.message(part, SUM, d).start()

    def finish(self):
        for part in BOTH:
            for d in BOTH:
                self.message(part, FREE, d).wait_recv()
                self.message(part, SUM, d).wait_recv()
            add(self.stage(part, OWN), self.landed.at[part, UP], self.landed.at[part, DOWN])

    def store(self, out_ref):
        rows = self.landed.shape[2]
        for part in BOTH:
            out_ref[part * rows:(part + 1) * rows] = self.stage(part, OWN)[...]
        for part in BOTH:
            for kind in range(3):
                for d in BOTH:
                    self.message(part, kind, d).wait_send()


def fast_scratch(rows, cols):
    return [pltpu.VMEM((2, 2, rows // 2, cols), BF), pltpu.VMEM((2, 2, rows, cols), BF)]


def comm_params(collective_id, limit=VMEM_MOST):
    return pltpu.CompilerParams(collective_id=collective_id, has_side_effects=True, vmem_limit_bytes=limit)


WO_CHUNKS = 4


def attend_kernel(side, adapters, scale, n_keep, ids_ref, x_ref, gain_ref, cos_ref, sin_ref, *rest):
    w_heads, a_heads, b_heads, (wo_ref, ao_ref), a_mlp, b_rows, rest = rest[:3], rest[3:6], rest[6:9], rest[9:11], rest[11:13], rest[13:15], rest[15:]
    given, rest = rest[:n_keep], rest[n_keep:]
    (out_ref, a_all, b_all), rest = rest[:3], rest[3:]
    kept, rest = rest[:n_keep], rest[n_keep:]
    (w, a_raw, b_raw, a_rows, bx, xbuf, h, z, lows, att, act, wo, stage, near, landed, am_raw, am_rows, pair_send, pair_recv, load_sem, x_sem, own_sem,
     wo_load, wo_send, wo_recv, bulk_send, bulk_recv, swap_send, swap_recv,
     send_sem, recv_sem, a_send, a_recv, b_send, b_recv, fast_send, fast_recv) = rest
    place = Place(side)
    place.announce(place.partner, place.device(0, FAR), place.device(FAR, 0))
    head, seq_len, depth = cos_ref.shape[1], x_ref.shape[1], x_ref.shape[2]
    cols = len(w_heads) * head
    chips = side * side
    per = a_raw.shape[3]
    half_depth = depth // 4
    heads = a_heads + w_heads + b_heads
    spots = [[a_raw.at[place.core, i] for i in range(3)] + [w.at[:, pl.ds(at * cols + i * head, head)] for i in range(3)] + [b_raw.at[at, i] for i in range(3)]
             for at in BOTH]
    few = len(a_heads)
    steps = chips // 2
    loads = ends([pltpu.make_async_copy(src, dst, load_sem) for src, dst in zip(heads, spots[0])])

    def x_loads(step):
        slot = lax.rem(step, 2)
        return [pltpu.make_async_copy(x_ref.at[4 * lax.rem(step, steps) + 2 * i + place.core], xbuf.at[slot, i], x_sem.at[slot]) for i in BOTH]

    ends(x_loads(0))

    def every(ref):
        return lambda part, ds: ref.at[place.core, part, :, place.turn(place.x, ds)] if part else ref.at[place.core, part, place.turn(place.y, ds)]

    def spot_of(part):
        return place.y if part else place.x

    def own_of(ref, part):
        return ref.at[place.core, part, place.y, place.x]

    own_loads = ends([pltpu.make_async_copy(a_mlp[i], am_raw.at[i], own_sem) for i in BOTH])
    own_b = [pltpu.make_async_copy(b_rows[half].at[part], own_of(b_all, part).at[half], load_sem) for part in BOTH for half in BOTH]
    ends(own_b)
    width = wo_ref.shape[1]
    rank = ao_ref.shape[2]
    wo_loads = []
    for part in BOTH:
        wo_loads.append(pltpu.make_async_copy(wo_ref, wo.at[part, OWN, 0, :, first(width)], wo_load))
        for a in range(adapters):
            wo_loads.append(pltpu.make_async_copy(ao_ref.at[a], wo.at[part, OWN, 0, :, pl.ds(width + a * rank, rank)], wo_load))
    ends(wo_loads)
    wait(own_loads)
    am_rows[...] = jnp.concatenate([am_raw[i, a] for i in BOTH for a in range(adapters)], axis=0)
    place.meet()
    pair = [remote(src, dst, pair_send.at[i], pair_recv.at[i], place.partner) for i, (src, dst) in
            enumerate(list(zip(heads, spots[1])) + list(zip(given, kept)))]
    ends(pair[:len(heads)])
    a_own = ends([pltpu.make_async_copy(am_rows.at[:, pl.ds((2 * part + half) * half_depth, half_depth)], own_of(a_all, part).at[half], own_sem)
                  for part in BOTH for half in BOTH])

    piece = head // WO_CHUNKS

    def wo_message(part, passed, d, i):
        src, dst = (wo.at[part, s, 0, pl.ds(i * piece, piece)] for s in ((FROM[d], FAR) if passed else (OWN, FROM[d])))
        sems = (part, passed, d, i)
        return remote(src, dst, wo_send.at[sems], wo_recv.at[sems], place.neighbour(part, SLOW, STEP[d]))

    def wo_to_partner(part, s):
        remote(wo.at[part, s, 0], wo.at[part, s, 1], bulk_send, bulk_recv, place.partner).start()

    passes = [range(d * WO_CHUNKS // 2, (d + 1) * WO_CHUNKS // 2) for d in BOTH]

    def wo_start(i):
        for d in BOTH:
            for part in BOTH:
                wo_message(part, 0, d, i).start()

    def wo_pass(k):
        for d in BOTH:
            for part in BOTH:
                wo_message(part, 0, d, passes[d][k]).wait_recv()
                wo_message(part, 1, d, passes[d][k]).start()

    def wo_arrived():
        for d in BOTH:
            for part in BOTH:
                for i in passes[1 - d]:
                    wo_message(part, 0, d, i).wait_recv()
                wo_to_partner(part, FROM[d])

    def wo_last():
        for part in BOTH:
            for d in BOTH:
                for i in passes[d]:
                    wo_message(part, 1, d, i).wait_recv()
            wo_to_partner(part, FAR)

    wait(wo_loads)
    early = WO_CHUNKS - 1
    for i in range(early):
        wo_start(i)
    wait(a_own)
    wait(loads)
    wait(own_b)
    gathers = [RowGather(place, every(a_all), spot_of, a_send, a_recv), RowGather(place, every(b_all), spot_of, b_send, b_recv)]

    def both(stage_of):
        for g in gathers:
            getattr(g, stage_of)()

    for copy in pair[:few]:
        copy.wait_recv()
    for core in BOTH:
        pieces = [a_raw[core, i, a] if i < len(w_heads) else jnp.zeros((per, depth), BF) for a in range(adapters) for i in RING]
        a_rows[core * 2 * TILE:(core + 1) * 2 * TILE, :] = jnp.concatenate(pieces, axis=0)
    mine = [(place.y, place.x), (place.x, place.y)]

    low_gather = RowGather(place, lambda part, ds: lows.at[part, place.turn(mine[part][0], ds)], spot_of, send_sem, recv_sem)

    def norm(step, last):
        slot = lax.rem(step, 2)

        @pl.when(step + 1 < last)
        def _():
            ends(x_loads(step + 1))

        wait(x_loads(step))
        for i in BOTH:
            h[i * seq_len:(i + 1) * seq_len, :] = normed(xbuf[slot, i].astype(F32), gain_ref[...])

    def products(step):
        norm(step, 2 * steps)
        low = dot_rows(a_rows[...], h[...])
        half, at = step // (steps // 2), lax.rem(step, steps // 2) * 2 * seq_len
        for part in BOTH:
            pieces = []
            for i in BOTH:
                options = [low[TILE * (2 * part + a):TILE * (2 * part + a + 1), i * seq_len:(i + 1) * seq_len] for a in range(adapters)]
                chosen = options[0]
                for a in range(1, adapters):
                    chosen = jnp.where(ids_ref[4 * step + 2 * i + place.core] == a, options[a], chosen)
                pieces.append(chosen)
            lows[part, mine[part][0], mine[part][1], half, :, pl.ds(pl.multiple_of(at, LANE), 2 * seq_len)] = jnp.concatenate(pieces, axis=1).astype(BF)

    loop(steps, products)
    low_gather.own()
    for copy in pair[few:len(heads)]:
        copy.wait_recv()
    for part in BOTH:
        wo_to_partner(part, OWN)
    events = {0: lambda: ends(pair[len(heads):]), 3: low_gather.near, 5: lambda: (low_gather.row(), wo_start(early))}

    def project(step):
        for at, what in events.items():
            pl.when(step == at)(lambda what=what: (what(), None)[1])
        norm(step + steps, 2 * steps)
        rows = pl.ds(pl.multiple_of(step * 2 * seq_len, LANE), 2 * seq_len)
        chunk = fit(2 * cols, 256)
        for n in range(2 * cols // chunk):
            z[rows, n * chunk:(n + 1) * chunk] = dot(h[...], w[:, n * chunk:(n + 1) * chunk])

    loop(steps, project)
    row, col = (lax.broadcasted_iota(jnp.int32, (2 * rank, rank), axis) for axis in BOTH)
    spot, kind = row // TILE, lax.rem(row, TILE) // per
    for part in BOTH:
        chip_of = spot if part == 0 else lax.rem(spot, side) * side + spot // side
        to = chip_of * 2 * per + part * per + lax.rem(row, per)
        for i in range(3):
            spread_rows = jnp.where((kind == i) & (col == to), 1.0, 0.0).astype(BF)
            for a in range(adapters):
                for o in BOTH:
                    bx[a, part, :, o * cols + i * head:o * cols + (i + 1) * head] = dot(spread_rows, b_raw[o, i, a]).astype(BF)
    low_gather.sides()
    wo_pass(0)
    low_gather.far()
    causal = lax.broadcasted_iota(jnp.int32, (seq_len, seq_len), 0) >= lax.broadcasted_iota(jnp.int32, (seq_len, seq_len), 1)

    def swap(part, ds):
        sems = (part, ds)
        to = place.neighbour(part, SLOW, ds)
        return remote(att.at[sems], act.at[part, lax.rem(len(RING) - ds, len(RING))], swap_send.at[sems], swap_recv.at[sems], to)

    def attention(i):
        dy, dx = side - 1 - i // side, side - 1 - lax.rem(i, side)
        chip = place.turn(place.y, dy) * side + place.turn(place.x, dx)
        adapter = ids_ref[2 * chip + place.core]
        half, at = chip // steps, pl.ds(pl.multiple_of(lax.rem(chip, steps) * seq_len, LANE), seq_len)
        zs = z[pl.ds(pl.multiple_of(chip * seq_len, LANE), seq_len), :]
        for part in BOTH:
            zs += scale * dot_columns(lows[part, :, :, half, :, at].reshape(-1, seq_len), bx[adapter, part])
        for i_head in BOTH:
            q, k, v = (zs[:, i_head * cols + i * head:i_head * cols + (i + 1) * head] for i in range(3))
            q, k = ((r * cos_ref[...] + pltpu.roll(r, head // 2, axis=1) * sin_ref[...]).astype(BF) for r in (q, k))
            scores = jnp.where(causal, dot_rows(q, k) * head ** -0.5, -1e30)
            e = jnp.exp(scores - jnp.max(scores, axis=-1, keepdims=True))
            prob = (e / jnp.sum(e, axis=-1, keepdims=True)).astype(BF)
            mixed = dot(prob, v.astype(BF)).astype(BF)
            for part, (ds, df) in enumerate(((dy, dx), (dx, dy))):
                att[part, ds, df, :, i_head * head:(i_head + 1) * head] = mixed[part * seq_len // 2:(part + 1) * seq_len // 2]

    def attention_pair(k):
        for i in BOTH:
            attention(2 * k + i)
        row = side - 1 - 2 * k // side
        pl.when((lax.rem(2 * k + 2, side) == 0) & (row != OWN))(lambda: swap(0, row).start())
        pl.when(k == 1)(lambda: wo_pass(1))

    loop(chips // 2, attention_pair)
    for ds in AWAY:
        swap(1, ds).start()
    wo_arrived()
    both('own')
    wo_last()
    for part in BOTH:
        act[part, OWN] = att[part, OWN]
    bulk = [remote(ref.at[place.core], ref.at[place.core], pair_send.at[len(pair) + i], pair_recv.at[len(pair) + i], place.partner) for i, ref in enumerate((a_all, b_all))]
    pltpu.make_async_copy(wo.at[:, :, 1], wo.at[:, :, 1], bulk_recv).wait()
    chunk = fit(width, 512)
    rows = seq_len // 2
    blocks = (len(RING), rows)
    fast = FastScatter(place, lambda part, df: stage.at[part, df], near, landed, fast_send, fast_recv)

    def sum_heads(part, at):
        return sum(dot(act[part, s].reshape(-1, 2 * head), wo[part, s, :, :, at].reshape(2 * head, -1)) for s in RING)

    for part in BOTH:
        for ds in AWAY:
            swap(part, ds).wait_recv()

        def columns(n):
            at = pl.ds(pl.multiple_of(n * chunk, chunk), chunk)
            stage[part, :, :, at] = sum_heads(part, at).reshape(blocks + (chunk,)).astype(BF)

        loop(width // chunk, columns)
        chosen = rows_of_adapter(place, ids_ref, part, OWN, (len(RING) * rows, rank))
        stage[part, :, :, width:] = pick_columns(sum_heads(part, pl.ds(width, adapters * rank)), chosen).reshape(blocks + (rank,)).astype(BF)
        for df in (FAR, NEXT, LAST):
            fast.ready(part, df)
        both(('near', 'row')[part])
    both('sides')
    fast.sum()
    both('far')
    ends(bulk)
    fast.finish()
    fast.store(out_ref)
    for copy in pair[len(heads):] + bulk:
        copy.wait_recv()
    for copy in pair + bulk:
        copy.wait_send()
    for g in gathers + [low_gather]:
        g.sent()
    pltpu.make_async_copy(wo.at[:, :, 1], wo.at[:, :, 1], bulk_send).wait()
    for part in BOTH:
        for d in BOTH:
            for i in range(WO_CHUNKS):
                wo_message(part, 0, d, i).wait_send()
            for i in passes[d]:
                wo_message(part, 1, d, i).wait_send()
        for ds in AWAY:
            swap(part, ds).wait_send()


def attend(ids, x_in, gain, heads, w_o, a_o, a_mlp, b_rows, given, side, scale, collective_id):
    _, seq_len, depth = x_in.shape
    head = heads[0].shape[1]
    cols = 3 * head
    adapters, _, rank = a_o.shape
    per = a_mlp[0].shape[1]
    chips = side * side
    half_dim = head // 2
    inv_freq = ROPE_BASE ** (-2.0 * np.arange(half_dim) / head)
    angle = np.arange(seq_len)[:, None] * inv_freq[None, :]
    cos, sin = np.cos(angle), np.sin(angle)
    tables = [jnp.asarray(np.concatenate(pair, axis=1), F32) for pair in ((cos, cos), (-sin, sin))]
    n_pair = len(heads) + len(given) + 2
    rows, out_cols = seq_len // 2, depth + rank
    every = (2, 2, side, side, 2)
    return pl.pallas_call(
        functools.partial(attend_kernel, side, adapters, scale, len(given)),
        out_shape=[jax.ShapeDtypeStruct((seq_len, out_cols), BF), jax.ShapeDtypeStruct(every + (2 * adapters * per, depth // 4), BF),
                   jax.ShapeDtypeStruct(every + b_rows[0].shape[1:], BF)] + [jax.ShapeDtypeStruct(g.shape, g.dtype) for g in given],
        in_specs=[SMEM, HBM, VMEM, VMEM, VMEM] + [HBM] * (len(heads) + 6 + len(given)),
        out_specs=[VMEM] + [HBM] * (2 + len(given)),
        scratch_shapes=[
            pltpu.VMEM((depth, 2 * cols), BF),
            pltpu.VMEM((2, 3, adapters, per, depth), BF),
            pltpu.VMEM((2, 3, adapters, rank, head), BF),
            pltpu.VMEM((2 * 2 * TILE, depth), BF),
            pltpu.VMEM((adapters, 2, 2 * rank, 2 * cols), BF),
            pltpu.VMEM((2, 2, seq_len, depth), BF),
            pltpu.VMEM((2 * seq_len, depth), BF),
            pltpu.VMEM((chips * seq_len, 2 * cols), F32),
            pltpu.VMEM((2, side, side, 2, TILE, chips * seq_len // 2), BF),
            pltpu.VMEM((2, side, side, rows, 2 * head), BF),
            pltpu.VMEM((2, side, side, rows, 2 * head), BF),
            pltpu.VMEM((2, side, 2, head, depth + adapters * rank), BF),
            pltpu.VMEM((2, side, rows, out_cols), BF),
        ] + fast_scratch(rows, out_cols) + [
            pltpu.VMEM((2, adapters, per, depth), BF),
            pltpu.VMEM((2 * adapters * per, depth), BF),
            DMA((n_pair,)), DMA((n_pair,)), DMA, DMA((2,)), DMA, DMA, DMA((2, 2, 2, WO_CHUNKS)), DMA((2, 2, 2, WO_CHUNKS)), DMA, DMA, DMA((2, 4)), DMA((2, 4)),
        ] + ROW_SEMS * 3 + FAST_SEMS,
        compiler_params=comm_params(collective_id),
        name='attend',
    )(ids, x_in, gain.reshape(1, depth), *tables, *heads, w_o, a_o, *a_mlp, *b_rows, *given)


def row_proj_kernel(side, adapters, rank, ids_ref, act, w, out_ref, stage, near, landed, fast_near, fast_landed, slow_send, slow_recv, fast_send, fast_recv):
    place = Place(side)
    place.announce()
    rows, cols = stage.shape[3:]
    quarter = rows // 2
    width = cols - rank
    chunk = fit(width, 512)

    def unit(part, ds):
        def columns(n):
            at = pl.ds(pl.multiple_of(n * chunk, chunk), chunk)
            stage[part, ds, :, :, at] = dot(act[part, ds], w[:, at]).reshape(len(RING), rows, chunk).astype(BF)

        loop(width // chunk, columns)
        chosen = rows_of_adapter(place, ids_ref, part, ds, (len(RING) * rows, rank))
        stage[part, ds, :, :, width:] = pick_columns(dot(act[part, ds], w[:, width:]), chosen).reshape(len(RING), rows, rank).astype(BF)

    blocks = ((FAR, LAST), (OWN, NEXT))

    def slow(part, kind, d, i):
        df = blocks[1 - d][i] if kind == FREE else blocks[d][i]
        sems = (part, kind, d, i)
        src = stage.at[part, FAR if kind == PASS else TOWARD[d], df]
        dst = near.at[part, d, i] if kind == PASS else landed.at[part, d, df]
        return remote(src, dst, slow_send.at[sems], slow_recv.at[sems], place.neighbour(part, SLOW, STEP[d]))

    fast = FastScatter(place, lambda part, df: stage.at[part, OWN, df], fast_near, fast_landed, fast_send, fast_recv)
    for part in BOTH:
        unit(part, FAR)
        if part == 0:
            place.meet()
        for i in BOTH:
            for d in BOTH:
                slow(part, PASS, d, i).start()
    loop(len(RING), lambda i: unit(lax.rem(i, 2), NEXT + 2 * (i // 2)))
    for i in BOTH:
        for d in BOTH:
            for part in BOTH:
                slow(part, FREE, d, i).start()
    loop(2, lambda part: unit(part, OWN))
    for i in BOTH:
        for d in BOTH:
            for part in BOTH:
                slow(part, PASS, d, i).wait_recv()
                add(stage.at[part, TOWARD[d], blocks[d][i]], near.at[part, d, i])
                slow(part, SUM, d, i).start()
    for i in BOTH:
        for d in BOTH:
            df = blocks[d][i]
            for part in BOTH:
                slow(part, SUM, d, i).wait_recv()
                slow(part, FREE, 1 - d, i).wait_recv()
                add(stage.at[part, OWN, df], landed.at[part, UP, df], landed.at[part, DOWN, df])
                fast.ready(part, df)
    fast.sum()
    fast.finish()
    fast.store(out_ref)
    for part in BOTH:
        for kind in range(3):
            for d in BOTH:
                for i in BOTH:
                    slow(part, kind, d, i).wait_send()


def row_proj(ids, act, w, adapters, rank, side, collective_id):
    rows = act.shape[2] // side
    cols = w.shape[1] - (adapters - 1) * rank
    blocks = (rows, cols)
    return pl.pallas_call(
        functools.partial(row_proj_kernel, side, adapters, rank),
        out_shape=pltpu.VMEM((2 * rows, cols), BF),
        in_specs=[SMEM, VMEM, VMEM],
        out_specs=VMEM,
        scratch_shapes=[
            pltpu.VMEM((2, side, side) + blocks, BF),
            pltpu.VMEM((2, 2, 2) + blocks, BF),
            pltpu.VMEM((2, 2, side) + blocks, BF),
        ] + fast_scratch(rows, cols) + [DMA((2, 3, 2, 2))] * 2 + FAST_SEMS,
        compiler_params=comm_params(collective_id, VMEM_MOST * 5 // 8),
        name='row_proj',
    )(ids, act, w)


def finish(sums_ref, resid, b_ref, chosen, scale, adapters):
    _, _, side, _, rank, part = b_ref.shape
    width = sums_ref.shape[1] - rank
    low = spread(sums_ref[:, width:].astype(F32), chosen, adapters)
    delta = [dot(low, b_ref[core, :, y, x].reshape(adapters * rank, part)) for y in range(side) for x in range(side) for core in BOTH]
    return resid.astype(F32) + (sums_ref[:, :width].astype(F32) + scale * jnp.concatenate(delta, axis=1))


def own_rows(place, ids_ref, shape):
    return jnp.full(shape, ids_ref[place.device(0, 0)], jnp.int32)


def gate_up_kernel(side, adapters, scale, ids_ref, sums_ref, gain_ref, x_all, a_all, b_all, wg_own, wg_par, wu_own, wu_par, bg_own, bg_par, bu_own, bu_par,
                   wd_own, wd_par, ad_own, ad_par, hid, mid_ref, wd, gbuf, raw, w, b, x_ref, a_ref, b_ref, raw_sem, load_sem, a_sem, b_sem, wd_sem, send_sem, recv_sem):
    place = Place(side)
    place.announce()
    b_load = ends([pltpu.make_async_copy(b_all.at[:, :, :, :, 0], b_ref, b_sem), pltpu.make_async_copy(x_all.at[place.device(0, 0)], x_ref, b_sem)])
    a_load = ends([pltpu.make_async_copy(a_all, a_ref, a_sem)])
    share, width = wg_own.shape
    half = raw.shape[1]
    rank = bg_own.shape[2]
    seq_len = sums_ref.shape[0]
    edge = share // TILE * TILE
    shares = (wg_own, wg_par, wu_own, wu_par)

    def raw_load(i):
        return pltpu.make_async_copy(shares[i], raw.at[i % 2, first(share)], raw_sem.at[i % 2])

    for i in BOTH:
        raw[i, edge:] = jnp.zeros((half - edge, width), BF)
        raw_load(i).start()
        for kind in BOTH:
            b[kind, i * half + edge:(i + 1) * half] = jnp.zeros((half - edge, adapters * rank), BF)
        wd[i * half + edge:(i + 1) * half] = jnp.zeros((half - edge, wd.shape[1]), BF)
    loads, wd_loads = [], []
    for i, at in enumerate((0, half)):
        wd_loads.append(pltpu.make_async_copy((wd_own, wd_par)[i], wd.at[pl.ds(at, share), first(width)], wd_sem))
        for a in range(adapters):
            wd_loads.append(pltpu.make_async_copy((ad_own, ad_par)[i].at[a], wd.at[pl.ds(at, share), pl.ds(width + a * rank, rank)], wd_sem))
            for kind, pair in enumerate(((bg_own, bg_par), (bu_own, bu_par))):
                loads.append(pltpu.make_async_copy(pair[i].at[a], b.at[kind, pl.ds(at, share), pl.ds(a * rank, rank)], load_sem))
    ends(loads)
    rows = seq_len // 4
    chosen = own_rows(place, ids_ref, (seq_len, rank))
    wait(b_load)
    mid = finish(sums_ref, x_ref[...], b_ref, chosen, scale, adapters).astype(BF)
    mid_ref[...] = mid
    h2 = normed(mid.astype(F32), gain_ref[...])
    lows = []
    wait(a_load)
    for core in BOTH:
        pieces = [dot_rows(h2[:, i * width // 4:(i + 1) * width // 4], a_ref[core, i // 2, :, :, i % 2].reshape(-1, width // 4)) for i in RING]
        lows.append(sum(pieces).astype(BF))
    low = jnp.concatenate(lows, axis=1)
    per = rank // (2 * side * side)
    row, col = (lax.broadcasted_iota(jnp.int32, (low.shape[1], 2 * rank), axis) for axis in BOTH)
    kind, rank_at = col // rank, lax.rem(col, rank)
    chip, core = rank_at // (2 * per), lax.rem(rank_at // per, 2)
    pick = ((core * side * side + chip) * 2 + kind) * adapters * per + ids_ref[place.device(0, 0)] * per + lax.rem(rank_at, per)
    low = dot(low, jnp.where(row == pick, 1.0, 0.0).astype(BF)).astype(BF)
    for part in BOTH:
        for piece in BOTH:
            at = (2 * part + piece) * rows
            gbuf[part, OWN, OWN, piece, :, :width] = h2[at:at + rows]
            gbuf[part, OWN, OWN, piece, :, width:] = low[at:at + rows]
    place.meet()
    chunk = fit(2 * half, 256)

    def unit(ds, blocks=RING):
        lo, hi = min(blocks), max(blocks) + 1
        unit_rows = (hi - lo) * 2 * rows
        low = gbuf[:, ds, lo:hi, :, :, width:].reshape(2 * unit_rows, 2 * rank).astype(F32)
        chosen = jnp.concatenate([rows_of_adapter(place, ids_ref, part, ds, (len(RING) * 2 * rows, rank))[lo * 2 * rows:hi * 2 * rows] for part in BOTH], axis=0)
        lows = [spread(low[:, kind * rank:(kind + 1) * rank], chosen, adapters) for kind in BOTH]

        def columns(n):
            at = pl.ds(pl.multiple_of(n * chunk, chunk), chunk)
            act = gbuf[:, ds, lo:hi, :, :, :width].reshape(2 * unit_rows, width)
            gate, up = (dot(act, w[kind, :, at]) + scale * dot_rows(lows[kind], b[kind, at]) for kind in BOTH)
            hid[:, ds, lo * 2 * rows:hi * 2 * rows, at] = (gate * jax.nn.sigmoid(gate) * up).astype(BF).reshape(2, unit_rows, chunk)

        loop(2 * half // chunk, columns)

    gather = Gather(place, lambda part, ds, df: gbuf.at[part, ds, df], send_sem, recv_sem)
    gather.own()
    for i in range(len(shares)):
        raw_load(i).wait()

        def turn(n):
            at = pl.ds(pl.multiple_of(n * LANE, LANE), LANE)
            w[i // 2, at, i % 2 * half:(i % 2 + 1) * half] = raw[i % 2, :, at].T

        loop(width // LANE, turn)
        if i + 2 < len(shares):
            raw_load(i + 2).start()
    gather.near()
    gather.row()
    ends(wd_loads)
    wait(loads)
    unit(OWN)
    gather.sides(*AWAY)
    loop(2, lambda i: unit(NEXT + 2 * i))
    wait(wd_loads)
    for pair in PAIRS:
        gather.far(*pair)
        unit(FAR, pair)
    gather.sent()


def gate_up(ids, sums, gain, x_in, a_all, b_all, w, side, scale, collective_id):
    _, seq_len, depth = x_in.shape
    share = w[0].shape[0]
    adapters, _, rank = w[4].shape
    half = (share + LANE - 1) // LANE * LANE
    hidden = (2, side, side * seq_len // 2, 2 * half)
    return pl.pallas_call(
        functools.partial(gate_up_kernel, side, adapters, scale),
        out_shape=[pltpu.VMEM(hidden, BF), pltpu.VMEM((seq_len, depth), BF), pltpu.VMEM((2 * half, depth + adapters * rank), BF)],
        in_specs=[SMEM] + [VMEM] * 2 + [HBM] * (3 + len(w)),
        out_specs=[VMEM] * 3,
        scratch_shapes=[
            pltpu.VMEM((2, side, side, 2, seq_len // 4, depth + 2 * rank), BF),
            pltpu.VMEM((2, half, depth), BF),
            pltpu.VMEM((2, depth, 2 * half), BF),
            pltpu.VMEM((2, 2 * half, adapters * rank), BF),
            pltpu.VMEM((seq_len, depth), BF),
            pltpu.VMEM(a_all.shape, BF),
            pltpu.VMEM(b_all.shape[:4] + b_all.shape[5:], BF),
            DMA((2,)), DMA, DMA, DMA, DMA,
        ] + GATHER_SEMS,
        compiler_params=comm_params(collective_id, VMEM_MOST * 51 // 64),
        name='gate_up',
    )(ids, sums, gain.reshape(1, depth), x_in, a_all, b_all, *w)


def deliver_kernel(side, adapters, scale, ids_ref, sums_ref, x_ref, b_all, out_ref, b_ref, b_sem, pair_send, pair_recv, send_sem, recv_sem):
    place = Place(side)
    place.announce(place.partner)
    b_load = ends([pltpu.make_async_copy(b_all.at[:, :, :, :, 1], b_ref, b_sem)])
    seq_len = sums_ref.shape[0]
    rows = seq_len // 4
    chosen = own_rows(place, ids_ref, (seq_len, b_ref.shape[4]))
    wait(b_load)
    y = finish(sums_ref, x_ref[...], b_ref, chosen, scale, adapters).astype(BF)
    for part in BOTH:
        for piece in BOTH:
            at = (2 * part + piece) * rows
            out_ref[place.device(0, 0), part, piece] = y[at:at + rows]
    place.meet()

    def block(part, ds, df):
        return out_ref.at[place.sequence(part, ds, df), part]

    def seen(part, ds, df, half):
        ref = block(part, ds, df) if half is None else block(part, ds, df).at[half]
        remote(ref, ref, pair_send, pair_recv, place.partner).start()

    for part in BOTH:
        seen(part, OWN, OWN, None)
    gather = Gather(place, block, send_sem, recv_sem, absolute=True, seen=seen)
    gather.own()
    gather.near()
    gather.row()
    gather.sides(*AWAY)
    gather.far(*RING)
    gather.sent()
    every = out_ref.at[first(side * side)]
    for sem in (pair_send, pair_recv):
        pltpu.make_async_copy(every, every, sem).wait()


def put_kernel(y_ref, out_ref, sem):
    wait(ends([pltpu.make_async_copy(y_ref.at[i], out_ref.at[i], sem) for i in range(y_ref.shape[0])]))


def deliver(ids, sums, x_mid, b_all, side, scale, collective_id):
    seq_len, depth = x_mid.shape
    rows = seq_len // 4
    y = pl.pallas_call(
        functools.partial(deliver_kernel, side, b_all.shape[1], scale),
        out_shape=pltpu.VMEM((2 * side * side, 2, 2, rows, depth), BF),
        in_specs=[SMEM] + [VMEM] * 2 + [HBM],
        scratch_shapes=[pltpu.VMEM(b_all.shape[:4] + b_all.shape[5:], BF), DMA, DMA, DMA] + GATHER_SEMS,
        compiler_params=comm_params(collective_id, VMEM_SMALL),
        name='deliver',
    )(ids, sums, x_mid, b_all)
    return pl.pallas_call(
        put_kernel,
        out_shape=jax.ShapeDtypeStruct(y.shape, BF),
        in_specs=[pl.BlockSpec(memory_space=pl.ANY)],
        out_specs=HBM,
        scratch_shapes=[DMA],
        compiler_params=pltpu.CompilerParams(vmem_limit_bytes=VMEM_LEAST),
        name='put',
    )(y)


def solution(mesh):
    tp_size = mesh.shape['tensor']
    side = math.isqrt(tp_size // 2)
    rows_only = P('tensor', None)
    head_split = P(None, 'tensor', None)
    last_split = P(None, None, 'tensor')
    b_head_split = P(None, None, 'tensor', None)
    in_specs = (P('data', None, None), P('data'), P(None), P(None),
                head_split, head_split, head_split, P('tensor', None, None),
                P(None, 'tensor'), P(None, 'tensor'), rows_only,
                last_split, b_head_split, last_split, b_head_split, last_split, b_head_split,
                P(None, 'tensor', None, None), last_split,
                last_split, last_split, last_split, last_split,
                head_split, last_split)

    def local_layer(x_in, adapter_ids, gain_attn, gain_mlp, w_q, w_k, w_v, w_o, w_gate, w_up, w_down, a_q, b_q, a_k, b_k, a_v, b_v, a_o, b_o, a_gate, b_gate, a_up, b_up, a_down, b_down):
        scale = ALPHA / b_q.shape[1]

        def across(a):
            return a.swapaxes(-1, -2)

        heads = [w[:, 0] for w in (w_q, w_k, w_v)] + [across(a) for a in (a_q, a_k, a_v)] + [b[:, :, 0] for b in (b_q, b_k, b_v)]
        given = [across(w_gate), across(w_up), across(b_gate), across(b_up), w_down, a_down]
        sums, all_a, all_b, *kept = attend(adapter_ids, x_in, gain_attn, heads, w_o[0], a_o[:, 0], (across(a_gate), across(a_up)), (b_o, b_down), given, side, scale, 0)
        w = [piece for pair in zip(given, kept) for piece in pair]
        hidden, x_mid, w_d = gate_up(adapter_ids, sums, gain_mlp, x_in, all_a, all_b, w, side, scale, 1)
        sums = row_proj(adapter_ids, hidden, w_d, *a_o.shape[::3], side, 2)
        y = deliver(adapter_ids, sums, x_mid, pltpu.with_memory_space_constraint(all_b, pltpu.HBM), side, scale, 3)
        return y.reshape(x_in.shape)

    return jax.shard_map(local_layer, mesh=mesh, in_specs=in_specs, out_specs=P('data', None, None), check_vma=False)
```

```python
import functools
import math

import jax
import jax.numpy as jnp
import numpy as np
from jax import lax
from jax.experimental import pallas as pl
from jax.experimental.pallas import tpu as pltpu
from jax.sharding import PartitionSpec as P

ALPHA = 16.0
ROPE_BASE = 10000.0
EPSILON = 1e-5
BF = jnp.bfloat16
F32 = jnp.float32
LANE = 128
TILE = 16
VMEM_MOST = 67043328
VMEM_SMALL = VMEM_MOST // 6
VMEM_LEAST = VMEM_MOST // 32
MESH = pl.DeviceIdType.MESH
HBM = pl.BlockSpec(memory_space=pltpu.HBM)
VMEM = pl.BlockSpec(memory_space=pltpu.VMEM)
SMEM = pl.BlockSpec(memory_space=pltpu.SMEM)
DMA = pltpu.SemaphoreType.DMA

OWN, NEXT, FAR, LAST = RING = range(4)
UP, DOWN = BOTH = range(2)
STEP = (NEXT, -NEXT)
FROM = (LAST, NEXT)
AWAY = (NEXT, LAST, FAR)
PAIRS = ((OWN, NEXT), (LAST, FAR))
TOWARD = (NEXT, LAST)
FAST, SLOW = BOTH


def fit(size, most):
    return max(c for c in range(LANE, most + 1, LANE) if size % c == 0)


def first(size):
    return pl.ds(0, size)


def dot(a, b):
    return jnp.dot(a, b, preferred_element_type=F32)


def dot_rows(a, b):
    return lax.dot_general(a, b, (((1,), (1,)), ((), ())), preferred_element_type=F32)


def dot_columns(a, b):
    return lax.dot_general(a, b, (((0,), (0,)), ((), ())), preferred_element_type=F32)


def normed(act, gain):
    return (act * lax.rsqrt(jnp.mean(act * act, axis=-1, keepdims=True) + EPSILON) * gain).astype(BF)


def ends(copies):
    for copy in copies:
        copy.start()
    return copies


def wait(copies):
    for copy in copies:
        copy.wait()


def loop(count, body):
    lax.fori_loop(0, count, lambda i, carry: (body(i), carry)[1], 0)


class Place:
    def __init__(self, side):
        index = lax.axis_index('tensor')
        self.side = side
        self.core = lax.rem(index, 2)
        chip = index // 2
        self.y, self.x = chip // side, lax.rem(chip, side)
        self.partner = index + 1 - 2 * self.core

    def turn(self, at, steps):
        return lax.rem(at + steps + self.side, self.side)

    def device(self, dy, dx):
        return (self.turn(self.y, dy) * self.side + self.turn(self.x, dx)) * 2 + self.core

    def neighbour(self, part, ring, step):
        return self.device(0, step) if part == ring else self.device(step, 0)

    def sequence(self, part, ds, df):
        return self.device(jnp.where(part == 0, ds, df), jnp.where(part == 0, df, ds))

    def announce(self, *more):
        to = [self.neighbour(0, ring, step) for ring in BOTH for step in STEP] + list(more)
        for device in to:
            pl.semaphore_signal(pltpu.get_barrier_semaphore(), inc=1, device_id={'tensor': device}, device_id_type=MESH)
        self.announced = len(to)

    def meet(self):
        pl.semaphore_wait(pltpu.get_barrier_semaphore(), self.announced)


def remote(src, dst, send_sem, recv_sem, to):
    return pltpu.make_async_remote_copy(src_ref=src, dst_ref=dst, send_sem=send_sem, recv_sem=recv_sem, device_id={'tensor': to}, device_id_type=MESH)


GATHER_SEMS = [DMA((2, 2, 2, 2, 4))] * 2


class Gather:
    def __init__(self, place, block, send_sem, recv_sem, absolute=False, seen=None):
        self.place, self.block, self.sems, self.absolute, self.seen = place, block, (send_sem, recv_sem), absolute, seen

    def message(self, part, ring, passed, d, j=OWN):
        spot = (lambda s: (s, j)) if ring == SLOW else (lambda s: (OWN, s))
        src, dst = (FROM[d], FAR) if passed else (OWN, FROM[d])
        a, b = self.block(part, *spot(src)), self.block(part, *spot(src if self.absolute else dst))
        if passed:
            a, b = a.at[d], b.at[d]
        return remote(a, b, *(sem.at[part, ring, passed, d, j] for sem in self.sems), self.place.neighbour(part, ring, STEP[d]))

    def arrived(self, part, ring, passed, d, j=OWN):
        self.message(part, ring, passed, d, j).wait_recv()
        if self.seen:
            at = FAR if passed else FROM[d]
            self.seen(part, *((at, j) if ring == SLOW else (OWN, at)), d if passed else None)

    def own(self):
        for ring in BOTH:
            for d in BOTH:
                for part in BOTH:
                    self.message(part, ring, 0, d).start()

    def near(self):
        for d in BOTH:
            for part in BOTH:
                self.arrived(part, FAST, 0, d)
                self.message(part, FAST, 1, d).start()
                for e in BOTH:
                    self.message(part, SLOW, 0, e, FROM[d]).start()

    def row(self):
        for part in BOTH:
            for d in BOTH:
                self.arrived(part, FAST, 1, d)
            for e in BOTH:
                self.message(part, SLOW, 0, e, FAR).start()
        self.sides(OWN)

    def sides(self, *blocks):
        for j in blocks:
            for part in BOTH:
                for d in BOTH:
                    self.arrived(part, SLOW, 0, d, j)
                    self.message(part, SLOW, 1, d, j).start()

    def far(self, *blocks):
        for j in blocks:
            for part in BOTH:
                for d in BOTH:
                    self.arrived(part, SLOW, 1, d, j)

    def sent(self):
        for part in BOTH:
            for d in BOTH:
                for passed in BOTH:
                    self.message(part, FAST, passed, d).wait_send()
                    for j in RING:
                        self.message(part, SLOW, passed, d, j).wait_send()


ROW_SEMS = [DMA((2, 2, 2, 2))] * 2


class RowGather:
    def __init__(self, place, row, mine, send_sem, recv_sem):
        self.place, self.row_at, self.mine, self.sems = place, row, mine, (send_sem, recv_sem)

    def message(self, part, ring, passed, d):
        if ring == SLOW:
            ref = self.row_at(part, FROM[d] if passed else OWN)
            ref = ref.at[:, d] if passed else ref
        else:
            ref = self.row_at(part, OWN).at[self.place.turn(self.mine(part), FROM[d] if passed else OWN)]
            ref = ref.at[d] if passed else ref
        return remote(ref, ref, *(sem.at[part, ring, passed, d] for sem in self.sems), self.place.neighbour(part, ring, STEP[d]))

    def pass_on(self, ring, passed):
        for part in BOTH:
            for d in BOTH:
                self.landing(part, ring, passed, d).wait_recv()
                if not passed:
                    self.message(part, ring, 1, d).start()
            if passed and ring == FAST:
                for d in BOTH:
                    self.message(part, SLOW, 0, d).start()

    def landing(self, part, ring, passed, d):
        at = FAR if passed else FROM[d]
        ref = self.row_at(part, at) if ring == SLOW else self.row_at(part, OWN).at[self.place.turn(self.mine(part), at)]
        if passed:
            ref = ref.at[:, d] if ring == SLOW else ref.at[d]
        return remote(ref, ref, *(sem.at[part, ring, passed, d] for sem in self.sems), self.place.neighbour(part, ring, STEP[d]))

    def own(self):
        for d in BOTH:
            for part in BOTH:
                self.message(part, FAST, 0, d).start()

    def near(self):
        self.pass_on(FAST, 0)

    def row(self):
        self.pass_on(FAST, 1)

    def sides(self):
        self.pass_on(SLOW, 0)

    def far(self):
        self.pass_on(SLOW, 1)

    def sent(self):
        for part in BOTH:
            for ring in BOTH:
                for passed in BOTH:
                    for d in BOTH:
                        self.message(part, ring, passed, d).wait_send()


def rows_of_adapter(place, ids_ref, part, ds, shape):
    block = lax.broadcasted_iota(jnp.int32, shape, 0) // (shape[0] // len(RING))
    chosen = jnp.zeros(shape, jnp.int32)
    for df in RING:
        chosen = jnp.where(block == df, ids_ref[place.sequence(part, ds, df)], chosen)
    return chosen


def pick_columns(low, chosen):
    rank = chosen.shape[1]
    kept = low[:, :rank]
    for a in range(1, low.shape[1] // rank):
        kept = jnp.where(chosen == a, low[:, a * rank:(a + 1) * rank], kept)
    return kept


def spread(low, chosen, adapters):
    return jnp.concatenate([jnp.where(chosen == a, low, 0.0) for a in range(adapters)], axis=1).astype(BF)


PASS, FREE, SUM = range(3)
FAST_SEMS = [DMA((2, 3, 2))] * 2


def add(into, *others):
    def some(i):
        at = pl.ds(pl.multiple_of(i * TILE, TILE), TILE)
        total = into[at, :].astype(F32)
        for other in others:
            total += other[at, :].astype(F32)
        into[at, :] = total.astype(BF)

    loop(into.shape[0] // TILE, some)


class FastScatter:
    def __init__(self, place, stage, near, landed, send_sem, recv_sem):
        self.place, self.stage, self.near, self.landed, self.sems = place, stage, near, landed, (send_sem, recv_sem)
        quarter = near.shape[2]
        self.halves = (first(quarter), pl.ds(quarter, quarter))

    def message(self, part, kind, d):
        at = self.halves[1 - d] if kind == FREE else self.halves[d]
        src = self.stage(part, FAR if kind == PASS else TOWARD[d]).at[at]
        dst = self.near.at[part, d] if kind == PASS else self.landed.at[part, d, at]
        sems = [sem.at[part, kind, d] for sem in self.sems]
        return remote(src, dst, *sems, self.place.neighbour(part, FAST, STEP[d]))

    def ready(self, part, df):
        for d in BOTH:
            if df == FAR:
                self.message(part, PASS, d).start()
            elif df == TOWARD[d]:
                self.message(part, FREE, d).start()

    def sum(self):
        for d in BOTH:
            for part in BOTH:
                self.message(part, PASS, d).wait_recv()
                add(self.stage(part, TOWARD[d]).at[self.halves[d]], self.near.at[part, d])
                self.message(part, SUM, d).start()

    def finish(self):
        for part in BOTH:
            for d in BOTH:
                self.message(part, FREE, d).wait_recv()
                self.message(part, SUM, d).wait_recv()
            add(self.stage(part, OWN), self.landed.at[part, UP], self.landed.at[part, DOWN])

    def store(self, out_ref):
        rows = self.landed.shape[2]
        for part in BOTH:
            out_ref[part * rows:(part + 1) * rows] = self.stage(part, OWN)[...]
        for part in BOTH:
            for kind in range(3):
                for d in BOTH:
                    self.message(part, kind, d).wait_send()


def fast_scratch(rows, cols):
    return [pltpu.VMEM((2, 2, rows // 2, cols), BF), pltpu.VMEM((2, 2, rows, cols), BF)]


def comm_params(collective_id, limit=VMEM_MOST):
    return pltpu.CompilerParams(collective_id=collective_id, has_side_effects=True, vmem_limit_bytes=limit)


WO_CHUNKS = 4


def attend_kernel(side, adapters, scale, ids_ref, x_ref, gain_ref, cos_ref, sin_ref, *rest):
    w_heads, a_heads, b_heads, (wo_ref, ao_ref), a_mlp, b_rows, rest = rest[:3], rest[3:6], rest[6:9], rest[9:11], rest[11:13], rest[13:15], rest[15:]
    (out_ref, a_all, b_all), rest = rest[:3], rest[3:]
    (w, a_raw, b_raw, a_rows, bx, xbuf, h, z, lows, att, act, wo, stage, near, landed, am_raw, a_mine, b_mine, pair_send, pair_recv, load_sem, x_sem, own_sem,
     wo_load, wo_send, wo_recv, bulk_send, bulk_recv, swap_send, swap_recv,
     send_sem, recv_sem, a_send, a_recv, b_send, b_recv, fast_send, fast_recv) = rest
    place = Place(side)
    place.announce(place.partner, place.device(0, FAR), place.device(FAR, 0))
    head, seq_len, depth = cos_ref.shape[1], x_ref.shape[1], x_ref.shape[2]
    cols = len(w_heads) * head
    chips = side * side
    per = a_raw.shape[3]
    half_depth = depth // 4
    loads = ends([pltpu.make_async_copy(src, dst, load_sem) for i in range(3) for src, dst in
                  ((a_heads[i], a_raw.at[place.core, i]), (w_heads[i], w.at[:, pl.ds(i * head, head)]), (b_heads[i], b_raw.at[0, i]))])
    steps = chips // 2

    def x_loads(step):
        slot = lax.rem(step, 2)
        return [pltpu.make_async_copy(x_ref.at[4 * lax.rem(step, steps) + 2 * i + place.core], xbuf.at[slot, i], x_sem.at[slot]) for i in BOTH]

    ends(x_loads(0))

    def every(ref):
        return lambda part, ds: ref.at[part, :, place.turn(place.x, ds)] if part else ref.at[part, place.turn(place.y, ds)]

    def spot_of(part):
        return place.y if part else place.x

    own_loads = ends([pltpu.make_async_copy(a_mlp[i], am_raw.at[i], own_sem) for i in BOTH] +
                     [pltpu.make_async_copy(b_rows[half].at[part], b_mine.at[part, place.y, place.x, half], own_sem) for part in BOTH for half in BOTH])
    width = wo_ref.shape[1]
    rank = ao_ref.shape[2]
    wo_loads = []
    for part in BOTH:
        wo_loads.append(pltpu.make_async_copy(wo_ref, wo.at[part, OWN, 0, :, first(width)], wo_load))
        for a in range(adapters):
            wo_loads.append(pltpu.make_async_copy(ao_ref.at[a], wo.at[part, OWN, 0, :, pl.ds(width + a * rank, rank)], wo_load))
    ends(wo_loads)
    wait(own_loads)
    wait(loads)
    am_rows = jnp.concatenate([am_raw[i, a] for i in BOTH for a in range(adapters)], axis=0)
    for part in BOTH:
        for half in BOTH:
            at = (2 * part + half) * half_depth
            a_mine[part, place.y, place.x, half] = am_rows[:, at:at + half_depth]
    place.meet()
    moves = [(a_raw.at[place.core], a_raw.at[place.core]), (w.at[:, first(cols)], w.at[:, pl.ds(cols, cols)]), (b_raw.at[0], b_raw.at[1])]
    pair = ends([remote(src, dst, pair_send.at[i], pair_recv.at[i], place.partner) for i, (src, dst) in enumerate(moves)])

    piece = head // WO_CHUNKS

    def wo_message(part, passed, d, i):
        src, dst = (wo.at[part, s, 0, pl.ds(i * piece, piece)] for s in ((FROM[d], FAR) if passed else (OWN, FROM[d])))
        sems = (part, passed, d, i)
        return remote(src, dst, wo_send.at[sems], wo_recv.at[sems], place.neighbour(part, SLOW, STEP[d]))

    def wo_to_partner(part, s):
        remote(wo.at[part, s, 0], wo.at[part, s, 1], bulk_send, bulk_recv, place.partner).start()

    passes = [range(d * WO_CHUNKS // 2, (d + 1) * WO_CHUNKS // 2) for d in BOTH]

    def wo_start(i):
        for d in BOTH:
            for part in BOTH:
                wo_message(part, 0, d, i).start()

    def wo_pass(k):
        for d in BOTH:
            for part in BOTH:
                wo_message(part, 0, d, passes[d][k]).wait_recv()
                wo_message(part, 1, d, passes[d][k]).start()

    def wo_arrived():
        for d in BOTH:
            for part in BOTH:
                for i in passes[1 - d]:
                    wo_message(part, 0, d, i).wait_recv()
                wo_to_partner(part, FROM[d])

    def wo_last():
        for part in BOTH:
            for d in BOTH:
                for i in passes[d]:
                    wo_message(part, 1, d, i).wait_recv()
            wo_to_partner(part, FAR)

    wait(wo_loads)
    early = WO_CHUNKS - 1
    for i in range(early):
        wo_start(i)
    gathers = [RowGather(place, every(a_mine), spot_of, a_send, a_recv), RowGather(place, every(b_mine), spot_of, b_send, b_recv)]

    def both(stage_of):
        for g in gathers:
            getattr(g, stage_of)()

    pair[0].wait_recv()
    for core in BOTH:
        pieces = [a_raw[core, i, a] if i < len(w_heads) else jnp.zeros((per, depth), BF) for a in range(adapters) for i in RING]
        a_rows[core * 2 * TILE:(core + 1) * 2 * TILE, :] = jnp.concatenate(pieces, axis=0)
    mine = [(place.y, place.x), (place.x, place.y)]

    low_gather = RowGather(place, lambda part, ds: lows.at[part, place.turn(mine[part][0], ds)], spot_of, send_sem, recv_sem)

    def norm(step, last):
        slot = lax.rem(step, 2)

        @pl.when(step + 1 < last)
        def _():
            ends(x_loads(step + 1))

        wait(x_loads(step))
        for i in BOTH:
            h[i * seq_len:(i + 1) * seq_len, :] = normed(xbuf[slot, i].astype(F32), gain_ref[...])

    def products(step):
        norm(step, 2 * steps)
        low = dot_rows(a_rows[...], h[...])
        half, at = step // (steps // 2), lax.rem(step, steps // 2) * 2 * seq_len
        for part in BOTH:
            pieces = []
            for i in BOTH:
                options = [low[TILE * (2 * part + a):TILE * (2 * part + a + 1), i * seq_len:(i + 1) * seq_len] for a in range(adapters)]
                chosen = options[0]
                for a in range(1, adapters):
                    chosen = jnp.where(ids_ref[4 * step + 2 * i + place.core] == a, options[a], chosen)
                pieces.append(chosen)
            lows[part, mine[part][0], mine[part][1], half, :, pl.ds(pl.multiple_of(at, LANE), 2 * seq_len)] = jnp.concatenate(pieces, axis=1).astype(BF)

    loop(steps, products)
    low_gather.own()
    for copy in pair[1:]:
        copy.wait_recv()
    for part in BOTH:
        wo_to_partner(part, OWN)
    events = {3: low_gather.near, 5: lambda: (low_gather.row(), wo_start(early))}

    def project(step):
        for at, what in events.items():
            pl.when(step == at)(lambda what=what: (what(), None)[1])
        norm(step + steps, 2 * steps)
        rows = pl.ds(pl.multiple_of(step * 2 * seq_len, LANE), 2 * seq_len)
        chunk = fit(2 * cols, 256)
        for n in range(2 * cols // chunk):
            z[rows, n * chunk:(n + 1) * chunk] = dot(h[...], w[:, n * chunk:(n + 1) * chunk])

    loop(steps, project)
    row, col = (lax.broadcasted_iota(jnp.int32, (2 * rank, rank), axis) for axis in BOTH)
    spot, kind = row // TILE, lax.rem(row, TILE) // per
    for part in BOTH:
        chip_of = spot if part == 0 else lax.rem(spot, side) * side + spot // side
        to = chip_of * 2 * per + part * per + lax.rem(row, per)
        for i in range(3):
            spread_rows = jnp.where((kind == i) & (col == to), 1.0, 0.0).astype(BF)
            for a in range(adapters):
                for o in BOTH:
                    bx[a, part, :, o * cols + i * head:o * cols + (i + 1) * head] = dot(spread_rows, b_raw[o, i, a]).astype(BF)
    low_gather.sides()
    wo_pass(0)
    low_gather.far()
    causal = lax.broadcasted_iota(jnp.int32, (seq_len, seq_len), 0) >= lax.broadcasted_iota(jnp.int32, (seq_len, seq_len), 1)

    def swap(part, ds):
        sems = (part, ds)
        to = place.neighbour(part, SLOW, ds)
        return remote(att.at[sems], act.at[part, lax.rem(len(RING) - ds, len(RING))], swap_send.at[sems], swap_recv.at[sems], to)

    def attention(i):
        dy, dx = side - 1 - i // side, side - 1 - lax.rem(i, side)
        chip = place.turn(place.y, dy) * side + place.turn(place.x, dx)
        adapter = ids_ref[2 * chip + place.core]
        half, at = chip // steps, pl.ds(pl.multiple_of(lax.rem(chip, steps) * seq_len, LANE), seq_len)
        zs = z[pl.ds(pl.multiple_of(chip * seq_len, LANE), seq_len), :]
        for part in BOTH:
            zs += scale * dot_columns(lows[part, :, :, half, :, at].reshape(-1, seq_len), bx[adapter, part])
        for i_head in BOTH:
            q, k, v = (zs[:, i_head * cols + i * head:i_head * cols + (i + 1) * head] for i in range(3))
            q, k = ((r * cos_ref[...] + pltpu.roll(r, head // 2, axis=1) * sin_ref[...]).astype(BF) for r in (q, k))
            scores = jnp.where(causal, dot_rows(q, k) * head ** -0.5, -1e30)
            e = jnp.exp(scores - jnp.max(scores, axis=-1, keepdims=True))
            prob = (e / jnp.sum(e, axis=-1, keepdims=True)).astype(BF)
            mixed = dot(prob, v.astype(BF)).astype(BF)
            for part, (ds, df) in enumerate(((dy, dx), (dx, dy))):
                att[part, ds, df, :, i_head * head:(i_head + 1) * head] = mixed[part * seq_len // 2:(part + 1) * seq_len // 2]

    def attention_pair(k):
        for i in BOTH:
            attention(2 * k + i)
        row = side - 1 - 2 * k // side
        pl.when((lax.rem(2 * k + 2, side) == 0) & (row != OWN))(lambda: swap(0, row).start())
        pl.when(k == 1)(lambda: wo_pass(1))

    loop(chips // 2, attention_pair)
    for ds in AWAY:
        swap(1, ds).start()
    wo_arrived()
    both('own')
    wo_last()
    for part in BOTH:
        act[part, OWN] = att[part, OWN]
    bulk = [remote(src, dst.at[place.core], pair_send.at[len(pair) + i], pair_recv.at[len(pair) + i], place.partner)
            for i, (src, dst) in enumerate(((a_mine, a_all), (b_mine, b_all)))]
    kept = [pltpu.make_async_copy(src, dst.at[place.core], load_sem) for src, dst in ((a_mine, a_all), (b_mine, b_all))]
    pltpu.make_async_copy(wo.at[:, :, 1], wo.at[:, :, 1], bulk_recv).wait()
    chunk = fit(width, 512)
    rows = seq_len // 2
    blocks = (len(RING), rows)
    fast = FastScatter(place, lambda part, df: stage.at[part, df], near, landed, fast_send, fast_recv)

    def sum_heads(part, at):
        return sum(dot(act[part, s].reshape(-1, 2 * head), wo[part, s, :, :, at].reshape(2 * head, -1)) for s in RING)

    for part in BOTH:
        for ds in AWAY:
            swap(part, ds).wait_recv()

        def columns(n):
            at = pl.ds(pl.multiple_of(n * chunk, chunk), chunk)
            stage[part, :, :, at] = sum_heads(part, at).reshape(blocks + (chunk,)).astype(BF)

        loop(width // chunk, columns)
        chosen = rows_of_adapter(place, ids_ref, part, OWN, (len(RING) * rows, rank))
        stage[part, :, :, width:] = pick_columns(sum_heads(part, pl.ds(width, adapters * rank)), chosen).reshape(blocks + (rank,)).astype(BF)
        for df in (FAR, NEXT, LAST):
            fast.ready(part, df)
        both(('near', 'row')[part])
    both('sides')
    fast.sum()
    both('far')
    ends(bulk)
    ends(kept)
    fast.finish()
    fast.store(out_ref)
    wait(kept)
    for copy in bulk:
        copy.wait_recv()
    for copy in pair + bulk:
        copy.wait_send()
    for g in gathers + [low_gather]:
        g.sent()
    pltpu.make_async_copy(wo.at[:, :, 1], wo.at[:, :, 1], bulk_send).wait()
    for part in BOTH:
        for d in BOTH:
            for i in range(WO_CHUNKS):
                wo_message(part, 0, d, i).wait_send()
            for i in passes[d]:
                wo_message(part, 1, d, i).wait_send()
        for ds in AWAY:
            swap(part, ds).wait_send()


def attend(ids, x_in, gain, heads, w_o, a_o, a_mlp, b_rows, side, scale, collective_id):
    _, seq_len, depth = x_in.shape
    head = heads[0].shape[1]
    cols = 3 * head
    adapters, _, rank = a_o.shape
    per = a_mlp[0].shape[1]
    chips = side * side
    half_dim = head // 2
    inv_freq = ROPE_BASE ** (-2.0 * np.arange(half_dim) / head)
    angle = np.arange(seq_len)[:, None] * inv_freq[None, :]
    cos, sin = np.cos(angle), np.sin(angle)
    tables = [jnp.asarray(np.concatenate(pair, axis=1), F32) for pair in ((cos, cos), (-sin, sin))]
    n_pair = 3 + 2
    rows, out_cols = seq_len // 2, depth + rank
    every = (2, 2, side, side, 2)
    return pl.pallas_call(
        functools.partial(attend_kernel, side, adapters, scale),
        out_shape=[jax.ShapeDtypeStruct((seq_len, out_cols), BF), jax.ShapeDtypeStruct(every + (2 * adapters * per, depth // 4), BF),
                   jax.ShapeDtypeStruct(every + b_rows[0].shape[1:], BF)],
        in_specs=[SMEM, HBM, VMEM, VMEM, VMEM] + [HBM] * (len(heads) + 6),
        out_specs=[VMEM] + [HBM] * 2,
        scratch_shapes=[
            pltpu.VMEM((depth, 2 * cols), BF),
            pltpu.VMEM((2, 3, adapters, per, depth), BF),
            pltpu.VMEM((2, 3, adapters, rank, head), BF),
            pltpu.VMEM((2 * 2 * TILE, depth), BF),
            pltpu.VMEM((adapters, 2, 2 * rank, 2 * cols), BF),
            pltpu.VMEM((2, 2, seq_len, depth), BF),
            pltpu.VMEM((2 * seq_len, depth), BF),
            pltpu.VMEM((chips * seq_len, 2 * cols), F32),
            pltpu.VMEM((2, side, side, 2, TILE, chips * seq_len // 2), BF),
            pltpu.VMEM((2, side, side, rows, 2 * head), BF),
            pltpu.VMEM((2, side, side, rows, 2 * head), BF),
            pltpu.VMEM((2, side, 2, head, depth + adapters * rank), BF),
            pltpu.VMEM((2, side, rows, out_cols), BF),
        ] + fast_scratch(rows, out_cols) + [
            pltpu.VMEM((2, adapters, per, depth), BF),
            pltpu.VMEM(every[1:] + (2 * adapters * per, depth // 4), BF),
            pltpu.VMEM(every[1:] + b_rows[0].shape[1:], BF),
            DMA((n_pair,)), DMA((n_pair,)), DMA, DMA((2,)), DMA, DMA, DMA((2, 2, 2, WO_CHUNKS)), DMA((2, 2, 2, WO_CHUNKS)), DMA, DMA, DMA((2, 4)), DMA((2, 4)),
        ] + ROW_SEMS * 3 + FAST_SEMS,
        compiler_params=comm_params(collective_id),
        name='attend',
    )(ids, x_in, gain.reshape(1, depth), *tables, *heads, w_o, a_o, *a_mlp, *b_rows)


def row_proj_kernel(side, adapters, rank, ids_ref, act, w, out_ref, stage, near, landed, fast_near, fast_landed, slow_send, slow_recv, fast_send, fast_recv):
    place = Place(side)
    place.announce()
    rows, cols = stage.shape[3:]
    quarter = rows // 2
    width = cols - rank
    chunk = fit(width, 512)

    def unit(part, ds):
        def columns(n):
            at = pl.ds(pl.multiple_of(n * chunk, chunk), chunk)
            stage[part, ds, :, :, at] = dot(act[part, ds], w[:, at]).reshape(len(RING), rows, chunk).astype(BF)

        loop(width // chunk, columns)
        chosen = rows_of_adapter(place, ids_ref, part, ds, (len(RING) * rows, rank))
        stage[part, ds, :, :, width:] = pick_columns(dot(act[part, ds], w[:, width:]), chosen).reshape(len(RING), rows, rank).astype(BF)

    blocks = ((FAR, LAST), (OWN, NEXT))

    def slow(part, kind, d, i):
        df = blocks[1 - d][i] if kind == FREE else blocks[d][i]
        sems = (part, kind, d, i)
        src = stage.at[part, FAR if kind == PASS else TOWARD[d], df]
        dst = near.at[part, d, i] if kind == PASS else landed.at[part, d, df]
        return remote(src, dst, slow_send.at[sems], slow_recv.at[sems], place.neighbour(part, SLOW, STEP[d]))

    fast = FastScatter(place, lambda part, df: stage.at[part, OWN, df], fast_near, fast_landed, fast_send, fast_recv)
    for part in BOTH:
        unit(part, FAR)
        if part == 0:
            place.meet()
        for i in BOTH:
            for d in BOTH:
                slow(part, PASS, d, i).start()
    loop(len(RING), lambda i: unit(lax.rem(i, 2), NEXT + 2 * (i // 2)))
    for i in BOTH:
        for d in BOTH:
            for part in BOTH:
                slow(part, FREE, d, i).start()
    loop(2, lambda part: unit(part, OWN))
    for i in BOTH:
        for d in BOTH:
            for part in BOTH:
                slow(part, PASS, d, i).wait_recv()
                add(stage.at[part, TOWARD[d], blocks[d][i]], near.at[part, d, i])
                slow(part, SUM, d, i).start()
    for i in BOTH:
        for d in BOTH:
            df = blocks[d][i]
            for part in BOTH:
                slow(part, SUM, d, i).wait_recv()
                slow(part, FREE, 1 - d, i).wait_recv()
                add(stage.at[part, OWN, df], landed.at[part, UP, df], landed.at[part, DOWN, df])
                fast.ready(part, df)
    fast.sum()
    fast.finish()
    fast.store(out_ref)
    for part in BOTH:
        for kind in range(3):
            for d in BOTH:
                for i in BOTH:
                    slow(part, kind, d, i).wait_send()


def row_proj(ids, act, w, adapters, rank, side, collective_id):
    rows = act.shape[2] // side
    cols = w.shape[1] - (adapters - 1) * rank
    blocks = (rows, cols)
    return pl.pallas_call(
        functools.partial(row_proj_kernel, side, adapters, rank),
        out_shape=pltpu.VMEM((2 * rows, cols), BF),
        in_specs=[SMEM, VMEM, VMEM],
        out_specs=VMEM,
        scratch_shapes=[
            pltpu.VMEM((2, side, side) + blocks, BF),
            pltpu.VMEM((2, 2, 2) + blocks, BF),
            pltpu.VMEM((2, 2, side) + blocks, BF),
        ] + fast_scratch(rows, cols) + [DMA((2, 3, 2, 2))] * 2 + FAST_SEMS,
        compiler_params=comm_params(collective_id, VMEM_MOST * 5 // 8),
        name='row_proj',
    )(ids, act, w)


def finish(sums_ref, resid, b_ref, chosen, scale, adapters):
    _, _, side, _, rank, part = b_ref.shape
    width = sums_ref.shape[1] - rank
    low = spread(sums_ref[:, width:].astype(F32), chosen, adapters)
    delta = [dot(low, b_ref[core, :, y, x].reshape(adapters * rank, part)) for y in range(side) for x in range(side) for core in BOTH]
    return resid.astype(F32) + (sums_ref[:, :width].astype(F32) + scale * jnp.concatenate(delta, axis=1))


def own_rows(place, ids_ref, shape):
    return jnp.full(shape, ids_ref[place.device(0, 0)], jnp.int32)


def gate_up_kernel(side, adapters, scale, ids_ref, sums_ref, gain_ref, x_all, a_all, b_all, wg_ref, wu_ref, bg_ref, bu_ref, wd_ref, ad_ref,
                   hid, mid_ref, wd, gbuf, raw, w, b, x_ref, a_ref, b_ref, raw_sem, load_sem, a_sem, b_sem, credit, pair_send, pair_recv, send_sem, recv_sem):
    place = Place(side)
    share, width = wg_ref.shape
    half = raw.shape[1]
    rank = bg_ref.shape[2]
    seq_len = sums_ref.shape[0]
    edge = share // TILE * TILE
    for i in BOTH:
        raw[i, edge:] = jnp.zeros((half - edge, width), BF)
        for kind in BOTH:
            b[kind, i * half + edge:(i + 1) * half] = jnp.zeros((half - edge, adapters * rank), BF)
        wd[i * half + edge:(i + 1) * half] = jnp.zeros((half - edge, wd.shape[1]), BF)
    place.announce(place.partner)
    b_load = ends([pltpu.make_async_copy(b_all.at[:, :, :, :, 0], b_ref, b_sem), pltpu.make_async_copy(x_all.at[place.device(0, 0)], x_ref, b_sem)])
    a_load = ends([pltpu.make_async_copy(a_all, a_ref, a_sem)])
    mine = first(share)

    def raw_load(kind):
        return pltpu.make_async_copy((wg_ref, wu_ref)[kind], raw.at[0, mine], raw_sem)

    raw_load(0).start()
    loads = [pltpu.make_async_copy(wd_ref, wd.at[mine, first(width)], load_sem)]
    for a in range(adapters):
        loads.append(pltpu.make_async_copy(ad_ref.at[a], wd.at[mine, pl.ds(width + a * rank, rank)], load_sem))
        for kind, ref in enumerate((bg_ref, bu_ref)):
            loads.append(pltpu.make_async_copy(ref.at[a], b.at[kind, mine, pl.ds(a * rank, rank)], load_sem))
    ends(loads)
    other = pl.ds(half, share)
    moves = [(raw.at[0, mine], raw.at[1, mine])] * 2 + [(wd.at[mine], wd.at[other])] + [(b.at[kind, mine], b.at[kind, other]) for kind in BOTH]
    pair = [remote(src, dst, pair_send.at[i], pair_recv.at[i], place.partner) for i, (src, dst) in enumerate(moves)]
    rows = seq_len // 4
    chosen = own_rows(place, ids_ref, (seq_len, rank))
    wait(b_load)
    mid = finish(sums_ref, x_ref[...], b_ref, chosen, scale, adapters).astype(BF)
    mid_ref[...] = mid
    h2 = normed(mid.astype(F32), gain_ref[...])
    lows = []
    wait(a_load)
    for core in BOTH:
        pieces = [dot_rows(h2[:, i * width // 4:(i + 1) * width // 4], a_ref[core, i // 2, :, :, i % 2].reshape(-1, width // 4)) for i in RING]
        lows.append(sum(pieces).astype(BF))
    low = jnp.concatenate(lows, axis=1)
    per = rank // (2 * side * side)
    row, col = (lax.broadcasted_iota(jnp.int32, (low.shape[1], 2 * rank), axis) for axis in BOTH)
    kind, rank_at = col // rank, lax.rem(col, rank)
    chip, core = rank_at // (2 * per), lax.rem(rank_at // per, 2)
    pick = ((core * side * side + chip) * 2 + kind) * adapters * per + ids_ref[place.device(0, 0)] * per + lax.rem(rank_at, per)
    low = dot(low, jnp.where(row == pick, 1.0, 0.0).astype(BF)).astype(BF)
    for part in BOTH:
        for piece in BOTH:
            at = (2 * part + piece) * rows
            gbuf[part, OWN, OWN, piece, :, :width] = h2[at:at + rows]
            gbuf[part, OWN, OWN, piece, :, width:] = low[at:at + rows]
    place.meet()
    chunk = fit(2 * half, 256)

    def unit(ds, blocks=RING):
        lo, hi = min(blocks), max(blocks) + 1
        unit_rows = (hi - lo) * 2 * rows
        low = gbuf[:, ds, lo:hi, :, :, width:].reshape(2 * unit_rows, 2 * rank).astype(F32)
        chosen = jnp.concatenate([rows_of_adapter(place, ids_ref, part, ds, (len(RING) * 2 * rows, rank))[lo * 2 * rows:hi * 2 * rows] for part in BOTH], axis=0)
        lows = [spread(low[:, kind * rank:(kind + 1) * rank], chosen, adapters) for kind in BOTH]

        def columns(n):
            at = pl.ds(pl.multiple_of(n * chunk, chunk), chunk)
            act = gbuf[:, ds, lo:hi, :, :, :width].reshape(2 * unit_rows, width)
            gate, up = (dot(act, w[kind, :, at]) + scale * dot_rows(lows[kind], b[kind, at]) for kind in BOTH)
            hid[:, ds, lo * 2 * rows:hi * 2 * rows, at] = (gate * jax.nn.sigmoid(gate) * up).astype(BF).reshape(2, unit_rows, chunk)

        loop(2 * half // chunk, columns)

    gather = Gather(place, lambda part, ds, df: gbuf.at[part, ds, df], send_sem, recv_sem)
    gather.own()
    def turned(kind, i):
        def turn(n):
            at = pl.ds(pl.multiple_of(n * LANE, LANE), LANE)
            w[kind, at, i * half:(i + 1) * half] = raw[i, :, at].T

        loop(width // LANE, turn)

    for kind in BOTH:
        raw_load(kind).wait()
        if kind:
            pl.semaphore_wait(credit, 1)
        pair[kind].start()
        turned(kind, 0)
        if kind == 0:
            wait(loads)
            ends(pair[2:])
        pair[kind].wait_recv()
        turned(kind, 1)
        pair[kind].wait_send()
        if kind == 0:
            pl.semaphore_signal(credit, inc=1, device_id={'tensor': place.partner}, device_id_type=MESH)
            raw_load(1).start()
    gather.near()
    gather.row()
    for copy in pair[2:]:
        copy.wait_recv()
    unit(OWN)
    gather.sides(*AWAY)
    loop(2, lambda i: unit(NEXT + 2 * i))
    for blocks in PAIRS:
        gather.far(*blocks)
        unit(FAR, blocks)
    gather.sent()
    for copy in pair[2:]:
        copy.wait_send()


def gate_up(ids, sums, gain, x_in, a_all, b_all, w, side, scale, collective_id):
    _, seq_len, depth = x_in.shape
    share = w[0].shape[0]
    adapters, _, rank = w[2].shape
    half = (share + LANE - 1) // LANE * LANE
    hidden = (2, side, side * seq_len // 2, 2 * half)
    return pl.pallas_call(
        functools.partial(gate_up_kernel, side, adapters, scale),
        out_shape=[pltpu.VMEM(hidden, BF), pltpu.VMEM((seq_len, depth), BF), pltpu.VMEM((2 * half, depth + adapters * rank), BF)],
        in_specs=[SMEM] + [VMEM] * 2 + [HBM] * (3 + len(w)),
        out_specs=[VMEM] * 3,
        scratch_shapes=[
            pltpu.VMEM((2, side, side, 2, seq_len // 4, depth + 2 * rank), BF),
            pltpu.VMEM((2, half, depth), BF),
            pltpu.VMEM((2, depth, 2 * half), BF),
            pltpu.VMEM((2, 2 * half, adapters * rank), BF),
            pltpu.VMEM((seq_len, depth), BF),
            pltpu.VMEM(a_all.shape, BF),
            pltpu.VMEM(b_all.shape[:4] + b_all.shape[5:], BF),
            DMA, DMA, DMA, DMA, pltpu.SemaphoreType.REGULAR, DMA((5,)), DMA((5,)),
        ] + GATHER_SEMS,
        compiler_params=comm_params(collective_id, VMEM_MOST * 51 // 64),
        name='gate_up',
    )(ids, sums, gain.reshape(1, depth), x_in, a_all, b_all, *w)


def deliver_kernel(side, adapters, scale, ids_ref, sums_ref, x_ref, b_all, out_ref, b_ref, b_sem, pair_send, pair_recv, send_sem, recv_sem):
    place = Place(side)
    place.announce(place.partner)
    b_load = ends([pltpu.make_async_copy(b_all.at[:, :, :, :, 1], b_ref, b_sem)])
    seq_len = sums_ref.shape[0]
    rows = seq_len // 4
    chosen = own_rows(place, ids_ref, (seq_len, b_ref.shape[4]))
    wait(b_load)
    y = finish(sums_ref, x_ref[...], b_ref, chosen, scale, adapters).astype(BF)
    for part in BOTH:
        for piece in BOTH:
            at = (2 * part + piece) * rows
            out_ref[place.device(0, 0), part, piece] = y[at:at + rows]
    place.meet()

    def block(part, ds, df):
        return out_ref.at[place.sequence(part, ds, df), part]

    def seen(part, ds, df, half):
        ref = block(part, ds, df) if half is None else block(part, ds, df).at[half]
        remote(ref, ref, pair_send, pair_recv, place.partner).start()

    for part in BOTH:
        seen(part, OWN, OWN, None)
    gather = Gather(place, block, send_sem, recv_sem, absolute=True, seen=seen)
    gather.own()
    gather.near()
    gather.row()
    gather.sides(*AWAY)
    gather.far(*RING)
    gather.sent()
    every = out_ref.at[first(side * side)]
    for sem in (pair_send, pair_recv):
        pltpu.make_async_copy(every, every, sem).wait()


def put_kernel(y_ref, out_ref, sem):
    wait(ends([pltpu.make_async_copy(y_ref.at[i], out_ref.at[i], sem) for i in range(y_ref.shape[0])]))


def deliver(ids, sums, x_mid, b_all, side, scale, collective_id):
    seq_len, depth = x_mid.shape
    rows = seq_len // 4
    y = pl.pallas_call(
        functools.partial(deliver_kernel, side, b_all.shape[1], scale),
        out_shape=pltpu.VMEM((2 * side * side, 2, 2, rows, depth), BF),
        in_specs=[SMEM] + [VMEM] * 2 + [HBM],
        scratch_shapes=[pltpu.VMEM(b_all.shape[:4] + b_all.shape[5:], BF), DMA, DMA, DMA] + GATHER_SEMS,
        compiler_params=comm_params(collective_id, VMEM_SMALL),
        name='deliver',
    )(ids, sums, x_mid, b_all)
    return pl.pallas_call(
        put_kernel,
        out_shape=jax.ShapeDtypeStruct(y.shape, BF),
        in_specs=[pl.BlockSpec(memory_space=pl.ANY)],
        out_specs=HBM,
        scratch_shapes=[DMA],
        compiler_params=pltpu.CompilerParams(vmem_limit_bytes=VMEM_LEAST),
        name='put',
    )(y)


def solution(mesh):
    tp_size = mesh.shape['tensor']
    side = math.isqrt(tp_size // 2)
    rows_only = P('tensor', None)
    head_split = P(None, 'tensor', None)
    last_split = P(None, None, 'tensor')
    b_head_split = P(None, None, 'tensor', None)
    in_specs = (P('data', None, None), P('data'), P(None), P(None),
                head_split, head_split, head_split, P('tensor', None, None),
                P(None, 'tensor'), P(None, 'tensor'), rows_only,
                last_split, b_head_split, last_split, b_head_split, last_split, b_head_split,
                P(None, 'tensor', None, None), last_split,
                last_split, last_split, last_split, last_split,
                head_split, last_split)

    def local_layer(x_in, adapter_ids, gain_attn, gain_mlp, w_q, w_k, w_v, w_o, w_gate, w_up, w_down, a_q, b_q, a_k, b_k, a_v, b_v, a_o, b_o, a_gate, b_gate, a_up, b_up, a_down, b_down):
        scale = ALPHA / b_q.shape[1]

        def across(a):
            return a.swapaxes(-1, -2)

        heads = [w[:, 0] for w in (w_q, w_k, w_v)] + [across(a) for a in (a_q, a_k, a_v)] + [b[:, :, 0] for b in (b_q, b_k, b_v)]
        sums, all_a, all_b = attend(adapter_ids, x_in, gain_attn, heads, w_o[0], a_o[:, 0], (across(a_gate), across(a_up)), (b_o, b_down), side, scale, 0)

        w = [across(w_gate), across(w_up), across(b_gate), across(b_up), w_down, a_down]
        hidden, x_mid, w_d = gate_up(adapter_ids, sums, gain_mlp, x_in, all_a, all_b, w, side, scale, 1)
        sums = row_proj(adapter_ids, hidden, w_d, *a_o.shape[::3], side, 2)
        y = deliver(adapter_ids, sums, x_mid, pltpu.with_memory_space_constraint(all_b, pltpu.HBM), side, scale, 3)
        return y.reshape(x_in.shape)

    return jax.shard_map(local_layer, mesh=mesh, in_specs=in_specs, out_specs=P('data', None, None), check_vma=False)
```

```python
import functools
import math

import jax
import jax.numpy as jnp
import numpy as np
from jax import lax
from jax.experimental import pallas as pl
from jax.experimental.pallas import tpu as pltpu
from jax.sharding import PartitionSpec as P

ALPHA = 16.0
ROPE_BASE = 10000.0
EPSILON = 1e-5
BF = jnp.bfloat16
F32 = jnp.float32
LANE = 128
TILE = 16
VMEM_MOST = 67043328
VMEM_SMALL = VMEM_MOST // 6
VMEM_LEAST = VMEM_MOST // 32
MESH = pl.DeviceIdType.MESH
HBM = pl.BlockSpec(memory_space=pltpu.HBM)
VMEM = pl.BlockSpec(memory_space=pltpu.VMEM)
SMEM = pl.BlockSpec(memory_space=pltpu.SMEM)
DMA = pltpu.SemaphoreType.DMA

OWN, NEXT, FAR, LAST = RING = range(4)
UP, DOWN = BOTH = range(2)
STEP = (NEXT, -NEXT)
FROM = (LAST, NEXT)
AWAY = (NEXT, LAST, FAR)
PAIRS = ((OWN, NEXT), (LAST, FAR))
TOWARD = (NEXT, LAST)
FAST, SLOW = BOTH


def fit(size, most):
    return max(c for c in range(LANE, most + 1, LANE) if size % c == 0)


def first(size):
    return pl.ds(0, size)


def dot(a, b):
    return jnp.dot(a, b, preferred_element_type=F32)


def dot_rows(a, b):
    return lax.dot_general(a, b, (((1,), (1,)), ((), ())), preferred_element_type=F32)


def dot_columns(a, b):
    return lax.dot_general(a, b, (((0,), (0,)), ((), ())), preferred_element_type=F32)


def normed(act, gain):
    return (act * lax.rsqrt(jnp.mean(act * act, axis=-1, keepdims=True) + EPSILON) * gain).astype(BF)


def ends(copies):
    for copy in copies:
        copy.start()
    return copies


def wait(copies):
    for copy in copies:
        copy.wait()


def loop(count, body):
    lax.fori_loop(0, count, lambda i, carry: (body(i), carry)[1], 0)


class Place:
    def __init__(self, side):
        index = lax.axis_index('tensor')
        self.side = side
        self.core = lax.rem(index, 2)
        chip = index // 2
        self.y, self.x = chip // side, lax.rem(chip, side)
        self.partner = index + 1 - 2 * self.core

    def turn(self, at, steps):
        return lax.rem(at + steps + self.side, self.side)

    def device(self, dy, dx):
        return (self.turn(self.y, dy) * self.side + self.turn(self.x, dx)) * 2 + self.core

    def neighbour(self, part, ring, step):
        return self.device(0, step) if part == ring else self.device(step, 0)

    def sequence(self, part, ds, df):
        return self.device(jnp.where(part == 0, ds, df), jnp.where(part == 0, df, ds))

    def announce(self, *more):
        to = [self.neighbour(0, ring, step) for ring in BOTH for step in STEP] + list(more)
        for device in to:
            pl.semaphore_signal(pltpu.get_barrier_semaphore(), inc=1, device_id={'tensor': device}, device_id_type=MESH)
        self.announced = len(to)

    def meet(self):
        pl.semaphore_wait(pltpu.get_barrier_semaphore(), self.announced)


def remote(src, dst, send_sem, recv_sem, to):
    return pltpu.make_async_remote_copy(src_ref=src, dst_ref=dst, send_sem=send_sem, recv_sem=recv_sem, device_id={'tensor': to}, device_id_type=MESH)


GATHER_SEMS = [DMA((2, 2, 2, 2, 4))] * 2


class Gather:
    def __init__(self, place, block, send_sem, recv_sem, absolute=False, seen=None):
        self.place, self.block, self.sems, self.absolute, self.seen = place, block, (send_sem, recv_sem), absolute, seen

    def message(self, part, ring, passed, d, j=OWN):
        spot = (lambda s: (s, j)) if ring == SLOW else (lambda s: (OWN, s))
        src, dst = (FROM[d], FAR) if passed else (OWN, FROM[d])
        a, b = self.block(part, *spot(src)), self.block(part, *spot(src if self.absolute else dst))
        if passed:
            a, b = a.at[d], b.at[d]
        return remote(a, b, *(sem.at[part, ring, passed, d, j] for sem in self.sems), self.place.neighbour(part, ring, STEP[d]))

    def arrived(self, part, ring, passed, d, j=OWN):
        self.message(part, ring, passed, d, j).wait_recv()
        if self.seen:
            at = FAR if passed else FROM[d]
            self.seen(part, *((at, j) if ring == SLOW else (OWN, at)), d if passed else None)

    def own(self):
        for ring in BOTH:
            for d in BOTH:
                for part in BOTH:
                    self.message(part, ring, 0, d).start()

    def near(self):
        for d in BOTH:
            for part in BOTH:
                self.arrived(part, FAST, 0, d)
                self.message(part, FAST, 1, d).start()
                for e in BOTH:
                    self.message(part, SLOW, 0, e, FROM[d]).start()

    def row(self):
        for part in BOTH:
            for d in BOTH:
                self.arrived(part, FAST, 1, d)
            for e in BOTH:
                self.message(part, SLOW, 0, e, FAR).start()
        self.sides(OWN)

    def sides(self, *blocks):
        for j in blocks:
            for part in BOTH:
                for d in BOTH:
                    self.arrived(part, SLOW, 0, d, j)
                    self.message(part, SLOW, 1, d, j).start()

    def far(self, *blocks):
        for j in blocks:
            for part in BOTH:
                for d in BOTH:
                    self.arrived(part, SLOW, 1, d, j)

    def sent(self):
        for part in BOTH:
            for d in BOTH:
                for passed in BOTH:
                    self.message(part, FAST, passed, d).wait_send()
                    for j in RING:
                        self.message(part, SLOW, passed, d, j).wait_send()


ROW_SEMS = [DMA((2, 2, 2, 2))] * 2


class RowGather:
    def __init__(self, place, row, mine, send_sem, recv_sem):
        self.place, self.row_at, self.mine, self.sems = place, row, mine, (send_sem, recv_sem)

    def message(self, part, ring, passed, d):
        if ring == SLOW:
            ref = self.row_at(part, FROM[d] if passed else OWN)
            ref = ref.at[:, d] if passed else ref
        else:
            ref = self.row_at(part, OWN).at[self.place.turn(self.mine(part), FROM[d] if passed else OWN)]
            ref = ref.at[d] if passed else ref
        return remote(ref, ref, *(sem.at[part, ring, passed, d] for sem in self.sems), self.place.neighbour(part, ring, STEP[d]))

    def pass_on(self, ring, passed):
        for part in BOTH:
            for d in BOTH:
                self.landing(part, ring, passed, d).wait_recv()
                if not passed:
                    self.message(part, ring, 1, d).start()
            if passed and ring == FAST:
                for d in BOTH:
                    self.message(part, SLOW, 0, d).start()

    def landing(self, part, ring, passed, d):
        at = FAR if passed else FROM[d]
        ref = self.row_at(part, at) if ring == SLOW else self.row_at(part, OWN).at[self.place.turn(self.mine(part), at)]
        if passed:
            ref = ref.at[:, d] if ring == SLOW else ref.at[d]
        return remote(ref, ref, *(sem.at[part, ring, passed, d] for sem in self.sems), self.place.neighbour(part, ring, STEP[d]))

    def own(self):
        for d in BOTH:
            for part in BOTH:
                self.message(part, FAST, 0, d).start()

    def near(self):
        self.pass_on(FAST, 0)

    def row(self):
        self.pass_on(FAST, 1)

    def sides(self):
        self.pass_on(SLOW, 0)

    def far(self):
        self.pass_on(SLOW, 1)

    def sent(self):
        for part in BOTH:
            for ring in BOTH:
                for passed in BOTH:
                    for d in BOTH:
                        self.message(part, ring, passed, d).wait_send()


def rows_of_adapter(place, ids_ref, part, ds, shape):
    block = lax.broadcasted_iota(jnp.int32, shape, 0) // (shape[0] // len(RING))
    chosen = jnp.zeros(shape, jnp.int32)
    for df in RING:
        chosen = jnp.where(block == df, ids_ref[place.sequence(part, ds, df)], chosen)
    return chosen


def pick_columns(low, chosen):
    rank = chosen.shape[1]
    kept = low[:, :rank]
    for a in range(1, low.shape[1] // rank):
        kept = jnp.where(chosen == a, low[:, a * rank:(a + 1) * rank], kept)
    return kept


def spread(low, chosen, adapters):
    return jnp.concatenate([jnp.where(chosen == a, low, 0.0) for a in range(adapters)], axis=1).astype(BF)


PASS, FREE, SUM = range(3)
FAST_SEMS = [DMA((2, 3, 2))] * 2


def add(into, *others):
    def some(i):
        at = pl.ds(pl.multiple_of(i * TILE, TILE), TILE)
        total = into[at, :].astype(F32)
        for other in others:
            total += other[at, :].astype(F32)
        into[at, :] = total.astype(BF)

    loop(into.shape[0] // TILE, some)


class FastScatter:
    def __init__(self, place, stage, near, landed, send_sem, recv_sem):
        self.place, self.stage, self.near, self.landed, self.sems = place, stage, near, landed, (send_sem, recv_sem)
        quarter = near.shape[2]
        self.halves = (first(quarter), pl.ds(quarter, quarter))

    def message(self, part, kind, d):
        at = self.halves[1 - d] if kind == FREE else self.halves[d]
        src = self.stage(part, FAR if kind == PASS else TOWARD[d]).at[at]
        dst = self.near.at[part, d] if kind == PASS else self.landed.at[part, d, at]
        sems = [sem.at[part, kind, d] for sem in self.sems]
        return remote(src, dst, *sems, self.place.neighbour(part, FAST, STEP[d]))

    def ready(self, part, df):
        for d in BOTH:
            if df == FAR:
                self.message(part, PASS, d).start()
            elif df == TOWARD[d]:
                self.message(part, FREE, d).start()

    def sum(self):
        for d in BOTH:
            for part in BOTH:
                self.message(part, PASS, d).wait_recv()
                add(self.stage(part, TOWARD[d]).at[self.halves[d]], self.near.at[part, d])
                self.message(part, SUM, d).start()

    def finish(self):
        for part in BOTH:
            for d in BOTH:
                self.message(part, FREE, d).wait_recv()
                self.message(part, SUM, d).wait_recv()
            add(self.stage(part, OWN), self.landed.at[part, UP], self.landed.at[part, DOWN])

    def store(self, out_ref):
        rows = self.landed.shape[2]
        for part in BOTH:
            out_ref[part * rows:(part + 1) * rows] = self.stage(part, OWN)[...]
        for part in BOTH:
            for kind in range(3):
                for d in BOTH:
                    self.message(part, kind, d).wait_send()


def fast_scratch(rows, cols):
    return [pltpu.VMEM((2, 2, rows // 2, cols), BF), pltpu.VMEM((2, 2, rows, cols), BF)]


def comm_params(collective_id, limit=VMEM_MOST):
    return pltpu.CompilerParams(collective_id=collective_id, has_side_effects=True, vmem_limit_bytes=limit)


WO_CHUNKS = 4


def attend_kernel(side, adapters, scale, ids_ref, x_ref, gain_ref, cos_ref, sin_ref, *rest):
    w_heads, a_heads, b_heads, (wo_ref, ao_ref), a_mlp, b_rows, rest = rest[:3], rest[3:6], rest[6:9], rest[9:11], rest[11:13], rest[13:15], rest[15:]
    (out_ref, a_all, b_all), rest = rest[:3], rest[3:]
    (w, a_raw, b_raw, a_rows, bx, xbuf, h, z, lows, att, act, wo, stage, near, landed, am_raw, a_mine, b_mine, pair_send, pair_recv, load_sem, x_sem, own_sem,
     kept_sem, hand_send, hand_recv, wo_load, wo_send, wo_recv, bulk_send, bulk_recv, swap_send, swap_recv,
     send_sem, recv_sem, a_send, a_recv, b_send, b_recv, fast_send, fast_recv) = rest
    place = Place(side)
    place.announce(place.partner, place.device(0, FAR), place.device(FAR, 0))
    head, seq_len, depth = cos_ref.shape[1], x_ref.shape[1], x_ref.shape[2]
    cols = len(w_heads) * head
    chips = side * side
    per = a_raw.shape[3]
    half_depth = depth // 4
    loads = ends([pltpu.make_async_copy(src, dst, load_sem) for i in range(3) for src, dst in
                  ((a_heads[i], a_raw.at[place.core, i]), (w_heads[i], w.at[:, pl.ds(i * head, head)]), (b_heads[i], b_raw.at[0, i]))])
    steps = chips // 2

    def x_loads(step):
        slot = lax.rem(step, 2)
        return [pltpu.make_async_copy(x_ref.at[4 * lax.rem(step, steps) + 2 * i + place.core], xbuf.at[slot, i], x_sem.at[slot]) for i in BOTH]

    ends(x_loads(0))

    def every(ref):
        return lambda part, ds: ref.at[part, :, place.turn(place.x, ds)] if part else ref.at[part, place.turn(place.y, ds)]

    def spot_of(part):
        return place.y if part else place.x

    own_loads = ends([pltpu.make_async_copy(a_mlp[i], am_raw.at[i], own_sem) for i in BOTH] +
                     [pltpu.make_async_copy(b_rows[half].at[part], b_mine.at[part, place.y, place.x, half], own_sem) for part in BOTH for half in BOTH])
    width = wo_ref.shape[1]
    rank = ao_ref.shape[2]
    wo_loads = []
    for part in BOTH:
        wo_loads.append(pltpu.make_async_copy(wo_ref, wo.at[part, OWN, 0, :, first(width)], wo_load))
        for a in range(adapters):
            wo_loads.append(pltpu.make_async_copy(ao_ref.at[a], wo.at[part, OWN, 0, :, pl.ds(width + a * rank, rank)], wo_load))
    ends(wo_loads)
    wait(own_loads)
    wait(loads)
    am_rows = jnp.concatenate([am_raw[i, a] for i in BOTH for a in range(adapters)], axis=0)
    for part in BOTH:
        for half in BOTH:
            at = (2 * part + half) * half_depth
            a_mine[part, place.y, place.x, half] = am_rows[:, at:at + half_depth]
    place.meet()
    moves = [(a_raw.at[place.core], a_raw.at[place.core]), (w.at[:, first(cols)], w.at[:, pl.ds(cols, cols)]), (b_raw.at[0], b_raw.at[1])]
    pair = ends([remote(src, dst, pair_send.at[i], pair_recv.at[i], place.partner) for i, (src, dst) in enumerate(moves)])

    piece = head // WO_CHUNKS

    def wo_message(part, passed, d, i):
        src, dst = (wo.at[part, s, 0, pl.ds(i * piece, piece)] for s in ((FROM[d], FAR) if passed else (OWN, FROM[d])))
        sems = (part, passed, d, i)
        return remote(src, dst, wo_send.at[sems], wo_recv.at[sems], place.neighbour(part, SLOW, STEP[d]))

    def wo_to_partner(part, s):
        remote(wo.at[part, s, 0], wo.at[part, s, 1], bulk_send, bulk_recv, place.partner).start()

    passes = [range(d * WO_CHUNKS // 2, (d + 1) * WO_CHUNKS // 2) for d in BOTH]

    def wo_start(i):
        for d in BOTH:
            for part in BOTH:
                wo_message(part, 0, d, i).start()

    def wo_pass(k):
        for d in BOTH:
            for part in BOTH:
                wo_message(part, 0, d, passes[d][k]).wait_recv()
                wo_message(part, 1, d, passes[d][k]).start()

    def wo_arrived():
        for d in BOTH:
            for part in BOTH:
                for i in passes[1 - d]:
                    wo_message(part, 0, d, i).wait_recv()
                wo_to_partner(part, FROM[d])

    def wo_last():
        for part in BOTH:
            for d in BOTH:
                for i in passes[d]:
                    wo_message(part, 1, d, i).wait_recv()
            wo_to_partner(part, FAR)

    wait(wo_loads)
    early = WO_CHUNKS // 2
    gathers = [RowGather(place, every(a_mine), spot_of, a_send, a_recv), RowGather(place, every(b_mine), spot_of, b_send, b_recv)]

    def both(stage_of):
        for g in gathers:
            getattr(g, stage_of)()

    def hand(*distances):
        for ds in distances:
            for part in BOTH:
                for i, dst in enumerate((a_all, b_all)):
                    here, there = gathers[i].row_at(part, ds), every(dst.at[place.core])(part, ds)
                    pltpu.make_async_copy(here, there, kept_sem.at[i]).start()
                    remote(here, there, hand_send.at[i], hand_recv.at[i], place.partner).start()

    both('own')
    for i in range(early):
        wo_start(i)
    pair[0].wait_recv()
    for core in BOTH:
        pieces = [a_raw[core, i, a] if i < len(w_heads) else jnp.zeros((per, depth), BF) for a in range(adapters) for i in RING]
        a_rows[core * 2 * TILE:(core + 1) * 2 * TILE, :] = jnp.concatenate(pieces, axis=0)
    mine = [(place.y, place.x), (place.x, place.y)]

    low_gather = RowGather(place, lambda part, ds: lows.at[part, place.turn(mine[part][0], ds)], spot_of, send_sem, recv_sem)

    def norm(step, last):
        slot = lax.rem(step, 2)

        @pl.when(step + 1 < last)
        def _():
            ends(x_loads(step + 1))

        wait(x_loads(step))
        for i in BOTH:
            h[i * seq_len:(i + 1) * seq_len, :] = normed(xbuf[slot, i].astype(F32), gain_ref[...])

    def products(step):
        pl.when(step == 3)(lambda: both('near'))
        norm(step, 2 * steps)
        low = dot_rows(a_rows[...], h[...])
        half, at = step // (steps // 2), lax.rem(step, steps // 2) * 2 * seq_len
        for part in BOTH:
            pieces = []
            for i in BOTH:
                options = [low[TILE * (2 * part + a):TILE * (2 * part + a + 1), i * seq_len:(i + 1) * seq_len] for a in range(adapters)]
                chosen = options[0]
                for a in range(1, adapters):
                    chosen = jnp.where(ids_ref[4 * step + 2 * i + place.core] == a, options[a], chosen)
                pieces.append(chosen)
            lows[part, mine[part][0], mine[part][1], half, :, pl.ds(pl.multiple_of(at, LANE), 2 * seq_len)] = jnp.concatenate(pieces, axis=1).astype(BF)

    loop(steps, products)
    low_gather.own()
    for copy in pair[1:]:
        copy.wait_recv()
    for part in BOTH:
        wo_to_partner(part, OWN)
    events = {1: lambda: wo_start(early), 4: lambda: (low_gather.near(), wo_start(early + 1)), 7: low_gather.row}

    def project(step):
        for at, what in events.items():
            pl.when(step == at)(lambda what=what: (what(), None)[1])
        norm(step + steps, 2 * steps)
        rows = pl.ds(pl.multiple_of(step * 2 * seq_len, LANE), 2 * seq_len)
        chunk = fit(2 * cols, 256)
        for n in range(2 * cols // chunk):
            z[rows, n * chunk:(n + 1) * chunk] = dot(h[...], w[:, n * chunk:(n + 1) * chunk])

    loop(steps, project)
    row, col = (lax.broadcasted_iota(jnp.int32, (2 * rank, rank), axis) for axis in BOTH)
    spot, kind = row // TILE, lax.rem(row, TILE) // per
    for part in BOTH:
        chip_of = spot if part == 0 else lax.rem(spot, side) * side + spot // side
        to = chip_of * 2 * per + part * per + lax.rem(row, per)
        for i in range(3):
            spread_rows = jnp.where((kind == i) & (col == to), 1.0, 0.0).astype(BF)
            for a in range(adapters):
                for o in BOTH:
                    bx[a, part, :, o * cols + i * head:o * cols + (i + 1) * head] = dot(spread_rows, b_raw[o, i, a]).astype(BF)
    low_gather.sides()
    wo_pass(0)
    wo_pass(1)
    low_gather.far()
    causal = lax.broadcasted_iota(jnp.int32, (seq_len, seq_len), 0) >= lax.broadcasted_iota(jnp.int32, (seq_len, seq_len), 1)

    def swap(part, ds):
        sems = (part, ds)
        to = place.neighbour(part, SLOW, ds)
        return remote(att.at[sems], act.at[part, lax.rem(len(RING) - ds, len(RING))], swap_send.at[sems], swap_recv.at[sems], to)

    def attention(i):
        dy, dx = side - 1 - i // side, side - 1 - lax.rem(i, side)
        chip = place.turn(place.y, dy) * side + place.turn(place.x, dx)
        adapter = ids_ref[2 * chip + place.core]
        half, at = chip // steps, pl.ds(pl.multiple_of(lax.rem(chip, steps) * seq_len, LANE), seq_len)
        zs = z[pl.ds(pl.multiple_of(chip * seq_len, LANE), seq_len), :]
        for part in BOTH:
            zs += scale * dot_columns(lows[part, :, :, half, :, at].reshape(-1, seq_len), bx[adapter, part])
        for i_head in BOTH:
            q, k, v = (zs[:, i_head * cols + i * head:i_head * cols + (i + 1) * head] for i in range(3))
            q, k = ((r * cos_ref[...] + pltpu.roll(r, head // 2, axis=1) * sin_ref[...]).astype(BF) for r in (q, k))
            scores = jnp.where(causal, dot_rows(q, k) * head ** -0.5, -1e30)
            e = jnp.exp(scores - jnp.max(scores, axis=-1, keepdims=True))
            prob = (e / jnp.sum(e, axis=-1, keepdims=True)).astype(BF)
            mixed = dot(prob, v.astype(BF)).astype(BF)
            for part, (ds, df) in enumerate(((dy, dx), (dx, dy))):
                att[part, ds, df, :, i_head * head:(i_head + 1) * head] = mixed[part * seq_len // 2:(part + 1) * seq_len // 2]

    def attention_pair(k):
        for i in BOTH:
            attention(2 * k + i)
        row = side - 1 - 2 * k // side
        pl.when((lax.rem(2 * k + 2, side) == 0) & (row != OWN))(lambda: swap(0, row).start())

    loop(chips // 2, attention_pair)
    for ds in AWAY:
        swap(1, ds).start()
    both('row')
    hand(OWN)
    wo_arrived()
    wo_last()
    for part in BOTH:
        act[part, OWN] = att[part, OWN]
    pltpu.make_async_copy(wo.at[:, :, 1], wo.at[:, :, 1], bulk_recv).wait()
    chunk = fit(width, 512)
    rows = seq_len // 2
    blocks = (len(RING), rows)
    fast = FastScatter(place, lambda part, df: stage.at[part, df], near, landed, fast_send, fast_recv)

    def sum_heads(part, at):
        return sum(dot(act[part, s].reshape(-1, 2 * head), wo[part, s, :, :, at].reshape(2 * head, -1)) for s in RING)

    for part in BOTH:
        for ds in AWAY:
            swap(part, ds).wait_recv()

        def columns(n):
            at = pl.ds(pl.multiple_of(n * chunk, chunk), chunk)
            stage[part, :, :, at] = sum_heads(part, at).reshape(blocks + (chunk,)).astype(BF)

        loop(width // chunk, columns)
        chosen = rows_of_adapter(place, ids_ref, part, OWN, (len(RING) * rows, rank))
        stage[part, :, :, width:] = pick_columns(sum_heads(part, pl.ds(width, adapters * rank)), chosen).reshape(blocks + (rank,)).astype(BF)
        for df in (FAR, NEXT, LAST):
            fast.ready(part, df)
    both('sides')
    hand(NEXT, LAST)
    fast.sum()
    both('far')
    hand(FAR)
    fast.finish()
    fast.store(out_ref)
    for sem in (kept_sem, hand_send, hand_recv):
        for i, ref in enumerate((a_mine, b_mine)):
            pltpu.make_async_copy(ref, ref, sem.at[i]).wait()
    for copy in pair:
        copy.wait_send()
    for g in gathers + [low_gather]:
        g.sent()
    pltpu.make_async_copy(wo.at[:, :, 1], wo.at[:, :, 1], bulk_send).wait()
    for part in BOTH:
        for d in BOTH:
            for i in range(WO_CHUNKS):
                wo_message(part, 0, d, i).wait_send()
            for i in passes[d]:
                wo_message(part, 1, d, i).wait_send()
        for ds in AWAY:
            swap(part, ds).wait_send()


def attend(ids, x_in, gain, heads, w_o, a_o, a_mlp, b_rows, side, scale, collective_id):
    _, seq_len, depth = x_in.shape
    head = heads[0].shape[1]
    cols = 3 * head
    adapters, _, rank = a_o.shape
    per = a_mlp[0].shape[1]
    chips = side * side
    half_dim = head // 2
    inv_freq = ROPE_BASE ** (-2.0 * np.arange(half_dim) / head)
    angle = np.arange(seq_len)[:, None] * inv_freq[None, :]
    cos, sin = np.cos(angle), np.sin(angle)
    tables = [jnp.asarray(np.concatenate(pair, axis=1), F32) for pair in ((cos, cos), (-sin, sin))]
    n_pair = 3
    rows, out_cols = seq_len // 2, depth + rank
    every = (2, 2, side, side, 2)
    return pl.pallas_call(
        functools.partial(attend_kernel, side, adapters, scale),
        out_shape=[jax.ShapeDtypeStruct((seq_len, out_cols), BF), jax.ShapeDtypeStruct(every + (2 * adapters * per, depth // 4), BF),
                   jax.ShapeDtypeStruct(every + b_rows[0].shape[1:], BF)],
        in_specs=[SMEM, HBM, VMEM, VMEM, VMEM] + [HBM] * (len(heads) + 6),
        out_specs=[VMEM] + [HBM] * 2,
        scratch_shapes=[
            pltpu.VMEM((depth, 2 * cols), BF),
            pltpu.VMEM((2, 3, adapters, per, depth), BF),
            pltpu.VMEM((2, 3, adapters, rank, head), BF),
            pltpu.VMEM((2 * 2 * TILE, depth), BF),
            pltpu.VMEM((adapters, 2, 2 * rank, 2 * cols), BF),
            pltpu.VMEM((2, 2, seq_len, depth), BF),
            pltpu.VMEM((2 * seq_len, depth), BF),
            pltpu.VMEM((chips * seq_len, 2 * cols), F32),
            pltpu.VMEM((2, side, side, 2, TILE, chips * seq_len // 2), BF),
            pltpu.VMEM((2, side, side, rows, 2 * head), BF),
            pltpu.VMEM((2, side, side, rows, 2 * head), BF),
            pltpu.VMEM((2, side, 2, head, depth + adapters * rank), BF),
            pltpu.VMEM((2, side, rows, out_cols), BF),
        ] + fast_scratch(rows, out_cols) + [
            pltpu.VMEM((2, adapters, per, depth), BF),
            pltpu.VMEM(every[1:] + (2 * adapters * per, depth // 4), BF),
            pltpu.VMEM(every[1:] + b_rows[0].shape[1:], BF),
            DMA((n_pair,)), DMA((n_pair,)), DMA, DMA((2,)), DMA, DMA((2,)), DMA((2,)), DMA((2,)), DMA, DMA((2, 2, 2, WO_CHUNKS)), DMA((2, 2, 2, WO_CHUNKS)), DMA, DMA, DMA((2, 4)), DMA((2, 4)),
        ] + ROW_SEMS * 3 + FAST_SEMS,
        compiler_params=comm_params(collective_id),
        name='attend',
    )(ids, x_in, gain.reshape(1, depth), *tables, *heads, w_o, a_o, *a_mlp, *b_rows)


def row_proj_kernel(side, adapters, rank, ids_ref, act, w, out_ref, stage, near, landed, fast_near, fast_landed, slow_send, slow_recv, fast_send, fast_recv):
    place = Place(side)
    place.announce()
    rows, cols = stage.shape[3:]
    quarter = rows // 2
    width = cols - rank
    chunk = fit(width, 512)

    def unit(part, ds):
        def columns(n):
            at = pl.ds(pl.multiple_of(n * chunk, chunk), chunk)
            stage[part, ds, :, :, at] = dot(act[part, ds], w[:, at]).reshape(len(RING), rows, chunk).astype(BF)

        loop(width // chunk, columns)
        chosen = rows_of_adapter(place, ids_ref, part, ds, (len(RING) * rows, rank))
        stage[part, ds, :, :, width:] = pick_columns(dot(act[part, ds], w[:, width:]), chosen).reshape(len(RING), rows, rank).astype(BF)

    blocks = ((FAR, LAST), (OWN, NEXT))

    def slow(part, kind, d, i):
        df = blocks[1 - d][i] if kind == FREE else blocks[d][i]
        sems = (part, kind, d, i)
        src = stage.at[part, FAR if kind == PASS else TOWARD[d], df]
        dst = near.at[part, d, i] if kind == PASS else landed.at[part, d, df]
        return remote(src, dst, slow_send.at[sems], slow_recv.at[sems], place.neighbour(part, SLOW, STEP[d]))

    fast = FastScatter(place, lambda part, df: stage.at[part, OWN, df], fast_near, fast_landed, fast_send, fast_recv)
    for part in BOTH:
        unit(part, FAR)
        if part == 0:
            place.meet()
        for i in BOTH:
            for d in BOTH:
                slow(part, PASS, d, i).start()
    loop(len(RING), lambda i: unit(lax.rem(i, 2), NEXT + 2 * (i // 2)))
    for i in BOTH:
        for d in BOTH:
            for part in BOTH:
                slow(part, FREE, d, i).start()
    loop(2, lambda part: unit(part, OWN))
    for i in BOTH:
        for d in BOTH:
            for part in BOTH:
                slow(part, PASS, d, i).wait_recv()
                add(stage.at[part, TOWARD[d], blocks[d][i]], near.at[part, d, i])
                slow(part, SUM, d, i).start()
    for i in BOTH:
        for d in BOTH:
            df = blocks[d][i]
            for part in BOTH:
                slow(part, SUM, d, i).wait_recv()
                slow(part, FREE, 1 - d, i).wait_recv()
                add(stage.at[part, OWN, df], landed.at[part, UP, df], landed.at[part, DOWN, df])
                fast.ready(part, df)
    fast.sum()
    fast.finish()
    fast.store(out_ref)
    for part in BOTH:
        for kind in range(3):
            for d in BOTH:
                for i in BOTH:
                    slow(part, kind, d, i).wait_send()


def row_proj(ids, act, w, adapters, rank, side, collective_id):
    rows = act.shape[2] // side
    cols = w.shape[1] - (adapters - 1) * rank
    blocks = (rows, cols)
    return pl.pallas_call(
        functools.partial(row_proj_kernel, side, adapters, rank),
        out_shape=pltpu.VMEM((2 * rows, cols), BF),
        in_specs=[SMEM, VMEM, VMEM],
        out_specs=VMEM,
        scratch_shapes=[
            pltpu.VMEM((2, side, side) + blocks, BF),
            pltpu.VMEM((2, 2, 2) + blocks, BF),
            pltpu.VMEM((2, 2, side) + blocks, BF),
        ] + fast_scratch(rows, cols) + [DMA((2, 3, 2, 2))] * 2 + FAST_SEMS,
        compiler_params=comm_params(collective_id, VMEM_MOST * 5 // 8),
        name='row_proj',
    )(ids, act, w)


def finish(sums_ref, resid, b_ref, chosen, scale, adapters):
    _, _, side, _, rank, part = b_ref.shape
    width = sums_ref.shape[1] - rank
    low = spread(sums_ref[:, width:].astype(F32), chosen, adapters)
    delta = [dot(low, b_ref[core, :, y, x].reshape(adapters * rank, part)) for y in range(side) for x in range(side) for core in BOTH]
    return resid.astype(F32) + (sums_ref[:, :width].astype(F32) + scale * jnp.concatenate(delta, axis=1))


def own_rows(place, ids_ref, shape):
    return jnp.full(shape, ids_ref[place.device(0, 0)], jnp.int32)


def gate_up_kernel(side, adapters, scale, ids_ref, sums_ref, gain_ref, x_all, a_all, b_all, wg_ref, wu_ref, bg_ref, bu_ref, wd_ref, ad_ref,
                   hid, mid_ref, wd, gbuf, raw, w, b, x_ref, a_ref, b_ref, raw_sem, load_sem, a_sem, b_sem, credit, pair_send, pair_recv, send_sem, recv_sem):
    place = Place(side)
    share, width = wg_ref.shape
    half = raw.shape[1]
    rank = bg_ref.shape[2]
    seq_len = sums_ref.shape[0]
    edge = share // TILE * TILE
    for i in BOTH:
        raw[i, edge:] = jnp.zeros((half - edge, width), BF)
        for kind in BOTH:
            b[kind, i * half + edge:(i + 1) * half] = jnp.zeros((half - edge, adapters * rank), BF)
        wd[i * half + edge:(i + 1) * half] = jnp.zeros((half - edge, wd.shape[1]), BF)
    place.announce(place.partner)
    b_load = ends([pltpu.make_async_copy(b_all.at[:, :, :, :, 0], b_ref, b_sem), pltpu.make_async_copy(x_all.at[place.device(0, 0)], x_ref, b_sem)])
    a_load = ends([pltpu.make_async_copy(a_all, a_ref, a_sem)])
    mine = first(share)

    def raw_load(kind):
        return pltpu.make_async_copy((wg_ref, wu_ref)[kind], raw.at[0, mine], raw_sem)

    raw_load(0).start()
    loads = [pltpu.make_async_copy(wd_ref, wd.at[mine, first(width)], load_sem)]
    for a in range(adapters):
        loads.append(pltpu.make_async_copy(ad_ref.at[a], wd.at[mine, pl.ds(width + a * rank, rank)], load_sem))
        for kind, ref in enumerate((bg_ref, bu_ref)):
            loads.append(pltpu.make_async_copy(ref.at[a], b.at[kind, mine, pl.ds(a * rank, rank)], load_sem))
    ends(loads)
    other = pl.ds(half, share)
    moves = [(raw.at[0, mine], raw.at[1, mine])] * 2 + [(wd.at[mine], wd.at[other])] + [(b.at[kind, mine], b.at[kind, other]) for kind in BOTH]
    pair = [remote(src, dst, pair_send.at[i], pair_recv.at[i], place.partner) for i, (src, dst) in enumerate(moves)]
    rows = seq_len // 4
    chosen = own_rows(place, ids_ref, (seq_len, rank))
    wait(b_load)
    mid = finish(sums_ref, x_ref[...], b_ref, chosen, scale, adapters).astype(BF)
    mid_ref[...] = mid
    h2 = normed(mid.astype(F32), gain_ref[...])
    lows = []
    wait(a_load)
    for core in BOTH:
        pieces = [dot_rows(h2[:, i * width // 4:(i + 1) * width // 4], a_ref[core, i // 2, :, :, i % 2].reshape(-1, width // 4)) for i in RING]
        lows.append(sum(pieces).astype(BF))
    low = jnp.concatenate(lows, axis=1)
    per = rank // (2 * side * side)
    row, col = (lax.broadcasted_iota(jnp.int32, (low.shape[1], 2 * rank), axis) for axis in BOTH)
    kind, rank_at = col // rank, lax.rem(col, rank)
    chip, core = rank_at // (2 * per), lax.rem(rank_at // per, 2)
    pick = ((core * side * side + chip) * 2 + kind) * adapters * per + ids_ref[place.device(0, 0)] * per + lax.rem(rank_at, per)
    low = dot(low, jnp.where(row == pick, 1.0, 0.0).astype(BF)).astype(BF)
    for part in BOTH:
        for piece in BOTH:
            at = (2 * part + piece) * rows
            gbuf[part, OWN, OWN, piece, :, :width] = h2[at:at + rows]
            gbuf[part, OWN, OWN, piece, :, width:] = low[at:at + rows]
    place.meet()
    chunk = fit(2 * half, 256)

    def unit(ds, blocks=RING):
        lo, hi = min(blocks), max(blocks) + 1
        unit_rows = (hi - lo) * 2 * rows
        low = gbuf[:, ds, lo:hi, :, :, width:].reshape(2 * unit_rows, 2 * rank).astype(F32)
        chosen = jnp.concatenate([rows_of_adapter(place, ids_ref, part, ds, (len(RING) * 2 * rows, rank))[lo * 2 * rows:hi * 2 * rows] for part in BOTH], axis=0)
        lows = [spread(low[:, kind * rank:(kind + 1) * rank], chosen, adapters) for kind in BOTH]

        def columns(n):
            at = pl.ds(pl.multiple_of(n * chunk, chunk), chunk)
            act = gbuf[:, ds, lo:hi, :, :, :width].reshape(2 * unit_rows, width)
            gate, up = (dot(act, w[kind, :, at]) + scale * dot_rows(lows[kind], b[kind, at]) for kind in BOTH)
            hid[:, ds, lo * 2 * rows:hi * 2 * rows, at] = (gate * jax.nn.sigmoid(gate) * up).astype(BF).reshape(2, unit_rows, chunk)

        loop(2 * half // chunk, columns)

    gather = Gather(place, lambda part, ds, df: gbuf.at[part, ds, df], send_sem, recv_sem)
    gather.own()
    def turned(kind, i):
        def turn(n):
            at = pl.ds(pl.multiple_of(n * LANE, LANE), LANE)
            w[kind, at, i * half:(i + 1) * half] = raw[i, :, at].T

        loop(width // LANE, turn)

    for kind in BOTH:
        raw_load(kind).wait()
        if kind:
            pl.semaphore_wait(credit, 1)
        pair[kind].start()
        turned(kind, 0)
        if kind == 0:
            wait(loads)
            ends(pair[2:])
        pair[kind].wait_recv()
        turned(kind, 1)
        pair[kind].wait_send()
        if kind == 0:
            pl.semaphore_signal(credit, inc=1, device_id={'tensor': place.partner}, device_id_type=MESH)
            raw_load(1).start()
    gather.near()
    gather.row()
    for copy in pair[2:]:
        copy.wait_recv()
    unit(OWN)
    gather.sides(*AWAY)
    loop(2, lambda i: unit(NEXT + 2 * i))
    for blocks in PAIRS:
        gather.far(*blocks)
        unit(FAR, blocks)
    gather.sent()
    for copy in pair[2:]:
        copy.wait_send()


def gate_up(ids, sums, gain, x_in, a_all, b_all, w, side, scale, collective_id):
    _, seq_len, depth = x_in.shape
    share = w[0].shape[0]
    adapters, _, rank = w[2].shape
    half = (share + LANE - 1) // LANE * LANE
    hidden = (2, side, side * seq_len // 2, 2 * half)
    return pl.pallas_call(
        functools.partial(gate_up_kernel, side, adapters, scale),
        out_shape=[pltpu.VMEM(hidden, BF), pltpu.VMEM((seq_len, depth), BF), pltpu.VMEM((2 * half, depth + adapters * rank), BF)],
        in_specs=[SMEM] + [VMEM] * 2 + [HBM] * (3 + len(w)),
        out_specs=[VMEM] * 3,
        scratch_shapes=[
            pltpu.VMEM((2, side, side, 2, seq_len // 4, depth + 2 * rank), BF),
            pltpu.VMEM((2, half, depth), BF),
            pltpu.VMEM((2, depth, 2 * half), BF),
            pltpu.VMEM((2, 2 * half, adapters * rank), BF),
            pltpu.VMEM((seq_len, depth), BF),
            pltpu.VMEM(a_all.shape, BF),
            pltpu.VMEM(b_all.shape[:4] + b_all.shape[5:], BF),
            DMA, DMA, DMA, DMA, pltpu.SemaphoreType.REGULAR, DMA((5,)), DMA((5,)),
        ] + GATHER_SEMS,
        compiler_params=comm_params(collective_id, VMEM_MOST * 51 // 64),
        name='gate_up',
    )(ids, sums, gain.reshape(1, depth), x_in, a_all, b_all, *w)


def deliver_kernel(side, adapters, scale, ids_ref, sums_ref, x_ref, b_all, out_ref, b_ref, b_sem, pair_send, pair_recv, send_sem, recv_sem):
    place = Place(side)
    place.announce(place.partner)
    b_load = ends([pltpu.make_async_copy(b_all.at[:, :, :, :, 1], b_ref, b_sem)])
    seq_len = sums_ref.shape[0]
    rows = seq_len // 4
    chosen = own_rows(place, ids_ref, (seq_len, b_ref.shape[4]))
    wait(b_load)
    y = finish(sums_ref, x_ref[...], b_ref, chosen, scale, adapters).astype(BF)
    for part in BOTH:
        for piece in BOTH:
            at = (2 * part + piece) * rows
            out_ref[place.device(0, 0), part, piece] = y[at:at + rows]
    place.meet()

    def block(part, ds, df):
        return out_ref.at[place.sequence(part, ds, df), part]

    def seen(part, ds, df, half):
        ref = block(part, ds, df) if half is None else block(part, ds, df).at[half]
        remote(ref, ref, pair_send, pair_recv, place.partner).start()

    for part in BOTH:
        seen(part, OWN, OWN, None)
    gather = Gather(place, block, send_sem, recv_sem, absolute=True, seen=seen)
    gather.own()
    gather.near()
    gather.row()
    gather.sides(*AWAY)
    gather.far(*RING)
    gather.sent()
    every = out_ref.at[first(side * side)]
    for sem in (pair_send, pair_recv):
        pltpu.make_async_copy(every, every, sem).wait()


def put_kernel(y_ref, out_ref, sem):
    wait(ends([pltpu.make_async_copy(y_ref.at[i], out_ref.at[i], sem) for i in range(y_ref.shape[0])]))


def deliver(ids, sums, x_mid, b_all, side, scale, collective_id):
    seq_len, depth = x_mid.shape
    rows = seq_len // 4
    y = pl.pallas_call(
        functools.partial(deliver_kernel, side, b_all.shape[1], scale),
        out_shape=pltpu.VMEM((2 * side * side, 2, 2, rows, depth), BF),
        in_specs=[SMEM] + [VMEM] * 2 + [HBM],
        scratch_shapes=[pltpu.VMEM(b_all.shape[:4] + b_all.shape[5:], BF), DMA, DMA, DMA] + GATHER_SEMS,
        compiler_params=comm_params(collective_id, VMEM_SMALL),
        name='deliver',
    )(ids, sums, x_mid, b_all)
    return pl.pallas_call(
        put_kernel,
        out_shape=jax.ShapeDtypeStruct(y.shape, BF),
        in_specs=[pl.BlockSpec(memory_space=pl.ANY)],
        out_specs=HBM,
        scratch_shapes=[DMA],
        compiler_params=pltpu.CompilerParams(vmem_limit_bytes=VMEM_LEAST),
        name='put',
    )(y)


def solution(mesh):
    tp_size = mesh.shape['tensor']
    side = math.isqrt(tp_size // 2)
    rows_only = P('tensor', None)
    head_split = P(None, 'tensor', None)
    last_split = P(None, None, 'tensor')
    b_head_split = P(None, None, 'tensor', None)
    in_specs = (P('data', None, None), P('data'), P(None), P(None),
                head_split, head_split, head_split, P('tensor', None, None),
                P(None, 'tensor'), P(None, 'tensor'), rows_only,
                last_split, b_head_split, last_split, b_head_split, last_split, b_head_split,
                P(None, 'tensor', None, None), last_split,
                last_split, last_split, last_split, last_split,
                head_split, last_split)

    def local_layer(x_in, adapter_ids, gain_attn, gain_mlp, w_q, w_k, w_v, w_o, w_gate, w_up, w_down, a_q, b_q, a_k, b_k, a_v, b_v, a_o, b_o, a_gate, b_gate, a_up, b_up, a_down, b_down):
        scale = ALPHA / b_q.shape[1]

        def across(a):
            return a.swapaxes(-1, -2)

        heads = [w[:, 0] for w in (w_q, w_k, w_v)] + [across(a) for a in (a_q, a_k, a_v)] + [b[:, :, 0] for b in (b_q, b_k, b_v)]
        sums, all_a, all_b = attend(adapter_ids, x_in, gain_attn, heads, w_o[0], a_o[:, 0], (across(a_gate), across(a_up)), (b_o, b_down), side, scale, 0)

        w = [across(w_gate), across(w_up), across(b_gate), across(b_up), w_down, a_down]
        hidden, x_mid, w_d = gate_up(adapter_ids, sums, gain_mlp, x_in, all_a, all_b, w, side, scale, 1)
        sums = row_proj(adapter_ids, hidden, w_d, *a_o.shape[::3], side, 2)
        y = deliver(adapter_ids, sums, x_mid, pltpu.with_memory_space_constraint(all_b, pltpu.HBM), side, scale, 3)
        return y.reshape(x_in.shape)

    return jax.shard_map(local_layer, mesh=mesh, in_specs=in_specs, out_specs=P('data', None, None), check_vma=False)
```

```python
import functools
import math

import jax
import jax.numpy as jnp
import numpy as np
from jax import lax
from jax.experimental import pallas as pl
from jax.experimental.pallas import tpu as pltpu
from jax.sharding import PartitionSpec as P

ALPHA = 16.0
ROPE_BASE = 10000.0
EPSILON = 1e-5
BF = jnp.bfloat16
F32 = jnp.float32
LANE = 128
TILE = 16
VMEM_MOST = 67043328
VMEM_SMALL = VMEM_MOST // 6
VMEM_LEAST = VMEM_MOST // 32
MESH = pl.DeviceIdType.MESH
HBM = pl.BlockSpec(memory_space=pltpu.HBM)
VMEM = pl.BlockSpec(memory_space=pltpu.VMEM)
SMEM = pl.BlockSpec(memory_space=pltpu.SMEM)
DMA = pltpu.SemaphoreType.DMA

OWN, NEXT, FAR, LAST = RING = range(4)
UP, DOWN = BOTH = range(2)
STEP = (NEXT, -NEXT)
FROM = (LAST, NEXT)
AWAY = (NEXT, LAST, FAR)
PAIRS = ((OWN, NEXT), (LAST, FAR))
TOWARD = (NEXT, LAST)
FAST, SLOW = BOTH


def fit(size, most):
    return max(c for c in range(LANE, most + 1, LANE) if size % c == 0)


def first(size):
    return pl.ds(0, size)


def dot(a, b):
    return jnp.dot(a, b, preferred_element_type=F32)


def dot_rows(a, b):
    return lax.dot_general(a, b, (((1,), (1,)), ((), ())), preferred_element_type=F32)


def dot_columns(a, b):
    return lax.dot_general(a, b, (((0,), (0,)), ((), ())), preferred_element_type=F32)


def normed(act, gain):
    return (act * lax.rsqrt(jnp.mean(act * act, axis=-1, keepdims=True) + EPSILON) * gain).astype(BF)


def ends(copies):
    for copy in copies:
        copy.start()
    return copies


def wait(copies):
    for copy in copies:
        copy.wait()


def loop(count, body):
    lax.fori_loop(0, count, lambda i, carry: (body(i), carry)[1], 0)


class Place:
    def __init__(self, side):
        index = lax.axis_index('tensor')
        self.side = side
        self.core = lax.rem(index, 2)
        chip = index // 2
        self.y, self.x = chip // side, lax.rem(chip, side)
        self.partner = index + 1 - 2 * self.core

    def turn(self, at, steps):
        return lax.rem(at + steps + self.side, self.side)

    def device(self, dy, dx):
        return (self.turn(self.y, dy) * self.side + self.turn(self.x, dx)) * 2 + self.core

    def neighbour(self, part, ring, step):
        return self.device(0, step) if part == ring else self.device(step, 0)

    def sequence(self, part, ds, df):
        return self.device(jnp.where(part == 0, ds, df), jnp.where(part == 0, df, ds))

    def rows(self, ref):
        return lambda part, ds: ref.at[part, :, self.turn(self.x, ds)] if part else ref.at[part, self.turn(self.y, ds)]

    def spot(self, part):
        return self.y if part else self.x

    def announce(self, *more):
        to = [self.neighbour(0, ring, step) for ring in BOTH for step in STEP] + list(more)
        for device in to:
            pl.semaphore_signal(pltpu.get_barrier_semaphore(), inc=1, device_id={'tensor': device}, device_id_type=MESH)
        self.announced = len(to)

    def meet(self):
        pl.semaphore_wait(pltpu.get_barrier_semaphore(), self.announced)


def remote(src, dst, send_sem, recv_sem, to):
    return pltpu.make_async_remote_copy(src_ref=src, dst_ref=dst, send_sem=send_sem, recv_sem=recv_sem, device_id={'tensor': to}, device_id_type=MESH)


GATHER_SEMS = [DMA((2, 2, 2, 2, 4))] * 2


class Gather:
    def __init__(self, place, block, send_sem, recv_sem, absolute=False, seen=None):
        self.place, self.block, self.sems, self.absolute, self.seen = place, block, (send_sem, recv_sem), absolute, seen

    def message(self, part, ring, passed, d, j=OWN):
        spot = (lambda s: (s, j)) if ring == SLOW else (lambda s: (OWN, s))
        src, dst = (FROM[d], FAR) if passed else (OWN, FROM[d])
        a, b = self.block(part, *spot(src)), self.block(part, *spot(src if self.absolute else dst))
        if passed:
            a, b = a.at[d], b.at[d]
        return remote(a, b, *(sem.at[part, ring, passed, d, j] for sem in self.sems), self.place.neighbour(part, ring, STEP[d]))

    def arrived(self, part, ring, passed, d, j=OWN):
        self.message(part, ring, passed, d, j).wait_recv()
        if self.seen:
            at = FAR if passed else FROM[d]
            self.seen(part, *((at, j) if ring == SLOW else (OWN, at)), d if passed else None)

    def own(self):
        for ring in BOTH:
            for d in BOTH:
                for part in BOTH:
                    self.message(part, ring, 0, d).start()

    def near(self):
        for d in BOTH:
            for part in BOTH:
                self.arrived(part, FAST, 0, d)
                self.message(part, FAST, 1, d).start()
                for e in BOTH:
                    self.message(part, SLOW, 0, e, FROM[d]).start()

    def row(self):
        for part in BOTH:
            for d in BOTH:
                self.arrived(part, FAST, 1, d)
            for e in BOTH:
                self.message(part, SLOW, 0, e, FAR).start()
        self.sides(OWN)

    def sides(self, *blocks):
        for j in blocks:
            for part in BOTH:
                for d in BOTH:
                    self.arrived(part, SLOW, 0, d, j)
                    self.message(part, SLOW, 1, d, j).start()

    def far(self, *blocks):
        for j in blocks:
            for part in BOTH:
                for d in BOTH:
                    self.arrived(part, SLOW, 1, d, j)

    def sent(self):
        for part in BOTH:
            for d in BOTH:
                for passed in BOTH:
                    self.message(part, FAST, passed, d).wait_send()
                    for j in RING:
                        self.message(part, SLOW, passed, d, j).wait_send()


ROW_SEMS = [DMA((2, 2, 2, 2))] * 2


class RowGather:
    def __init__(self, place, row, mine, send_sem, recv_sem):
        self.place, self.row_at, self.mine, self.sems = place, row, mine, (send_sem, recv_sem)

    def message(self, part, ring, passed, d):
        if ring == SLOW:
            ref = self.row_at(part, FROM[d] if passed else OWN)
            ref = ref.at[:, d] if passed else ref
        else:
            ref = self.row_at(part, OWN).at[self.place.turn(self.mine(part), FROM[d] if passed else OWN)]
            ref = ref.at[d] if passed else ref
        return remote(ref, ref, *(sem.at[part, ring, passed, d] for sem in self.sems), self.place.neighbour(part, ring, STEP[d]))

    def pass_on(self, ring, passed):
        for part in BOTH:
            for d in BOTH:
                self.landing(part, ring, passed, d).wait_recv()
                if not passed:
                    self.message(part, ring, 1, d).start()
            if passed and ring == FAST:
                for d in BOTH:
                    self.message(part, SLOW, 0, d).start()

    def landing(self, part, ring, passed, d):
        at = FAR if passed else FROM[d]
        ref = self.row_at(part, at) if ring == SLOW else self.row_at(part, OWN).at[self.place.turn(self.mine(part), at)]
        if passed:
            ref = ref.at[:, d] if ring == SLOW else ref.at[d]
        return remote(ref, ref, *(sem.at[part, ring, passed, d] for sem in self.sems), self.place.neighbour(part, ring, STEP[d]))

    def own(self):
        for d in BOTH:
            for part in BOTH:
                self.message(part, FAST, 0, d).start()

    def near(self):
        self.pass_on(FAST, 0)

    def row(self):
        self.pass_on(FAST, 1)

    def sides(self):
        self.pass_on(SLOW, 0)

    def far(self):
        self.pass_on(SLOW, 1)

    def sent(self):
        for part in BOTH:
            for ring in BOTH:
                for passed in BOTH:
                    for d in BOTH:
                        self.message(part, ring, passed, d).wait_send()


def rows_of_adapter(place, ids_ref, part, ds, shape):
    block = lax.broadcasted_iota(jnp.int32, shape, 0) // (shape[0] // len(RING))
    chosen = jnp.zeros(shape, jnp.int32)
    for df in RING:
        chosen = jnp.where(block == df, ids_ref[place.sequence(part, ds, df)], chosen)
    return chosen


def pick_columns(low, chosen):
    rank = chosen.shape[1]
    kept = low[:, :rank]
    for a in range(1, low.shape[1] // rank):
        kept = jnp.where(chosen == a, low[:, a * rank:(a + 1) * rank], kept)
    return kept


def spread(low, chosen, adapters):
    return jnp.concatenate([jnp.where(chosen == a, low, 0.0) for a in range(adapters)], axis=1).astype(BF)


PASS, FREE, SUM = range(3)
FAST_SEMS = [DMA((2, 3, 2))] * 2


def add(into, *others):
    def some(i):
        at = pl.ds(pl.multiple_of(i * TILE, TILE), TILE)
        total = into[at, :].astype(F32)
        for other in others:
            total += other[at, :].astype(F32)
        into[at, :] = total.astype(BF)

    loop(into.shape[0] // TILE, some)


class FastScatter:
    def __init__(self, place, stage, near, landed, send_sem, recv_sem):
        self.place, self.stage, self.near, self.landed, self.sems = place, stage, near, landed, (send_sem, recv_sem)
        quarter = near.shape[2]
        self.halves = (first(quarter), pl.ds(quarter, quarter))

    def message(self, part, kind, d):
        at = self.halves[1 - d] if kind == FREE else self.halves[d]
        src = self.stage(part, FAR if kind == PASS else TOWARD[d]).at[at]
        dst = self.near.at[part, d] if kind == PASS else self.landed.at[part, d, at]
        sems = [sem.at[part, kind, d] for sem in self.sems]
        return remote(src, dst, *sems, self.place.neighbour(part, FAST, STEP[d]))

    def ready(self, part, df):
        for d in BOTH:
            if df == FAR:
                self.message(part, PASS, d).start()
            elif df == TOWARD[d]:
                self.message(part, FREE, d).start()

    def sum(self):
        for d in BOTH:
            for part in BOTH:
                self.message(part, PASS, d).wait_recv()
                add(self.stage(part, TOWARD[d]).at[self.halves[d]], self.near.at[part, d])
                self.message(part, SUM, d).start()

    def finish(self):
        for part in BOTH:
            for d in BOTH:
                self.message(part, FREE, d).wait_recv()
                self.message(part, SUM, d).wait_recv()
            add(self.stage(part, OWN), self.landed.at[part, UP], self.landed.at[part, DOWN])

    def store(self, out_ref):
        rows = self.landed.shape[2]
        for part in BOTH:
            out_ref[part * rows:(part + 1) * rows] = self.stage(part, OWN)[...]
        for part in BOTH:
            for kind in range(3):
                for d in BOTH:
                    self.message(part, kind, d).wait_send()


def fast_scratch(rows, cols):
    return [pltpu.VMEM((2, 2, rows // 2, cols), BF), pltpu.VMEM((2, 2, rows, cols), BF)]


def comm_params(collective_id, limit=VMEM_MOST):
    return pltpu.CompilerParams(collective_id=collective_id, has_side_effects=True, vmem_limit_bytes=limit)


WO_CHUNKS = 4


def attend_kernel(side, adapters, scale, ids_ref, x_ref, gain_ref, cos_ref, sin_ref, *rest):
    w_heads, a_heads, b_heads, (wo_ref, ao_ref), b_rows, rest = rest[:3], rest[3:6], rest[6:9], rest[9:11], rest[11:13], rest[13:]
    (out_ref, b_all), rest = rest[:2], rest[2:]
    (w, a_raw, b_raw, a_rows, bx, xbuf, h, z, lows, att, act, wo, stage, near, landed, b_mine, pair_send, pair_recv, load_sem, x_sem, own_sem,
     kept_sem, hand_send, hand_recv, wo_load, wo_send, wo_recv, bulk_send, bulk_recv, swap_send, swap_recv,
     send_sem, recv_sem, b_send, b_recv, fast_send, fast_recv) = rest
    place = Place(side)
    place.announce(place.partner, place.device(0, FAR), place.device(FAR, 0))
    head, seq_len, depth = cos_ref.shape[1], x_ref.shape[1], x_ref.shape[2]
    cols = len(w_heads) * head
    chips = side * side
    per = a_raw.shape[3]
    loads = ends([pltpu.make_async_copy(src, dst, load_sem) for i in range(3) for src, dst in
                  ((a_heads[i], a_raw.at[place.core, i]), (w_heads[i], w.at[:, pl.ds(i * head, head)]), (b_heads[i], b_raw.at[0, i]))])
    steps = chips // 2

    def x_loads(step):
        slot = lax.rem(step, 2)
        return [pltpu.make_async_copy(x_ref.at[4 * lax.rem(step, steps) + 2 * i + place.core], xbuf.at[slot, i], x_sem.at[slot]) for i in BOTH]

    ends(x_loads(0))

    own_loads = ends([pltpu.make_async_copy(b_rows[half].at[part], b_mine.at[part, place.y, place.x, half], own_sem) for part in BOTH for half in BOTH])
    width = wo_ref.shape[1]
    rank = ao_ref.shape[2]
    wo_loads = []
    for part in BOTH:
        wo_loads.append(pltpu.make_async_copy(wo_ref, wo.at[part, OWN, 0, :, first(width)], wo_load))
        for a in range(adapters):
            wo_loads.append(pltpu.make_async_copy(ao_ref.at[a], wo.at[part, OWN, 0, :, pl.ds(width + a * rank, rank)], wo_load))
    ends(wo_loads)
    wait(own_loads)
    wait(loads)
    place.meet()
    moves = [(a_raw.at[place.core], a_raw.at[place.core]), (w.at[:, first(cols)], w.at[:, pl.ds(cols, cols)]), (b_raw.at[0], b_raw.at[1])]
    pair = ends([remote(src, dst, pair_send.at[i], pair_recv.at[i], place.partner) for i, (src, dst) in enumerate(moves)])

    piece = head // WO_CHUNKS

    def wo_message(part, passed, d, i):
        src, dst = (wo.at[part, s, 0, pl.ds(i * piece, piece)] for s in ((FROM[d], FAR) if passed else (OWN, FROM[d])))
        sems = (part, passed, d, i)
        return remote(src, dst, wo_send.at[sems], wo_recv.at[sems], place.neighbour(part, SLOW, STEP[d]))

    def wo_to_partner(part, s):
        remote(wo.at[part, s, 0], wo.at[part, s, 1], bulk_send, bulk_recv, place.partner).start()

    passes = [range(d * WO_CHUNKS // 2, (d + 1) * WO_CHUNKS // 2) for d in BOTH]

    def wo_start(i):
        for d in BOTH:
            for part in BOTH:
                wo_message(part, 0, d, i).start()

    def wo_pass(k):
        for d in BOTH:
            for part in BOTH:
                wo_message(part, 0, d, passes[d][k]).wait_recv()
                wo_message(part, 1, d, passes[d][k]).start()

    def wo_arrived():
        for d in BOTH:
            for part in BOTH:
                for i in passes[1 - d]:
                    wo_message(part, 0, d, i).wait_recv()
                wo_to_partner(part, FROM[d])

    def wo_last():
        for part in BOTH:
            for d in BOTH:
                for i in passes[d]:
                    wo_message(part, 1, d, i).wait_recv()
            wo_to_partner(part, FAR)

    wait(wo_loads)
    early = WO_CHUNKS // 2
    b_gather = RowGather(place, place.rows(b_mine), place.spot, b_send, b_recv)

    def hand(*distances):
        for ds in distances:
            for part in BOTH:
                here, there = b_gather.row_at(part, ds), place.rows(b_all.at[place.core])(part, ds)
                pltpu.make_async_copy(here, there, kept_sem).start()
                remote(here, there, hand_send, hand_recv, place.partner).start()

    b_gather.own()
    for i in range(early):
        wo_start(i)
    pair[0].wait_recv()
    for core in BOTH:
        pieces = [a_raw[core, i, a] if i < len(w_heads) else jnp.zeros((per, depth), BF) for a in range(adapters) for i in RING]
        a_rows[core * 2 * TILE:(core + 1) * 2 * TILE, :] = jnp.concatenate(pieces, axis=0)
    mine = [(place.y, place.x), (place.x, place.y)]

    low_gather = RowGather(place, lambda part, ds: lows.at[part, place.turn(mine[part][0], ds)], place.spot, send_sem, recv_sem)

    def norm(step, last):
        slot = lax.rem(step, 2)

        @pl.when(step + 1 < last)
        def _():
            ends(x_loads(step + 1))

        wait(x_loads(step))
        for i in BOTH:
            h[i * seq_len:(i + 1) * seq_len, :] = normed(xbuf[slot, i].astype(F32), gain_ref[...])

    def products(step):
        pl.when(step == 3)(b_gather.near)
        norm(step, 2 * steps)
        low = dot_rows(a_rows[...], h[...])
        half, at = step // (steps // 2), lax.rem(step, steps // 2) * 2 * seq_len
        for part in BOTH:
            pieces = []
            for i in BOTH:
                options = [low[TILE * (2 * part + a):TILE * (2 * part + a + 1), i * seq_len:(i + 1) * seq_len] for a in range(adapters)]
                chosen = options[0]
                for a in range(1, adapters):
                    chosen = jnp.where(ids_ref[4 * step + 2 * i + place.core] == a, options[a], chosen)
                pieces.append(chosen)
            lows[part, mine[part][0], mine[part][1], half, :, pl.ds(pl.multiple_of(at, LANE), 2 * seq_len)] = jnp.concatenate(pieces, axis=1).astype(BF)

    loop(steps, products)
    low_gather.own()
    for copy in pair[1:]:
        copy.wait_recv()
    for part in BOTH:
        wo_to_partner(part, OWN)
    events = {1: lambda: wo_start(early), 4: lambda: (low_gather.near(), wo_start(early + 1)), 7: low_gather.row}

    def project(step):
        for at, what in events.items():
            pl.when(step == at)(lambda what=what: (what(), None)[1])
        norm(step + steps, 2 * steps)
        rows = pl.ds(pl.multiple_of(step * 2 * seq_len, LANE), 2 * seq_len)
        chunk = fit(2 * cols, 256)
        for n in range(2 * cols // chunk):
            z[rows, n * chunk:(n + 1) * chunk] = dot(h[...], w[:, n * chunk:(n + 1) * chunk])

    loop(steps, project)
    row, col = (lax.broadcasted_iota(jnp.int32, (2 * rank, rank), axis) for axis in BOTH)
    spot, kind = row // TILE, lax.rem(row, TILE) // per
    for part in BOTH:
        chip_of = spot if part == 0 else lax.rem(spot, side) * side + spot // side
        to = chip_of * 2 * per + part * per + lax.rem(row, per)
        for i in range(3):
            spread_rows = jnp.where((kind == i) & (col == to), 1.0, 0.0).astype(BF)
            for a in range(adapters):
                for o in BOTH:
                    bx[a, part, :, o * cols + i * head:o * cols + (i + 1) * head] = dot(spread_rows, b_raw[o, i, a]).astype(BF)
    low_gather.sides()
    wo_pass(0)
    wo_pass(1)
    low_gather.far()
    causal = lax.broadcasted_iota(jnp.int32, (seq_len, seq_len), 0) >= lax.broadcasted_iota(jnp.int32, (seq_len, seq_len), 1)

    def swap(part, ds):
        sems = (part, ds)
        to = place.neighbour(part, SLOW, ds)
        return remote(att.at[sems], act.at[part, lax.rem(len(RING) - ds, len(RING))], swap_send.at[sems], swap_recv.at[sems], to)

    def attention(i):
        dy, dx = side - 1 - i // side, side - 1 - lax.rem(i, side)
        chip = place.turn(place.y, dy) * side + place.turn(place.x, dx)
        adapter = ids_ref[2 * chip + place.core]
        half, at = chip // steps, pl.ds(pl.multiple_of(lax.rem(chip, steps) * seq_len, LANE), seq_len)
        zs = z[pl.ds(pl.multiple_of(chip * seq_len, LANE), seq_len), :]
        for part in BOTH:
            zs += scale * dot_columns(lows[part, :, :, half, :, at].reshape(-1, seq_len), bx[adapter, part])
        for i_head in BOTH:
            q, k, v = (zs[:, i_head * cols + i * head:i_head * cols + (i + 1) * head] for i in range(3))
            q, k = ((r * cos_ref[...] + pltpu.roll(r, head // 2, axis=1) * sin_ref[...]).astype(BF) for r in (q, k))
            scores = jnp.where(causal, dot_rows(q, k) * head ** -0.5, -1e30)
            e = jnp.exp(scores - jnp.max(scores, axis=-1, keepdims=True))
            prob = (e / jnp.sum(e, axis=-1, keepdims=True)).astype(BF)
            mixed = dot(prob, v.astype(BF)).astype(BF)
            for part, (ds, df) in enumerate(((dy, dx), (dx, dy))):
                att[part, ds, df, :, i_head * head:(i_head + 1) * head] = mixed[part * seq_len // 2:(part + 1) * seq_len // 2]

    def attention_pair(k):
        for i in BOTH:
            attention(2 * k + i)
        row = side - 1 - 2 * k // side
        pl.when((lax.rem(2 * k + 2, side) == 0) & (row != OWN))(lambda: swap(0, row).start())

    loop(chips // 2, attention_pair)
    for ds in AWAY:
        swap(1, ds).start()
    b_gather.row()
    hand(OWN)
    wo_arrived()
    wo_last()
    for part in BOTH:
        act[part, OWN] = att[part, OWN]
    pltpu.make_async_copy(wo.at[:, :, 1], wo.at[:, :, 1], bulk_recv).wait()
    chunk = fit(width, 512)
    rows = seq_len // 2
    blocks = (len(RING), rows)
    fast = FastScatter(place, lambda part, df: stage.at[part, df], near, landed, fast_send, fast_recv)

    def sum_heads(part, at):
        return sum(dot(act[part, s].reshape(-1, 2 * head), wo[part, s, :, :, at].reshape(2 * head, -1)) for s in RING)

    for part in BOTH:
        for ds in AWAY:
            swap(part, ds).wait_recv()

        def columns(n):
            at = pl.ds(pl.multiple_of(n * chunk, chunk), chunk)
            stage[part, :, :, at] = sum_heads(part, at).reshape(blocks + (chunk,)).astype(BF)

        loop(width // chunk, columns)
        chosen = rows_of_adapter(place, ids_ref, part, OWN, (len(RING) * rows, rank))
        stage[part, :, :, width:] = pick_columns(sum_heads(part, pl.ds(width, adapters * rank)), chosen).reshape(blocks + (rank,)).astype(BF)
        for df in (FAR, NEXT, LAST):
            fast.ready(part, df)
    b_gather.sides()
    hand(NEXT, LAST)
    fast.sum()
    b_gather.far()
    hand(FAR)
    fast.finish()
    fast.store(out_ref)
    for sem in (kept_sem, hand_send, hand_recv):
        pltpu.make_async_copy(b_mine, b_mine, sem).wait()
    for copy in pair:
        copy.wait_send()
    for g in (b_gather, low_gather):
        g.sent()
    pltpu.make_async_copy(wo.at[:, :, 1], wo.at[:, :, 1], bulk_send).wait()
    for part in BOTH:
        for d in BOTH:
            for i in range(WO_CHUNKS):
                wo_message(part, 0, d, i).wait_send()
            for i in passes[d]:
                wo_message(part, 1, d, i).wait_send()
        for ds in AWAY:
            swap(part, ds).wait_send()


def attend(ids, x_in, gain, heads, w_o, a_o, b_rows, side, scale, collective_id):
    _, seq_len, depth = x_in.shape
    head = heads[0].shape[1]
    cols = 3 * head
    adapters, _, rank = a_o.shape
    per = heads[3].shape[1]
    chips = side * side
    half_dim = head // 2
    inv_freq = ROPE_BASE ** (-2.0 * np.arange(half_dim) / head)
    angle = np.arange(seq_len)[:, None] * inv_freq[None, :]
    cos, sin = np.cos(angle), np.sin(angle)
    tables = [jnp.asarray(np.concatenate(pair, axis=1), F32) for pair in ((cos, cos), (-sin, sin))]
    n_pair = 3
    rows, out_cols = seq_len // 2, depth + rank
    every = (2, 2, side, side, 2)
    return pl.pallas_call(
        functools.partial(attend_kernel, side, adapters, scale),
        out_shape=[jax.ShapeDtypeStruct((seq_len, out_cols), BF),
                   jax.ShapeDtypeStruct(every + b_rows[0].shape[1:], BF)],
        in_specs=[SMEM, HBM, VMEM, VMEM, VMEM] + [HBM] * (len(heads) + 4),
        out_specs=[VMEM, HBM],
        scratch_shapes=[
            pltpu.VMEM((depth, 2 * cols), BF),
            pltpu.VMEM((2, 3, adapters, per, depth), BF),
            pltpu.VMEM((2, 3, adapters, rank, head), BF),
            pltpu.VMEM((2 * 2 * TILE, depth), BF),
            pltpu.VMEM((adapters, 2, 2 * rank, 2 * cols), BF),
            pltpu.VMEM((2, 2, seq_len, depth), BF),
            pltpu.VMEM((2 * seq_len, depth), BF),
            pltpu.VMEM((chips * seq_len, 2 * cols), F32),
            pltpu.VMEM((2, side, side, 2, TILE, chips * seq_len // 2), BF),
            pltpu.VMEM((2, side, side, rows, 2 * head), BF),
            pltpu.VMEM((2, side, side, rows, 2 * head), BF),
            pltpu.VMEM((2, side, 2, head, depth + adapters * rank), BF),
            pltpu.VMEM((2, side, rows, out_cols), BF),
        ] + fast_scratch(rows, out_cols) + [
            pltpu.VMEM(every[1:] + b_rows[0].shape[1:], BF),
            DMA((n_pair,)), DMA((n_pair,)), DMA, DMA((2,)), DMA, DMA, DMA, DMA, DMA, DMA((2, 2, 2, WO_CHUNKS)), DMA((2, 2, 2, WO_CHUNKS)), DMA, DMA, DMA((2, 4)), DMA((2, 4)),
        ] + ROW_SEMS * 2 + FAST_SEMS,
        compiler_params=comm_params(collective_id),
        name='attend',
    )(ids, x_in, gain.reshape(1, depth), *tables, *heads, w_o, a_o, *b_rows)


def row_proj_kernel(side, adapters, rank, ids_ref, act, w, out_ref, stage, near, landed, fast_near, fast_landed, slow_send, slow_recv, fast_send, fast_recv):
    place = Place(side)
    place.announce()
    rows, cols = stage.shape[3:]
    quarter = rows // 2
    width = cols - rank
    chunk = fit(width, 512)

    def unit(part, ds):
        def columns(n):
            at = pl.ds(pl.multiple_of(n * chunk, chunk), chunk)
            stage[part, ds, :, :, at] = dot(act[part, ds], w[:, at]).reshape(len(RING), rows, chunk).astype(BF)

        loop(width // chunk, columns)
        chosen = rows_of_adapter(place, ids_ref, part, ds, (len(RING) * rows, rank))
        stage[part, ds, :, :, width:] = pick_columns(dot(act[part, ds], w[:, width:]), chosen).reshape(len(RING), rows, rank).astype(BF)

    blocks = ((FAR, LAST), (OWN, NEXT))

    def slow(part, kind, d, i):
        df = blocks[1 - d][i] if kind == FREE else blocks[d][i]
        sems = (part, kind, d, i)
        src = stage.at[part, FAR if kind == PASS else TOWARD[d], df]
        dst = near.at[part, d, i] if kind == PASS else landed.at[part, d, df]
        return remote(src, dst, slow_send.at[sems], slow_recv.at[sems], place.neighbour(part, SLOW, STEP[d]))

    fast = FastScatter(place, lambda part, df: stage.at[part, OWN, df], fast_near, fast_landed, fast_send, fast_recv)
    for part in BOTH:
        unit(part, FAR)
        if part == 0:
            place.meet()
        for i in BOTH:
            for d in BOTH:
                slow(part, PASS, d, i).start()
    loop(len(RING), lambda i: unit(lax.rem(i, 2), NEXT + 2 * (i // 2)))
    for i in BOTH:
        for d in BOTH:
            for part in BOTH:
                slow(part, FREE, d, i).start()
    loop(2, lambda part: unit(part, OWN))
    for i in BOTH:
        for d in BOTH:
            for part in BOTH:
                slow(part, PASS, d, i).wait_recv()
                add(stage.at[part, TOWARD[d], blocks[d][i]], near.at[part, d, i])
                slow(part, SUM, d, i).start()
    for i in BOTH:
        for d in BOTH:
            df = blocks[d][i]
            for part in BOTH:
                slow(part, SUM, d, i).wait_recv()
                slow(part, FREE, 1 - d, i).wait_recv()
                add(stage.at[part, OWN, df], landed.at[part, UP, df], landed.at[part, DOWN, df])
                fast.ready(part, df)
    fast.sum()
    fast.finish()
    fast.store(out_ref)
    for part in BOTH:
        for kind in range(3):
            for d in BOTH:
                for i in BOTH:
                    slow(part, kind, d, i).wait_send()


def row_proj(ids, act, w, adapters, rank, side, collective_id):
    rows = act.shape[2] // side
    cols = w.shape[1] - (adapters - 1) * rank
    blocks = (rows, cols)
    return pl.pallas_call(
        functools.partial(row_proj_kernel, side, adapters, rank),
        out_shape=pltpu.VMEM((2 * rows, cols), BF),
        in_specs=[SMEM, VMEM, VMEM],
        out_specs=VMEM,
        scratch_shapes=[
            pltpu.VMEM((2, side, side) + blocks, BF),
            pltpu.VMEM((2, 2, 2) + blocks, BF),
            pltpu.VMEM((2, 2, side) + blocks, BF),
        ] + fast_scratch(rows, cols) + [DMA((2, 3, 2, 2))] * 2 + FAST_SEMS,
        compiler_params=comm_params(collective_id, VMEM_MOST * 5 // 8),
        name='row_proj',
    )(ids, act, w)


def finish(sums_ref, resid, b_ref, chosen, scale, adapters):
    _, _, side, _, rank, part = b_ref.shape
    width = sums_ref.shape[1] - rank
    low = spread(sums_ref[:, width:].astype(F32), chosen, adapters)
    delta = [dot(low, b_ref[core, :, y, x].reshape(adapters * rank, part)) for y in range(side) for x in range(side) for core in BOTH]
    return resid.astype(F32) + (sums_ref[:, :width].astype(F32) + scale * jnp.concatenate(delta, axis=1))


def own_rows(place, ids_ref, shape):
    return jnp.full(shape, ids_ref[place.device(0, 0)], jnp.int32)


def gate_up_kernel(side, adapters, scale, ids_ref, sums_ref, gain_ref, x_all, b_all, ag_ref, au_ref, wg_ref, wu_ref, bg_ref, bu_ref, wd_ref, ad_ref,
                   hid, mid_ref, wd, gbuf, raw, w, b, bx, x_ref, a_raw, a_ref, a_cols, b_ref, raw_sem, load_sem, a_sem, b_sem, credit, pair_send, pair_recv, hand_send, hand_recv,
                   send_sem, recv_sem, a_send, a_recv):
    place = Place(side)
    share, width = wg_ref.shape
    half = raw.shape[1]
    rank = bg_ref.shape[2]
    seq_len = sums_ref.shape[0]
    edge = share // TILE * TILE
    for i in BOTH:
        raw[i, edge:] = jnp.zeros((half - edge, width), BF)
        for kind in BOTH:
            b[kind, i * half + edge:(i + 1) * half] = jnp.zeros((half - edge, adapters * rank), BF)
        wd[i * half + edge:(i + 1) * half] = jnp.zeros((half - edge, wd.shape[1]), BF)
    place.announce(place.partner)
    b_load = ends([pltpu.make_async_copy(b_all.at[:, :, :, :, 0], b_ref, b_sem), pltpu.make_async_copy(x_all.at[place.device(0, 0)], x_ref, b_sem)])
    a_load = ends([pltpu.make_async_copy(ref, a_raw.at[i], a_sem) for i, ref in enumerate((ag_ref, au_ref))])
    mine = first(share)

    def raw_load(kind):
        return pltpu.make_async_copy((wg_ref, wu_ref)[kind], raw.at[0, mine], raw_sem)

    raw_load(0).start()
    loads = [pltpu.make_async_copy(wd_ref, wd.at[mine, first(width)], load_sem)]
    for a in range(adapters):
        loads.append(pltpu.make_async_copy(ad_ref.at[a], wd.at[mine, pl.ds(width + a * rank, rank)], load_sem))
        for kind, ref in enumerate((bg_ref, bu_ref)):
            loads.append(pltpu.make_async_copy(ref.at[a], b.at[kind, mine, pl.ds(a * rank, rank)], load_sem))
    ends(loads)
    other = pl.ds(half, share)
    moves = [(raw.at[0, mine], raw.at[1, mine])] * 2 + [(wd.at[mine], wd.at[other])] + [(b.at[kind, mine], b.at[kind, other]) for kind in BOTH]
    pair = [remote(src, dst, pair_send.at[i], pair_recv.at[i], place.partner) for i, (src, dst) in enumerate(moves)]
    quarter = width // 4
    wait(a_load)
    a_own = jnp.concatenate([a_raw[i, a] for i in BOTH for a in range(adapters)], axis=0)
    group = a_own.shape[0]
    for i in RING:
        a_ref[place.core, i // 2, place.y, place.x, i % 2] = a_own[:, i * quarter:(i + 1) * quarter]
    a_gather = RowGather(place, place.rows(a_ref.at[place.core]), place.spot, a_send, a_recv)

    def hand(*distances):
        for ds in distances:
            for part in BOTH:
                ref = a_gather.row_at(part, ds)
                remote(ref, ref, hand_send, hand_recv, place.partner).start()

    place.meet()
    a_gather.own()
    rows = seq_len // 4
    chosen = own_rows(place, ids_ref, (seq_len, rank))
    wait(b_load)
    mid = finish(sums_ref, x_ref[...], b_ref, chosen, scale, adapters).astype(BF)
    mid_ref[...] = mid
    h2 = normed(mid.astype(F32), gain_ref[...])
    for part in BOTH:
        for piece in BOTH:
            at = (2 * part + piece) * rows
            gbuf[part, OWN, OWN, piece] = h2[at:at + rows]
    chunk = fit(2 * half, 256)

    n_low = 2 * side * side * group
    per = group // (2 * adapters)

    def unit(ds, blocks=RING):
        lo, hi = min(blocks), max(blocks) + 1
        unit_rows = (hi - lo) * 2 * rows
        act_of = lambda: gbuf[:, ds, lo:hi].reshape(2 * unit_rows, width)
        chosen = jnp.concatenate([rows_of_adapter(place, ids_ref, part, ds, (len(RING) * 2 * rows, n_low))[lo * 2 * rows:hi * 2 * rows] for part in BOTH], axis=0)
        adapter = lax.rem(lax.broadcasted_iota(jnp.int32, chosen.shape, 1) // per, adapters)
        lows = jnp.where(adapter == chosen, dot(act_of(), a_cols[...]), 0.0).astype(BF)

        def columns(n):
            at = pl.ds(pl.multiple_of(n * chunk, chunk), chunk)
            act = act_of()
            gate, up = (dot(act, w[kind, :, at]) + scale * dot_rows(lows, bx[kind, at]) for kind in BOTH)
            hid[:, ds, lo * 2 * rows:hi * 2 * rows, at] = (gate * jax.nn.sigmoid(gate) * up).astype(BF).reshape(2, unit_rows, chunk)

        loop(2 * half // chunk, columns)

    gather = Gather(place, lambda part, ds, df: gbuf.at[part, ds, df], send_sem, recv_sem)
    gather.own()
    a_gather.near()
    def turned(kind, i):
        def turn(n):
            at = pl.ds(pl.multiple_of(n * LANE, LANE), LANE)
            w[kind, at, i * half:(i + 1) * half] = raw[i, :, at].T

        loop(width // LANE, turn)

    for kind in BOTH:
        raw_load(kind).wait()
        if kind:
            pl.semaphore_wait(credit, 1)
        pair[kind].start()
        turned(kind, 0)
        if kind == 0:
            wait(loads)
            ends(pair[2:])
            a_gather.row()
            hand(OWN)
        pair[kind].wait_recv()
        turned(kind, 1)
        pair[kind].wait_send()
        if kind == 0:
            pl.semaphore_signal(credit, inc=1, device_id={'tensor': place.partner}, device_id_type=MESH)
            raw_load(1).start()
    gather.near()
    gather.row()
    a_gather.sides()
    hand(NEXT, LAST)
    for copy in pair[2:]:
        copy.wait_recv()
    row, col = (lax.broadcasted_iota(jnp.int32, (adapters * rank, n_low), axis) for axis in BOTH)
    core, chip = col // (n_low // 2), lax.rem(col, n_low // 2) // group
    kind_of, a_of = lax.rem(col, group) // (group // 2), lax.rem(col // per, adapters)
    to = a_of * rank + chip * 2 * per + core * per + lax.rem(col, per)
    for kind in BOTH:
        bx[kind] = dot(b[kind], jnp.where((row == to) & (kind_of == kind), 1.0, 0.0).astype(BF)).astype(BF)
    a_gather.far()
    hand(FAR)
    pltpu.make_async_copy(a_ref.at[0], a_ref.at[0], hand_recv).wait()
    for core in BOTH:
        for i in RING:

            def turn_a(n):
                at = pl.ds(pl.multiple_of(n * LANE, LANE), LANE)
                to = pl.ds(pl.multiple_of(i * quarter + n * LANE, LANE), LANE)
                a_cols[to, core * n_low // 2:(core + 1) * n_low // 2] = a_ref[core, i // 2, :, :, i % 2, :, at].reshape(n_low // 2, LANE).T

            loop(quarter // LANE, turn_a)
    unit(OWN)
    for blocks in PAIRS:
        gather.sides(*(j for j in blocks if j != OWN))
        loop(2, lambda i: unit(NEXT + 2 * i, blocks))
    for blocks in PAIRS:
        gather.far(*blocks)
        unit(FAR, blocks)
    gather.sent()
    a_gather.sent()
    pltpu.make_async_copy(a_ref.at[0], a_ref.at[0], hand_send).wait()
    for copy in pair[2:]:
        copy.wait_send()


def gate_up(ids, sums, gain, x_in, b_all, a_mlp, w, side, scale, collective_id):
    _, seq_len, depth = x_in.shape
    share = w[0].shape[0]
    adapters, _, rank = w[2].shape
    half = (share + LANE - 1) // LANE * LANE
    hidden = (2, side, side * seq_len // 2, 2 * half)
    n_low = 2 * adapters * rank
    return pl.pallas_call(
        functools.partial(gate_up_kernel, side, adapters, scale),
        out_shape=[pltpu.VMEM(hidden, BF), pltpu.VMEM((seq_len, depth), BF), pltpu.VMEM((2 * half, depth + adapters * rank), BF)],
        in_specs=[SMEM] + [VMEM] * 2 + [HBM] * (4 + len(w)),
        out_specs=[VMEM] * 3,
        scratch_shapes=[
            pltpu.VMEM((2, side, side, 2, seq_len // 4, depth), BF),
            pltpu.VMEM((2, half, depth), BF),
            pltpu.VMEM((2, depth, 2 * half), BF),
            pltpu.VMEM((2, 2 * half, adapters * rank), BF),
            pltpu.VMEM((2, 2 * half, n_low), BF),
            pltpu.VMEM((seq_len, depth), BF),
            pltpu.VMEM((2,) + a_mlp[0].shape, BF),
            pltpu.VMEM((2, 2, side, side, 2, n_low // (2 * side * side), depth // 4), BF),
            pltpu.VMEM((depth, n_low), BF),
            pltpu.VMEM(b_all.shape[:4] + b_all.shape[5:], BF),
            DMA, DMA, DMA, DMA, pltpu.SemaphoreType.REGULAR, DMA((5,)), DMA((5,)), DMA, DMA,
        ] + GATHER_SEMS + ROW_SEMS,
        compiler_params=comm_params(collective_id, VMEM_MOST * 51 // 64),
        name='gate_up',
    )(ids, sums, gain.reshape(1, depth), x_in, b_all, *a_mlp, *w)


def deliver_kernel(side, adapters, scale, ids_ref, sums_ref, x_ref, b_all, out_ref, b_ref, b_sem, pair_send, pair_recv, send_sem, recv_sem):
    place = Place(side)
    place.announce(place.partner)
    b_load = ends([pltpu.make_async_copy(b_all.at[:, :, :, :, 1], b_ref, b_sem)])
    seq_len = sums_ref.shape[0]
    rows = seq_len // 4
    chosen = own_rows(place, ids_ref, (seq_len, b_ref.shape[4]))
    wait(b_load)
    y = finish(sums_ref, x_ref[...], b_ref, chosen, scale, adapters).astype(BF)
    for part in BOTH:
        for piece in BOTH:
            at = (2 * part + piece) * rows
            out_ref[place.device(0, 0), part, piece] = y[at:at + rows]
    place.meet()

    def block(part, ds, df):
        return out_ref.at[place.sequence(part, ds, df), part]

    def seen(part, ds, df, half):
        ref = block(part, ds, df) if half is None else block(part, ds, df).at[half]
        remote(ref, ref, pair_send, pair_recv, place.partner).start()

    for part in BOTH:
        seen(part, OWN, OWN, None)
    gather = Gather(place, block, send_sem, recv_sem, absolute=True, seen=seen)
    gather.own()
    gather.near()
    gather.row()
    gather.sides(*AWAY)
    gather.far(*RING)
    gather.sent()
    every = out_ref.at[first(side * side)]
    for sem in (pair_send, pair_recv):
        pltpu.make_async_copy(every, every, sem).wait()


def put_kernel(y_ref, out_ref, sem):
    wait(ends([pltpu.make_async_copy(y_ref.at[i], out_ref.at[i], sem) for i in range(y_ref.shape[0])]))


def deliver(ids, sums, x_mid, b_all, side, scale, collective_id):
    seq_len, depth = x_mid.shape
    rows = seq_len // 4
    y = pl.pallas_call(
        functools.partial(deliver_kernel, side, b_all.shape[1], scale),
        out_shape=pltpu.VMEM((2 * side * side, 2, 2, rows, depth), BF),
        in_specs=[SMEM] + [VMEM] * 2 + [HBM],
        scratch_shapes=[pltpu.VMEM(b_all.shape[:4] + b_all.shape[5:], BF), DMA, DMA, DMA] + GATHER_SEMS,
        compiler_params=comm_params(collective_id, VMEM_SMALL),
        name='deliver',
    )(ids, sums, x_mid, b_all)
    return pl.pallas_call(
        put_kernel,
        out_shape=jax.ShapeDtypeStruct(y.shape, BF),
        in_specs=[pl.BlockSpec(memory_space=pl.ANY)],
        out_specs=HBM,
        scratch_shapes=[DMA],
        compiler_params=pltpu.CompilerParams(vmem_limit_bytes=VMEM_LEAST),
        name='put',
    )(y)


def solution(mesh):
    tp_size = mesh.shape['tensor']
    side = math.isqrt(tp_size // 2)
    rows_only = P('tensor', None)
    head_split = P(None, 'tensor', None)
    last_split = P(None, None, 'tensor')
    b_head_split = P(None, None, 'tensor', None)
    in_specs = (P('data', None, None), P('data'), P(None), P(None),
                head_split, head_split, head_split, P('tensor', None, None),
                P(None, 'tensor'), P(None, 'tensor'), rows_only,
                last_split, b_head_split, last_split, b_head_split, last_split, b_head_split,
                P(None, 'tensor', None, None), last_split,
                last_split, last_split, last_split, last_split,
                head_split, last_split)

    def local_layer(x_in, adapter_ids, gain_attn, gain_mlp, w_q, w_k, w_v, w_o, w_gate, w_up, w_down, a_q, b_q, a_k, b_k, a_v, b_v, a_o, b_o, a_gate, b_gate, a_up, b_up, a_down, b_down):
        scale = ALPHA / b_q.shape[1]

        def across(a):
            return a.swapaxes(-1, -2)

        heads = [w[:, 0] for w in (w_q, w_k, w_v)] + [across(a) for a in (a_q, a_k, a_v)] + [b[:, :, 0] for b in (b_q, b_k, b_v)]
        sums, all_b = attend(adapter_ids, x_in, gain_attn, heads, w_o[0], a_o[:, 0], (b_o, b_down), side, scale, 0)

        w = [across(w_gate), across(w_up), across(b_gate), across(b_up), w_down, a_down]
        hidden, x_mid, w_d = gate_up(adapter_ids, sums, gain_mlp, x_in, all_b, (across(a_gate), across(a_up)), w, side, scale, 1)
        sums = row_proj(adapter_ids, hidden, w_d, *a_o.shape[::3], side, 2)
        y = deliver(adapter_ids, sums, x_mid, pltpu.with_memory_space_constraint(all_b, pltpu.HBM), side, scale, 3)
        return y.reshape(x_in.shape)

    return jax.shard_map(local_layer, mesh=mesh, in_specs=in_specs, out_specs=P('data', None, None), check_vma=False)
```

```python
import functools
import math

import jax
import jax.numpy as jnp
import numpy as np
from jax import lax
from jax.experimental import pallas as pl
from jax.experimental.pallas import tpu as pltpu
from jax.sharding import PartitionSpec as P

ALPHA = 16.0
ROPE_BASE = 10000.0
EPSILON = 1e-5
BF = jnp.bfloat16
F32 = jnp.float32
LANE = 128
TILE = 16
VMEM_MOST = 67043328
VMEM_SMALL = VMEM_MOST // 6
VMEM_LEAST = VMEM_MOST // 32
MESH = pl.DeviceIdType.MESH
HBM = pl.BlockSpec(memory_space=pltpu.HBM)
VMEM = pl.BlockSpec(memory_space=pltpu.VMEM)
SMEM = pl.BlockSpec(memory_space=pltpu.SMEM)
DMA = pltpu.SemaphoreType.DMA

OWN, NEXT, FAR, LAST = RING = range(4)
UP, DOWN = BOTH = range(2)
STEP = (NEXT, -NEXT)
FROM = (LAST, NEXT)
AWAY = (NEXT, LAST, FAR)
PAIRS = ((OWN, NEXT), (LAST, FAR))
TOWARD = (NEXT, LAST)
FAST, SLOW = BOTH


def fit(size, most):
    return max(c for c in range(LANE, most + 1, LANE) if size % c == 0)


def first(size):
    return pl.ds(0, size)


def dot(a, b):
    return jnp.dot(a, b, preferred_element_type=F32)


def dot_rows(a, b):
    return lax.dot_general(a, b, (((1,), (1,)), ((), ())), preferred_element_type=F32)


def dot_columns(a, b):
    return lax.dot_general(a, b, (((0,), (0,)), ((), ())), preferred_element_type=F32)


def normed(act, gain):
    return (act * lax.rsqrt(jnp.mean(act * act, axis=-1, keepdims=True) + EPSILON) * gain).astype(BF)


def ends(copies):
    for copy in copies:
        copy.start()
    return copies


def wait(copies):
    for copy in copies:
        copy.wait()


def loop(count, body):
    lax.fori_loop(0, count, lambda i, carry: (body(i), carry)[1], 0)


class Place:
    def __init__(self, side):
        index = lax.axis_index('tensor')
        self.side = side
        self.core = lax.rem(index, 2)
        chip = index // 2
        self.y, self.x = chip // side, lax.rem(chip, side)
        self.partner = index + 1 - 2 * self.core

    def turn(self, at, steps):
        return lax.rem(at + steps + self.side, self.side)

    def device(self, dy, dx):
        return (self.turn(self.y, dy) * self.side + self.turn(self.x, dx)) * 2 + self.core

    def neighbour(self, part, ring, step):
        return self.device(0, step) if part == ring else self.device(step, 0)

    def sequence(self, part, ds, df):
        return self.device(jnp.where(part == 0, ds, df), jnp.where(part == 0, df, ds))

    def rows(self, ref):
        return lambda part, ds: ref.at[part, :, self.turn(self.x, ds)] if part else ref.at[part, self.turn(self.y, ds)]

    def spot(self, part):
        return self.y if part else self.x

    def announce(self, *more):
        to = [self.neighbour(0, ring, step) for ring in BOTH for step in STEP] + list(more)
        for device in to:
            pl.semaphore_signal(pltpu.get_barrier_semaphore(), inc=1, device_id={'tensor': device}, device_id_type=MESH)
        self.announced = len(to)

    def meet(self):
        pl.semaphore_wait(pltpu.get_barrier_semaphore(), self.announced)


def remote(src, dst, send_sem, recv_sem, to):
    return pltpu.make_async_remote_copy(src_ref=src, dst_ref=dst, send_sem=send_sem, recv_sem=recv_sem, device_id={'tensor': to}, device_id_type=MESH)


GATHER_SEMS = [DMA((2, 2, 2, 2, 4))] * 2


class Gather:
    def __init__(self, place, block, send_sem, recv_sem, absolute=False, seen=None):
        self.place, self.block, self.sems, self.absolute, self.seen = place, block, (send_sem, recv_sem), absolute, seen

    def message(self, part, ring, passed, d, j=OWN):
        spot = (lambda s: (s, j)) if ring == SLOW else (lambda s: (OWN, s))
        src, dst = (FROM[d], FAR) if passed else (OWN, FROM[d])
        a, b = self.block(part, *spot(src)), self.block(part, *spot(src if self.absolute else dst))
        if passed:
            a, b = a.at[d], b.at[d]
        return remote(a, b, *(sem.at[part, ring, passed, d, j] for sem in self.sems), self.place.neighbour(part, ring, STEP[d]))

    def arrived(self, part, ring, passed, d, j=OWN):
        self.message(part, ring, passed, d, j).wait_recv()
        if self.seen:
            at = FAR if passed else FROM[d]
            self.seen(part, *((at, j) if ring == SLOW else (OWN, at)), d if passed else None)

    def own(self, *rings):
        for ring in rings:
            for d in BOTH:
                for part in BOTH:
                    self.message(part, ring, 0, d).start()

    def near(self):
        for d in BOTH:
            for part in BOTH:
                self.arrived(part, FAST, 0, d)
                self.message(part, FAST, 1, d).start()
                for e in BOTH:
                    self.message(part, SLOW, 0, e, FROM[d]).start()

    def row(self):
        for part in BOTH:
            for d in BOTH:
                self.arrived(part, FAST, 1, d)
            for e in BOTH:
                self.message(part, SLOW, 0, e, FAR).start()
        self.sides(OWN)

    def sides(self, *blocks):
        for j in blocks:
            for part in BOTH:
                for d in BOTH:
                    self.arrived(part, SLOW, 0, d, j)
                    self.message(part, SLOW, 1, d, j).start()

    def far(self, *blocks):
        for j in blocks:
            for part in BOTH:
                for d in BOTH:
                    self.arrived(part, SLOW, 1, d, j)

    def sent(self):
        for part in BOTH:
            for d in BOTH:
                for passed in BOTH:
                    self.message(part, FAST, passed, d).wait_send()
                    for j in RING:
                        self.message(part, SLOW, passed, d, j).wait_send()


ROW_SEMS = [DMA((2, 2, 2, 2))] * 2


class RowGather:
    def __init__(self, place, row, mine, send_sem, recv_sem):
        self.place, self.row_at, self.mine, self.sems = place, row, mine, (send_sem, recv_sem)

    def message(self, part, ring, passed, d):
        if ring == SLOW:
            ref = self.row_at(part, FROM[d] if passed else OWN)
            ref = ref.at[:, d] if passed else ref
        else:
            ref = self.row_at(part, OWN).at[self.place.turn(self.mine(part), FROM[d] if passed else OWN)]
            ref = ref.at[d] if passed else ref
        return remote(ref, ref, *(sem.at[part, ring, passed, d] for sem in self.sems), self.place.neighbour(part, ring, STEP[d]))

    def pass_on(self, ring, passed):
        for part in BOTH:
            for d in BOTH:
                self.landing(part, ring, passed, d).wait_recv()
                if not passed:
                    self.message(part, ring, 1, d).start()
            if passed and ring == FAST:
                for d in BOTH:
                    self.message(part, SLOW, 0, d).start()

    def landing(self, part, ring, passed, d):
        at = FAR if passed else FROM[d]
        ref = self.row_at(part, at) if ring == SLOW else self.row_at(part, OWN).at[self.place.turn(self.mine(part), at)]
        if passed:
            ref = ref.at[:, d] if ring == SLOW else ref.at[d]
        return remote(ref, ref, *(sem.at[part, ring, passed, d] for sem in self.sems), self.place.neighbour(part, ring, STEP[d]))

    def own(self):
        for d in BOTH:
            for part in BOTH:
                self.message(part, FAST, 0, d).start()

    def near(self):
        self.pass_on(FAST, 0)

    def row(self):
        self.pass_on(FAST, 1)

    def sides(self):
        self.pass_on(SLOW, 0)

    def far(self):
        self.pass_on(SLOW, 1)

    def sent(self):
        for part in BOTH:
            for ring in BOTH:
                for passed in BOTH:
                    for d in BOTH:
                        self.message(part, ring, passed, d).wait_send()


def rows_of_adapter(place, ids_ref, part, ds, shape):
    block = lax.broadcasted_iota(jnp.int32, shape, 0) // (shape[0] // len(RING))
    chosen = jnp.zeros(shape, jnp.int32)
    for df in RING:
        chosen = jnp.where(block == df, ids_ref[place.sequence(part, ds, df)], chosen)
    return chosen


def pick_columns(low, chosen):
    rank = chosen.shape[1]
    kept = low[:, :rank]
    for a in range(1, low.shape[1] // rank):
        kept = jnp.where(chosen == a, low[:, a * rank:(a + 1) * rank], kept)
    return kept


def spread(low, chosen, adapters):
    return jnp.concatenate([jnp.where(chosen == a, low, 0.0) for a in range(adapters)], axis=1).astype(BF)


PASS, FREE, SUM = range(3)
FAST_SEMS = [DMA((2, 3, 2))] * 2


def add(into, *others):
    def some(i):
        at = pl.ds(pl.multiple_of(i * TILE, TILE), TILE)
        total = into[at, :].astype(F32)
        for other in others:
            total += other[at, :].astype(F32)
        into[at, :] = total.astype(BF)

    loop(into.shape[0] // TILE, some)


class FastScatter:
    def __init__(self, place, stage, near, landed, send_sem, recv_sem):
        self.place, self.stage, self.near, self.landed, self.sems = place, stage, near, landed, (send_sem, recv_sem)
        quarter = near.shape[2]
        self.halves = (first(quarter), pl.ds(quarter, quarter))

    def message(self, part, kind, d):
        at = self.halves[1 - d] if kind == FREE else self.halves[d]
        src = self.stage(part, FAR if kind == PASS else TOWARD[d]).at[at]
        dst = self.near.at[part, d] if kind == PASS else self.landed.at[part, d, at]
        sems = [sem.at[part, kind, d] for sem in self.sems]
        return remote(src, dst, *sems, self.place.neighbour(part, FAST, STEP[d]))

    def ready(self, part, df):
        for d in BOTH:
            if df == FAR:
                self.message(part, PASS, d).start()
            elif df == TOWARD[d]:
                self.message(part, FREE, d).start()

    def sum(self):
        for d in BOTH:
            for part in BOTH:
                self.message(part, PASS, d).wait_recv()
                add(self.stage(part, TOWARD[d]).at[self.halves[d]], self.near.at[part, d])
                self.message(part, SUM, d).start()

    def finish(self):
        for part in BOTH:
            for d in BOTH:
                self.message(part, FREE, d).wait_recv()
                self.message(part, SUM, d).wait_recv()
            add(self.stage(part, OWN), self.landed.at[part, UP], self.landed.at[part, DOWN])

    def store(self, out_ref):
        rows = self.landed.shape[2]
        for part in BOTH:
            out_ref[part * rows:(part + 1) * rows] = self.stage(part, OWN)[...]
        for part in BOTH:
            for kind in range(3):
                for d in BOTH:
                    self.message(part, kind, d).wait_send()


def fast_scratch(rows, cols):
    return [pltpu.VMEM((2, 2, rows // 2, cols), BF), pltpu.VMEM((2, 2, rows, cols), BF)]


def comm_params(collective_id, limit=VMEM_MOST):
    return pltpu.CompilerParams(collective_id=collective_id, has_side_effects=True, vmem_limit_bytes=limit)


WO_CHUNKS = 8
X_SLOTS = 3


def attend_kernel(side, adapters, scale, ids_ref, x_ref, gain_ref, cos_ref, sin_ref, *rest):
    w_heads, a_heads, b_heads, (wo_ref, ao_ref), b_rows, rest = rest[:3], rest[3:6], rest[6:9], rest[9:11], rest[11:13], rest[13:]
    (out_ref, b_all), rest = rest[:2], rest[2:]
    (w, a_raw, b_raw, a_rows, bx, xbuf, h, z, lows, att, act, wo, stage, near, landed, b_mine, pair_send, pair_recv, load_sem, x_sem, own_sem,
     kept_sem, hand_send, hand_recv, wo_load, wo_send, wo_recv, bulk_send, bulk_recv, swap_send, swap_recv,
     send_sem, recv_sem, b_send, b_recv, fast_send, fast_recv) = rest
    place = Place(side)
    place.announce(place.partner, place.device(0, FAR), place.device(FAR, 0))
    head, seq_len, depth = cos_ref.shape[1], x_ref.shape[1], x_ref.shape[2]
    cols = len(w_heads) * head
    chips = side * side
    per = a_raw.shape[3]
    loads = ends([pltpu.make_async_copy(src, dst, load_sem) for i in range(3) for src, dst in
                  ((a_heads[i], a_raw.at[place.core, i]), (w_heads[i], w.at[:, pl.ds(i * head, head)]), (b_heads[i], b_raw.at[0, i]))])
    steps = chips // 2

    def x_loads(step):
        slot = lax.rem(step, X_SLOTS)
        return [pltpu.make_async_copy(x_ref.at[4 * lax.rem(step, steps) + 2 * i + place.core], xbuf.at[slot, i], x_sem.at[slot]) for i in BOTH]

    for step in range(X_SLOTS - 1):
        ends(x_loads(step))

    own_loads = ends([pltpu.make_async_copy(b_rows[half].at[part], b_mine.at[part, place.y, place.x, half], own_sem) for part in BOTH for half in BOTH])
    width = wo_ref.shape[1]
    rank = ao_ref.shape[2]
    wo_loads = []
    for part in BOTH:
        wo_loads.append(pltpu.make_async_copy(wo_ref, wo.at[part, OWN, 0, :, first(width)], wo_load))
        for a in range(adapters):
            wo_loads.append(pltpu.make_async_copy(ao_ref.at[a], wo.at[part, OWN, 0, :, pl.ds(width + a * rank, rank)], wo_load))
    ends(wo_loads)
    wait(own_loads)
    wait(loads)
    place.meet()
    moves = [(a_raw.at[place.core], a_raw.at[place.core]), (w.at[:, first(cols)], w.at[:, pl.ds(cols, cols)]), (b_raw.at[0], b_raw.at[1])]
    pair = ends([remote(src, dst, pair_send.at[i], pair_recv.at[i], place.partner) for i, (src, dst) in enumerate(moves)])

    piece = head // WO_CHUNKS

    def wo_message(part, passed, d, i):
        src, dst = (wo.at[part, s, 0, pl.ds(i * piece, piece)] for s in ((FROM[d], FAR) if passed else (OWN, FROM[d])))
        sems = (part, passed, d, i)
        return remote(src, dst, wo_send.at[sems], wo_recv.at[sems], place.neighbour(part, SLOW, STEP[d]))

    def wo_to_partner(part, s):
        remote(wo.at[part, s, 0], wo.at[part, s, 1], bulk_send, bulk_recv, place.partner).start()

    passes = [range(d * WO_CHUNKS // 2, (d + 1) * WO_CHUNKS // 2) for d in BOTH]

    def wo_start(i):
        for d in BOTH:
            for part in BOTH:
                wo_message(part, 0, d, i).start()

    def wo_pass(k):
        for d in BOTH:
            for part in BOTH:
                wo_message(part, 0, d, passes[d][k]).wait_recv()
                wo_message(part, 1, d, passes[d][k]).start()

    def wo_arrived():
        for d in BOTH:
            for part in BOTH:
                for i in passes[1 - d]:
                    wo_message(part, 0, d, i).wait_recv()
                wo_to_partner(part, FROM[d])

    def wo_last():
        for part in BOTH:
            for d in BOTH:
                for i in passes[d]:
                    wo_message(part, 1, d, i).wait_recv()
            wo_to_partner(part, FAR)

    wait(wo_loads)
    early = WO_CHUNKS // 2
    b_gather = RowGather(place, place.rows(b_mine), place.spot, b_send, b_recv)

    def hand(*distances):
        for ds in distances:
            for part in BOTH:
                here, there = b_gather.row_at(part, ds), place.rows(b_all.at[place.core])(part, ds)
                pltpu.make_async_copy(here, there, kept_sem).start()
                remote(here, there, hand_send, hand_recv, place.partner).start()

    b_gather.own()
    for i in range(early):
        wo_start(i)
    pair[0].wait_recv()
    for core in BOTH:
        pieces = [a_raw[core, i, a] if i < len(w_heads) else jnp.zeros((per, depth), BF) for a in range(adapters) for i in RING]
        a_rows[core * 2 * TILE:(core + 1) * 2 * TILE, :] = jnp.concatenate(pieces, axis=0)
    mine = [(place.y, place.x), (place.x, place.y)]

    low_gather = RowGather(place, lambda part, ds: lows.at[part, place.turn(mine[part][0], ds)], place.spot, send_sem, recv_sem)

    def norm(step, last):
        slot = lax.rem(step, X_SLOTS)

        @pl.when(step + X_SLOTS - 1 < last)
        def _():
            ends(x_loads(step + X_SLOTS - 1))

        wait(x_loads(step))
        for i in BOTH:
            h[i * seq_len:(i + 1) * seq_len, :] = normed(xbuf[slot, i].astype(F32), gain_ref[...])

    def products(step):
        pl.when(step == 3)(b_gather.near)
        norm(step, 2 * steps)
        low = dot_rows(a_rows[...], h[...])
        half, at = step // (steps // 2), lax.rem(step, steps // 2) * 2 * seq_len
        for part in BOTH:
            pieces = []
            for i in BOTH:
                options = [low[TILE * (2 * part + a):TILE * (2 * part + a + 1), i * seq_len:(i + 1) * seq_len] for a in range(adapters)]
                chosen = options[0]
                for a in range(1, adapters):
                    chosen = jnp.where(ids_ref[4 * step + 2 * i + place.core] == a, options[a], chosen)
                pieces.append(chosen)
            lows[part, mine[part][0], mine[part][1], half, :, pl.ds(pl.multiple_of(at, LANE), 2 * seq_len)] = jnp.concatenate(pieces, axis=1).astype(BF)

    loop(steps, products)
    low_gather.own()
    for copy in pair[1:]:
        copy.wait_recv()
    for part in BOTH:
        wo_to_partner(part, OWN)
    events = {0: lambda: wo_start(early), 3: lambda: (low_gather.near(), wo_start(early + 1)), 7: lambda: (low_gather.row(), wo_start(early + 2)),
              14: lambda: (low_gather.sides(), wo_start(early + 3))}

    def happen(half_step):
        for at, what in events.items():
            pl.when(half_step == at)(lambda what=what: (what(), None)[1])

    def project(step):
        happen(2 * step)
        norm(step + steps, 2 * steps)
        happen(2 * step + 1)
        rows = pl.ds(pl.multiple_of(step * 2 * seq_len, LANE), 2 * seq_len)
        chunk = fit(2 * cols, 256)
        for n in range(2 * cols // chunk):
            z[rows, n * chunk:(n + 1) * chunk] = dot(h[...], w[:, n * chunk:(n + 1) * chunk])

    loop(steps, project)
    row, col = (lax.broadcasted_iota(jnp.int32, (2 * rank, rank), axis) for axis in BOTH)
    spot, kind = row // TILE, lax.rem(row, TILE) // per
    for part in BOTH:
        chip_of = spot if part == 0 else lax.rem(spot, side) * side + spot // side
        to = chip_of * 2 * per + part * per + lax.rem(row, per)
        for i in range(3):
            spread_rows = jnp.where((kind == i) & (col == to), 1.0, 0.0).astype(BF)
            for a in range(adapters):
                for o in BOTH:
                    bx[a, part, :, o * cols + i * head:o * cols + (i + 1) * head] = dot(spread_rows, b_raw[o, i, a]).astype(BF)
    wo_pass(0)
    wo_pass(1)
    low_gather.far()
    wo_pass(2)
    wo_pass(3)
    causal = lax.broadcasted_iota(jnp.int32, (seq_len, seq_len), 0) >= lax.broadcasted_iota(jnp.int32, (seq_len, seq_len), 1)

    def swap(part, ds):
        sems = (part, ds)
        to = place.neighbour(part, SLOW, ds)
        return remote(att.at[sems], act.at[part, lax.rem(len(RING) - ds, len(RING))], swap_send.at[sems], swap_recv.at[sems], to)

    def attention(i):
        dy, dx = side - 1 - i // side, side - 1 - lax.rem(i, side)
        chip = place.turn(place.y, dy) * side + place.turn(place.x, dx)
        adapter = ids_ref[2 * chip + place.core]
        half, at = chip // steps, pl.ds(pl.multiple_of(lax.rem(chip, steps) * seq_len, LANE), seq_len)
        zs = z[pl.ds(pl.multiple_of(chip * seq_len, LANE), seq_len), :]
        for part in BOTH:
            zs += scale * dot_columns(lows[part, :, :, half, :, at].reshape(-1, seq_len), bx[adapter, part])
        for i_head in BOTH:
            q, k, v = (zs[:, i_head * cols + i * head:i_head * cols + (i + 1) * head] for i in range(3))
            q, k = ((r * cos_ref[...] + pltpu.roll(r, head // 2, axis=1) * sin_ref[...]).astype(BF) for r in (q, k))
            scores = jnp.where(causal, dot_rows(q, k) * head ** -0.5, -1e30)
            e = jnp.exp(scores - jnp.max(scores, axis=-1, keepdims=True))
            prob = (e / jnp.sum(e, axis=-1, keepdims=True)).astype(BF)
            mixed = dot(prob, v.astype(BF)).astype(BF)
            for part, (ds, df) in enumerate(((dy, dx), (dx, dy))):
                att[part, ds, df, :, i_head * head:(i_head + 1) * head] = mixed[part * seq_len // 2:(part + 1) * seq_len // 2]

    def attention_pair(k):
        for i in BOTH:
            attention(2 * k + i)
        row = side - 1 - 2 * k // side
        pl.when((lax.rem(2 * k + 2, side) == 0) & (row != OWN))(lambda: swap(0, row).start())

    loop(chips // 2, attention_pair)
    for ds in AWAY:
        swap(1, ds).start()
    b_gather.row()
    hand(OWN)
    wo_arrived()
    wo_last()
    for part in BOTH:
        act[part, OWN] = att[part, OWN]
    pltpu.make_async_copy(wo.at[:, :, 1], wo.at[:, :, 1], bulk_recv).wait()
    chunk = fit(width, 512)
    rows = seq_len // 2
    blocks = (len(RING), rows)
    fast = FastScatter(place, lambda part, df: stage.at[part, df], near, landed, fast_send, fast_recv)

    def sum_heads(part, at):
        return sum(dot(act[part, s].reshape(-1, 2 * head), wo[part, s, :, :, at].reshape(2 * head, -1)) for s in RING)

    for part in BOTH:
        for ds in AWAY:
            swap(part, ds).wait_recv()

        def columns(n):
            at = pl.ds(pl.multiple_of(n * chunk, chunk), chunk)
            stage[part, :, :, at] = sum_heads(part, at).reshape(blocks + (chunk,)).astype(BF)

        loop(width // chunk, columns)
        chosen = rows_of_adapter(place, ids_ref, part, OWN, (len(RING) * rows, rank))
        stage[part, :, :, width:] = pick_columns(sum_heads(part, pl.ds(width, adapters * rank)), chosen).reshape(blocks + (rank,)).astype(BF)
        for df in (FAR, NEXT, LAST):
            fast.ready(part, df)
    b_gather.sides()
    hand(NEXT, LAST)
    fast.sum()
    b_gather.far()
    hand(FAR)
    fast.finish()
    fast.store(out_ref)
    for sem in (kept_sem, hand_send, hand_recv):
        pltpu.make_async_copy(b_mine, b_mine, sem).wait()
    for copy in pair:
        copy.wait_send()
    for g in (b_gather, low_gather):
        g.sent()
    pltpu.make_async_copy(wo.at[:, :, 1], wo.at[:, :, 1], bulk_send).wait()
    for part in BOTH:
        for d in BOTH:
            for i in range(WO_CHUNKS):
                wo_message(part, 0, d, i).wait_send()
            for i in passes[d]:
                wo_message(part, 1, d, i).wait_send()
        for ds in AWAY:
            swap(part, ds).wait_send()


def attend(ids, x_in, gain, heads, w_o, a_o, b_rows, side, scale, collective_id):
    _, seq_len, depth = x_in.shape
    head = heads[0].shape[1]
    cols = 3 * head
    adapters, _, rank = a_o.shape
    per = heads[3].shape[1]
    chips = side * side
    half_dim = head // 2
    inv_freq = ROPE_BASE ** (-2.0 * np.arange(half_dim) / head)
    angle = np.arange(seq_len)[:, None] * inv_freq[None, :]
    cos, sin = np.cos(angle), np.sin(angle)
    tables = [jnp.asarray(np.concatenate(pair, axis=1), F32) for pair in ((cos, cos), (-sin, sin))]
    n_pair = 3
    rows, out_cols = seq_len // 2, depth + rank
    every = (2, 2, side, side, 2)
    return pl.pallas_call(
        functools.partial(attend_kernel, side, adapters, scale),
        out_shape=[jax.ShapeDtypeStruct((seq_len, out_cols), BF),
                   jax.ShapeDtypeStruct(every + b_rows[0].shape[1:], BF)],
        in_specs=[SMEM, HBM, VMEM, VMEM, VMEM] + [HBM] * (len(heads) + 4),
        out_specs=[VMEM, HBM],
        scratch_shapes=[
            pltpu.VMEM((depth, 2 * cols), BF),
            pltpu.VMEM((2, 3, adapters, per, depth), BF),
            pltpu.VMEM((2, 3, adapters, rank, head), BF),
            pltpu.VMEM((2 * 2 * TILE, depth), BF),
            pltpu.VMEM((adapters, 2, 2 * rank, 2 * cols), BF),
            pltpu.VMEM((X_SLOTS, 2, seq_len, depth), BF),
            pltpu.VMEM((2 * seq_len, depth), BF),
            pltpu.VMEM((chips * seq_len, 2 * cols), F32),
            pltpu.VMEM((2, side, side, 2, TILE, chips * seq_len // 2), BF),
            pltpu.VMEM((2, side, side, rows, 2 * head), BF),
            pltpu.VMEM((2, side, side, rows, 2 * head), BF),
            pltpu.VMEM((2, side, 2, head, depth + adapters * rank), BF),
            pltpu.VMEM((2, side, rows, out_cols), BF),
        ] + fast_scratch(rows, out_cols) + [
            pltpu.VMEM(every[1:] + b_rows[0].shape[1:], BF),
            DMA((n_pair,)), DMA((n_pair,)), DMA, DMA((X_SLOTS,)), DMA, DMA, DMA, DMA, DMA, DMA((2, 2, 2, WO_CHUNKS)), DMA((2, 2, 2, WO_CHUNKS)), DMA, DMA, DMA((2, 4)), DMA((2, 4)),
        ] + ROW_SEMS * 2 + FAST_SEMS,
        compiler_params=comm_params(collective_id),
        name='attend',
    )(ids, x_in, gain.reshape(1, depth), *tables, *heads, w_o, a_o, *b_rows)


def row_proj_kernel(side, adapters, rank, ids_ref, act, w, out_ref, stage, near, landed, fast_near, fast_landed, slow_send, slow_recv, fast_send, fast_recv):
    place = Place(side)
    place.announce()
    rows, cols = stage.shape[3:]
    quarter = rows // 2
    width = cols - rank
    chunk = fit(width, 512)

    def unit(part, ds):
        def columns(n):
            at = pl.ds(pl.multiple_of(n * chunk, chunk), chunk)
            stage[part, ds, :, :, at] = dot(act[part, ds], w[:, at]).reshape(len(RING), rows, chunk).astype(BF)

        loop(width // chunk, columns)
        chosen = rows_of_adapter(place, ids_ref, part, ds, (len(RING) * rows, rank))
        stage[part, ds, :, :, width:] = pick_columns(dot(act[part, ds], w[:, width:]), chosen).reshape(len(RING), rows, rank).astype(BF)

    blocks = ((FAR, LAST), (OWN, NEXT))

    def slow(part, kind, d, i):
        df = blocks[1 - d][i] if kind == FREE else blocks[d][i]
        sems = (part, kind, d, i)
        src = stage.at[part, FAR if kind == PASS else TOWARD[d], df]
        dst = near.at[part, d, i] if kind == PASS else landed.at[part, d, df]
        return remote(src, dst, slow_send.at[sems], slow_recv.at[sems], place.neighbour(part, SLOW, STEP[d]))

    fast = FastScatter(place, lambda part, df: stage.at[part, OWN, df], fast_near, fast_landed, fast_send, fast_recv)
    for part in BOTH:
        unit(part, FAR)
        if part == 0:
            place.meet()
        for i in BOTH:
            for d in BOTH:
                slow(part, PASS, d, i).start()
    loop(len(RING), lambda i: unit(lax.rem(i, 2), NEXT + 2 * (i // 2)))
    for i in BOTH:
        for d in BOTH:
            for part in BOTH:
                slow(part, FREE, d, i).start()
    loop(2, lambda part: unit(part, OWN))
    for i in BOTH:
        for d in BOTH:
            for part in BOTH:
                slow(part, PASS, d, i).wait_recv()
                add(stage.at[part, TOWARD[d], blocks[d][i]], near.at[part, d, i])
                slow(part, SUM, d, i).start()
    for i in BOTH:
        for d in BOTH:
            df = blocks[d][i]
            for part in BOTH:
                slow(part, SUM, d, i).wait_recv()
                slow(part, FREE, 1 - d, i).wait_recv()
                add(stage.at[part, OWN, df], landed.at[part, UP, df], landed.at[part, DOWN, df])
                fast.ready(part, df)
    fast.sum()
    fast.finish()
    fast.store(out_ref)
    for part in BOTH:
        for kind in range(3):
            for d in BOTH:
                for i in BOTH:
                    slow(part, kind, d, i).wait_send()


def row_proj(ids, act, w, adapters, rank, side, collective_id):
    rows = act.shape[2] // side
    cols = w.shape[1] - (adapters - 1) * rank
    blocks = (rows, cols)
    return pl.pallas_call(
        functools.partial(row_proj_kernel, side, adapters, rank),
        out_shape=pltpu.VMEM((2 * rows, cols), BF),
        in_specs=[SMEM, VMEM, VMEM],
        out_specs=VMEM,
        scratch_shapes=[
            pltpu.VMEM((2, side, side) + blocks, BF),
            pltpu.VMEM((2, 2, 2) + blocks, BF),
            pltpu.VMEM((2, 2, side) + blocks, BF),
        ] + fast_scratch(rows, cols) + [DMA((2, 3, 2, 2))] * 2 + FAST_SEMS,
        compiler_params=comm_params(collective_id, VMEM_MOST * 5 // 8),
        name='row_proj',
    )(ids, act, w)


def finish(sums_ref, resid, b_ref, chosen, scale, adapters):
    _, _, side, _, rank, part = b_ref.shape
    width = sums_ref.shape[1] - rank
    low = spread(sums_ref[:, width:].astype(F32), chosen, adapters)
    delta = [dot(low, b_ref[core, :, y, x].reshape(adapters * rank, part)) for y in range(side) for x in range(side) for core in BOTH]
    return resid.astype(F32) + (sums_ref[:, :width].astype(F32) + scale * jnp.concatenate(delta, axis=1))


def own_rows(place, ids_ref, shape):
    return jnp.full(shape, ids_ref[place.device(0, 0)], jnp.int32)


def gate_up_kernel(side, adapters, scale, ids_ref, sums_ref, gain_ref, x_all, b_all, ag_ref, au_ref, wg_ref, wu_ref, bg_ref, bu_ref, wd_ref, ad_ref,
                   hid, mid_ref, wd, gbuf, raw, w, b, bx, x_ref, a_raw, a_ref, a_cols, b_ref, raw_sem, load_sem, a_sem, b_sem, credit, pair_send, pair_recv, hand_send, hand_recv,
                   send_sem, recv_sem, a_send, a_recv):
    place = Place(side)
    share, width = wg_ref.shape
    half = raw.shape[1]
    rank = bg_ref.shape[2]
    seq_len = sums_ref.shape[0]
    edge = share // TILE * TILE
    for i in BOTH:
        raw[i, edge:] = jnp.zeros((half - edge, width), BF)
        for kind in BOTH:
            b[kind, i * half + edge:(i + 1) * half] = jnp.zeros((half - edge, adapters * rank), BF)
        wd[i * half + edge:(i + 1) * half] = jnp.zeros((half - edge, wd.shape[1]), BF)
    place.announce(place.partner)
    b_load = ends([pltpu.make_async_copy(b_all.at[:, :, :, :, 0], b_ref, b_sem), pltpu.make_async_copy(x_all.at[place.device(0, 0)], x_ref, b_sem)])
    a_load = ends([pltpu.make_async_copy(ref, a_raw.at[i], a_sem) for i, ref in enumerate((ag_ref, au_ref))])
    mine = first(share)

    def raw_load(kind):
        return pltpu.make_async_copy((wg_ref, wu_ref)[kind], raw.at[0, mine], raw_sem)

    raw_load(0).start()
    loads = [pltpu.make_async_copy(wd_ref, wd.at[mine, first(width)], load_sem)]
    for a in range(adapters):
        loads.append(pltpu.make_async_copy(ad_ref.at[a], wd.at[mine, pl.ds(width + a * rank, rank)], load_sem))
        for kind, ref in enumerate((bg_ref, bu_ref)):
            loads.append(pltpu.make_async_copy(ref.at[a], b.at[kind, mine, pl.ds(a * rank, rank)], load_sem))
    ends(loads)
    other = pl.ds(half, share)
    moves = [(raw.at[0, mine], raw.at[1, mine])] * 2 + [(wd.at[mine], wd.at[other])] + [(b.at[kind, mine], b.at[kind, other]) for kind in BOTH]
    pair = [remote(src, dst, pair_send.at[i], pair_recv.at[i], place.partner) for i, (src, dst) in enumerate(moves)]
    quarter = width // 4
    wait(a_load)
    a_own = jnp.concatenate([a_raw[i, a] for i in BOTH for a in range(adapters)], axis=0)
    group = a_own.shape[0]
    for i in RING:
        a_ref[place.core, i // 2, place.y, place.x, i % 2] = a_own[:, i * quarter:(i + 1) * quarter]
    a_gather = RowGather(place, place.rows(a_ref.at[place.core]), place.spot, a_send, a_recv)

    def hand(*distances):
        for ds in distances:
            for part in BOTH:
                ref = a_gather.row_at(part, ds)
                remote(ref, ref, hand_send, hand_recv, place.partner).start()

    place.meet()
    a_gather.own()
    rows = seq_len // 4
    chosen = own_rows(place, ids_ref, (seq_len, rank))
    wait(b_load)
    mid = finish(sums_ref, x_ref[...], b_ref, chosen, scale, adapters).astype(BF)
    mid_ref[...] = mid
    h2 = normed(mid.astype(F32), gain_ref[...])
    for part in BOTH:
        for piece in BOTH:
            at = (2 * part + piece) * rows
            gbuf[part, OWN, OWN, piece] = h2[at:at + rows]
    chunk = fit(2 * half, 256)

    n_low = 2 * side * side * group
    per = group // (2 * adapters)

    def unit(ds, blocks=RING):
        lo, hi = min(blocks), max(blocks) + 1
        unit_rows = (hi - lo) * 2 * rows
        act_of = lambda: gbuf[:, ds, lo:hi].reshape(2 * unit_rows, width)
        chosen = jnp.concatenate([rows_of_adapter(place, ids_ref, part, ds, (len(RING) * 2 * rows, n_low))[lo * 2 * rows:hi * 2 * rows] for part in BOTH], axis=0)
        adapter = lax.rem(lax.broadcasted_iota(jnp.int32, chosen.shape, 1) // per, adapters)
        lows = jnp.where(adapter == chosen, dot(act_of(), a_cols[...]), 0.0).astype(BF)

        def columns(n):
            at = pl.ds(pl.multiple_of(n * chunk, chunk), chunk)
            act = act_of()
            gate, up = (dot(act, w[kind, :, at]) + scale * dot_rows(lows, bx[kind, at]) for kind in BOTH)
            hid[:, ds, lo * 2 * rows:hi * 2 * rows, at] = (gate * jax.nn.sigmoid(gate) * up).astype(BF).reshape(2, unit_rows, chunk)

        loop(2 * half // chunk, columns)

    gather = Gather(place, lambda part, ds, df: gbuf.at[part, ds, df], send_sem, recv_sem)
    a_gather.near()
    gather.own(FAST)
    a_gather.row()
    hand(OWN)
    gather.own(SLOW)
    def turned(kind, i):
        def turn(n):
            at = pl.ds(pl.multiple_of(n * LANE, LANE), LANE)
            w[kind, at, i * half:(i + 1) * half] = raw[i, :, at].T

        loop(width // LANE, turn)

    for kind in BOTH:
        raw_load(kind).wait()
        if kind:
            pl.semaphore_wait(credit, 1)
        pair[kind].start()
        turned(kind, 0)
        if kind == 0:
            wait(loads)
            ends(pair[2:])
        pair[kind].wait_recv()
        turned(kind, 1)
        pair[kind].wait_send()
        if kind == 0:
            pl.semaphore_signal(credit, inc=1, device_id={'tensor': place.partner}, device_id_type=MESH)
            raw_load(1).start()
    a_gather.sides()
    gather.near()
    hand(NEXT, LAST)
    for copy in pair[2:]:
        copy.wait_recv()
    row, col = (lax.broadcasted_iota(jnp.int32, (adapters * rank, n_low), axis) for axis in BOTH)
    core, chip = col // (n_low // 2), lax.rem(col, n_low // 2) // group
    kind_of, a_of = lax.rem(col, group) // (group // 2), lax.rem(col // per, adapters)
    to = a_of * rank + chip * 2 * per + core * per + lax.rem(col, per)
    for kind in BOTH:
        bx[kind] = dot(b[kind], jnp.where((row == to) & (kind_of == kind), 1.0, 0.0).astype(BF)).astype(BF)
    a_gather.far()
    hand(FAR)
    pltpu.make_async_copy(a_ref.at[0], a_ref.at[0], hand_recv).wait()
    for core in BOTH:
        for i in RING:

            def turn_a(n):
                at = pl.ds(pl.multiple_of(n * LANE, LANE), LANE)
                to = pl.ds(pl.multiple_of(i * quarter + n * LANE, LANE), LANE)
                a_cols[to, core * n_low // 2:(core + 1) * n_low // 2] = a_ref[core, i // 2, :, :, i % 2, :, at].reshape(n_low // 2, LANE).T

            loop(quarter // LANE, turn_a)
    gather.row()
    unit(OWN)
    for blocks in PAIRS:
        gather.sides(*(j for j in blocks if j != OWN))
        loop(2, lambda i: unit(NEXT + 2 * i, blocks))
    for blocks in PAIRS:
        gather.far(*blocks)
        unit(FAR, blocks)
    gather.sent()
    a_gather.sent()
    pltpu.make_async_copy(a_ref.at[0], a_ref.at[0], hand_send).wait()
    for copy in pair[2:]:
        copy.wait_send()


def gate_up(ids, sums, gain, x_in, b_all, a_mlp, w, side, scale, collective_id):
    _, seq_len, depth = x_in.shape
    share = w[0].shape[0]
    adapters, _, rank = w[2].shape
    half = (share + LANE - 1) // LANE * LANE
    hidden = (2, side, side * seq_len // 2, 2 * half)
    n_low = 2 * adapters * rank
    return pl.pallas_call(
        functools.partial(gate_up_kernel, side, adapters, scale),
        out_shape=[pltpu.VMEM(hidden, BF), pltpu.VMEM((seq_len, depth), BF), pltpu.VMEM((2 * half, depth + adapters * rank), BF)],
        in_specs=[SMEM] + [VMEM] * 2 + [HBM] * (4 + len(w)),
        out_specs=[VMEM] * 3,
        scratch_shapes=[
            pltpu.VMEM((2, side, side, 2, seq_len // 4, depth), BF),
            pltpu.VMEM((2, half, depth), BF),
            pltpu.VMEM((2, depth, 2 * half), BF),
            pltpu.VMEM((2, 2 * half, adapters * rank), BF),
            pltpu.VMEM((2, 2 * half, n_low), BF),
            pltpu.VMEM((seq_len, depth), BF),
            pltpu.VMEM((2,) + a_mlp[0].shape, BF),
            pltpu.VMEM((2, 2, side, side, 2, n_low // (2 * side * side), depth // 4), BF),
            pltpu.VMEM((depth, n_low), BF),
            pltpu.VMEM(b_all.shape[:4] + b_all.shape[5:], BF),
            DMA, DMA, DMA, DMA, pltpu.SemaphoreType.REGULAR, DMA((5,)), DMA((5,)), DMA, DMA,
        ] + GATHER_SEMS + ROW_SEMS,
        compiler_params=comm_params(collective_id, VMEM_MOST * 51 // 64),
        name='gate_up',
    )(ids, sums, gain.reshape(1, depth), x_in, b_all, *a_mlp, *w)


def deliver_kernel(side, adapters, scale, ids_ref, sums_ref, x_ref, b_all, out_ref, b_ref, b_sem, pair_send, pair_recv, send_sem, recv_sem):
    place = Place(side)
    place.announce(place.partner)
    b_load = ends([pltpu.make_async_copy(b_all.at[:, :, :, :, 1], b_ref, b_sem)])
    seq_len = sums_ref.shape[0]
    rows = seq_len // 4
    chosen = own_rows(place, ids_ref, (seq_len, b_ref.shape[4]))
    wait(b_load)
    y = finish(sums_ref, x_ref[...], b_ref, chosen, scale, adapters).astype(BF)
    for part in BOTH:
        for piece in BOTH:
            at = (2 * part + piece) * rows
            out_ref[place.device(0, 0), part, piece] = y[at:at + rows]
    place.meet()

    def block(part, ds, df):
        return out_ref.at[place.sequence(part, ds, df), part]

    def seen(part, ds, df, half):
        ref = block(part, ds, df) if half is None else block(part, ds, df).at[half]
        remote(ref, ref, pair_send, pair_recv, place.partner).start()

    for part in BOTH:
        seen(part, OWN, OWN, None)
    gather = Gather(place, block, send_sem, recv_sem, absolute=True, seen=seen)
    gather.own(*BOTH)
    gather.near()
    gather.row()
    gather.sides(*AWAY)
    gather.far(*RING)
    gather.sent()
    every = out_ref.at[first(side * side)]
    for sem in (pair_send, pair_recv):
        pltpu.make_async_copy(every, every, sem).wait()


def put_kernel(y_ref, out_ref, sem):
    wait(ends([pltpu.make_async_copy(y_ref.at[i], out_ref.at[i], sem) for i in range(y_ref.shape[0])]))


def deliver(ids, sums, x_mid, b_all, side, scale, collective_id):
    seq_len, depth = x_mid.shape
    rows = seq_len // 4
    y = pl.pallas_call(
        functools.partial(deliver_kernel, side, b_all.shape[1], scale),
        out_shape=pltpu.VMEM((2 * side * side, 2, 2, rows, depth), BF),
        in_specs=[SMEM] + [VMEM] * 2 + [HBM],
        scratch_shapes=[pltpu.VMEM(b_all.shape[:4] + b_all.shape[5:], BF), DMA, DMA, DMA] + GATHER_SEMS,
        compiler_params=comm_params(collective_id, VMEM_SMALL),
        name='deliver',
    )(ids, sums, x_mid, b_all)
    return pl.pallas_call(
        put_kernel,
        out_shape=jax.ShapeDtypeStruct(y.shape, BF),
        in_specs=[pl.BlockSpec(memory_space=pl.ANY)],
        out_specs=HBM,
        scratch_shapes=[DMA],
        compiler_params=pltpu.CompilerParams(vmem_limit_bytes=VMEM_LEAST),
        name='put',
    )(y)


def solution(mesh):
    tp_size = mesh.shape['tensor']
    side = math.isqrt(tp_size // 2)
    rows_only = P('tensor', None)
    head_split = P(None, 'tensor', None)
    last_split = P(None, None, 'tensor')
    b_head_split = P(None, None, 'tensor', None)
    in_specs = (P('data', None, None), P('data'), P(None), P(None),
                head_split, head_split, head_split, P('tensor', None, None),
                P(None, 'tensor'), P(None, 'tensor'), rows_only,
                last_split, b_head_split, last_split, b_head_split, last_split, b_head_split,
                P(None, 'tensor', None, None), last_split,
                last_split, last_split, last_split, last_split,
                head_split, last_split)

    def local_layer(x_in, adapter_ids, gain_attn, gain_mlp, w_q, w_k, w_v, w_o, w_gate, w_up, w_down, a_q, b_q, a_k, b_k, a_v, b_v, a_o, b_o, a_gate, b_gate, a_up, b_up, a_down, b_down):
        scale = ALPHA / b_q.shape[1]

        def across(a):
            return a.swapaxes(-1, -2)

        heads = [w[:, 0] for w in (w_q, w_k, w_v)] + [across(a) for a in (a_q, a_k, a_v)] + [b[:, :, 0] for b in (b_q, b_k, b_v)]
        sums, all_b = attend(adapter_ids, x_in, gain_attn, heads, w_o[0], a_o[:, 0], (b_o, b_down), side, scale, 0)

        w = [across(w_gate), across(w_up), across(b_gate), across(b_up), w_down, a_down]
        hidden, x_mid, w_d = gate_up(adapter_ids, sums, gain_mlp, x_in, all_b, (across(a_gate), across(a_up)), w, side, scale, 1)
        sums = row_proj(adapter_ids, hidden, w_d, *a_o.shape[::3], side, 2)
        y = deliver(adapter_ids, sums, x_mid, pltpu.with_memory_space_constraint(all_b, pltpu.HBM), side, scale, 3)
        return y.reshape(x_in.shape)

    return jax.shard_map(local_layer, mesh=mesh, in_specs=in_specs, out_specs=P('data', None, None), check_vma=False)
```

```python
import functools
import math

import jax
import jax.numpy as jnp
import numpy as np
from jax import lax
from jax.experimental import pallas as pl
from jax.experimental.pallas import tpu as pltpu
from jax.sharding import PartitionSpec as P

ALPHA = 16.0
ROPE_BASE = 10000.0
EPSILON = 1e-5
BF = jnp.bfloat16
F32 = jnp.float32
LANE = 128
TILE = 16
VMEM_MOST = 67043328
VMEM_SMALL = VMEM_MOST // 6
VMEM_LEAST = VMEM_MOST // 32
MESH = pl.DeviceIdType.MESH
HBM = pl.BlockSpec(memory_space=pltpu.HBM)
VMEM = pl.BlockSpec(memory_space=pltpu.VMEM)
SMEM = pl.BlockSpec(memory_space=pltpu.SMEM)
DMA = pltpu.SemaphoreType.DMA

OWN, NEXT, FAR, LAST = RING = range(4)
UP, DOWN = BOTH = range(2)
STEP = (NEXT, -NEXT)
FROM = (LAST, NEXT)
AWAY = (NEXT, LAST, FAR)
PAIRS = ((OWN, NEXT), (LAST, FAR))
TOWARD = (NEXT, LAST)
FAST, SLOW = BOTH


def fit(size, most):
    return max(c for c in range(LANE, most + 1, LANE) if size % c == 0)


def first(size):
    return pl.ds(0, size)


def dot(a, b):
    return jnp.dot(a, b, preferred_element_type=F32)


def dot_rows(a, b):
    return lax.dot_general(a, b, (((1,), (1,)), ((), ())), preferred_element_type=F32)


def dot_columns(a, b):
    return lax.dot_general(a, b, (((0,), (0,)), ((), ())), preferred_element_type=F32)


def normed(act, gain):
    return (act * lax.rsqrt(jnp.mean(act * act, axis=-1, keepdims=True) + EPSILON) * gain).astype(BF)


def ends(copies):
    for copy in copies:
        copy.start()
    return copies


def wait(copies):
    for copy in copies:
        copy.wait()


def loop(count, body):
    lax.fori_loop(0, count, lambda i, carry: (body(i), carry)[1], 0)


class Place:
    def __init__(self, side):
        index = lax.axis_index('tensor')
        self.side = side
        self.core = lax.rem(index, 2)
        chip = index // 2
        self.y, self.x = chip // side, lax.rem(chip, side)
        self.partner = index + 1 - 2 * self.core

    def turn(self, at, steps):
        return lax.rem(at + steps + self.side, self.side)

    def device(self, dy, dx):
        return (self.turn(self.y, dy) * self.side + self.turn(self.x, dx)) * 2 + self.core

    def neighbour(self, part, ring, step):
        return self.device(0, step) if part == ring else self.device(step, 0)

    def sequence(self, part, ds, df):
        return self.device(jnp.where(part == 0, ds, df), jnp.where(part == 0, df, ds))

    def rows(self, ref):
        return lambda part, ds: ref.at[part, :, self.turn(self.x, ds)] if part else ref.at[part, self.turn(self.y, ds)]

    def spot(self, part):
        return self.y if part else self.x

    def announce(self, *more):
        to = [self.neighbour(0, ring, step) for ring in BOTH for step in STEP] + list(more)
        for device in to:
            pl.semaphore_signal(pltpu.get_barrier_semaphore(), inc=1, device_id={'tensor': device}, device_id_type=MESH)
        self.announced = len(to)

    def meet(self):
        pl.semaphore_wait(pltpu.get_barrier_semaphore(), self.announced)


def remote(src, dst, send_sem, recv_sem, to):
    return pltpu.make_async_remote_copy(src_ref=src, dst_ref=dst, send_sem=send_sem, recv_sem=recv_sem, device_id={'tensor': to}, device_id_type=MESH)


GATHER_SEMS = [DMA((2, 2, 2, 2, 4))] * 2


class Gather:
    def __init__(self, place, block, send_sem, recv_sem, absolute=False, seen=None):
        self.place, self.block, self.sems, self.absolute, self.seen = place, block, (send_sem, recv_sem), absolute, seen

    def message(self, part, ring, passed, d, j=OWN):
        spot = (lambda s: (s, j)) if ring == SLOW else (lambda s: (OWN, s))
        src, dst = (FROM[d], FAR) if passed else (OWN, FROM[d])
        a, b = self.block(part, *spot(src)), self.block(part, *spot(src if self.absolute else dst))
        if passed:
            a, b = a.at[d], b.at[d]
        return remote(a, b, *(sem.at[part, ring, passed, d, j] for sem in self.sems), self.place.neighbour(part, ring, STEP[d]))

    def arrived(self, part, ring, passed, d, j=OWN):
        self.message(part, ring, passed, d, j).wait_recv()
        if self.seen:
            at = FAR if passed else FROM[d]
            self.seen(part, *((at, j) if ring == SLOW else (OWN, at)), d if passed else None)

    def own(self, *rings):
        for ring in rings:
            for d in BOTH:
                for part in BOTH:
                    self.message(part, ring, 0, d).start()

    def near(self):
        for d in BOTH:
            for part in BOTH:
                self.arrived(part, FAST, 0, d)
                self.message(part, FAST, 1, d).start()
                for e in BOTH:
                    self.message(part, SLOW, 0, e, FROM[d]).start()

    def row(self):
        for part in BOTH:
            for d in BOTH:
                self.arrived(part, FAST, 1, d)
            for e in BOTH:
                self.message(part, SLOW, 0, e, FAR).start()
        self.sides(OWN)

    def sides(self, *blocks):
        for j in blocks:
            for part in BOTH:
                for d in BOTH:
                    self.arrived(part, SLOW, 0, d, j)
                    self.message(part, SLOW, 1, d, j).start()

    def far(self, *blocks):
        for j in blocks:
            for part in BOTH:
                for d in BOTH:
                    self.arrived(part, SLOW, 1, d, j)

    def sent(self):
        for part in BOTH:
            for d in BOTH:
                for passed in BOTH:
                    self.message(part, FAST, passed, d).wait_send()
                    for j in RING:
                        self.message(part, SLOW, passed, d, j).wait_send()


ROW_SEMS = [DMA((2, 2, 2, 2))] * 2


class RowGather:
    def __init__(self, place, row, mine, send_sem, recv_sem):
        self.place, self.row_at, self.mine, self.sems = place, row, mine, (send_sem, recv_sem)

    def message(self, part, ring, passed, d):
        if ring == SLOW:
            ref = self.row_at(part, FROM[d] if passed else OWN)
            ref = ref.at[:, d] if passed else ref
        else:
            ref = self.row_at(part, OWN).at[self.place.turn(self.mine(part), FROM[d] if passed else OWN)]
            ref = ref.at[d] if passed else ref
        return remote(ref, ref, *(sem.at[part, ring, passed, d] for sem in self.sems), self.place.neighbour(part, ring, STEP[d]))

    def pass_on(self, ring, passed):
        for part in BOTH:
            for d in BOTH:
                self.landing(part, ring, passed, d).wait_recv()
                if not passed:
                    self.message(part, ring, 1, d).start()
            if passed and ring == FAST:
                for d in BOTH:
                    self.message(part, SLOW, 0, d).start()

    def landing(self, part, ring, passed, d):
        at = FAR if passed else FROM[d]
        ref = self.row_at(part, at) if ring == SLOW else self.row_at(part, OWN).at[self.place.turn(self.mine(part), at)]
        if passed:
            ref = ref.at[:, d] if ring == SLOW else ref.at[d]
        return remote(ref, ref, *(sem.at[part, ring, passed, d] for sem in self.sems), self.place.neighbour(part, ring, STEP[d]))

    def own(self):
        for d in BOTH:
            for part in BOTH:
                self.message(part, FAST, 0, d).start()

    def near(self):
        self.pass_on(FAST, 0)

    def row(self):
        self.pass_on(FAST, 1)

    def sides(self):
        self.pass_on(SLOW, 0)

    def far(self):
        self.pass_on(SLOW, 1)

    def sent(self):
        for part in BOTH:
            for ring in BOTH:
                for passed in BOTH:
                    for d in BOTH:
                        self.message(part, ring, passed, d).wait_send()


def rows_of_adapter(place, ids_ref, part, ds, shape):
    block = lax.broadcasted_iota(jnp.int32, shape, 0) // (shape[0] // len(RING))
    chosen = jnp.zeros(shape, jnp.int32)
    for df in RING:
        chosen = jnp.where(block == df, ids_ref[place.sequence(part, ds, df)], chosen)
    return chosen


def pick_columns(low, chosen):
    rank = chosen.shape[1]
    kept = low[:, :rank]
    for a in range(1, low.shape[1] // rank):
        kept = jnp.where(chosen == a, low[:, a * rank:(a + 1) * rank], kept)
    return kept


def spread(low, chosen, adapters):
    return jnp.concatenate([jnp.where(chosen == a, low, 0.0) for a in range(adapters)], axis=1).astype(BF)


PASS, FREE, SUM = range(3)
FAST_SEMS = [DMA((2, 3, 2))] * 2


def add(into, *others):
    def some(i):
        at = pl.ds(pl.multiple_of(i * TILE, TILE), TILE)
        total = into[at, :].astype(F32)
        for other in others:
            total += other[at, :].astype(F32)
        into[at, :] = total.astype(BF)

    loop(into.shape[0] // TILE, some)


class FastScatter:
    def __init__(self, place, stage, near, landed, send_sem, recv_sem):
        self.place, self.stage, self.near, self.landed, self.sems = place, stage, near, landed, (send_sem, recv_sem)
        quarter = near.shape[2]
        self.halves = (first(quarter), pl.ds(quarter, quarter))

    def message(self, part, kind, d):
        at = self.halves[1 - d] if kind == FREE else self.halves[d]
        src = self.stage(part, FAR if kind == PASS else TOWARD[d]).at[at]
        dst = self.near.at[part, d] if kind == PASS else self.landed.at[part, d, at]
        sems = [sem.at[part, kind, d] for sem in self.sems]
        return remote(src, dst, *sems, self.place.neighbour(part, FAST, STEP[d]))

    def ready(self, part, df):
        for d in BOTH:
            if df == FAR:
                self.message(part, PASS, d).start()
            elif df == TOWARD[d]:
                self.message(part, FREE, d).start()

    def sum(self):
        for d in BOTH:
            for part in BOTH:
                self.message(part, PASS, d).wait_recv()
                add(self.stage(part, TOWARD[d]).at[self.halves[d]], self.near.at[part, d])
                self.message(part, SUM, d).start()

    def finish(self):
        for part in BOTH:
            for d in BOTH:
                self.message(part, FREE, d).wait_recv()
                self.message(part, SUM, d).wait_recv()
            add(self.stage(part, OWN), self.landed.at[part, UP], self.landed.at[part, DOWN])

    def store(self, out_ref):
        rows = self.landed.shape[2]
        for part in BOTH:
            out_ref[part * rows:(part + 1) * rows] = self.stage(part, OWN)[...]
        for part in BOTH:
            for kind in range(3):
                for d in BOTH:
                    self.message(part, kind, d).wait_send()


def fast_scratch(rows, cols):
    return [pltpu.VMEM((2, 2, rows // 2, cols), BF), pltpu.VMEM((2, 2, rows, cols), BF)]


def comm_params(collective_id, limit=VMEM_MOST):
    return pltpu.CompilerParams(collective_id=collective_id, has_side_effects=True, vmem_limit_bytes=limit)


WO_CHUNKS = 8
X_SLOTS = 3


def attend_kernel(side, adapters, scale, ids_ref, x_ref, gain_ref, cos_ref, sin_ref, *rest):
    w_heads, a_heads, b_heads, (wo_ref, ao_ref), a_mlp, b_rows, rest = rest[:3], rest[3:6], rest[6:9], rest[9:11], rest[11:13], rest[13:15], rest[15:]
    (out_ref, a_all, b_all), rest = rest[:3], rest[3:]
    (w, a_raw, b_raw, a_rows, bx, xbuf, h, z, lows, att, act, wo, stage, near, landed, am_raw, a_mine, b_mine, pair_send, pair_recv, load_sem, x_sem, own_sem,
     kept_sem, hand_send, hand_recv, wo_load, wo_send, wo_recv, bulk_send, bulk_recv, swap_send, swap_recv,
     send_sem, recv_sem, a_send, a_recv, b_send, b_recv, fast_send, fast_recv) = rest
    place = Place(side)
    place.announce(place.partner, place.device(0, FAR), place.device(FAR, 0))
    head, seq_len, depth = cos_ref.shape[1], x_ref.shape[1], x_ref.shape[2]
    cols = len(w_heads) * head
    chips = side * side
    per = a_raw.shape[3]
    loads = ends([pltpu.make_async_copy(src, dst, load_sem) for i in range(3) for src, dst in
                  ((a_heads[i], a_raw.at[place.core, i]), (w_heads[i], w.at[:, pl.ds(i * head, head)]), (b_heads[i], b_raw.at[0, i]))])
    steps = chips // 2

    def x_loads(step):
        slot = lax.rem(step, X_SLOTS)
        return [pltpu.make_async_copy(x_ref.at[4 * lax.rem(step, steps) + 2 * i + place.core], xbuf.at[slot, i], x_sem.at[slot]) for i in BOTH]

    for step in range(X_SLOTS - 1):
        ends(x_loads(step))

    own_loads = ends([pltpu.make_async_copy(a_mlp[i], am_raw.at[i], own_sem) for i in BOTH] +
                     [pltpu.make_async_copy(b_rows[half].at[part], b_mine.at[part, place.y, place.x, half], own_sem) for part in BOTH for half in BOTH])
    width = wo_ref.shape[1]
    rank = ao_ref.shape[2]
    wo_loads = []
    for part in BOTH:
        wo_loads.append(pltpu.make_async_copy(wo_ref, wo.at[part, OWN, 0, :, first(width)], wo_load))
        for a in range(adapters):
            wo_loads.append(pltpu.make_async_copy(ao_ref.at[a], wo.at[part, OWN, 0, :, pl.ds(width + a * rank, rank)], wo_load))
    ends(wo_loads)
    wait(own_loads)
    wait(loads)
    am_rows = jnp.concatenate([am_raw[i, a] for i in BOTH for a in range(adapters)], axis=0)
    for i in RING:
        a_mine[i // 2, place.y, place.x, i % 2] = am_rows[:, i * depth // 4:(i + 1) * depth // 4]
    place.meet()
    moves = [(a_raw.at[place.core], a_raw.at[place.core]), (w.at[:, first(cols)], w.at[:, pl.ds(cols, cols)]), (b_raw.at[0], b_raw.at[1])]
    pair = ends([remote(src, dst, pair_send.at[i], pair_recv.at[i], place.partner) for i, (src, dst) in enumerate(moves)])

    piece = head // WO_CHUNKS

    def wo_message(part, passed, d, i):
        src, dst = (wo.at[part, s, 0, pl.ds(i * piece, piece)] for s in ((FROM[d], FAR) if passed else (OWN, FROM[d])))
        sems = (part, passed, d, i)
        return remote(src, dst, wo_send.at[sems], wo_recv.at[sems], place.neighbour(part, SLOW, STEP[d]))

    def wo_to_partner(part, s):
        remote(wo.at[part, s, 0], wo.at[part, s, 1], bulk_send, bulk_recv, place.partner).start()

    passes = [range(d * WO_CHUNKS // 2, (d + 1) * WO_CHUNKS // 2) for d in BOTH]

    def wo_start(i):
        for d in BOTH:
            for part in BOTH:
                wo_message(part, 0, d, i).start()

    def wo_pass(k):
        for d in BOTH:
            for part in BOTH:
                wo_message(part, 0, d, passes[d][k]).wait_recv()
                wo_message(part, 1, d, passes[d][k]).start()

    def wo_arrived():
        for d in BOTH:
            for part in BOTH:
                for i in passes[1 - d]:
                    wo_message(part, 0, d, i).wait_recv()
                wo_to_partner(part, FROM[d])

    def wo_last():
        for part in BOTH:
            for d in BOTH:
                for i in passes[d]:
                    wo_message(part, 1, d, i).wait_recv()
            wo_to_partner(part, FAR)

    wait(wo_loads)
    early = WO_CHUNKS // 2
    gathers = [RowGather(place, place.rows(a_mine), place.spot, a_send, a_recv), RowGather(place, place.rows(b_mine), place.spot, b_send, b_recv)]

    def both(stage_of):
        for g in gathers:
            getattr(g, stage_of)()

    def hand(*distances):
        for ds in distances:
            for part in BOTH:
                for i, dst in enumerate((a_all, b_all)):
                    here, there = gathers[i].row_at(part, ds), place.rows(dst.at[place.core])(part, ds)
                    pltpu.make_async_copy(here, there, kept_sem.at[i]).start()
                    remote(here, there, hand_send.at[i], hand_recv.at[i], place.partner).start()

    both('own')
    for i in range(early):
        wo_start(i)
    pair[0].wait_recv()
    for core in BOTH:
        pieces = [a_raw[core, i, a] if i < len(w_heads) else jnp.zeros((per, depth), BF) for a in range(adapters) for i in RING]
        a_rows[core * 2 * TILE:(core + 1) * 2 * TILE, :] = jnp.concatenate(pieces, axis=0)
    mine = [(place.y, place.x), (place.x, place.y)]

    low_gather = RowGather(place, lambda part, ds: lows.at[part, place.turn(mine[part][0], ds)], place.spot, send_sem, recv_sem)

    def norm(step, last):
        slot = lax.rem(step, X_SLOTS)

        @pl.when(step + X_SLOTS - 1 < last)
        def _():
            ends(x_loads(step + X_SLOTS - 1))

        wait(x_loads(step))
        for i in BOTH:
            h[i * seq_len:(i + 1) * seq_len, :] = normed(xbuf[slot, i].astype(F32), gain_ref[...])

    def products(step):
        pl.when(step == 3)(lambda: both('near'))
        norm(step, 2 * steps)
        low = dot_rows(a_rows[...], h[...])
        half, at = step // (steps // 2), lax.rem(step, steps // 2) * 2 * seq_len
        for part in BOTH:
            pieces = []
            for i in BOTH:
                options = [low[TILE * (2 * part + a):TILE * (2 * part + a + 1), i * seq_len:(i + 1) * seq_len] for a in range(adapters)]
                chosen = options[0]
                for a in range(1, adapters):
                    chosen = jnp.where(ids_ref[4 * step + 2 * i + place.core] == a, options[a], chosen)
                pieces.append(chosen)
            lows[part, mine[part][0], mine[part][1], half, :, pl.ds(pl.multiple_of(at, LANE), 2 * seq_len)] = jnp.concatenate(pieces, axis=1).astype(BF)

    loop(steps, products)
    low_gather.own()
    for copy in pair[1:]:
        copy.wait_recv()
    for part in BOTH:
        wo_to_partner(part, OWN)
    events = {0: lambda: wo_start(early), 3: lambda: (low_gather.near(), wo_start(early + 1)), 7: lambda: (low_gather.row(), wo_start(early + 2)),
              14: lambda: (low_gather.sides(), wo_start(early + 3))}

    def happen(half_step):
        for at, what in events.items():
            pl.when(half_step == at)(lambda what=what: (what(), None)[1])

    def project(step):
        happen(2 * step)
        norm(step + steps, 2 * steps)
        happen(2 * step + 1)
        rows = pl.ds(pl.multiple_of(step * 2 * seq_len, LANE), 2 * seq_len)
        chunk = fit(2 * cols, 256)
        for n in range(2 * cols // chunk):
            z[rows, n * chunk:(n + 1) * chunk] = dot(h[...], w[:, n * chunk:(n + 1) * chunk])

    loop(steps, project)
    row, col = (lax.broadcasted_iota(jnp.int32, (2 * rank, rank), axis) for axis in BOTH)
    spot, kind = row // TILE, lax.rem(row, TILE) // per
    for part in BOTH:
        chip_of = spot if part == 0 else lax.rem(spot, side) * side + spot // side
        to = chip_of * 2 * per + part * per + lax.rem(row, per)
        for i in range(3):
            spread_rows = jnp.where((kind == i) & (col == to), 1.0, 0.0).astype(BF)
            for a in range(adapters):
                for o in BOTH:
                    bx[a, part, :, o * cols + i * head:o * cols + (i + 1) * head] = dot(spread_rows, b_raw[o, i, a]).astype(BF)
    wo_pass(0)
    wo_pass(1)
    low_gather.far()
    wo_pass(2)
    wo_pass(3)
    causal = lax.broadcasted_iota(jnp.int32, (seq_len, seq_len), 0) >= lax.broadcasted_iota(jnp.int32, (seq_len, seq_len), 1)

    def swap(part, ds):
        sems = (part, ds)
        to = place.neighbour(part, SLOW, ds)
        return remote(att.at[sems], act.at[part, lax.rem(len(RING) - ds, len(RING))], swap_send.at[sems], swap_recv.at[sems], to)

    def attention(i):
        dy, dx = side - 1 - i // side, side - 1 - lax.rem(i, side)
        chip = place.turn(place.y, dy) * side + place.turn(place.x, dx)
        adapter = ids_ref[2 * chip + place.core]
        half, at = chip // steps, pl.ds(pl.multiple_of(lax.rem(chip, steps) * seq_len, LANE), seq_len)
        zs = z[pl.ds(pl.multiple_of(chip * seq_len, LANE), seq_len), :]
        for part in BOTH:
            zs += scale * dot_columns(lows[part, :, :, half, :, at].reshape(-1, seq_len), bx[adapter, part])
        for i_head in BOTH:
            q, k, v = (zs[:, i_head * cols + i * head:i_head * cols + (i + 1) * head] for i in range(3))
            q, k = ((r * cos_ref[...] + pltpu.roll(r, head // 2, axis=1) * sin_ref[...]).astype(BF) for r in (q, k))
            scores = jnp.where(causal, dot_rows(q, k) * head ** -0.5, -1e30)
            e = jnp.exp(scores - jnp.max(scores, axis=-1, keepdims=True))
            prob = (e / jnp.sum(e, axis=-1, keepdims=True)).astype(BF)
            mixed = dot(prob, v.astype(BF)).astype(BF)
            for part, (ds, df) in enumerate(((dy, dx), (dx, dy))):
                att[part, ds, df, :, i_head * head:(i_head + 1) * head] = mixed[part * seq_len // 2:(part + 1) * seq_len // 2]

    def attention_pair(k):
        for i in BOTH:
            attention(2 * k + i)
        row = side - 1 - 2 * k // side
        pl.when((lax.rem(2 * k + 2, side) == 0) & (row != OWN))(lambda: swap(0, row).start())

    loop(chips // 2, attention_pair)
    for ds in AWAY:
        swap(1, ds).start()
    both('row')
    hand(OWN)
    wo_arrived()
    wo_last()
    for part in BOTH:
        act[part, OWN] = att[part, OWN]
    pltpu.make_async_copy(wo.at[:, :, 1], wo.at[:, :, 1], bulk_recv).wait()
    chunk = fit(width, 512)
    rows = seq_len // 2
    blocks = (len(RING), rows)
    fast = FastScatter(place, lambda part, df: stage.at[part, df], near, landed, fast_send, fast_recv)

    def sum_heads(part, at):
        return sum(dot(act[part, s].reshape(-1, 2 * head), wo[part, s, :, :, at].reshape(2 * head, -1)) for s in RING)

    for part in BOTH:
        for ds in AWAY:
            swap(part, ds).wait_recv()

        def columns(n):
            at = pl.ds(pl.multiple_of(n * chunk, chunk), chunk)
            stage[part, :, :, at] = sum_heads(part, at).reshape(blocks + (chunk,)).astype(BF)

        loop(width // chunk, columns)
        chosen = rows_of_adapter(place, ids_ref, part, OWN, (len(RING) * rows, rank))
        stage[part, :, :, width:] = pick_columns(sum_heads(part, pl.ds(width, adapters * rank)), chosen).reshape(blocks + (rank,)).astype(BF)
        for df in (FAR, NEXT, LAST):
            fast.ready(part, df)
    both('sides')
    hand(NEXT, LAST)
    fast.sum()
    both('far')
    hand(FAR)
    fast.finish()
    fast.store(out_ref)
    for sem in (kept_sem, hand_send, hand_recv):
        for i, ref in enumerate((a_mine, b_mine)):
            pltpu.make_async_copy(ref, ref, sem.at[i]).wait()
    for copy in pair:
        copy.wait_send()
    for g in gathers + [low_gather]:
        g.sent()
    pltpu.make_async_copy(wo.at[:, :, 1], wo.at[:, :, 1], bulk_send).wait()
    for part in BOTH:
        for d in BOTH:
            for i in range(WO_CHUNKS):
                wo_message(part, 0, d, i).wait_send()
            for i in passes[d]:
                wo_message(part, 1, d, i).wait_send()
        for ds in AWAY:
            swap(part, ds).wait_send()


def attend(ids, x_in, gain, heads, w_o, a_o, a_mlp, b_rows, side, scale, collective_id):
    _, seq_len, depth = x_in.shape
    head = heads[0].shape[1]
    cols = 3 * head
    adapters, _, rank = a_o.shape
    per = heads[3].shape[1]
    chips = side * side
    half_dim = head // 2
    inv_freq = ROPE_BASE ** (-2.0 * np.arange(half_dim) / head)
    angle = np.arange(seq_len)[:, None] * inv_freq[None, :]
    cos, sin = np.cos(angle), np.sin(angle)
    tables = [jnp.asarray(np.concatenate(pair, axis=1), F32) for pair in ((cos, cos), (-sin, sin))]
    n_pair = 3
    rows, out_cols = seq_len // 2, depth + rank
    every = (2, 2, side, side, 2)
    return pl.pallas_call(
        functools.partial(attend_kernel, side, adapters, scale),
        out_shape=[jax.ShapeDtypeStruct((seq_len, out_cols), BF), jax.ShapeDtypeStruct(every + (2 * adapters * per, depth // 4), BF),
                   jax.ShapeDtypeStruct(every + b_rows[0].shape[1:], BF)],
        in_specs=[SMEM, HBM, VMEM, VMEM, VMEM] + [HBM] * (len(heads) + 6),
        out_specs=[VMEM] + [HBM] * 2,
        scratch_shapes=[
            pltpu.VMEM((depth, 2 * cols), BF),
            pltpu.VMEM((2, 3, adapters, per, depth), BF),
            pltpu.VMEM((2, 3, adapters, rank, head), BF),
            pltpu.VMEM((2 * 2 * TILE, depth), BF),
            pltpu.VMEM((adapters, 2, 2 * rank, 2 * cols), BF),
            pltpu.VMEM((X_SLOTS, 2, seq_len, depth), BF),
            pltpu.VMEM((2 * seq_len, depth), BF),
            pltpu.VMEM((chips * seq_len, 2 * cols), F32),
            pltpu.VMEM((2, side, side, 2, TILE, chips * seq_len // 2), BF),
            pltpu.VMEM((2, side, side, rows, 2 * head), BF),
            pltpu.VMEM((2, side, side, rows, 2 * head), BF),
            pltpu.VMEM((2, side, 2, head, depth + adapters * rank), BF),
            pltpu.VMEM((2, side, rows, out_cols), BF),
        ] + fast_scratch(rows, out_cols) + [
            pltpu.VMEM((2, adapters, per, depth), BF),
            pltpu.VMEM(every[1:] + (2 * adapters * per, depth // 4), BF),
            pltpu.VMEM(every[1:] + b_rows[0].shape[1:], BF),
            DMA((n_pair,)), DMA((n_pair,)), DMA, DMA((X_SLOTS,)), DMA, DMA((2,)), DMA((2,)), DMA((2,)), DMA, DMA((2, 2, 2, WO_CHUNKS)), DMA((2, 2, 2, WO_CHUNKS)), DMA, DMA, DMA((2, 4)), DMA((2, 4)),
        ] + ROW_SEMS * 3 + FAST_SEMS,
        compiler_params=comm_params(collective_id),
        name='attend',
    )(ids, x_in, gain.reshape(1, depth), *tables, *heads, w_o, a_o, *a_mlp, *b_rows)


def row_proj_kernel(side, adapters, rank, ids_ref, act, w, out_ref, stage, near, landed, fast_near, fast_landed, slow_send, slow_recv, fast_send, fast_recv):
    place = Place(side)
    place.announce()
    rows, cols = stage.shape[3:]
    quarter = rows // 2
    width = cols - rank
    chunk = fit(width, 1024)

    def unit(part, ds):
        def columns(n):
            at = pl.ds(pl.multiple_of(n * chunk, chunk), chunk)
            stage[part, ds, :, :, at] = dot(act[part, ds], w[:, at]).reshape(len(RING), rows, chunk).astype(BF)

        loop(width // chunk, columns)
        chosen = rows_of_adapter(place, ids_ref, part, ds, (len(RING) * rows, rank))
        stage[part, ds, :, :, width:] = pick_columns(dot(act[part, ds], w[:, width:]), chosen).reshape(len(RING), rows, rank).astype(BF)

    blocks = ((FAR, LAST), (OWN, NEXT))

    def slow(part, kind, d, i):
        df = blocks[1 - d][i] if kind == FREE else blocks[d][i]
        sems = (part, kind, d, i)
        src = stage.at[part, FAR if kind == PASS else TOWARD[d], df]
        dst = near.at[part, d, i] if kind == PASS else landed.at[part, d, df]
        return remote(src, dst, slow_send.at[sems], slow_recv.at[sems], place.neighbour(part, SLOW, STEP[d]))

    fast = FastScatter(place, lambda part, df: stage.at[part, OWN, df], fast_near, fast_landed, fast_send, fast_recv)
    for part in BOTH:
        unit(part, FAR)
        if part == 0:
            place.meet()
        for i in BOTH:
            for d in BOTH:
                slow(part, PASS, d, i).start()
    loop(len(RING), lambda i: unit(lax.rem(i, 2), NEXT + 2 * (i // 2)))
    for i in BOTH:
        for d in BOTH:
            for part in BOTH:
                slow(part, FREE, d, i).start()
    loop(2, lambda part: unit(part, OWN))
    for i in BOTH:
        for d in BOTH:
            for part in BOTH:
                slow(part, PASS, d, i).wait_recv()
                add(stage.at[part, TOWARD[d], blocks[d][i]], near.at[part, d, i])
                slow(part, SUM, d, i).start()
    for i in BOTH:
        for d in BOTH:
            df = blocks[d][i]
            for part in BOTH:
                slow(part, SUM, d, i).wait_recv()
                slow(part, FREE, 1 - d, i).wait_recv()
                add(stage.at[part, OWN, df], landed.at[part, UP, df], landed.at[part, DOWN, df])
                fast.ready(part, df)
    fast.sum()
    fast.finish()
    fast.store(out_ref)
    for part in BOTH:
        for kind in range(3):
            for d in BOTH:
                for i in BOTH:
                    slow(part, kind, d, i).wait_send()


def row_proj(ids, act, w, adapters, rank, side, collective_id):
    rows = act.shape[2] // side
    cols = w.shape[1] - (adapters - 1) * rank
    blocks = (rows, cols)
    return pl.pallas_call(
        functools.partial(row_proj_kernel, side, adapters, rank),
        out_shape=pltpu.VMEM((2 * rows, cols), BF),
        in_specs=[SMEM, VMEM, VMEM],
        out_specs=VMEM,
        scratch_shapes=[
            pltpu.VMEM((2, side, side) + blocks, BF),
            pltpu.VMEM((2, 2, 2) + blocks, BF),
            pltpu.VMEM((2, 2, side) + blocks, BF),
        ] + fast_scratch(rows, cols) + [DMA((2, 3, 2, 2))] * 2 + FAST_SEMS,
        compiler_params=comm_params(collective_id, VMEM_MOST * 5 // 8),
        name='row_proj',
    )(ids, act, w)


def finish(sums_ref, resid, b_ref, chosen, scale, adapters):
    _, _, side, _, rank, part = b_ref.shape
    width = sums_ref.shape[1] - rank
    low = spread(sums_ref[:, width:].astype(F32), chosen, adapters)
    delta = [dot(low, b_ref[core, :, y, x].reshape(adapters * rank, part)) for y in range(side) for x in range(side) for core in BOTH]
    return resid.astype(F32) + (sums_ref[:, :width].astype(F32) + scale * jnp.concatenate(delta, axis=1))


def own_rows(place, ids_ref, shape):
    return jnp.full(shape, ids_ref[place.device(0, 0)], jnp.int32)


def gate_up_kernel(side, adapters, scale, ids_ref, sums_ref, gain_ref, x_all, a_all, b_all, wg_ref, wu_ref, bg_ref, bu_ref, wd_ref, ad_ref,
                   hid, mid_ref, wd, gbuf, raw, w, b, bx, x_ref, a_ref, a_cols, b_ref, raw_sem, load_sem, a_sem, b_sem, credit, pair_send, pair_recv, send_sem, recv_sem):
    place = Place(side)
    share, width = wg_ref.shape
    half = raw.shape[1]
    rank = bg_ref.shape[2]
    seq_len = sums_ref.shape[0]
    edge = share // TILE * TILE
    for i in BOTH:
        raw[i, edge:] = jnp.zeros((half - edge, width), BF)
        for kind in BOTH:
            b[kind, i * half + edge:(i + 1) * half] = jnp.zeros((half - edge, adapters * rank), BF)
        wd[i * half + edge:(i + 1) * half] = jnp.zeros((half - edge, wd.shape[1]), BF)
    place.announce(place.partner)
    b_load = ends([pltpu.make_async_copy(b_all.at[:, :, :, :, 0], b_ref, b_sem), pltpu.make_async_copy(x_all.at[place.device(0, 0)], x_ref, b_sem)])
    a_load = ends([pltpu.make_async_copy(a_all, a_ref, a_sem)])
    mine = first(share)

    def raw_load(kind):
        return pltpu.make_async_copy((wg_ref, wu_ref)[kind], raw.at[0, mine], raw_sem)

    raw_load(0).start()
    loads = [pltpu.make_async_copy(wd_ref, wd.at[mine, first(width)], load_sem)]
    for a in range(adapters):
        loads.append(pltpu.make_async_copy(ad_ref.at[a], wd.at[mine, pl.ds(width + a * rank, rank)], load_sem))
        for kind, ref in enumerate((bg_ref, bu_ref)):
            loads.append(pltpu.make_async_copy(ref.at[a], b.at[kind, mine, pl.ds(a * rank, rank)], load_sem))
    ends(loads)
    other = pl.ds(half, share)
    moves = [(raw.at[0, mine], raw.at[1, mine])] * 2 + [(wd.at[mine], wd.at[other])] + [(b.at[kind, mine], b.at[kind, other]) for kind in BOTH]
    pair = [remote(src, dst, pair_send.at[i], pair_recv.at[i], place.partner) for i, (src, dst) in enumerate(moves)]
    rows = seq_len // 4
    chosen = own_rows(place, ids_ref, (seq_len, rank))
    wait(b_load)
    mid = finish(sums_ref, x_ref[...], b_ref, chosen, scale, adapters).astype(BF)
    mid_ref[...] = mid
    h2 = normed(mid.astype(F32), gain_ref[...])
    for part in BOTH:
        for piece in BOTH:
            at = (2 * part + piece) * rows
            gbuf[part, OWN, OWN, piece] = h2[at:at + rows]
    place.meet()
    chunk = fit(2 * half, 256)

    group, quarter = a_ref.shape[5:]
    n_low = 2 * side * side * group
    per = group // (2 * adapters)

    def unit(ds, blocks=RING):
        lo, hi = min(blocks), max(blocks) + 1
        unit_rows = (hi - lo) * 2 * rows
        act_of = lambda: gbuf[:, ds, lo:hi].reshape(2 * unit_rows, width)
        chosen = jnp.concatenate([rows_of_adapter(place, ids_ref, part, ds, (len(RING) * 2 * rows, n_low))[lo * 2 * rows:hi * 2 * rows] for part in BOTH], axis=0)
        adapter = lax.rem(lax.broadcasted_iota(jnp.int32, chosen.shape, 1) // per, adapters)
        lows = jnp.where(adapter == chosen, dot(act_of(), a_cols[...]), 0.0).astype(BF)

        def columns(n):
            at = pl.ds(pl.multiple_of(n * chunk, chunk), chunk)
            act = act_of()
            gate, up = (dot(act, w[kind, :, at]) + scale * dot_rows(lows, bx[kind, at]) for kind in BOTH)
            hid[:, ds, lo * 2 * rows:hi * 2 * rows, at] = (gate * jax.nn.sigmoid(gate) * up).astype(BF).reshape(2, unit_rows, chunk)

        loop(2 * half // chunk, columns)

    gather = Gather(place, lambda part, ds, df: gbuf.at[part, ds, df], send_sem, recv_sem)
    gather.own(*BOTH)
    def turned(kind, i):
        def turn(n):
            at = pl.ds(pl.multiple_of(n * LANE, LANE), LANE)
            w[kind, at, i * half:(i + 1) * half] = raw[i, :, at].T

        loop(width // LANE, turn)

    for kind in BOTH:
        raw_load(kind).wait()
        if kind:
            pl.semaphore_wait(credit, 1)
        pair[kind].start()
        turned(kind, 0)
        if kind == 0:
            wait(loads)
            ends(pair[2:])
        pair[kind].wait_recv()
        turned(kind, 1)
        pair[kind].wait_send()
        if kind == 0:
            pl.semaphore_signal(credit, inc=1, device_id={'tensor': place.partner}, device_id_type=MESH)
            raw_load(1).start()
    gather.near()
    wait(a_load)
    for copy in pair[2:]:
        copy.wait_recv()
    row, col = (lax.broadcasted_iota(jnp.int32, (adapters * rank, n_low), axis) for axis in BOTH)
    core, chip = col // (n_low // 2), lax.rem(col, n_low // 2) // group
    kind_of, a_of = lax.rem(col, group) // (group // 2), lax.rem(col // per, adapters)
    to = a_of * rank + chip * 2 * per + core * per + lax.rem(col, per)
    for kind in BOTH:
        bx[kind] = dot(b[kind], jnp.where((row == to) & (kind_of == kind), 1.0, 0.0).astype(BF)).astype(BF)
    for core in BOTH:
        for i in RING:

            def turn_a(n):
                at = pl.ds(pl.multiple_of(n * LANE, LANE), LANE)
                to = pl.ds(pl.multiple_of(i * quarter + n * LANE, LANE), LANE)
                a_cols[to, core * n_low // 2:(core + 1) * n_low // 2] = a_ref[core, i // 2, :, :, i % 2, :, at].reshape(n_low // 2, LANE).T

            loop(quarter // LANE, turn_a)
    gather.row()
    unit(OWN)
    for blocks in PAIRS:
        gather.sides(*(j for j in blocks if j != OWN))
        loop(2, lambda i: unit(NEXT + 2 * i, blocks))
    for blocks in PAIRS:
        gather.far(*blocks)
        unit(FAR, blocks)
    gather.sent()
    for copy in pair[2:]:
        copy.wait_send()


def gate_up(ids, sums, gain, x_in, a_all, b_all, w, side, scale, collective_id):
    _, seq_len, depth = x_in.shape
    share = w[0].shape[0]
    adapters, _, rank = w[2].shape
    half = (share + LANE - 1) // LANE * LANE
    hidden = (2, side, side * seq_len // 2, 2 * half)
    n_low = 2 * adapters * rank
    return pl.pallas_call(
        functools.partial(gate_up_kernel, side, adapters, scale),
        out_shape=[pltpu.VMEM(hidden, BF), pltpu.VMEM((seq_len, depth), BF), pltpu.VMEM((2 * half, depth + adapters * rank), BF)],
        in_specs=[SMEM] + [VMEM] * 2 + [HBM] * (3 + len(w)),
        out_specs=[VMEM] * 3,
        scratch_shapes=[
            pltpu.VMEM((2, side, side, 2, seq_len // 4, depth), BF),
            pltpu.VMEM((2, half, depth), BF),
            pltpu.VMEM((2, depth, 2 * half), BF),
            pltpu.VMEM((2, 2 * half, adapters * rank), BF),
            pltpu.VMEM((2, 2 * half, n_low), BF),
            pltpu.VMEM((seq_len, depth), BF),
            pltpu.VMEM(a_all.shape, BF),
            pltpu.VMEM((depth, n_low), BF),
            pltpu.VMEM(b_all.shape[:4] + b_all.shape[5:], BF),
            DMA, DMA, DMA, DMA, pltpu.SemaphoreType.REGULAR, DMA((5,)), DMA((5,)),
        ] + GATHER_SEMS,
        compiler_params=comm_params(collective_id, VMEM_MOST * 51 // 64),
        name='gate_up',
    )(ids, sums, gain.reshape(1, depth), x_in, a_all, b_all, *w)


def deliver_kernel(side, adapters, scale, ids_ref, sums_ref, x_ref, b_all, out_ref, b_ref, b_sem, pair_send, pair_recv, send_sem, recv_sem):
    place = Place(side)
    place.announce(place.partner)
    b_load = ends([pltpu.make_async_copy(b_all.at[:, :, :, :, 1], b_ref, b_sem)])
    seq_len = sums_ref.shape[0]
    rows = seq_len // 4
    chosen = own_rows(place, ids_ref, (seq_len, b_ref.shape[4]))
    wait(b_load)
    y = finish(sums_ref, x_ref[...], b_ref, chosen, scale, adapters).astype(BF)
    for part in BOTH:
        for piece in BOTH:
            at = (2 * part + piece) * rows
            out_ref[place.device(0, 0), part, piece] = y[at:at + rows]
    place.meet()

    def block(part, ds, df):
        return out_ref.at[place.sequence(part, ds, df), part]

    def seen(part, ds, df, half):
        ref = block(part, ds, df) if half is None else block(part, ds, df).at[half]
        remote(ref, ref, pair_send, pair_recv, place.partner).start()

    for part in BOTH:
        seen(part, OWN, OWN, None)
    gather = Gather(place, block, send_sem, recv_sem, absolute=True, seen=seen)
    gather.own(*BOTH)
    gather.near()
    gather.row()
    gather.sides(*AWAY)
    gather.far(*RING)
    gather.sent()
    every = out_ref.at[first(side * side)]
    for sem in (pair_send, pair_recv):
        pltpu.make_async_copy(every, every, sem).wait()


def put_kernel(y_ref, out_ref, sem):
    wait(ends([pltpu.make_async_copy(y_ref.at[i], out_ref.at[i], sem) for i in range(y_ref.shape[0])]))


def deliver(ids, sums, x_mid, b_all, side, scale, collective_id):
    seq_len, depth = x_mid.shape
    rows = seq_len // 4
    y = pl.pallas_call(
        functools.partial(deliver_kernel, side, b_all.shape[1], scale),
        out_shape=pltpu.VMEM((2 * side * side, 2, 2, rows, depth), BF),
        in_specs=[SMEM] + [VMEM] * 2 + [HBM],
        scratch_shapes=[pltpu.VMEM(b_all.shape[:4] + b_all.shape[5:], BF), DMA, DMA, DMA] + GATHER_SEMS,
        compiler_params=comm_params(collective_id, VMEM_SMALL),
        name='deliver',
    )(ids, sums, x_mid, b_all)
    return pl.pallas_call(
        put_kernel,
        out_shape=jax.ShapeDtypeStruct(y.shape, BF),
        in_specs=[pl.BlockSpec(memory_space=pl.ANY)],
        out_specs=HBM,
        scratch_shapes=[DMA],
        compiler_params=pltpu.CompilerParams(vmem_limit_bytes=VMEM_LEAST),
        name='put',
    )(y)


def solution(mesh):
    tp_size = mesh.shape['tensor']
    side = math.isqrt(tp_size // 2)
    rows_only = P('tensor', None)
    head_split = P(None, 'tensor', None)
    last_split = P(None, None, 'tensor')
    b_head_split = P(None, None, 'tensor', None)
    in_specs = (P('data', None, None), P('data'), P(None), P(None),
                head_split, head_split, head_split, P('tensor', None, None),
                P(None, 'tensor'), P(None, 'tensor'), rows_only,
                last_split, b_head_split, last_split, b_head_split, last_split, b_head_split,
                P(None, 'tensor', None, None), last_split,
                last_split, last_split, last_split, last_split,
                head_split, last_split)

    def local_layer(x_in, adapter_ids, gain_attn, gain_mlp, w_q, w_k, w_v, w_o, w_gate, w_up, w_down, a_q, b_q, a_k, b_k, a_v, b_v, a_o, b_o, a_gate, b_gate, a_up, b_up, a_down, b_down):
        scale = ALPHA / b_q.shape[1]

        def across(a):
            return a.swapaxes(-1, -2)

        heads = [w[:, 0] for w in (w_q, w_k, w_v)] + [across(a) for a in (a_q, a_k, a_v)] + [b[:, :, 0] for b in (b_q, b_k, b_v)]
        sums, all_a, all_b = attend(adapter_ids, x_in, gain_attn, heads, w_o[0], a_o[:, 0], (across(a_gate), across(a_up)), (b_o, b_down), side, scale, 0)

        w = [across(w_gate), across(w_up), across(b_gate), across(b_up), w_down, a_down]
        hidden, x_mid, w_d = gate_up(adapter_ids, sums, gain_mlp, x_in, all_a, all_b, w, side, scale, 1)
        sums = row_proj(adapter_ids, hidden, w_d, *a_o.shape[::3], side, 2)
        y = deliver(adapter_ids, sums, x_mid, pltpu.with_memory_space_constraint(all_b, pltpu.HBM), side, scale, 3)
        return y.reshape(x_in.shape)

    return jax.shard_map(local_layer, mesh=mesh, in_specs=in_specs, out_specs=P('data', None, None), check_vma=False)
```

```python
import functools
import math

import jax
import jax.numpy as jnp
import numpy as np
from jax import lax
from jax.experimental import pallas as pl
from jax.experimental.pallas import tpu as pltpu
from jax.sharding import PartitionSpec as P

ALPHA = 16.0
ROPE_BASE = 10000.0
EPSILON = 1e-5
BF = jnp.bfloat16
F32 = jnp.float32
LANE = 128
TILE = 16
VMEM_MOST = 67043328
VMEM_SMALL = VMEM_MOST // 6
VMEM_LEAST = VMEM_MOST // 32
MESH = pl.DeviceIdType.MESH
HBM = pl.BlockSpec(memory_space=pltpu.HBM)
VMEM = pl.BlockSpec(memory_space=pltpu.VMEM)
SMEM = pl.BlockSpec(memory_space=pltpu.SMEM)
DMA = pltpu.SemaphoreType.DMA

OWN, NEXT, FAR, LAST = RING = range(4)
UP, DOWN = BOTH = range(2)
STEP = (NEXT, -NEXT)
FROM = (LAST, NEXT)
AWAY = (NEXT, LAST, FAR)
PAIRS = ((OWN, NEXT), (LAST, FAR))
TOWARD = (NEXT, LAST)
FAST, SLOW = BOTH


def fit(size, most):
    return max(c for c in range(LANE, most + 1, LANE) if size % c == 0)


def first(size):
    return pl.ds(0, size)


def dot(a, b):
    return jnp.dot(a, b, preferred_element_type=F32)


def dot_rows(a, b):
    return lax.dot_general(a, b, (((1,), (1,)), ((), ())), preferred_element_type=F32)


def dot_columns(a, b):
    return lax.dot_general(a, b, (((0,), (0,)), ((), ())), preferred_element_type=F32)


def normed(act, gain):
    return (act * lax.rsqrt(jnp.mean(act * act, axis=-1, keepdims=True) + EPSILON) * gain).astype(BF)


def ends(copies):
    for copy in copies:
        copy.start()
    return copies


def wait(copies):
    for copy in copies:
        copy.wait()


def loop(count, body):
    lax.fori_loop(0, count, lambda i, carry: (body(i), carry)[1], 0)


class Place:
    def __init__(self, side):
        index = lax.axis_index('tensor')
        self.side = side
        self.core = lax.rem(index, 2)
        chip = index // 2
        self.y, self.x = chip // side, lax.rem(chip, side)
        self.partner = index + 1 - 2 * self.core

    def turn(self, at, steps):
        return lax.rem(at + steps + self.side, self.side)

    def device(self, dy, dx):
        return (self.turn(self.y, dy) * self.side + self.turn(self.x, dx)) * 2 + self.core

    def neighbour(self, part, ring, step):
        return self.device(0, step) if part == ring else self.device(step, 0)

    def sequence(self, part, ds, df):
        return self.device(jnp.where(part == 0, ds, df), jnp.where(part == 0, df, ds))

    def rows(self, ref):
        return lambda part, ds: ref.at[part, :, self.turn(self.x, ds)] if part else ref.at[part, self.turn(self.y, ds)]

    def spot(self, part):
        return self.y if part else self.x

    def announce(self, *more):
        to = [self.neighbour(0, ring, step) for ring in BOTH for step in STEP] + list(more)
        for device in to:
            pl.semaphore_signal(pltpu.get_barrier_semaphore(), inc=1, device_id={'tensor': device}, device_id_type=MESH)
        self.announced = len(to)

    def meet(self):
        pl.semaphore_wait(pltpu.get_barrier_semaphore(), self.announced)


def remote(src, dst, send_sem, recv_sem, to):
    return pltpu.make_async_remote_copy(src_ref=src, dst_ref=dst, send_sem=send_sem, recv_sem=recv_sem, device_id={'tensor': to}, device_id_type=MESH)


GATHER_SEMS = [DMA((2, 2, 2, 2, 4))] * 2


class Gather:
    def __init__(self, place, block, send_sem, recv_sem, absolute=False, seen=None):
        self.place, self.block, self.sems, self.absolute, self.seen = place, block, (send_sem, recv_sem), absolute, seen

    def message(self, part, ring, passed, d, j=OWN):
        spot = (lambda s: (s, j)) if ring == SLOW else (lambda s: (OWN, s))
        src, dst = (FROM[d], FAR) if passed else (OWN, FROM[d])
        a, b = self.block(part, *spot(src)), self.block(part, *spot(src if self.absolute else dst))
        if passed:
            a, b = a.at[d], b.at[d]
        return remote(a, b, *(sem.at[part, ring, passed, d, j] for sem in self.sems), self.place.neighbour(part, ring, STEP[d]))

    def arrived(self, part, ring, passed, d, j=OWN):
        self.message(part, ring, passed, d, j).wait_recv()
        if self.seen:
            at = FAR if passed else FROM[d]
            self.seen(part, *((at, j) if ring == SLOW else (OWN, at)), d if passed else None)

    def own(self, *rings):
        for ring in rings:
            for d in BOTH:
                for part in BOTH:
                    self.message(part, ring, 0, d).start()

    def near(self):
        for d in BOTH:
            for part in BOTH:
                self.arrived(part, FAST, 0, d)
                self.message(part, FAST, 1, d).start()
                for e in BOTH:
                    self.message(part, SLOW, 0, e, FROM[d]).start()

    def row(self):
        for part in BOTH:
            for d in BOTH:
                self.arrived(part, FAST, 1, d)
            for e in BOTH:
                self.message(part, SLOW, 0, e, FAR).start()
        self.sides(OWN)

    def sides(self, *blocks):
        for j in blocks:
            for part in BOTH:
                for d in BOTH:
                    self.arrived(part, SLOW, 0, d, j)
                    self.message(part, SLOW, 1, d, j).start()

    def far(self, *blocks):
        for j in blocks:
            for part in BOTH:
                for d in BOTH:
                    self.arrived(part, SLOW, 1, d, j)

    def sent(self):
        for part in BOTH:
            for d in BOTH:
                for passed in BOTH:
                    self.message(part, FAST, passed, d).wait_send()
                    for j in RING:
                        self.message(part, SLOW, passed, d, j).wait_send()


ROW_SEMS = [DMA((2, 2, 2, 2))] * 2


class RowGather:
    def __init__(self, place, row, mine, send_sem, recv_sem):
        self.place, self.row_at, self.mine, self.sems = place, row, mine, (send_sem, recv_sem)

    def message(self, part, ring, passed, d):
        if ring == SLOW:
            ref = self.row_at(part, FROM[d] if passed else OWN)
            ref = ref.at[:, d] if passed else ref
        else:
            ref = self.row_at(part, OWN).at[self.place.turn(self.mine(part), FROM[d] if passed else OWN)]
            ref = ref.at[d] if passed else ref
        return remote(ref, ref, *(sem.at[part, ring, passed, d] for sem in self.sems), self.place.neighbour(part, ring, STEP[d]))

    def pass_on(self, ring, passed):
        for part in BOTH:
            for d in BOTH:
                self.landing(part, ring, passed, d).wait_recv()
                if not passed:
                    self.message(part, ring, 1, d).start()
            if passed and ring == FAST:
                for d in BOTH:
                    self.message(part, SLOW, 0, d).start()

    def landing(self, part, ring, passed, d):
        at = FAR if passed else FROM[d]
        ref = self.row_at(part, at) if ring == SLOW else self.row_at(part, OWN).at[self.place.turn(self.mine(part), at)]
        if passed:
            ref = ref.at[:, d] if ring == SLOW else ref.at[d]
        return remote(ref, ref, *(sem.at[part, ring, passed, d] for sem in self.sems), self.place.neighbour(part, ring, STEP[d]))

    def own(self):
        for d in BOTH:
            for part in BOTH:
                self.message(part, FAST, 0, d).start()

    def near(self):
        self.pass_on(FAST, 0)

    def row(self):
        self.pass_on(FAST, 1)

    def sides(self):
        self.pass_on(SLOW, 0)

    def far(self):
        self.pass_on(SLOW, 1)

    def sent(self):
        for part in BOTH:
            for ring in BOTH:
                for passed in BOTH:
                    for d in BOTH:
                        self.message(part, ring, passed, d).wait_send()


def rows_of_adapter(place, ids_ref, part, ds, shape):
    block = lax.broadcasted_iota(jnp.int32, shape, 0) // (shape[0] // len(RING))
    chosen = jnp.zeros(shape, jnp.int32)
    for df in RING:
        chosen = jnp.where(block == df, ids_ref[place.sequence(part, ds, df)], chosen)
    return chosen


def pick_columns(low, chosen):
    rank = chosen.shape[1]
    kept = low[:, :rank]
    for a in range(1, low.shape[1] // rank):
        kept = jnp.where(chosen == a, low[:, a * rank:(a + 1) * rank], kept)
    return kept


def spread(low, chosen, adapters):
    return jnp.concatenate([jnp.where(chosen == a, low, 0.0) for a in range(adapters)], axis=1).astype(BF)


PASS, FREE, SUM = range(3)
FAST_SEMS = [DMA((2, 3, 2))] * 2


def add(into, *others):
    def some(i):
        at = pl.ds(pl.multiple_of(i * TILE, TILE), TILE)
        total = into[at, :].astype(F32)
        for other in others:
            total += other[at, :].astype(F32)
        into[at, :] = total.astype(BF)

    loop(into.shape[0] // TILE, some)


class FastScatter:
    def __init__(self, place, stage, near, landed, send_sem, recv_sem):
        self.place, self.stage, self.near, self.landed, self.sems = place, stage, near, landed, (send_sem, recv_sem)
        quarter = near.shape[2]
        self.halves = (first(quarter), pl.ds(quarter, quarter))

    def message(self, part, kind, d):
        at = self.halves[1 - d] if kind == FREE else self.halves[d]
        src = self.stage(part, FAR if kind == PASS else TOWARD[d]).at[at]
        dst = self.near.at[part, d] if kind == PASS else self.landed.at[part, d, at]
        sems = [sem.at[part, kind, d] for sem in self.sems]
        return remote(src, dst, *sems, self.place.neighbour(part, FAST, STEP[d]))

    def ready(self, part, df):
        for d in BOTH:
            if df == FAR:
                self.message(part, PASS, d).start()
            elif df == TOWARD[d]:
                self.message(part, FREE, d).start()

    def sum(self):
        for d in BOTH:
            for part in BOTH:
                self.message(part, PASS, d).wait_recv()
                add(self.stage(part, TOWARD[d]).at[self.halves[d]], self.near.at[part, d])
                self.message(part, SUM, d).start()

    def finish(self):
        for part in BOTH:
            for d in BOTH:
                self.message(part, FREE, d).wait_recv()
                self.message(part, SUM, d).wait_recv()
            add(self.stage(part, OWN), self.landed.at[part, UP], self.landed.at[part, DOWN])

    def store(self, out_ref):
        rows = self.landed.shape[2]
        for part in BOTH:
            out_ref[part * rows:(part + 1) * rows] = self.stage(part, OWN)[...]

    def sent(self):
        for part in BOTH:
            for kind in range(3):
                for d in BOTH:
                    self.message(part, kind, d).wait_send()


def fast_scratch(rows, cols):
    return [pltpu.VMEM((2, 2, rows // 2, cols), BF), pltpu.VMEM((2, 2, rows, cols), BF)]


def comm_params(collective_id, limit=VMEM_MOST):
    return pltpu.CompilerParams(collective_id=collective_id, has_side_effects=True, vmem_limit_bytes=limit)


WO_CHUNKS = 8
X_SLOTS = 3


def attend_kernel(side, adapters, scale, ids_ref, x_ref, gain_in, cos_in, sin_in, *rest):
    w_heads, a_heads, b_heads, (wo_ref, ao_ref), a_mlp, b_rows, rest = rest[:3], rest[3:6], rest[6:9], rest[9:11], rest[11:13], rest[13:15], rest[15:]
    (out_ref, a_all, b_all), rest = rest[:3], rest[3:]
    (w, a_raw, b_raw, a_rows, bx, xbuf, h, z, lows, att, act, wo, stage, near, landed, am_raw, a_mine, b_mine, gain_ref, cos_ref, sin_ref, pair_send, pair_recv, table_sem, load_sem, x_sem, own_sem,
     kept_sem, hand_send, hand_recv, wo_load, wo_send, wo_recv, bulk_send, bulk_recv, swap_send, swap_recv,
     send_sem, recv_sem, a_send, a_recv, b_send, b_recv, fast_send, fast_recv) = rest
    place = Place(side)
    place.announce(place.partner, place.device(0, FAR), place.device(FAR, 0))
    head, seq_len, depth = cos_ref.shape[1], x_ref.shape[1], x_ref.shape[2]
    cols = len(w_heads) * head
    chips = side * side
    per = a_raw.shape[3]
    loads = ends([pltpu.make_async_copy(src, dst, load_sem) for i in range(3) for src, dst in
                  ((a_heads[i], a_raw.at[place.core, i]), (w_heads[i], w.at[:, pl.ds(i * head, head)]), (b_heads[i], b_raw.at[0, i]))])
    steps = chips // 2

    def x_loads(step):
        slot = lax.rem(step, X_SLOTS)
        return [pltpu.make_async_copy(x_ref.at[4 * lax.rem(step, steps) + 2 * i + place.core], xbuf.at[slot, i], x_sem.at[slot]) for i in BOTH]

    for step in range(X_SLOTS - 1):
        ends(x_loads(step))
    tables = ends([pltpu.make_async_copy(src, dst, table_sem) for src, dst in ((gain_in, gain_ref), (cos_in, cos_ref), (sin_in, sin_ref))])

    own_loads = ends([pltpu.make_async_copy(a_mlp[i], am_raw.at[i], own_sem) for i in BOTH] +
                     [pltpu.make_async_copy(b_rows[half].at[part], b_mine.at[part, place.y, place.x, half], own_sem) for part in BOTH for half in BOTH])
    width = wo_ref.shape[1]
    rank = ao_ref.shape[2]
    wo_loads = []
    for part in BOTH:
        wo_loads.append(pltpu.make_async_copy(wo_ref, wo.at[part, OWN, 0, :, first(width)], wo_load))
        for a in range(adapters):
            wo_loads.append(pltpu.make_async_copy(ao_ref.at[a], wo.at[part, OWN, 0, :, pl.ds(width + a * rank, rank)], wo_load))
    ends(wo_loads)
    wait(own_loads)
    wait(loads)
    am_rows = jnp.concatenate([am_raw[i, a] for i in BOTH for a in range(adapters)], axis=0)
    for i in RING:
        a_mine[i // 2, place.y, place.x, i % 2] = am_rows[:, i * depth // 4:(i + 1) * depth // 4]
    place.meet()
    moves = [(a_raw.at[place.core], a_raw.at[place.core]), (w.at[:, first(cols)], w.at[:, pl.ds(cols, cols)]), (b_raw.at[0], b_raw.at[1])]
    pair = ends([remote(src, dst, pair_send.at[i], pair_recv.at[i], place.partner) for i, (src, dst) in enumerate(moves)])

    piece = head // WO_CHUNKS

    def wo_message(part, passed, d, i):
        src, dst = (wo.at[part, s, 0, pl.ds(i * piece, piece)] for s in ((FROM[d], FAR) if passed else (OWN, FROM[d])))
        sems = (part, passed, d, i)
        return remote(src, dst, wo_send.at[sems], wo_recv.at[sems], place.neighbour(part, SLOW, STEP[d]))

    def wo_to_partner(part, s):
        remote(wo.at[part, s, 0], wo.at[part, s, 1], bulk_send, bulk_recv, place.partner).start()

    passes = [range(d * WO_CHUNKS // 2, (d + 1) * WO_CHUNKS // 2) for d in BOTH]

    def wo_start(i):
        for d in BOTH:
            for part in BOTH:
                wo_message(part, 0, d, i).start()

    def wo_pass(k):
        for d in BOTH:
            for part in BOTH:
                wo_message(part, 0, d, passes[d][k]).wait_recv()
                wo_message(part, 1, d, passes[d][k]).start()

    def wo_arrived():
        for d in BOTH:
            for part in BOTH:
                for i in passes[1 - d]:
                    wo_message(part, 0, d, i).wait_recv()
                wo_to_partner(part, FROM[d])

    def wo_last():
        for part in BOTH:
            for d in BOTH:
                for i in passes[d]:
                    wo_message(part, 1, d, i).wait_recv()
            wo_to_partner(part, FAR)

    wait(wo_loads)
    early = WO_CHUNKS // 2
    gathers = [RowGather(place, place.rows(a_mine), place.spot, a_send, a_recv), RowGather(place, place.rows(b_mine), place.spot, b_send, b_recv)]

    def both(stage_of):
        for g in gathers:
            getattr(g, stage_of)()

    def hand(*distances):
        for ds in distances:
            for part in BOTH:
                for i, dst in enumerate((a_all, b_all)):
                    here, there = gathers[i].row_at(part, ds), place.rows(dst.at[place.core])(part, ds)
                    pltpu.make_async_copy(here, there, kept_sem.at[i]).start()
                    remote(here, there, hand_send.at[i], hand_recv.at[i], place.partner).start()

    both('own')
    for i in range(early):
        wo_start(i)
    wait(tables)
    pair[0].wait_recv()
    for core in BOTH:
        pieces = [a_raw[core, i, a] if i < len(w_heads) else jnp.zeros((per, depth), BF) for a in range(adapters) for i in RING]
        a_rows[core * 2 * TILE:(core + 1) * 2 * TILE, :] = jnp.concatenate(pieces, axis=0)
    mine = [(place.y, place.x), (place.x, place.y)]

    low_gather = RowGather(place, lambda part, ds: lows.at[part, place.turn(mine[part][0], ds)], place.spot, send_sem, recv_sem)

    def norm(step, last):
        slot = lax.rem(step, X_SLOTS)

        @pl.when(step + X_SLOTS - 1 < last)
        def _():
            ends(x_loads(step + X_SLOTS - 1))

        wait(x_loads(step))
        for i in BOTH:
            h[i * seq_len:(i + 1) * seq_len, :] = normed(xbuf[slot, i].astype(F32), gain_ref[...])

    def products(step):
        pl.when(step == 3)(lambda: both('near'))
        norm(step, 2 * steps)
        low = dot_rows(a_rows[...], h[...])
        half, at = step // (steps // 2), lax.rem(step, steps // 2) * 2 * seq_len
        for part in BOTH:
            pieces = []
            for i in BOTH:
                options = [low[TILE * (2 * part + a):TILE * (2 * part + a + 1), i * seq_len:(i + 1) * seq_len] for a in range(adapters)]
                chosen = options[0]
                for a in range(1, adapters):
                    chosen = jnp.where(ids_ref[4 * step + 2 * i + place.core] == a, options[a], chosen)
                pieces.append(chosen)
            lows[part, mine[part][0], mine[part][1], half, :, pl.ds(pl.multiple_of(at, LANE), 2 * seq_len)] = jnp.concatenate(pieces, axis=1).astype(BF)

    loop(steps, products)
    low_gather.own()
    for copy in pair[1:]:
        copy.wait_recv()
    for part in BOTH:
        wo_to_partner(part, OWN)
    events = {0: lambda: wo_start(early), 3: lambda: (low_gather.near(), wo_start(early + 1)), 7: lambda: (low_gather.row(), wo_start(early + 2)),
              14: lambda: (low_gather.sides(), wo_start(early + 3))}

    def happen(half_step):
        for at, what in events.items():
            pl.when(half_step == at)(lambda what=what: (what(), None)[1])

    def project(step):
        happen(2 * step)
        norm(step + steps, 2 * steps)
        happen(2 * step + 1)
        rows = pl.ds(pl.multiple_of(step * 2 * seq_len, LANE), 2 * seq_len)
        chunk = fit(2 * cols, 256)
        for n in range(2 * cols // chunk):
            z[rows, n * chunk:(n + 1) * chunk] = dot(h[...], w[:, n * chunk:(n + 1) * chunk])

    loop(steps, project)
    row, col = (lax.broadcasted_iota(jnp.int32, (2 * rank, rank), axis) for axis in BOTH)
    spot, kind = row // TILE, lax.rem(row, TILE) // per
    for part in BOTH:
        chip_of = spot if part == 0 else lax.rem(spot, side) * side + spot // side
        to = chip_of * 2 * per + part * per + lax.rem(row, per)
        for i in range(3):
            spread_rows = jnp.where((kind == i) & (col == to), 1.0, 0.0).astype(BF)
            for a in range(adapters):
                for o in BOTH:
                    bx[a, part, :, o * cols + i * head:o * cols + (i + 1) * head] = dot(spread_rows, b_raw[o, i, a]).astype(BF)
    wo_pass(0)
    wo_pass(1)
    low_gather.far()
    wo_pass(2)
    wo_pass(3)
    causal = lax.broadcasted_iota(jnp.int32, (seq_len, seq_len), 0) >= lax.broadcasted_iota(jnp.int32, (seq_len, seq_len), 1)

    def swap(part, ds):
        sems = (part, ds)
        to = place.neighbour(part, SLOW, ds)
        return remote(att.at[sems], act.at[part, lax.rem(len(RING) - ds, len(RING))], swap_send.at[sems], swap_recv.at[sems], to)

    def attention(i):
        dy, dx = side - 1 - i // side, side - 1 - lax.rem(i, side)
        chip = place.turn(place.y, dy) * side + place.turn(place.x, dx)
        adapter = ids_ref[2 * chip + place.core]
        half, at = chip // steps, pl.ds(pl.multiple_of(lax.rem(chip, steps) * seq_len, LANE), seq_len)
        zs = z[pl.ds(pl.multiple_of(chip * seq_len, LANE), seq_len), :]
        for part in BOTH:
            zs += scale * dot_columns(lows[part, :, :, half, :, at].reshape(-1, seq_len), bx[adapter, part])
        for i_head in BOTH:
            q, k, v = (zs[:, i_head * cols + i * head:i_head * cols + (i + 1) * head] for i in range(3))
            q, k = ((r * cos_ref[...] + pltpu.roll(r, head // 2, axis=1) * sin_ref[...]).astype(BF) for r in (q, k))
            scores = jnp.where(causal, dot_rows(q, k) * head ** -0.5, -1e30)
            e = jnp.exp(scores - jnp.max(scores, axis=-1, keepdims=True))
            prob = (e / jnp.sum(e, axis=-1, keepdims=True)).astype(BF)
            mixed = dot(prob, v.astype(BF)).astype(BF)
            for part, (ds, df) in enumerate(((dy, dx), (dx, dy))):
                att[part, ds, df, :, i_head * head:(i_head + 1) * head] = mixed[part * seq_len // 2:(part + 1) * seq_len // 2]

    def attention_pair(k):
        for i in BOTH:
            attention(2 * k + i)
        row = side - 1 - 2 * k // side
        pl.when((lax.rem(2 * k + 2, side) == 0) & (row != OWN))(lambda: swap(0, row).start())

    loop(chips // 2, attention_pair)
    for ds in AWAY:
        swap(1, ds).start()
    both('row')
    hand(OWN)
    wo_arrived()
    wo_last()
    for part in BOTH:
        act[part, OWN] = att[part, OWN]
    pltpu.make_async_copy(wo.at[:, :, 1], wo.at[:, :, 1], bulk_recv).wait()
    chunk = fit(width, 512)
    rows = seq_len // 2
    blocks = (len(RING), rows)
    fast = FastScatter(place, lambda part, df: stage.at[part, df], near, landed, fast_send, fast_recv)

    def sum_heads(part, at):
        return sum(dot(act[part, s].reshape(-1, 2 * head), wo[part, s, :, :, at].reshape(2 * head, -1)) for s in RING)

    for part in BOTH:
        for ds in AWAY:
            swap(part, ds).wait_recv()

        def columns(n):
            at = pl.ds(pl.multiple_of(n * chunk, chunk), chunk)
            stage[part, :, :, at] = sum_heads(part, at).reshape(blocks + (chunk,)).astype(BF)

        loop(width // chunk, columns)
        chosen = rows_of_adapter(place, ids_ref, part, OWN, (len(RING) * rows, rank))
        stage[part, :, :, width:] = pick_columns(sum_heads(part, pl.ds(width, adapters * rank)), chosen).reshape(blocks + (rank,)).astype(BF)
        for df in (FAR, NEXT, LAST):
            fast.ready(part, df)
    both('sides')
    hand(NEXT, LAST)
    fast.sum()
    both('far')
    hand(FAR)
    fast.finish()
    out = ends([pltpu.make_async_copy(stage.at[part, OWN], out_ref.at[pl.ds(part * rows, rows)], load_sem) for part in BOTH])
    fast.sent()
    for sem in (kept_sem, hand_send, hand_recv):
        for i, ref in enumerate((a_mine, b_mine)):
            pltpu.make_async_copy(ref, ref, sem.at[i]).wait()
    for copy in pair:
        copy.wait_send()
    for g in gathers + [low_gather]:
        g.sent()
    pltpu.make_async_copy(wo.at[:, :, 1], wo.at[:, :, 1], bulk_send).wait()
    for part in BOTH:
        for d in BOTH:
            for i in range(WO_CHUNKS):
                wo_message(part, 0, d, i).wait_send()
            for i in passes[d]:
                wo_message(part, 1, d, i).wait_send()
        for ds in AWAY:
            swap(part, ds).wait_send()
    wait(out)


def attend(ids, x_in, gain, heads, w_o, a_o, a_mlp, b_rows, side, scale, collective_id):
    _, seq_len, depth = x_in.shape
    head = heads[0].shape[1]
    cols = 3 * head
    adapters, _, rank = a_o.shape
    per = heads[3].shape[1]
    chips = side * side
    half_dim = head // 2
    inv_freq = ROPE_BASE ** (-2.0 * np.arange(half_dim) / head)
    angle = np.arange(seq_len)[:, None] * inv_freq[None, :]
    cos, sin = np.cos(angle), np.sin(angle)
    tables = [jnp.asarray(np.concatenate(pair, axis=1), F32) for pair in ((cos, cos), (-sin, sin))]
    n_pair = 3
    rows, out_cols = seq_len // 2, depth + rank
    every = (2, 2, side, side, 2)
    return pl.pallas_call(
        functools.partial(attend_kernel, side, adapters, scale),
        out_shape=[jax.ShapeDtypeStruct((seq_len, out_cols), BF), jax.ShapeDtypeStruct(every + (2 * adapters * per, depth // 4), BF),
                   jax.ShapeDtypeStruct(every + b_rows[0].shape[1:], BF)],
        in_specs=[SMEM] + [HBM] * (4 + len(heads) + 6),
        out_specs=[HBM] * 3,
        scratch_shapes=[
            pltpu.VMEM((depth, 2 * cols), BF),
            pltpu.VMEM((2, 3, adapters, per, depth), BF),
            pltpu.VMEM((2, 3, adapters, rank, head), BF),
            pltpu.VMEM((2 * 2 * TILE, depth), BF),
            pltpu.VMEM((adapters, 2, 2 * rank, 2 * cols), BF),
            pltpu.VMEM((X_SLOTS, 2, seq_len, depth), BF),
            pltpu.VMEM((2 * seq_len, depth), BF),
            pltpu.VMEM((chips * seq_len, 2 * cols), F32),
            pltpu.VMEM((2, side, side, 2, TILE, chips * seq_len // 2), BF),
            pltpu.VMEM((2, side, side, rows, 2 * head), BF),
            pltpu.VMEM((2, side, side, rows, 2 * head), BF),
            pltpu.VMEM((2, side, 2, head, depth + adapters * rank), BF),
            pltpu.VMEM((2, side, rows, out_cols), BF),
        ] + fast_scratch(rows, out_cols) + [
            pltpu.VMEM((2, adapters, per, depth), BF),
            pltpu.VMEM(every[1:] + (2 * adapters * per, depth // 4), BF),
            pltpu.VMEM(every[1:] + b_rows[0].shape[1:], BF),
            pltpu.VMEM((1, depth), F32),
            pltpu.VMEM(tables[0].shape, F32),
            pltpu.VMEM(tables[0].shape, F32),
            DMA((n_pair,)), DMA((n_pair,)), DMA, DMA, DMA((X_SLOTS,)), DMA, DMA((2,)), DMA((2,)), DMA((2,)), DMA, DMA((2, 2, 2, WO_CHUNKS)), DMA((2, 2, 2, WO_CHUNKS)), DMA, DMA, DMA((2, 4)), DMA((2, 4)),
        ] + ROW_SEMS * 3 + FAST_SEMS,
        compiler_params=comm_params(collective_id),
        name='attend',
    )(ids, x_in, gain.reshape(1, depth), *tables, *heads, w_o, a_o, *a_mlp, *b_rows)


def row_proj_kernel(side, adapters, rank, ids_ref, act, w, out_ref, stage, near, landed, fast_near, fast_landed, slow_send, slow_recv, fast_send, fast_recv):
    place = Place(side)
    place.announce()
    rows, cols = stage.shape[3:]
    quarter = rows // 2
    width = cols - rank
    chunk = fit(width, 1024)

    def unit(part, ds):
        def columns(n):
            at = pl.ds(pl.multiple_of(n * chunk, chunk), chunk)
            stage[part, ds, :, :, at] = dot(act[part, ds], w[:, at]).reshape(len(RING), rows, chunk).astype(BF)

        loop(width // chunk, columns)
        chosen = rows_of_adapter(place, ids_ref, part, ds, (len(RING) * rows, rank))
        stage[part, ds, :, :, width:] = pick_columns(dot(act[part, ds], w[:, width:]), chosen).reshape(len(RING), rows, rank).astype(BF)

    blocks = ((FAR, LAST), (OWN, NEXT))

    def slow(part, kind, d, i):
        df = blocks[1 - d][i] if kind == FREE else blocks[d][i]
        sems = (part, kind, d, i)
        src = stage.at[part, FAR if kind == PASS else TOWARD[d], df]
        dst = near.at[part, d, i] if kind == PASS else landed.at[part, d, df]
        return remote(src, dst, slow_send.at[sems], slow_recv.at[sems], place.neighbour(part, SLOW, STEP[d]))

    fast = FastScatter(place, lambda part, df: stage.at[part, OWN, df], fast_near, fast_landed, fast_send, fast_recv)
    for part in BOTH:
        unit(part, FAR)
        if part == 0:
            place.meet()
        for i in BOTH:
            for d in BOTH:
                slow(part, PASS, d, i).start()
    loop(len(RING), lambda i: unit(lax.rem(i, 2), NEXT + 2 * (i // 2)))
    for i in BOTH:
        for d in BOTH:
            for part in BOTH:
                slow(part, FREE, d, i).start()
    loop(2, lambda part: unit(part, OWN))
    for i in BOTH:
        for d in BOTH:
            for part in BOTH:
                slow(part, PASS, d, i).wait_recv()
                add(stage.at[part, TOWARD[d], blocks[d][i]], near.at[part, d, i])
                slow(part, SUM, d, i).start()
    for i in BOTH:
        for d in BOTH:
            df = blocks[d][i]
            for part in BOTH:
                slow(part, SUM, d, i).wait_recv()
                slow(part, FREE, 1 - d, i).wait_recv()
                add(stage.at[part, OWN, df], landed.at[part, UP, df], landed.at[part, DOWN, df])
                fast.ready(part, df)
    fast.sum()
    fast.finish()
    fast.store(out_ref)
    fast.sent()
    for part in BOTH:
        for kind in range(3):
            for d in BOTH:
                for i in BOTH:
                    slow(part, kind, d, i).wait_send()


def row_proj(ids, act, w, adapters, rank, side, collective_id):
    rows = act.shape[2] // side
    cols = w.shape[1] - (adapters - 1) * rank
    blocks = (rows, cols)
    return pl.pallas_call(
        functools.partial(row_proj_kernel, side, adapters, rank),
        out_shape=pltpu.VMEM((2 * rows, cols), BF),
        in_specs=[SMEM, VMEM, VMEM],
        out_specs=VMEM,
        scratch_shapes=[
            pltpu.VMEM((2, side, side) + blocks, BF),
            pltpu.VMEM((2, 2, 2) + blocks, BF),
            pltpu.VMEM((2, 2, side) + blocks, BF),
        ] + fast_scratch(rows, cols) + [DMA((2, 3, 2, 2))] * 2 + FAST_SEMS,
        compiler_params=comm_params(collective_id, VMEM_MOST * 5 // 8),
        name='row_proj',
    )(ids, act, w)


def finish(sums_ref, resid, b_ref, chosen, scale, adapters):
    _, _, side, _, rank, part = b_ref.shape
    width = sums_ref.shape[1] - rank
    low = spread(sums_ref[:, width:].astype(F32), chosen, adapters)
    delta = [dot(low, b_ref[core, :, y, x].reshape(adapters * rank, part)) for y in range(side) for x in range(side) for core in BOTH]
    return resid.astype(F32) + (sums_ref[:, :width].astype(F32) + scale * jnp.concatenate(delta, axis=1))


def own_rows(place, ids_ref, shape):
    return jnp.full(shape, ids_ref[place.device(0, 0)], jnp.int32)


def gate_up_kernel(side, adapters, scale, ids_ref, sums_in, gain_in, x_all, a_all, b_all, wg_ref, wu_ref, bg_ref, bu_ref, wd_ref, ad_ref,
                   hid, mid_ref, wd, gbuf, raw, w, b, bx, gain_ref, sums_ref, a_ref, a_cols, b_ref, raw_sem, load_sem, a_sem, b_sem, credit, pair_send, pair_recv, send_sem, recv_sem):
    place = Place(side)
    share, width = wg_ref.shape
    half = raw.shape[1]
    rank = bg_ref.shape[2]
    seq_len = sums_ref.shape[0]
    edge = share // TILE * TILE
    for i in BOTH:
        raw[i, edge:] = jnp.zeros((half - edge, width), BF)
        for kind in BOTH:
            b[kind, i * half + edge:(i + 1) * half] = jnp.zeros((half - edge, adapters * rank), BF)
        wd[i * half + edge:(i + 1) * half] = jnp.zeros((half - edge, wd.shape[1]), BF)
    place.announce(place.partner)
    b_load = ends([pltpu.make_async_copy(b_all.at[:, :, :, :, 0], b_ref, b_sem), pltpu.make_async_copy(x_all.at[place.device(0, 0)], mid_ref, b_sem),
                   pltpu.make_async_copy(gain_in, gain_ref, b_sem), pltpu.make_async_copy(sums_in, sums_ref, b_sem)])
    a_load = ends([pltpu.make_async_copy(a_all, a_ref, a_sem)])
    mine = first(share)

    def raw_load(kind):
        return pltpu.make_async_copy((wg_ref, wu_ref)[kind], raw.at[0, mine], raw_sem)

    raw_load(0).start()
    loads = [pltpu.make_async_copy(wd_ref, wd.at[mine, first(width)], load_sem)]
    for a in range(adapters):
        loads.append(pltpu.make_async_copy(ad_ref.at[a], wd.at[mine, pl.ds(width + a * rank, rank)], load_sem))
        for kind, ref in enumerate((bg_ref, bu_ref)):
            loads.append(pltpu.make_async_copy(ref.at[a], b.at[kind, mine, pl.ds(a * rank, rank)], load_sem))
    ends(loads)
    other = pl.ds(half, share)
    moves = [(raw.at[0, mine], raw.at[1, mine])] * 2 + [(wd.at[mine], wd.at[other])] + [(b.at[kind, mine], b.at[kind, other]) for kind in BOTH]
    pair = [remote(src, dst, pair_send.at[i], pair_recv.at[i], place.partner) for i, (src, dst) in enumerate(moves)]
    rows = seq_len // 4
    chosen = own_rows(place, ids_ref, (seq_len, rank))
    wait(b_load)
    mid = finish(sums_ref, mid_ref[...], b_ref, chosen, scale, adapters).astype(BF)
    mid_ref[...] = mid
    h2 = normed(mid.astype(F32), gain_ref[...])
    for part in BOTH:
        for piece in BOTH:
            at = (2 * part + piece) * rows
            gbuf[part, OWN, OWN, piece] = h2[at:at + rows]
    place.meet()
    chunk = fit(2 * half, 256)

    group, quarter = a_ref.shape[5:]
    n_low = 2 * side * side * group
    per = group // (2 * adapters)

    def unit(ds, blocks=RING):
        lo, hi = min(blocks), max(blocks) + 1
        unit_rows = (hi - lo) * 2 * rows
        act_of = lambda: gbuf[:, ds, lo:hi].reshape(2 * unit_rows, width)
        chosen = jnp.concatenate([rows_of_adapter(place, ids_ref, part, ds, (len(RING) * 2 * rows, n_low))[lo * 2 * rows:hi * 2 * rows] for part in BOTH], axis=0)
        adapter = lax.rem(lax.broadcasted_iota(jnp.int32, chosen.shape, 1) // per, adapters)
        lows = jnp.where(adapter == chosen, dot(act_of(), a_cols[...]), 0.0).astype(BF)

        def columns(n):
            at = pl.ds(pl.multiple_of(n * chunk, chunk), chunk)
            act = act_of()
            gate, up = (dot(act, w[kind, :, at]) + scale * dot_rows(lows, bx[kind, at]) for kind in BOTH)
            hid[:, ds, lo * 2 * rows:hi * 2 * rows, at] = (gate * jax.nn.sigmoid(gate) * up).astype(BF).reshape(2, unit_rows, chunk)

        loop(2 * half // chunk, columns)

    gather = Gather(place, lambda part, ds, df: gbuf.at[part, ds, df], send_sem, recv_sem)
    gather.own(*BOTH)
    def turned(kind, i):
        def turn(n):
            at = pl.ds(pl.multiple_of(n * LANE, LANE), LANE)
            w[kind, at, i * half:(i + 1) * half] = raw[i, :, at].T

        loop(width // LANE, turn)

    for kind in BOTH:
        raw_load(kind).wait()
        if kind:
            pl.semaphore_wait(credit, 1)
        pair[kind].start()
        turned(kind, 0)
        if kind == 0:
            wait(loads)
            ends(pair[2:])
        pair[kind].wait_recv()
        turned(kind, 1)
        pair[kind].wait_send()
        if kind == 0:
            pl.semaphore_signal(credit, inc=1, device_id={'tensor': place.partner}, device_id_type=MESH)
            raw_load(1).start()
    gather.near()
    wait(a_load)
    for copy in pair[2:]:
        copy.wait_recv()
    row, col = (lax.broadcasted_iota(jnp.int32, (adapters * rank, n_low), axis) for axis in BOTH)
    core, chip = col // (n_low // 2), lax.rem(col, n_low // 2) // group
    kind_of, a_of = lax.rem(col, group) // (group // 2), lax.rem(col // per, adapters)
    to = a_of * rank + chip * 2 * per + core * per + lax.rem(col, per)
    for kind in BOTH:
        bx[kind] = dot(b[kind], jnp.where((row == to) & (kind_of == kind), 1.0, 0.0).astype(BF)).astype(BF)
    for core in BOTH:
        for i in RING:

            def turn_a(n):
                at = pl.ds(pl.multiple_of(n * LANE, LANE), LANE)
                to = pl.ds(pl.multiple_of(i * quarter + n * LANE, LANE), LANE)
                a_cols[to, core * n_low // 2:(core + 1) * n_low // 2] = a_ref[core, i // 2, :, :, i % 2, :, at].reshape(n_low // 2, LANE).T

            loop(quarter // LANE, turn_a)
    gather.row()
    unit(OWN)
    for blocks in PAIRS:
        gather.sides(*(j for j in blocks if j != OWN))
        loop(2, lambda i: unit(NEXT + 2 * i, blocks))
    for blocks in PAIRS:
        gather.far(*blocks)
        unit(FAR, blocks)
    gather.sent()
    for copy in pair[2:]:
        copy.wait_send()


def gate_up(ids, sums, gain, x_in, a_all, b_all, w, side, scale, collective_id):
    _, seq_len, depth = x_in.shape
    share = w[0].shape[0]
    adapters, _, rank = w[2].shape
    half = (share + LANE - 1) // LANE * LANE
    hidden = (2, side, side * seq_len // 2, 2 * half)
    n_low = 2 * adapters * rank
    return pl.pallas_call(
        functools.partial(gate_up_kernel, side, adapters, scale),
        out_shape=[pltpu.VMEM(hidden, BF), pltpu.VMEM((seq_len, depth), BF), pltpu.VMEM((2 * half, depth + adapters * rank), BF)],
        in_specs=[SMEM] + [HBM] * (5 + len(w)),
        out_specs=[VMEM] * 3,
        scratch_shapes=[
            pltpu.VMEM((2, side, side, 2, seq_len // 4, depth), BF),
            pltpu.VMEM((2, half, depth), BF),
            pltpu.VMEM((2, depth, 2 * half), BF),
            pltpu.VMEM((2, 2 * half, adapters * rank), BF),
            pltpu.VMEM((2, 2 * half, n_low), BF),
            pltpu.VMEM((1, depth), F32),
            pltpu.VMEM(sums.shape, BF),
            pltpu.VMEM(a_all.shape, BF),
            pltpu.VMEM((depth, n_low), BF),
            pltpu.VMEM(b_all.shape[:4] + b_all.shape[5:], BF),
            DMA, DMA, DMA, DMA, pltpu.SemaphoreType.REGULAR, DMA((5,)), DMA((5,)),
        ] + GATHER_SEMS,
        compiler_params=comm_params(collective_id, VMEM_MOST * 51 // 64),
        name='gate_up',
    )(ids, sums, gain.reshape(1, depth), x_in, a_all, b_all, *w)


def deliver_kernel(side, adapters, scale, ids_ref, sums_ref, x_ref, b_all, out_ref, b_ref, b_sem, pair_send, pair_recv, send_sem, recv_sem):
    place = Place(side)
    place.announce(place.partner)
    b_load = ends([pltpu.make_async_copy(b_all.at[:, :, :, :, 1], b_ref, b_sem)])
    seq_len = sums_ref.shape[0]
    rows = seq_len // 4
    chosen = own_rows(place, ids_ref, (seq_len, b_ref.shape[4]))
    wait(b_load)
    y = finish(sums_ref, x_ref[...], b_ref, chosen, scale, adapters).astype(BF)
    for part in BOTH:
        for piece in BOTH:
            at = (2 * part + piece) * rows
            out_ref[place.device(0, 0), part, piece] = y[at:at + rows]
    place.meet()

    def block(part, ds, df):
        return out_ref.at[place.sequence(part, ds, df), part]

    def seen(part, ds, df, half):
        ref = block(part, ds, df) if half is None else block(part, ds, df).at[half]
        remote(ref, ref, pair_send, pair_recv, place.partner).start()

    for part in BOTH:
        seen(part, OWN, OWN, None)
    gather = Gather(place, block, send_sem, recv_sem, absolute=True, seen=seen)
    gather.own(*BOTH)
    gather.near()
    gather.row()
    gather.sides(*AWAY)
    gather.far(*RING)
    gather.sent()
    every = out_ref.at[first(side * side)]
    for sem in (pair_send, pair_recv):
        pltpu.make_async_copy(every, every, sem).wait()


def put_kernel(y_ref, out_ref, sem):
    wait(ends([pltpu.make_async_copy(y_ref.at[i], out_ref.at[i], sem) for i in range(y_ref.shape[0])]))


def deliver(ids, sums, x_mid, b_all, side, scale, collective_id):
    seq_len, depth = x_mid.shape
    rows = seq_len // 4
    y = pl.pallas_call(
        functools.partial(deliver_kernel, side, b_all.shape[1], scale),
        out_shape=pltpu.VMEM((2 * side * side, 2, 2, rows, depth), BF),
        in_specs=[SMEM] + [VMEM] * 2 + [HBM],
        scratch_shapes=[pltpu.VMEM(b_all.shape[:4] + b_all.shape[5:], BF), DMA, DMA, DMA] + GATHER_SEMS,
        compiler_params=comm_params(collective_id, VMEM_SMALL),
        name='deliver',
    )(ids, sums, x_mid, b_all)
    return pl.pallas_call(
        put_kernel,
        out_shape=jax.ShapeDtypeStruct(y.shape, BF),
        in_specs=[pl.BlockSpec(memory_space=pl.ANY)],
        out_specs=HBM,
        scratch_shapes=[DMA],
        compiler_params=pltpu.CompilerParams(vmem_limit_bytes=VMEM_LEAST),
        name='put',
    )(y)


def solution(mesh):
    tp_size = mesh.shape['tensor']
    side = math.isqrt(tp_size // 2)
    rows_only = P('tensor', None)
    head_split = P(None, 'tensor', None)
    last_split = P(None, None, 'tensor')
    b_head_split = P(None, None, 'tensor', None)
    in_specs = (P('data', None, None), P('data'), P(None), P(None),
                head_split, head_split, head_split, P('tensor', None, None),
                P(None, 'tensor'), P(None, 'tensor'), rows_only,
                last_split, b_head_split, last_split, b_head_split, last_split, b_head_split,
                P(None, 'tensor', None, None), last_split,
                last_split, last_split, last_split, last_split,
                head_split, last_split)

    def local_layer(x_in, adapter_ids, gain_attn, gain_mlp, w_q, w_k, w_v, w_o, w_gate, w_up, w_down, a_q, b_q, a_k, b_k, a_v, b_v, a_o, b_o, a_gate, b_gate, a_up, b_up, a_down, b_down):
        scale = ALPHA / b_q.shape[1]

        def across(a):
            return a.swapaxes(-1, -2)

        heads = [w[:, 0] for w in (w_q, w_k, w_v)] + [across(a) for a in (a_q, a_k, a_v)] + [b[:, :, 0] for b in (b_q, b_k, b_v)]
        sums, all_a, all_b = attend(adapter_ids, x_in, gain_attn, heads, w_o[0], a_o[:, 0], (across(a_gate), across(a_up)), (b_o, b_down), side, scale, 0)

        w = [across(w_gate), across(w_up), across(b_gate), across(b_up), w_down, a_down]
        hidden, x_mid, w_d = gate_up(adapter_ids, sums, gain_mlp, x_in, all_a, all_b, w, side, scale, 1)
        sums = row_proj(adapter_ids, hidden, w_d, *a_o.shape[::3], side, 2)
        y = deliver(adapter_ids, sums, x_mid, pltpu.with_memory_space_constraint(all_b, pltpu.HBM), side, scale, 3)
        return y.reshape(x_in.shape)

    return jax.shard_map(local_layer, mesh=mesh, in_specs=in_specs, out_specs=P('data', None, None), check_vma=False)
```

```python
import functools
import math

import jax
import jax.numpy as jnp
import numpy as np
from jax import lax
from jax.experimental import pallas as pl
from jax.experimental.pallas import tpu as pltpu
from jax.sharding import PartitionSpec as P

ALPHA = 16.0
ROPE_BASE = 10000.0
EPSILON = 1e-5
BF = jnp.bfloat16
F32 = jnp.float32
LANE = 128
TILE = 16
VMEM_MOST = 67043328
VMEM_SMALL = VMEM_MOST // 6
VMEM_LEAST = VMEM_MOST // 32
MESH = pl.DeviceIdType.MESH
HBM = pl.BlockSpec(memory_space=pltpu.HBM)
VMEM = pl.BlockSpec(memory_space=pltpu.VMEM)
SMEM = pl.BlockSpec(memory_space=pltpu.SMEM)
DMA = pltpu.SemaphoreType.DMA

OWN, NEXT, FAR, LAST = RING = range(4)
UP, DOWN = BOTH = range(2)
STEP = (NEXT, -NEXT)
FROM = (LAST, NEXT)
AWAY = (NEXT, LAST, FAR)
PAIRS = ((OWN, NEXT), (LAST, FAR))
TOWARD = (NEXT, LAST)
FAST, SLOW = BOTH


def fit(size, most):
    return max(c for c in range(LANE, most + 1, LANE) if size % c == 0)


def first(size):
    return pl.ds(0, size)


def dot(a, b):
    return jnp.dot(a, b, preferred_element_type=F32)


def dot_rows(a, b):
    return lax.dot_general(a, b, (((1,), (1,)), ((), ())), preferred_element_type=F32)


def dot_columns(a, b):
    return lax.dot_general(a, b, (((0,), (0,)), ((), ())), preferred_element_type=F32)


def normed(act, gain):
    return (act * lax.rsqrt(jnp.mean(act * act, axis=-1, keepdims=True) + EPSILON) * gain).astype(BF)


def ends(copies):
    for copy in copies:
        copy.start()
    return copies


def wait(copies):
    for copy in copies:
        copy.wait()


def loop(count, body):
    lax.fori_loop(0, count, lambda i, carry: (body(i), carry)[1], 0)


class Place:
    def __init__(self, side):
        index = lax.axis_index('tensor')
        self.side = side
        self.core = lax.rem(index, 2)
        chip = index // 2
        self.y, self.x = chip // side, lax.rem(chip, side)
        self.partner = index + 1 - 2 * self.core

    def turn(self, at, steps):
        return lax.rem(at + steps + self.side, self.side)

    def device(self, dy, dx):
        return (self.turn(self.y, dy) * self.side + self.turn(self.x, dx)) * 2 + self.core

    def neighbour(self, part, ring, step):
        return self.device(0, step) if part == ring else self.device(step, 0)

    def sequence(self, part, ds, df):
        return self.device(jnp.where(part == 0, ds, df), jnp.where(part == 0, df, ds))

    def rows(self, ref):
        return lambda part, ds: ref.at[part, :, self.turn(self.x, ds)] if part else ref.at[part, self.turn(self.y, ds)]

    def spot(self, part):
        return self.y if part else self.x

    def announce(self, *more):
        to = [self.neighbour(0, ring, step) for ring in BOTH for step in STEP] + list(more)
        for device in to:
            pl.semaphore_signal(pltpu.get_barrier_semaphore(), inc=1, device_id={'tensor': device}, device_id_type=MESH)
        self.announced = len(to)

    def meet(self):
        pl.semaphore_wait(pltpu.get_barrier_semaphore(), self.announced)


def remote(src, dst, send_sem, recv_sem, to):
    return pltpu.make_async_remote_copy(src_ref=src, dst_ref=dst, send_sem=send_sem, recv_sem=recv_sem, device_id={'tensor': to}, device_id_type=MESH)


GATHER_SEMS = [DMA((2, 2, 2, 2, 4))] * 2


class Gather:
    def __init__(self, place, block, send_sem, recv_sem, absolute=False, seen=None):
        self.place, self.block, self.sems, self.absolute, self.seen = place, block, (send_sem, recv_sem), absolute, seen

    def message(self, part, ring, passed, d, j=OWN):
        spot = (lambda s: (s, j)) if ring == SLOW else (lambda s: (OWN, s))
        src, dst = (FROM[d], FAR) if passed else (OWN, FROM[d])
        a, b = self.block(part, *spot(src)), self.block(part, *spot(src if self.absolute else dst))
        if passed:
            a, b = a.at[d], b.at[d]
        return remote(a, b, *(sem.at[part, ring, passed, d, j] for sem in self.sems), self.place.neighbour(part, ring, STEP[d]))

    def arrived(self, part, ring, passed, d, j=OWN):
        self.message(part, ring, passed, d, j).wait_recv()
        if self.seen:
            at = FAR if passed else FROM[d]
            self.seen(part, *((at, j) if ring == SLOW else (OWN, at)), d if passed else None)

    def own(self, *rings):
        for ring in rings:
            for d in BOTH:
                for part in BOTH:
                    self.message(part, ring, 0, d).start()

    def near(self):
        for d in BOTH:
            for part in BOTH:
                self.arrived(part, FAST, 0, d)
                self.message(part, FAST, 1, d).start()
                for e in BOTH:
                    self.message(part, SLOW, 0, e, FROM[d]).start()

    def row(self):
        for part in BOTH:
            for d in BOTH:
                self.arrived(part, FAST, 1, d)
            for e in BOTH:
                self.message(part, SLOW, 0, e, FAR).start()
        self.sides(OWN)

    def sides(self, *blocks):
        for j in blocks:
            for part in BOTH:
                for d in BOTH:
                    self.arrived(part, SLOW, 0, d, j)
                    self.message(part, SLOW, 1, d, j).start()

    def far(self, *blocks):
        for j in blocks:
            for part in BOTH:
                for d in BOTH:
                    self.arrived(part, SLOW, 1, d, j)

    def sent(self):
        for part in BOTH:
            for d in BOTH:
                for passed in BOTH:
                    self.message(part, FAST, passed, d).wait_send()
                    for j in RING:
                        self.message(part, SLOW, passed, d, j).wait_send()


ROW_SEMS = [DMA((2, 2, 2, 2))] * 2


class RowGather:
    def __init__(self, place, row, mine, send_sem, recv_sem):
        self.place, self.row_at, self.mine, self.sems = place, row, mine, (send_sem, recv_sem)

    def message(self, part, ring, passed, d):
        if ring == SLOW:
            ref = self.row_at(part, FROM[d] if passed else OWN)
            ref = ref.at[:, d] if passed else ref
        else:
            ref = self.row_at(part, OWN).at[self.place.turn(self.mine(part), FROM[d] if passed else OWN)]
            ref = ref.at[d] if passed else ref
        return remote(ref, ref, *(sem.at[part, ring, passed, d] for sem in self.sems), self.place.neighbour(part, ring, STEP[d]))

    def pass_on(self, ring, passed):
        for part in BOTH:
            for d in BOTH:
                self.landing(part, ring, passed, d).wait_recv()
                if not passed:
                    self.message(part, ring, 1, d).start()
            if passed and ring == FAST:
                for d in BOTH:
                    self.message(part, SLOW, 0, d).start()

    def landing(self, part, ring, passed, d):
        at = FAR if passed else FROM[d]
        ref = self.row_at(part, at) if ring == SLOW else self.row_at(part, OWN).at[self.place.turn(self.mine(part), at)]
        if passed:
            ref = ref.at[:, d] if ring == SLOW else ref.at[d]
        return remote(ref, ref, *(sem.at[part, ring, passed, d] for sem in self.sems), self.place.neighbour(part, ring, STEP[d]))

    def own(self):
        for d in BOTH:
            for part in BOTH:
                self.message(part, FAST, 0, d).start()

    def near(self):
        self.pass_on(FAST, 0)

    def row(self):
        self.pass_on(FAST, 1)

    def sides(self):
        self.pass_on(SLOW, 0)

    def far(self):
        self.pass_on(SLOW, 1)

    def sent(self):
        for part in BOTH:
            for ring in BOTH:
                for passed in BOTH:
                    for d in BOTH:
                        self.message(part, ring, passed, d).wait_send()


def rows_of_adapter(place, ids_ref, part, ds, shape):
    block = lax.broadcasted_iota(jnp.int32, shape, 0) // (shape[0] // len(RING))
    chosen = jnp.zeros(shape, jnp.int32)
    for df in RING:
        chosen = jnp.where(block == df, ids_ref[place.sequence(part, ds, df)], chosen)
    return chosen


def pick_columns(low, chosen):
    rank = chosen.shape[1]
    kept = low[:, :rank]
    for a in range(1, low.shape[1] // rank):
        kept = jnp.where(chosen == a, low[:, a * rank:(a + 1) * rank], kept)
    return kept


def spread(low, chosen, adapters):
    return jnp.concatenate([jnp.where(chosen == a, low, 0.0) for a in range(adapters)], axis=1).astype(BF)


PASS, FREE, SUM = range(3)
FAST_SEMS = [DMA((2, 3, 2))] * 2


def add(into, *others):
    def some(i):
        at = pl.ds(pl.multiple_of(i * TILE, TILE), TILE)
        total = into[at, :].astype(F32)
        for other in others:
            total += other[at, :].astype(F32)
        into[at, :] = total.astype(BF)

    loop(into.shape[0] // TILE, some)


class FastScatter:
    def __init__(self, place, stage, near, landed, send_sem, recv_sem):
        self.place, self.stage, self.near, self.landed, self.sems = place, stage, near, landed, (send_sem, recv_sem)
        quarter = near.shape[2]
        self.halves = (first(quarter), pl.ds(quarter, quarter))

    def message(self, part, kind, d):
        at = self.halves[1 - d] if kind == FREE else self.halves[d]
        src = self.stage(part, FAR if kind == PASS else TOWARD[d]).at[at]
        dst = self.near.at[part, d] if kind == PASS else self.landed.at[part, d, at]
        sems = [sem.at[part, kind, d] for sem in self.sems]
        return remote(src, dst, *sems, self.place.neighbour(part, FAST, STEP[d]))

    def ready(self, part, df):
        for d in BOTH:
            if df == FAR:
                self.message(part, PASS, d).start()
            elif df == TOWARD[d]:
                self.message(part, FREE, d).start()

    def sum(self):
        for d in BOTH:
            for part in BOTH:
                self.message(part, PASS, d).wait_recv()
                add(self.stage(part, TOWARD[d]).at[self.halves[d]], self.near.at[part, d])
                self.message(part, SUM, d).start()

    def finish(self):
        for part in BOTH:
            for d in BOTH:
                self.message(part, FREE, d).wait_recv()
                self.message(part, SUM, d).wait_recv()
            add(self.stage(part, OWN), self.landed.at[part, UP], self.landed.at[part, DOWN])

    def store(self, out_ref):
        rows = self.landed.shape[2]
        for part in BOTH:
            out_ref[part * rows:(part + 1) * rows] = self.stage(part, OWN)[...]

    def sent(self):
        for part in BOTH:
            for kind in range(3):
                for d in BOTH:
                    self.message(part, kind, d).wait_send()


def fast_scratch(rows, cols):
    return [pltpu.VMEM((2, 2, rows // 2, cols), BF), pltpu.VMEM((2, 2, rows, cols), BF)]


def comm_params(collective_id, limit=VMEM_MOST):
    return pltpu.CompilerParams(collective_id=collective_id, has_side_effects=True, vmem_limit_bytes=limit)


WO_CHUNKS = 8
X_SLOTS = 3


def attend_kernel(side, adapters, scale, ids_ref, x_ref, gain_in, cos_in, sin_in, *rest):
    w_heads, a_heads, b_heads, (wo_ref, ao_ref), a_mlp, b_rows, rest = rest[:3], rest[3:6], rest[6:9], rest[9:11], rest[11:13], rest[13:15], rest[15:]
    (out_ref, a_all, b_all), rest = rest[:3], rest[3:]
    (w, a_raw, b_raw, a_rows, bx, xbuf, h, z, lows, att, act, wo, stage, near, landed, am_raw, a_mine, b_mine, gain_ref, cos_ref, sin_ref, pair_send, pair_recv, table_sem, load_sem, x_sem, own_sem,
     kept_sem, hand_send, hand_recv, wo_load, wo_send, wo_recv, bulk_send, bulk_recv, swap_send, swap_recv,
     send_sem, recv_sem, a_send, a_recv, b_send, b_recv, fast_send, fast_recv) = rest
    place = Place(side)
    place.announce(place.partner, place.device(0, FAR), place.device(FAR, 0))
    head, seq_len, depth = cos_ref.shape[1], x_ref.shape[1], x_ref.shape[2]
    cols = len(w_heads) * head
    chips = side * side
    per = a_raw.shape[3]
    steps = chips // 2

    def x_loads(step):
        slot = lax.rem(step, X_SLOTS)
        return [pltpu.make_async_copy(x_ref.at[4 * lax.rem(step, steps) + 2 * i + place.core], xbuf.at[slot, i], x_sem.at[slot]) for i in BOTH]

    own_loads = ends([pltpu.make_async_copy(a_mlp[i], am_raw.at[i], own_sem) for i in BOTH] +
                     [pltpu.make_async_copy(b_rows[half].at[part], b_mine.at[part, place.y, place.x, half], own_sem) for part in BOTH for half in BOTH])
    width = wo_ref.shape[1]
    rank = ao_ref.shape[2]
    wo_loads = []
    for part in BOTH:
        wo_loads.append(pltpu.make_async_copy(wo_ref, wo.at[part, OWN, 0, :, first(width)], wo_load))
        for a in range(adapters):
            wo_loads.append(pltpu.make_async_copy(ao_ref.at[a], wo.at[part, OWN, 0, :, pl.ds(width + a * rank, rank)], wo_load))
    ends(wo_loads)
    loads = ends([pltpu.make_async_copy(src, dst, load_sem) for i in range(3) for src, dst in
                  ((a_heads[i], a_raw.at[place.core, i]), (w_heads[i], w.at[:, pl.ds(i * head, head)]), (b_heads[i], b_raw.at[0, i]))])
    for step in range(X_SLOTS - 1):
        ends(x_loads(step))
    tables = ends([pltpu.make_async_copy(src, dst, table_sem) for src, dst in ((gain_in, gain_ref), (cos_in, cos_ref), (sin_in, sin_ref))])
    wait(own_loads)
    am_rows = jnp.concatenate([am_raw[i, a] for i in BOTH for a in range(adapters)], axis=0)
    for i in RING:
        a_mine[i // 2, place.y, place.x, i % 2] = am_rows[:, i * depth // 4:(i + 1) * depth // 4]
    place.meet()
    piece = head // WO_CHUNKS

    def wo_message(part, passed, d, i):
        src, dst = (wo.at[part, s, 0, pl.ds(i * piece, piece)] for s in ((FROM[d], FAR) if passed else (OWN, FROM[d])))
        sems = (part, passed, d, i)
        return remote(src, dst, wo_send.at[sems], wo_recv.at[sems], place.neighbour(part, SLOW, STEP[d]))

    def wo_to_partner(part, s):
        remote(wo.at[part, s, 0], wo.at[part, s, 1], bulk_send, bulk_recv, place.partner).start()

    passes = [range(d * WO_CHUNKS // 2, (d + 1) * WO_CHUNKS // 2) for d in BOTH]

    def wo_start(i):
        for d in BOTH:
            for part in BOTH:
                wo_message(part, 0, d, i).start()

    def wo_pass(k):
        for d in BOTH:
            for part in BOTH:
                wo_message(part, 0, d, passes[d][k]).wait_recv()
                wo_message(part, 1, d, passes[d][k]).start()

    def wo_arrived():
        for d in BOTH:
            for part in BOTH:
                for i in passes[1 - d]:
                    wo_message(part, 0, d, i).wait_recv()
                wo_to_partner(part, FROM[d])

    def wo_last():
        for part in BOTH:
            for d in BOTH:
                for i in passes[d]:
                    wo_message(part, 1, d, i).wait_recv()
            wo_to_partner(part, FAR)

    early = WO_CHUNKS // 2
    gathers = [RowGather(place, place.rows(a_mine), place.spot, a_send, a_recv), RowGather(place, place.rows(b_mine), place.spot, b_send, b_recv)]

    def both(stage_of):
        for g in gathers:
            getattr(g, stage_of)()

    def hand(*distances):
        for ds in distances:
            for part in BOTH:
                for i, dst in enumerate((a_all, b_all)):
                    here, there = gathers[i].row_at(part, ds), place.rows(dst.at[place.core])(part, ds)
                    pltpu.make_async_copy(here, there, kept_sem.at[i]).start()
                    remote(here, there, hand_send.at[i], hand_recv.at[i], place.partner).start()

    both('own')
    wait(wo_loads)
    for i in range(early):
        wo_start(i)
    wait(loads)
    moves = [(a_raw.at[place.core], a_raw.at[place.core]), (w.at[:, first(cols)], w.at[:, pl.ds(cols, cols)]), (b_raw.at[0], b_raw.at[1])]
    pair = ends([remote(src, dst, pair_send.at[i], pair_recv.at[i], place.partner) for i, (src, dst) in enumerate(moves)])
    wait(tables)
    pair[0].wait_recv()
    for core in BOTH:
        pieces = [a_raw[core, i, a] if i < len(w_heads) else jnp.zeros((per, depth), BF) for a in range(adapters) for i in RING]
        a_rows[core * 2 * TILE:(core + 1) * 2 * TILE, :] = jnp.concatenate(pieces, axis=0)
    mine = [(place.y, place.x), (place.x, place.y)]

    low_gather = RowGather(place, lambda part, ds: lows.at[part, place.turn(mine[part][0], ds)], place.spot, send_sem, recv_sem)

    def norm(step, last):
        slot = lax.rem(step, X_SLOTS)

        @pl.when(step + X_SLOTS - 1 < last)
        def _():
            ends(x_loads(step + X_SLOTS - 1))

        wait(x_loads(step))
        for i in BOTH:
            h[i * seq_len:(i + 1) * seq_len, :] = normed(xbuf[slot, i].astype(F32), gain_ref[...])

    def products(step):
        pl.when(step == 3)(lambda: both('near'))
        norm(step, 2 * steps)
        low = dot_rows(a_rows[...], h[...])
        half, at = step // (steps // 2), lax.rem(step, steps // 2) * 2 * seq_len
        for part in BOTH:
            pieces = []
            for i in BOTH:
                options = [low[TILE * (2 * part + a):TILE * (2 * part + a + 1), i * seq_len:(i + 1) * seq_len] for a in range(adapters)]
                chosen = options[0]
                for a in range(1, adapters):
                    chosen = jnp.where(ids_ref[4 * step + 2 * i + place.core] == a, options[a], chosen)
                pieces.append(chosen)
            lows[part, mine[part][0], mine[part][1], half, :, pl.ds(pl.multiple_of(at, LANE), 2 * seq_len)] = jnp.concatenate(pieces, axis=1).astype(BF)

    loop(steps, products)
    low_gather.own()
    for copy in pair[1:]:
        copy.wait_recv()
    for part in BOTH:
        wo_to_partner(part, OWN)
    events = {0: lambda: wo_start(early), 3: lambda: (low_gather.near(), wo_start(early + 1)), 7: lambda: (low_gather.row(), wo_start(early + 2)),
              14: lambda: (low_gather.sides(), wo_start(early + 3))}

    def happen(half_step):
        for at, what in events.items():
            pl.when(half_step == at)(lambda what=what: (what(), None)[1])

    def project(step):
        happen(2 * step)
        norm(step + steps, 2 * steps)
        happen(2 * step + 1)
        rows = pl.ds(pl.multiple_of(step * 2 * seq_len, LANE), 2 * seq_len)
        chunk = fit(2 * cols, 256)
        for n in range(2 * cols // chunk):
            z[rows, n * chunk:(n + 1) * chunk] = dot(h[...], w[:, n * chunk:(n + 1) * chunk])

    loop(steps, project)
    row, col = (lax.broadcasted_iota(jnp.int32, (2 * rank, rank), axis) for axis in BOTH)
    spot, kind = row // TILE, lax.rem(row, TILE) // per
    for part in BOTH:
        chip_of = spot if part == 0 else lax.rem(spot, side) * side + spot // side
        to = chip_of * 2 * per + part * per + lax.rem(row, per)
        for i in range(3):
            spread_rows = jnp.where((kind == i) & (col == to), 1.0, 0.0).astype(BF)
            for a in range(adapters):
                for o in BOTH:
                    bx[a, part, :, o * cols + i * head:o * cols + (i + 1) * head] = dot(spread_rows, b_raw[o, i, a]).astype(BF)
    wo_pass(0)
    wo_pass(1)
    low_gather.far()
    wo_pass(2)
    wo_pass(3)
    causal = lax.broadcasted_iota(jnp.int32, (seq_len, seq_len), 0) >= lax.broadcasted_iota(jnp.int32, (seq_len, seq_len), 1)

    def swap(part, ds):
        sems = (part, ds)
        to = place.neighbour(part, SLOW, ds)
        return remote(att.at[sems], act.at[part, lax.rem(len(RING) - ds, len(RING))], swap_send.at[sems], swap_recv.at[sems], to)

    def attention(i):
        dy, dx = side - 1 - i // side, side - 1 - lax.rem(i, side)
        chip = place.turn(place.y, dy) * side + place.turn(place.x, dx)
        adapter = ids_ref[2 * chip + place.core]
        half, at = chip // steps, pl.ds(pl.multiple_of(lax.rem(chip, steps) * seq_len, LANE), seq_len)
        zs = z[pl.ds(pl.multiple_of(chip * seq_len, LANE), seq_len), :]
        for part in BOTH:
            zs += scale * dot_columns(lows[part, :, :, half, :, at].reshape(-1, seq_len), bx[adapter, part])
        for i_head in BOTH:
            q, k, v = (zs[:, i_head * cols + i * head:i_head * cols + (i + 1) * head] for i in range(3))
            q, k = ((r * cos_ref[...] + pltpu.roll(r, head // 2, axis=1) * sin_ref[...]).astype(BF) for r in (q, k))
            scores = jnp.where(causal, dot_rows(q, k) * head ** -0.5, -1e30)
            e = jnp.exp(scores - jnp.max(scores, axis=-1, keepdims=True))
            prob = (e / jnp.sum(e, axis=-1, keepdims=True)).astype(BF)
            mixed = dot(prob, v.astype(BF)).astype(BF)
            for part, (ds, df) in enumerate(((dy, dx), (dx, dy))):
                att[part, ds, df, :, i_head * head:(i_head + 1) * head] = mixed[part * seq_len // 2:(part + 1) * seq_len // 2]

    def attention_pair(k):
        for i in BOTH:
            attention(2 * k + i)
        row = side - 1 - 2 * k // side
        pl.when((lax.rem(2 * k + 2, side) == 0) & (row != OWN))(lambda: swap(0, row).start())

    loop(chips // 2, attention_pair)
    for ds in AWAY:
        swap(1, ds).start()
    both('row')
    hand(OWN)
    wo_arrived()
    wo_last()
    for part in BOTH:
        act[part, OWN] = att[part, OWN]
    pltpu.make_async_copy(wo.at[:, :, 1], wo.at[:, :, 1], bulk_recv).wait()
    chunk = fit(width, 512)
    rows = seq_len // 2
    blocks = (len(RING), rows)
    fast = FastScatter(place, lambda part, df: stage.at[part, df], near, landed, fast_send, fast_recv)

    def sum_heads(part, at):
        return sum(dot(act[part, s].reshape(-1, 2 * head), wo[part, s, :, :, at].reshape(2 * head, -1)) for s in RING)

    for part in BOTH:
        for ds in AWAY:
            swap(part, ds).wait_recv()

        def columns(n):
            at = pl.ds(pl.multiple_of(n * chunk, chunk), chunk)
            stage[part, :, :, at] = sum_heads(part, at).reshape(blocks + (chunk,)).astype(BF)

        loop(width // chunk, columns)
        chosen = rows_of_adapter(place, ids_ref, part, OWN, (len(RING) * rows, rank))
        stage[part, :, :, width:] = pick_columns(sum_heads(part, pl.ds(width, adapters * rank)), chosen).reshape(blocks + (rank,)).astype(BF)
        for df in (FAR, NEXT, LAST):
            fast.ready(part, df)
    both('sides')
    hand(NEXT, LAST)
    fast.sum()
    both('far')
    hand(FAR)
    fast.finish()
    out = ends([pltpu.make_async_copy(stage.at[part, OWN], out_ref.at[pl.ds(part * rows, rows)], load_sem) for part in BOTH])
    fast.sent()
    for sem in (kept_sem, hand_send, hand_recv):
        for i, ref in enumerate((a_mine, b_mine)):
            pltpu.make_async_copy(ref, ref, sem.at[i]).wait()
    for copy in pair:
        copy.wait_send()
    for g in gathers + [low_gather]:
        g.sent()
    pltpu.make_async_copy(wo.at[:, :, 1], wo.at[:, :, 1], bulk_send).wait()
    for part in BOTH:
        for d in BOTH:
            for i in range(WO_CHUNKS):
                wo_message(part, 0, d, i).wait_send()
            for i in passes[d]:
                wo_message(part, 1, d, i).wait_send()
        for ds in AWAY:
            swap(part, ds).wait_send()
    wait(out)


def attend(ids, x_in, gain, heads, w_o, a_o, a_mlp, b_rows, side, scale, collective_id):
    _, seq_len, depth = x_in.shape
    head = heads[0].shape[1]
    cols = 3 * head
    adapters, _, rank = a_o.shape
    per = heads[3].shape[1]
    chips = side * side
    half_dim = head // 2
    inv_freq = ROPE_BASE ** (-2.0 * np.arange(half_dim) / head)
    angle = np.arange(seq_len)[:, None] * inv_freq[None, :]
    cos, sin = np.cos(angle), np.sin(angle)
    tables = [jnp.asarray(np.concatenate(pair, axis=1), F32) for pair in ((cos, cos), (-sin, sin))]
    n_pair = 3
    rows, out_cols = seq_len // 2, depth + rank
    every = (2, 2, side, side, 2)
    return pl.pallas_call(
        functools.partial(attend_kernel, side, adapters, scale),
        out_shape=[jax.ShapeDtypeStruct((seq_len, out_cols), BF), jax.ShapeDtypeStruct(every + (2 * adapters * per, depth // 4), BF),
                   jax.ShapeDtypeStruct(every + b_rows[0].shape[1:], BF)],
        in_specs=[SMEM] + [HBM] * (4 + len(heads) + 6),
        out_specs=[HBM] * 3,
        scratch_shapes=[
            pltpu.VMEM((depth, 2 * cols), BF),
            pltpu.VMEM((2, 3, adapters, per, depth), BF),
            pltpu.VMEM((2, 3, adapters, rank, head), BF),
            pltpu.VMEM((2 * 2 * TILE, depth), BF),
            pltpu.VMEM((adapters, 2, 2 * rank, 2 * cols), BF),
            pltpu.VMEM((X_SLOTS, 2, seq_len, depth), BF),
            pltpu.VMEM((2 * seq_len, depth), BF),
            pltpu.VMEM((chips * seq_len, 2 * cols), F32),
            pltpu.VMEM((2, side, side, 2, TILE, chips * seq_len // 2), BF),
            pltpu.VMEM((2, side, side, rows, 2 * head), BF),
            pltpu.VMEM((2, side, side, rows, 2 * head), BF),
            pltpu.VMEM((2, side, 2, head, depth + adapters * rank), BF),
            pltpu.VMEM((2, side, rows, out_cols), BF),
        ] + fast_scratch(rows, out_cols) + [
            pltpu.VMEM((2, adapters, per, depth), BF),
            pltpu.VMEM(every[1:] + (2 * adapters * per, depth // 4), BF),
            pltpu.VMEM(every[1:] + b_rows[0].shape[1:], BF),
            pltpu.VMEM((1, depth), F32),
            pltpu.VMEM(tables[0].shape, F32),
            pltpu.VMEM(tables[0].shape, F32),
            DMA((n_pair,)), DMA((n_pair,)), DMA, DMA, DMA((X_SLOTS,)), DMA, DMA((2,)), DMA((2,)), DMA((2,)), DMA, DMA((2, 2, 2, WO_CHUNKS)), DMA((2, 2, 2, WO_CHUNKS)), DMA, DMA, DMA((2, 4)), DMA((2, 4)),
        ] + ROW_SEMS * 3 + FAST_SEMS,
        compiler_params=comm_params(collective_id),
        name='attend',
    )(ids, x_in, gain.reshape(1, depth), *tables, *heads, w_o, a_o, *a_mlp, *b_rows)


def row_proj_kernel(side, adapters, rank, ids_ref, act, w, b_all, out_ref, b_ref, b_sem, stage, near, landed, fast_near, fast_landed, slow_send, slow_recv, fast_send, fast_recv):
    place = Place(side)
    place.announce()
    rows, cols = stage.shape[3:]
    quarter = rows // 2
    b_load = ends([pltpu.make_async_copy(b_all.at[:, :, :, :, 1], b_ref, b_sem)])
    width = cols - rank
    chunk = fit(width, 1024)

    def unit(part, ds):
        def columns(n):
            at = pl.ds(pl.multiple_of(n * chunk, chunk), chunk)
            stage[part, ds, :, :, at] = dot(act[part, ds], w[:, at]).reshape(len(RING), rows, chunk).astype(BF)

        loop(width // chunk, columns)
        chosen = rows_of_adapter(place, ids_ref, part, ds, (len(RING) * rows, rank))
        stage[part, ds, :, :, width:] = pick_columns(dot(act[part, ds], w[:, width:]), chosen).reshape(len(RING), rows, rank).astype(BF)

    blocks = ((FAR, LAST), (OWN, NEXT))

    def slow(part, kind, d, i):
        df = blocks[1 - d][i] if kind == FREE else blocks[d][i]
        sems = (part, kind, d, i)
        src = stage.at[part, FAR if kind == PASS else TOWARD[d], df]
        dst = near.at[part, d, i] if kind == PASS else landed.at[part, d, df]
        return remote(src, dst, slow_send.at[sems], slow_recv.at[sems], place.neighbour(part, SLOW, STEP[d]))

    fast = FastScatter(place, lambda part, df: stage.at[part, OWN, df], fast_near, fast_landed, fast_send, fast_recv)
    for part in BOTH:
        unit(part, FAR)
        if part == 0:
            place.meet()
        for i in BOTH:
            for d in BOTH:
                slow(part, PASS, d, i).start()
    loop(len(RING), lambda i: unit(lax.rem(i, 2), NEXT + 2 * (i // 2)))
    for i in BOTH:
        for d in BOTH:
            for part in BOTH:
                slow(part, FREE, d, i).start()
    loop(2, lambda part: unit(part, OWN))
    for i in BOTH:
        for d in BOTH:
            for part in BOTH:
                slow(part, PASS, d, i).wait_recv()
                add(stage.at[part, TOWARD[d], blocks[d][i]], near.at[part, d, i])
                slow(part, SUM, d, i).start()
    for i in BOTH:
        for d in BOTH:
            df = blocks[d][i]
            for part in BOTH:
                slow(part, SUM, d, i).wait_recv()
                slow(part, FREE, 1 - d, i).wait_recv()
                add(stage.at[part, OWN, df], landed.at[part, UP, df], landed.at[part, DOWN, df])
                fast.ready(part, df)
    fast.sum()
    fast.finish()
    fast.store(out_ref)
    fast.sent()
    wait(b_load)
    for part in BOTH:
        for kind in range(3):
            for d in BOTH:
                for i in BOTH:
                    slow(part, kind, d, i).wait_send()


def row_proj(ids, act, w, b_all, adapters, rank, side, collective_id):
    rows = act.shape[2] // side
    cols = w.shape[1] - (adapters - 1) * rank
    blocks = (rows, cols)
    return pl.pallas_call(
        functools.partial(row_proj_kernel, side, adapters, rank),
        out_shape=[pltpu.VMEM((2 * rows, cols), BF), pltpu.VMEM(b_all.shape[:4] + b_all.shape[5:], BF)],
        in_specs=[SMEM, VMEM, VMEM, HBM],
        out_specs=[VMEM, VMEM],
        scratch_shapes=[
            DMA,
            pltpu.VMEM((2, side, side) + blocks, BF),
            pltpu.VMEM((2, 2, 2) + blocks, BF),
            pltpu.VMEM((2, 2, side) + blocks, BF),
        ] + fast_scratch(rows, cols) + [DMA((2, 3, 2, 2))] * 2 + FAST_SEMS,
        compiler_params=comm_params(collective_id, VMEM_MOST * 9 // 16),
        name='row_proj',
    )(ids, act, w, b_all)


def finish(sums_ref, resid, b_ref, chosen, scale, adapters):
    _, _, side, _, rank, part = b_ref.shape
    width = sums_ref.shape[1] - rank
    low = spread(sums_ref[:, width:].astype(F32), chosen, adapters)
    delta = [dot(low, b_ref[core, :, y, x].reshape(adapters * rank, part)) for y in range(side) for x in range(side) for core in BOTH]
    return resid.astype(F32) + (sums_ref[:, :width].astype(F32) + scale * jnp.concatenate(delta, axis=1))


def own_rows(place, ids_ref, shape):
    return jnp.full(shape, ids_ref[place.device(0, 0)], jnp.int32)


def gate_up_kernel(side, adapters, scale, ids_ref, sums_in, gain_in, x_all, a_all, b_all, wg_ref, wu_ref, bg_ref, bu_ref, wd_ref, ad_ref,
                   hid, mid_ref, wd, gbuf, raw, w, b, bx, gain_ref, sums_ref, a_ref, a_cols, b_ref, raw_sem, load_sem, a_sem, b_sem, credit, pair_send, pair_recv, send_sem, recv_sem):
    place = Place(side)
    share, width = wg_ref.shape
    half = raw.shape[1]
    rank = bg_ref.shape[2]
    seq_len = sums_ref.shape[0]
    edge = share // TILE * TILE
    for i in BOTH:
        raw[i, edge:] = jnp.zeros((half - edge, width), BF)
        for kind in BOTH:
            b[kind, i * half + edge:(i + 1) * half] = jnp.zeros((half - edge, adapters * rank), BF)
        wd[i * half + edge:(i + 1) * half] = jnp.zeros((half - edge, wd.shape[1]), BF)
    place.announce(place.partner)
    b_load = ends([pltpu.make_async_copy(b_all.at[:, :, :, :, 0], b_ref, b_sem), pltpu.make_async_copy(x_all.at[place.device(0, 0)], mid_ref, b_sem),
                   pltpu.make_async_copy(gain_in, gain_ref, b_sem), pltpu.make_async_copy(sums_in, sums_ref, b_sem)])
    a_load = ends([pltpu.make_async_copy(a_all, a_ref, a_sem)])
    mine = first(share)

    def raw_load(kind):
        return pltpu.make_async_copy((wg_ref, wu_ref)[kind], raw.at[0, mine], raw_sem)

    raw_load(0).start()
    loads = [pltpu.make_async_copy(wd_ref, wd.at[mine, first(width)], load_sem)]
    for a in range(adapters):
        loads.append(pltpu.make_async_copy(ad_ref.at[a], wd.at[mine, pl.ds(width + a * rank, rank)], load_sem))
        for kind, ref in enumerate((bg_ref, bu_ref)):
            loads.append(pltpu.make_async_copy(ref.at[a], b.at[kind, mine, pl.ds(a * rank, rank)], load_sem))
    ends(loads)
    other = pl.ds(half, share)
    moves = [(raw.at[0, mine], raw.at[1, mine])] * 2 + [(wd.at[mine], wd.at[other])] + [(b.at[kind, mine], b.at[kind, other]) for kind in BOTH]
    pair = [remote(src, dst, pair_send.at[i], pair_recv.at[i], place.partner) for i, (src, dst) in enumerate(moves)]
    rows = seq_len // 4
    chosen = own_rows(place, ids_ref, (seq_len, rank))
    wait(b_load)
    mid = finish(sums_ref, mid_ref[...], b_ref, chosen, scale, adapters).astype(BF)
    mid_ref[...] = mid
    h2 = normed(mid.astype(F32), gain_ref[...])
    for part in BOTH:
        for piece in BOTH:
            at = (2 * part + piece) * rows
            gbuf[part, OWN, OWN, piece] = h2[at:at + rows]
    place.meet()
    chunk = fit(2 * half, 256)

    group, quarter = a_ref.shape[5:]
    n_low = 2 * side * side * group
    per = group // (2 * adapters)

    def unit(ds, blocks=RING):
        lo, hi = min(blocks), max(blocks) + 1
        unit_rows = (hi - lo) * 2 * rows
        act_of = lambda: gbuf[:, ds, lo:hi].reshape(2 * unit_rows, width)
        chosen = jnp.concatenate([rows_of_adapter(place, ids_ref, part, ds, (len(RING) * 2 * rows, n_low))[lo * 2 * rows:hi * 2 * rows] for part in BOTH], axis=0)
        adapter = lax.rem(lax.broadcasted_iota(jnp.int32, chosen.shape, 1) // per, adapters)
        lows = jnp.where(adapter == chosen, dot(act_of(), a_cols[...]), 0.0).astype(BF)

        def columns(n):
            at = pl.ds(pl.multiple_of(n * chunk, chunk), chunk)
            act = act_of()
            gate, up = (dot(act, w[kind, :, at]) + scale * dot_rows(lows, bx[kind, at]) for kind in BOTH)
            hid[:, ds, lo * 2 * rows:hi * 2 * rows, at] = (gate * jax.nn.sigmoid(gate) * up).astype(BF).reshape(2, unit_rows, chunk)

        loop(2 * half // chunk, columns)

    gather = Gather(place, lambda part, ds, df: gbuf.at[part, ds, df], send_sem, recv_sem)
    gather.own(*BOTH)
    def turned(kind, i):
        def turn(n):
            at = pl.ds(pl.multiple_of(n * LANE, LANE), LANE)
            w[kind, at, i * half:(i + 1) * half] = raw[i, :, at].T

        loop(width // LANE, turn)

    for kind in BOTH:
        raw_load(kind).wait()
        if kind:
            pl.semaphore_wait(credit, 1)
        pair[kind].start()
        turned(kind, 0)
        if kind == 0:
            wait(loads)
            ends(pair[2:])
        pair[kind].wait_recv()
        turned(kind, 1)
        pair[kind].wait_send()
        if kind == 0:
            pl.semaphore_signal(credit, inc=1, device_id={'tensor': place.partner}, device_id_type=MESH)
            raw_load(1).start()
    gather.near()
    wait(a_load)
    for copy in pair[2:]:
        copy.wait_recv()
    row, col = (lax.broadcasted_iota(jnp.int32, (adapters * rank, n_low), axis) for axis in BOTH)
    core, chip = col // (n_low // 2), lax.rem(col, n_low // 2) // group
    kind_of, a_of = lax.rem(col, group) // (group // 2), lax.rem(col // per, adapters)
    to = a_of * rank + chip * 2 * per + core * per + lax.rem(col, per)
    for kind in BOTH:
        bx[kind] = dot(b[kind], jnp.where((row == to) & (kind_of == kind), 1.0, 0.0).astype(BF)).astype(BF)
    for core in BOTH:
        for i in RING:

            def turn_a(n):
                at = pl.ds(pl.multiple_of(n * LANE, LANE), LANE)
                to = pl.ds(pl.multiple_of(i * quarter + n * LANE, LANE), LANE)
                a_cols[to, core * n_low // 2:(core + 1) * n_low // 2] = a_ref[core, i // 2, :, :, i % 2, :, at].reshape(n_low // 2, LANE).T

            loop(quarter // LANE, turn_a)
    gather.row()
    unit(OWN)
    for blocks in PAIRS:
        gather.sides(*(j for j in blocks if j != OWN))
        loop(2, lambda i: unit(NEXT + 2 * i, blocks))
    for blocks in PAIRS:
        gather.far(*blocks)
        unit(FAR, blocks)
    gather.sent()
    for copy in pair[2:]:
        copy.wait_send()


def gate_up(ids, sums, gain, x_in, a_all, b_all, w, side, scale, collective_id):
    _, seq_len, depth = x_in.shape
    share = w[0].shape[0]
    adapters, _, rank = w[2].shape
    half = (share + LANE - 1) // LANE * LANE
    hidden = (2, side, side * seq_len // 2, 2 * half)
    n_low = 2 * adapters * rank
    return pl.pallas_call(
        functools.partial(gate_up_kernel, side, adapters, scale),
        out_shape=[pltpu.VMEM(hidden, BF), pltpu.VMEM((seq_len, depth), BF), pltpu.VMEM((2 * half, depth + adapters * rank), BF)],
        in_specs=[SMEM] + [HBM] * (5 + len(w)),
        out_specs=[VMEM] * 3,
        scratch_shapes=[
            pltpu.VMEM((2, side, side, 2, seq_len // 4, depth), BF),
            pltpu.VMEM((2, half, depth), BF),
            pltpu.VMEM((2, depth, 2 * half), BF),
            pltpu.VMEM((2, 2 * half, adapters * rank), BF),
            pltpu.VMEM((2, 2 * half, n_low), BF),
            pltpu.VMEM((1, depth), F32),
            pltpu.VMEM(sums.shape, BF),
            pltpu.VMEM(a_all.shape, BF),
            pltpu.VMEM((depth, n_low), BF),
            pltpu.VMEM(b_all.shape[:4] + b_all.shape[5:], BF),
            DMA, DMA, DMA, DMA, pltpu.SemaphoreType.REGULAR, DMA((5,)), DMA((5,)),
        ] + GATHER_SEMS,
        compiler_params=comm_params(collective_id, VMEM_MOST * 51 // 64),
        name='gate_up',
    )(ids, sums, gain.reshape(1, depth), x_in, a_all, b_all, *w)


def deliver_kernel(side, adapters, scale, ids_ref, sums_ref, x_ref, b_ref, out_ref, pair_send, pair_recv, send_sem, recv_sem):
    place = Place(side)
    place.announce(place.partner)
    seq_len = sums_ref.shape[0]
    rows = seq_len // 4
    chosen = own_rows(place, ids_ref, (seq_len, b_ref.shape[4]))
    y = finish(sums_ref, x_ref[...], b_ref, chosen, scale, adapters).astype(BF)
    for part in BOTH:
        for piece in BOTH:
            at = (2 * part + piece) * rows
            out_ref[place.device(0, 0), part, piece] = y[at:at + rows]
    place.meet()

    def block(part, ds, df):
        return out_ref.at[place.sequence(part, ds, df), part]

    def seen(part, ds, df, half):
        ref = block(part, ds, df) if half is None else block(part, ds, df).at[half]
        remote(ref, ref, pair_send, pair_recv, place.partner).start()

    for part in BOTH:
        seen(part, OWN, OWN, None)
    gather = Gather(place, block, send_sem, recv_sem, absolute=True, seen=seen)
    gather.own(*BOTH)
    gather.near()
    gather.row()
    gather.sides(*AWAY)
    gather.far(*RING)
    gather.sent()
    every = out_ref.at[first(side * side)]
    for sem in (pair_send, pair_recv):
        pltpu.make_async_copy(every, every, sem).wait()


def put_kernel(y_ref, out_ref, sem):
    wait(ends([pltpu.make_async_copy(y_ref.at[i], out_ref.at[i], sem) for i in range(y_ref.shape[0])]))


def deliver(ids, sums, x_mid, b_down, side, scale, collective_id):
    seq_len, depth = x_mid.shape
    rows = seq_len // 4
    y = pl.pallas_call(
        functools.partial(deliver_kernel, side, b_down.shape[1], scale),
        out_shape=pltpu.VMEM((2 * side * side, 2, 2, rows, depth), BF),
        in_specs=[SMEM] + [VMEM] * 3,
        scratch_shapes=[DMA, DMA] + GATHER_SEMS,
        compiler_params=comm_params(collective_id, VMEM_SMALL),
        name='deliver',
    )(ids, sums, x_mid, b_down)
    return pl.pallas_call(
        put_kernel,
        out_shape=jax.ShapeDtypeStruct(y.shape, BF),
        in_specs=[pl.BlockSpec(memory_space=pl.ANY)],
        out_specs=HBM,
        scratch_shapes=[DMA],
        compiler_params=pltpu.CompilerParams(vmem_limit_bytes=VMEM_LEAST),
        name='put',
    )(y)


def solution(mesh):
    tp_size = mesh.shape['tensor']
    side = math.isqrt(tp_size // 2)
    rows_only = P('tensor', None)
    head_split = P(None, 'tensor', None)
    last_split = P(None, None, 'tensor')
    b_head_split = P(None, None, 'tensor', None)
    in_specs = (P('data', None, None), P('data'), P(None), P(None),
                head_split, head_split, head_split, P('tensor', None, None),
                P(None, 'tensor'), P(None, 'tensor'), rows_only,
                last_split, b_head_split, last_split, b_head_split, last_split, b_head_split,
                P(None, 'tensor', None, None), last_split,
                last_split, last_split, last_split, last_split,
                head_split, last_split)

    def local_layer(x_in, adapter_ids, gain_attn, gain_mlp, w_q, w_k, w_v, w_o, w_gate, w_up, w_down, a_q, b_q, a_k, b_k, a_v, b_v, a_o, b_o, a_gate, b_gate, a_up, b_up, a_down, b_down):
        scale = ALPHA / b_q.shape[1]

        def across(a):
            return a.swapaxes(-1, -2)

        heads = [w[:, 0] for w in (w_q, w_k, w_v)] + [across(a) for a in (a_q, a_k, a_v)] + [b[:, :, 0] for b in (b_q, b_k, b_v)]
        sums, all_a, all_b = attend(adapter_ids, x_in, gain_attn, heads, w_o[0], a_o[:, 0], (across(a_gate), across(a_up)), (b_o, b_down), side, scale, 0)

        w = [across(w_gate), across(w_up), across(b_gate), across(b_up), w_down, a_down]
        hidden, x_mid, w_d = gate_up(adapter_ids, sums, gain_mlp, x_in, all_a, all_b, w, side, scale, 1)
        sums, b_d = row_proj(adapter_ids, hidden, w_d, pltpu.with_memory_space_constraint(all_b, pltpu.HBM), *a_o.shape[::3], side, 2)
        y = deliver(adapter_ids, sums, x_mid, b_d, side, scale, 3)
        return y.reshape(x_in.shape)

    return jax.shard_map(local_layer, mesh=mesh, in_specs=in_specs, out_specs=P('data', None, None), check_vma=False)
```

```python
import functools
import math

import jax
import jax.numpy as jnp
import numpy as np
from jax import lax
from jax.experimental import pallas as pl
from jax.experimental.pallas import tpu as pltpu
from jax.sharding import PartitionSpec as P

ALPHA = 16.0
ROPE_BASE = 10000.0
EPSILON = 1e-5
BF = jnp.bfloat16
F32 = jnp.float32
LANE = 128
TILE = 16
VMEM_MOST = 67043328
VMEM_SMALL = VMEM_MOST // 6
VMEM_LEAST = VMEM_MOST // 32
MESH = pl.DeviceIdType.MESH
HBM = pl.BlockSpec(memory_space=pltpu.HBM)
VMEM = pl.BlockSpec(memory_space=pltpu.VMEM)
SMEM = pl.BlockSpec(memory_space=pltpu.SMEM)
DMA = pltpu.SemaphoreType.DMA

OWN, NEXT, FAR, LAST = RING = range(4)
UP, DOWN = BOTH = range(2)
STEP = (NEXT, -NEXT)
FROM = (LAST, NEXT)
AWAY = (NEXT, LAST, FAR)
PAIRS = ((OWN, NEXT), (LAST, FAR))
TOWARD = (NEXT, LAST)
FAST, SLOW = BOTH


def fit(size, most):
    return max(c for c in range(LANE, most + 1, LANE) if size % c == 0)


def first(size):
    return pl.ds(0, size)


def dot(a, b):
    return jnp.dot(a, b, preferred_element_type=F32)


def dot_rows(a, b):
    return lax.dot_general(a, b, (((1,), (1,)), ((), ())), preferred_element_type=F32)


def dot_columns(a, b):
    return lax.dot_general(a, b, (((0,), (0,)), ((), ())), preferred_element_type=F32)


def normed(act, gain):
    return (act * lax.rsqrt(jnp.mean(act * act, axis=-1, keepdims=True) + EPSILON) * gain).astype(BF)


def ends(copies):
    for copy in copies:
        copy.start()
    return copies


def wait(copies):
    for copy in copies:
        copy.wait()


def loop(count, body):
    lax.fori_loop(0, count, lambda i, carry: (body(i), carry)[1], 0)


class Place:
    def __init__(self, side):
        index = lax.axis_index('tensor')
        self.side = side
        self.core = lax.rem(index, 2)
        chip = index // 2
        self.y, self.x = chip // side, lax.rem(chip, side)
        self.partner = index + 1 - 2 * self.core

    def turn(self, at, steps):
        return lax.rem(at + steps + self.side, self.side)

    def device(self, dy, dx):
        return (self.turn(self.y, dy) * self.side + self.turn(self.x, dx)) * 2 + self.core

    def neighbour(self, part, ring, step):
        return self.device(0, step) if part == ring else self.device(step, 0)

    def sequence(self, part, ds, df):
        return self.device(jnp.where(part == 0, ds, df), jnp.where(part == 0, df, ds))

    def rows(self, ref):
        return lambda part, ds: ref.at[part, :, self.turn(self.x, ds)] if part else ref.at[part, self.turn(self.y, ds)]

    def spot(self, part):
        return self.y if part else self.x

    def announce(self, *more):
        to = [self.neighbour(0, ring, step) for ring in BOTH for step in STEP] + list(more)
        for device in to:
            pl.semaphore_signal(pltpu.get_barrier_semaphore(), inc=1, device_id={'tensor': device}, device_id_type=MESH)
        self.announced = len(to)

    def meet(self):
        pl.semaphore_wait(pltpu.get_barrier_semaphore(), self.announced)


def remote(src, dst, send_sem, recv_sem, to):
    return pltpu.make_async_remote_copy(src_ref=src, dst_ref=dst, send_sem=send_sem, recv_sem=recv_sem, device_id={'tensor': to}, device_id_type=MESH)


GATHER_SEMS = [DMA((2, 2, 2, 2, 4))] * 2


class Gather:
    def __init__(self, place, block, send_sem, recv_sem, absolute=False, seen=None):
        self.place, self.block, self.sems, self.absolute, self.seen = place, block, (send_sem, recv_sem), absolute, seen

    def message(self, part, ring, passed, d, j=OWN):
        spot = (lambda s: (s, j)) if ring == SLOW else (lambda s: (OWN, s))
        src, dst = (FROM[d], FAR) if passed else (OWN, FROM[d])
        a, b = self.block(part, *spot(src)), self.block(part, *spot(src if self.absolute else dst))
        if passed:
            a, b = a.at[d], b.at[d]
        return remote(a, b, *(sem.at[part, ring, passed, d, j] for sem in self.sems), self.place.neighbour(part, ring, STEP[d]))

    def arrived(self, part, ring, passed, d, j=OWN):
        self.message(part, ring, passed, d, j).wait_recv()
        if self.seen:
            at = FAR if passed else FROM[d]
            self.seen(part, *((at, j) if ring == SLOW else (OWN, at)), d if passed else None)

    def own(self, *rings):
        for ring in rings:
            for d in BOTH:
                for part in BOTH:
                    self.message(part, ring, 0, d).start()

    def near(self):
        for d in BOTH:
            for part in BOTH:
                self.arrived(part, FAST, 0, d)
                self.message(part, FAST, 1, d).start()
                for e in BOTH:
                    self.message(part, SLOW, 0, e, FROM[d]).start()

    def row(self):
        for part in BOTH:
            for d in BOTH:
                self.arrived(part, FAST, 1, d)
            for e in BOTH:
                self.message(part, SLOW, 0, e, FAR).start()
        self.sides(OWN)

    def sides(self, *blocks):
        for j in blocks:
            for part in BOTH:
                for d in BOTH:
                    self.arrived(part, SLOW, 0, d, j)
                    self.message(part, SLOW, 1, d, j).start()

    def far(self, *blocks):
        for j in blocks:
            for part in BOTH:
                for d in BOTH:
                    self.arrived(part, SLOW, 1, d, j)

    def sent(self):
        for part in BOTH:
            for d in BOTH:
                for passed in BOTH:
                    self.message(part, FAST, passed, d).wait_send()
                    for j in RING:
                        self.message(part, SLOW, passed, d, j).wait_send()


ROW_SEMS = [DMA((2, 2, 2, 2))] * 2


class RowGather:
    def __init__(self, place, row, mine, send_sem, recv_sem):
        self.place, self.row_at, self.mine, self.sems = place, row, mine, (send_sem, recv_sem)

    def message(self, part, ring, passed, d):
        if ring == SLOW:
            ref = self.row_at(part, FROM[d] if passed else OWN)
            ref = ref.at[:, d] if passed else ref
        else:
            ref = self.row_at(part, OWN).at[self.place.turn(self.mine(part), FROM[d] if passed else OWN)]
            ref = ref.at[d] if passed else ref
        return remote(ref, ref, *(sem.at[part, ring, passed, d] for sem in self.sems), self.place.neighbour(part, ring, STEP[d]))

    def pass_on(self, ring, passed):
        for part in BOTH:
            for d in BOTH:
                self.landing(part, ring, passed, d).wait_recv()
                if not passed:
                    self.message(part, ring, 1, d).start()
            if passed and ring == FAST:
                for d in BOTH:
                    self.message(part, SLOW, 0, d).start()

    def landing(self, part, ring, passed, d):
        at = FAR if passed else FROM[d]
        ref = self.row_at(part, at) if ring == SLOW else self.row_at(part, OWN).at[self.place.turn(self.mine(part), at)]
        if passed:
            ref = ref.at[:, d] if ring == SLOW else ref.at[d]
        return remote(ref, ref, *(sem.at[part, ring, passed, d] for sem in self.sems), self.place.neighbour(part, ring, STEP[d]))

    def own(self):
        for d in BOTH:
            for part in BOTH:
                self.message(part, FAST, 0, d).start()

    def near(self):
        self.pass_on(FAST, 0)

    def row(self):
        self.pass_on(FAST, 1)

    def sides(self):
        self.pass_on(SLOW, 0)

    def far(self):
        self.pass_on(SLOW, 1)

    def sent(self):
        for part in BOTH:
            for ring in BOTH:
                for passed in BOTH:
                    for d in BOTH:
                        self.message(part, ring, passed, d).wait_send()


def rows_of_adapter(place, ids_ref, part, ds, shape):
    block = lax.broadcasted_iota(jnp.int32, shape, 0) // (shape[0] // len(RING))
    chosen = jnp.zeros(shape, jnp.int32)
    for df in RING:
        chosen = jnp.where(block == df, ids_ref[place.sequence(part, ds, df)], chosen)
    return chosen


def pick_columns(low, chosen):
    rank = chosen.shape[1]
    kept = low[:, :rank]
    for a in range(1, low.shape[1] // rank):
        kept = jnp.where(chosen == a, low[:, a * rank:(a + 1) * rank], kept)
    return kept


def spread(low, chosen, adapters):
    return jnp.concatenate([jnp.where(chosen == a, low, 0.0) for a in range(adapters)], axis=1).astype(BF)


PASS, FREE, SUM = range(3)
FAST_SEMS = [DMA((2, 3, 2))] * 2


def add(into, *others):
    def some(i):
        at = pl.ds(pl.multiple_of(i * TILE, TILE), TILE)
        total = into[at, :].astype(F32)
        for other in others:
            total += other[at, :].astype(F32)
        into[at, :] = total.astype(BF)

    loop(into.shape[0] // TILE, some)


class FastScatter:
    def __init__(self, place, stage, near, landed, send_sem, recv_sem):
        self.place, self.stage, self.near, self.landed, self.sems = place, stage, near, landed, (send_sem, recv_sem)
        quarter = near.shape[2]
        self.halves = (first(quarter), pl.ds(quarter, quarter))

    def message(self, part, kind, d):
        at = self.halves[1 - d] if kind == FREE else self.halves[d]
        src = self.stage(part, FAR if kind == PASS else TOWARD[d]).at[at]
        dst = self.near.at[part, d] if kind == PASS else self.landed.at[part, d, at]
        sems = [sem.at[part, kind, d] for sem in self.sems]
        return remote(src, dst, *sems, self.place.neighbour(part, FAST, STEP[d]))

    def ready(self, part, df):
        for d in BOTH:
            if df == FAR:
                self.message(part, PASS, d).start()
            elif df == TOWARD[d]:
                self.message(part, FREE, d).start()

    def sum(self):
        for d in BOTH:
            for part in BOTH:
                self.message(part, PASS, d).wait_recv()
                add(self.stage(part, TOWARD[d]).at[self.halves[d]], self.near.at[part, d])
                self.message(part, SUM, d).start()

    def finish(self):
        for part in BOTH:
            for d in BOTH:
                self.message(part, FREE, d).wait_recv()
                self.message(part, SUM, d).wait_recv()
            add(self.stage(part, OWN), self.landed.at[part, UP], self.landed.at[part, DOWN])

    def store(self, out_ref):
        rows = self.landed.shape[2]
        for part in BOTH:
            out_ref[part * rows:(part + 1) * rows] = self.stage(part, OWN)[...]

    def sent(self):
        for part in BOTH:
            for kind in range(3):
                for d in BOTH:
                    self.message(part, kind, d).wait_send()


def fast_scratch(rows, cols):
    return [pltpu.VMEM((2, 2, rows // 2, cols), BF), pltpu.VMEM((2, 2, rows, cols), BF)]


def comm_params(collective_id, limit=VMEM_MOST):
    return pltpu.CompilerParams(collective_id=collective_id, has_side_effects=True, vmem_limit_bytes=limit)


WO_CHUNKS = 8
X_SLOTS = 3


def attend_kernel(side, adapters, scale, ids_ref, x_ref, gain_in, cos_in, sin_in, *rest):
    w_heads, a_heads, b_heads, (wo_ref, ao_ref), a_mlp, b_rows, rest = rest[:3], rest[3:6], rest[6:9], rest[9:11], rest[11:13], rest[13:15], rest[15:]
    (out_ref, a_all, b_all), rest = rest[:3], rest[3:]
    (w, a_raw, b_raw, a_rows, bx, xbuf, h, z, lows, att, act, wo, stage, near, landed, am_raw, a_mine, b_mine, gain_ref, cos_ref, sin_ref, pair_send, pair_recv, table_sem, load_sem, x_sem, own_sem,
     kept_sem, hand_send, hand_recv, wo_load, wo_send, wo_recv, bulk_send, bulk_recv, swap_send, swap_recv,
     send_sem, recv_sem, a_send, a_recv, b_send, b_recv, fast_send, fast_recv) = rest
    place = Place(side)
    place.announce(place.partner, place.device(0, FAR), place.device(FAR, 0))
    head, seq_len, depth = cos_ref.shape[1], x_ref.shape[1], x_ref.shape[2]
    cols = len(w_heads) * head
    chips = side * side
    per = a_raw.shape[3]
    steps = chips // 2

    def x_loads(step):
        slot = lax.rem(step, X_SLOTS)
        return [pltpu.make_async_copy(x_ref.at[4 * lax.rem(step, steps) + 2 * i + place.core], xbuf.at[slot, i], x_sem.at[slot]) for i in BOTH]

    own_loads = ends([pltpu.make_async_copy(a_mlp[i], am_raw.at[i], own_sem) for i in BOTH] +
                     [pltpu.make_async_copy(b_rows[half].at[part], b_mine.at[part, place.y, place.x, half], own_sem) for part in BOTH for half in BOTH])
    width = wo_ref.shape[1]
    rank = ao_ref.shape[2]
    wo_loads = []
    for part in BOTH:
        wo_loads.append(pltpu.make_async_copy(wo_ref, wo.at[part, OWN, 0, :, first(width)], wo_load))
        for a in range(adapters):
            wo_loads.append(pltpu.make_async_copy(ao_ref.at[a], wo.at[part, OWN, 0, :, pl.ds(width + a * rank, rank)], wo_load))
    ends(wo_loads)
    loads = ends([pltpu.make_async_copy(src, dst, load_sem) for i in range(3) for src, dst in
                  ((a_heads[i], a_raw.at[place.core, i]), (w_heads[i], w.at[:, pl.ds(i * head, head)]), (b_heads[i], b_raw.at[0, i]))])
    for step in range(X_SLOTS - 1):
        ends(x_loads(step))
    tables = ends([pltpu.make_async_copy(src, dst, table_sem) for src, dst in ((gain_in, gain_ref), (cos_in, cos_ref), (sin_in, sin_ref))])
    wait(own_loads)
    am_rows = jnp.concatenate([am_raw[i, a] for i in BOTH for a in range(adapters)], axis=0)
    for i in RING:
        a_mine[i // 2, place.y, place.x, i % 2] = am_rows[:, i * depth // 4:(i + 1) * depth // 4]
    place.meet()
    piece = head // WO_CHUNKS

    def wo_message(part, passed, d, i):
        src, dst = (wo.at[part, s, 0, pl.ds(i * piece, piece)] for s in ((FROM[d], FAR) if passed else (OWN, FROM[d])))
        sems = (part, passed, d, i)
        return remote(src, dst, wo_send.at[sems], wo_recv.at[sems], place.neighbour(part, SLOW, STEP[d]))

    def wo_to_partner(part, s):
        remote(wo.at[part, s, 0], wo.at[part, s, 1], bulk_send, bulk_recv, place.partner).start()

    passes = [range(d * WO_CHUNKS // 2, (d + 1) * WO_CHUNKS // 2) for d in BOTH]

    def wo_start(i):
        for d in BOTH:
            for part in BOTH:
                wo_message(part, 0, d, i).start()

    def wo_pass(k):
        for d in BOTH:
            for part in BOTH:
                wo_message(part, 0, d, passes[d][k]).wait_recv()
                wo_message(part, 1, d, passes[d][k]).start()

    def wo_arrived():
        for d in BOTH:
            for part in BOTH:
                for i in passes[1 - d]:
                    wo_message(part, 0, d, i).wait_recv()
                wo_to_partner(part, FROM[d])

    def wo_last():
        for part in BOTH:
            for d in BOTH:
                for i in passes[d]:
                    wo_message(part, 1, d, i).wait_recv()
            wo_to_partner(part, FAR)

    early = WO_CHUNKS // 2
    gathers = [RowGather(place, place.rows(a_mine), place.spot, a_send, a_recv), RowGather(place, place.rows(b_mine), place.spot, b_send, b_recv)]

    def both(stage_of):
        for g in gathers:
            getattr(g, stage_of)()

    def hand(*distances):
        for ds in distances:
            for part in BOTH:
                for i, dst in enumerate((a_all, b_all)):
                    here, there = gathers[i].row_at(part, ds), place.rows(dst.at[place.core])(part, ds)
                    pltpu.make_async_copy(here, there, kept_sem.at[i]).start()
                    remote(here, there, hand_send.at[i], hand_recv.at[i], place.partner).start()

    both('own')
    wait(wo_loads)
    for i in range(early):
        wo_start(i)
    wait(loads)
    moves = [(a_raw.at[place.core], a_raw.at[place.core]), (w.at[:, first(cols)], w.at[:, pl.ds(cols, cols)]), (b_raw.at[0], b_raw.at[1])]
    pair = ends([remote(src, dst, pair_send.at[i], pair_recv.at[i], place.partner) for i, (src, dst) in enumerate(moves)])
    wait(tables)
    pair[0].wait_recv()
    for core in BOTH:
        pieces = [a_raw[core, i, a] if i < len(w_heads) else jnp.zeros((per, depth), BF) for a in range(adapters) for i in RING]
        a_rows[core * 2 * TILE:(core + 1) * 2 * TILE, :] = jnp.concatenate(pieces, axis=0)
    mine = [(place.y, place.x), (place.x, place.y)]

    low_gather = RowGather(place, lambda part, ds: lows.at[part, place.turn(mine[part][0], ds)], place.spot, send_sem, recv_sem)

    def norm(step, last):
        slot = lax.rem(step, X_SLOTS)

        @pl.when(step + X_SLOTS - 1 < last)
        def _():
            ends(x_loads(step + X_SLOTS - 1))

        wait(x_loads(step))
        for i in BOTH:
            h[i * seq_len:(i + 1) * seq_len, :] = normed(xbuf[slot, i].astype(F32), gain_ref[...])

    def products(step):
        pl.when(step == 3)(lambda: both('near'))
        norm(step, 2 * steps)
        low = dot_rows(a_rows[...], h[...])
        half, at = step // (steps // 2), lax.rem(step, steps // 2) * 2 * seq_len
        for part in BOTH:
            pieces = []
            for i in BOTH:
                options = [low[TILE * (2 * part + a):TILE * (2 * part + a + 1), i * seq_len:(i + 1) * seq_len] for a in range(adapters)]
                chosen = options[0]
                for a in range(1, adapters):
                    chosen = jnp.where(ids_ref[4 * step + 2 * i + place.core] == a, options[a], chosen)
                pieces.append(chosen)
            lows[part, mine[part][0], mine[part][1], half, :, pl.ds(pl.multiple_of(at, LANE), 2 * seq_len)] = jnp.concatenate(pieces, axis=1).astype(BF)

    loop(steps, products)
    low_gather.own()
    for copy in pair[1:]:
        copy.wait_recv()
    for part in BOTH:
        wo_to_partner(part, OWN)
    events = {0: lambda: wo_start(early), 3: lambda: (low_gather.near(), wo_start(early + 1)), 7: lambda: (low_gather.row(), wo_start(early + 2)),
              14: lambda: (low_gather.sides(), wo_start(early + 3))}

    def happen(half_step):
        for at, what in events.items():
            pl.when(half_step == at)(lambda what=what: (what(), None)[1])

    def project(step):
        happen(2 * step)
        norm(step + steps, 2 * steps)
        happen(2 * step + 1)
        rows = pl.ds(pl.multiple_of(step * 2 * seq_len, LANE), 2 * seq_len)
        chunk = fit(2 * cols, 256)
        for n in range(2 * cols // chunk):
            z[rows, n * chunk:(n + 1) * chunk] = dot(h[...], w[:, n * chunk:(n + 1) * chunk])

    loop(steps, project)
    row, col = (lax.broadcasted_iota(jnp.int32, (2 * rank, rank), axis) for axis in BOTH)
    spot, kind = row // TILE, lax.rem(row, TILE) // per
    for part in BOTH:
        chip_of = spot if part == 0 else lax.rem(spot, side) * side + spot // side
        to = chip_of * 2 * per + part * per + lax.rem(row, per)
        for i in range(3):
            spread_rows = jnp.where((kind == i) & (col == to), 1.0, 0.0).astype(BF)
            for a in range(adapters):
                for o in BOTH:
                    bx[a, part, :, o * cols + i * head:o * cols + (i + 1) * head] = dot(spread_rows, b_raw[o, i, a]).astype(BF)
    wo_pass(0)
    wo_pass(1)
    low_gather.far()
    wo_pass(2)
    wo_pass(3)
    causal = lax.broadcasted_iota(jnp.int32, (seq_len, seq_len), 0) >= lax.broadcasted_iota(jnp.int32, (seq_len, seq_len), 1)

    def swap(part, ds):
        sems = (part, ds)
        to = place.neighbour(part, SLOW, ds)
        return remote(att.at[sems], act.at[part, lax.rem(len(RING) - ds, len(RING))], swap_send.at[sems], swap_recv.at[sems], to)

    def attention(i):
        dy, dx = side - 1 - i // side, side - 1 - lax.rem(i, side)
        chip = place.turn(place.y, dy) * side + place.turn(place.x, dx)
        adapter = ids_ref[2 * chip + place.core]
        half, at = chip // steps, pl.ds(pl.multiple_of(lax.rem(chip, steps) * seq_len, LANE), seq_len)
        zs = z[pl.ds(pl.multiple_of(chip * seq_len, LANE), seq_len), :]
        for part in BOTH:
            zs += scale * dot_columns(lows[part, :, :, half, :, at].reshape(-1, seq_len), bx[adapter, part])
        for i_head in BOTH:
            q, k, v = (zs[:, i_head * cols + i * head:i_head * cols + (i + 1) * head] for i in range(3))
            q, k = ((r * cos_ref[...] + pltpu.roll(r, head // 2, axis=1) * sin_ref[...]).astype(BF) for r in (q, k))
            scores = jnp.where(causal, dot_rows(q, k) * head ** -0.5, -1e30)
            e = jnp.exp(scores - jnp.max(scores, axis=-1, keepdims=True))
            prob = (e / jnp.sum(e, axis=-1, keepdims=True)).astype(BF)
            mixed = dot(prob, v.astype(BF)).astype(BF)
            for part, (ds, df) in enumerate(((dy, dx), (dx, dy))):
                att[part, ds, df, :, i_head * head:(i_head + 1) * head] = mixed[part * seq_len // 2:(part + 1) * seq_len // 2]

    def attention_pair(k):
        for i in BOTH:
            attention(2 * k + i)
        row = side - 1 - 2 * k // side
        pl.when((lax.rem(2 * k + 2, side) == 0) & (row != OWN))(lambda: swap(0, row).start())

    loop(chips // 2, attention_pair)
    for ds in AWAY:
        swap(1, ds).start()
    both('row')
    hand(OWN)
    wo_arrived()
    wo_last()
    for part in BOTH:
        act[part, OWN] = att[part, OWN]
    pltpu.make_async_copy(wo.at[:, :, 1], wo.at[:, :, 1], bulk_recv).wait()
    chunk = fit(width, 512)
    rows = seq_len // 2
    blocks = (len(RING), rows)
    fast = FastScatter(place, lambda part, df: stage.at[part, df], near, landed, fast_send, fast_recv)

    def sum_heads(part, at):
        return sum(dot(act[part, s].reshape(-1, 2 * head), wo[part, s, :, :, at].reshape(2 * head, -1)) for s in RING)

    for part in BOTH:
        for ds in AWAY:
            swap(part, ds).wait_recv()

        def columns(n):
            at = pl.ds(pl.multiple_of(n * chunk, chunk), chunk)
            stage[part, :, :, at] = sum_heads(part, at).reshape(blocks + (chunk,)).astype(BF)

        loop(width // chunk, columns)
        chosen = rows_of_adapter(place, ids_ref, part, OWN, (len(RING) * rows, rank))
        stage[part, :, :, width:] = pick_columns(sum_heads(part, pl.ds(width, adapters * rank)), chosen).reshape(blocks + (rank,)).astype(BF)
        for df in (FAR, NEXT, LAST):
            fast.ready(part, df)
    both('sides')
    hand(NEXT, LAST)
    fast.sum()
    both('far')
    hand(FAR)
    fast.finish()
    out = ends([pltpu.make_async_copy(stage.at[part, OWN], out_ref.at[pl.ds(part * rows, rows)], load_sem) for part in BOTH])
    fast.sent()
    for sem in (kept_sem, hand_send, hand_recv):
        for i, ref in enumerate((a_mine, b_mine)):
            pltpu.make_async_copy(ref, ref, sem.at[i]).wait()
    for copy in pair:
        copy.wait_send()
    for g in gathers + [low_gather]:
        g.sent()
    pltpu.make_async_copy(wo.at[:, :, 1], wo.at[:, :, 1], bulk_send).wait()
    for part in BOTH:
        for d in BOTH:
            for i in range(WO_CHUNKS):
                wo_message(part, 0, d, i).wait_send()
            for i in passes[d]:
                wo_message(part, 1, d, i).wait_send()
        for ds in AWAY:
            swap(part, ds).wait_send()
    wait(out)


def attend(ids, x_in, gain, heads, w_o, a_o, a_mlp, b_rows, side, scale, collective_id):
    _, seq_len, depth = x_in.shape
    head = heads[0].shape[1]
    cols = 3 * head
    adapters, _, rank = a_o.shape
    per = heads[3].shape[1]
    chips = side * side
    half_dim = head // 2
    inv_freq = ROPE_BASE ** (-2.0 * np.arange(half_dim) / head)
    angle = np.arange(seq_len)[:, None] * inv_freq[None, :]
    cos, sin = np.cos(angle), np.sin(angle)
    tables = [jnp.asarray(np.concatenate(pair, axis=1), F32) for pair in ((cos, cos), (-sin, sin))]
    n_pair = 3
    rows, out_cols = seq_len // 2, depth + rank
    every = (2, 2, side, side, 2)
    return pl.pallas_call(
        functools.partial(attend_kernel, side, adapters, scale),
        out_shape=[jax.ShapeDtypeStruct((seq_len, out_cols), BF), jax.ShapeDtypeStruct(every + (2 * adapters * per, depth // 4), BF),
                   jax.ShapeDtypeStruct(every + b_rows[0].shape[1:], BF)],
        in_specs=[SMEM] + [HBM] * (4 + len(heads) + 6),
        out_specs=[HBM] * 3,
        scratch_shapes=[
            pltpu.VMEM((depth, 2 * cols), BF),
            pltpu.VMEM((2, 3, adapters, per, depth), BF),
            pltpu.VMEM((2, 3, adapters, rank, head), BF),
            pltpu.VMEM((2 * 2 * TILE, depth), BF),
            pltpu.VMEM((adapters, 2, 2 * rank, 2 * cols), BF),
            pltpu.VMEM((X_SLOTS, 2, seq_len, depth), BF),
            pltpu.VMEM((2 * seq_len, depth), BF),
            pltpu.VMEM((chips * seq_len, 2 * cols), F32),
            pltpu.VMEM((2, side, side, 2, TILE, chips * seq_len // 2), BF),
            pltpu.VMEM((2, side, side, rows, 2 * head), BF),
            pltpu.VMEM((2, side, side, rows, 2 * head), BF),
            pltpu.VMEM((2, side, 2, head, depth + adapters * rank), BF),
            pltpu.VMEM((2, side, rows, out_cols), BF),
        ] + fast_scratch(rows, out_cols) + [
            pltpu.VMEM((2, adapters, per, depth), BF),
            pltpu.VMEM(every[1:] + (2 * adapters * per, depth // 4), BF),
            pltpu.VMEM(every[1:] + b_rows[0].shape[1:], BF),
            pltpu.VMEM((1, depth), F32),
            pltpu.VMEM(tables[0].shape, F32),
            pltpu.VMEM(tables[0].shape, F32),
            DMA((n_pair,)), DMA((n_pair,)), DMA, DMA, DMA((X_SLOTS,)), DMA, DMA((2,)), DMA((2,)), DMA((2,)), DMA, DMA((2, 2, 2, WO_CHUNKS)), DMA((2, 2, 2, WO_CHUNKS)), DMA, DMA, DMA((2, 4)), DMA((2, 4)),
        ] + ROW_SEMS * 3 + FAST_SEMS,
        compiler_params=comm_params(collective_id),
        name='attend',
    )(ids, x_in, gain.reshape(1, depth), *tables, *heads, w_o, a_o, *a_mlp, *b_rows)


def row_proj_kernel(side, adapters, rank, ids_ref, act, w, b_all, out_ref, b_ref, b_sem, stage, near, landed, fast_near, fast_landed, slow_send, slow_recv, fast_send, fast_recv):
    place = Place(side)
    place.announce()
    rows, cols = stage.shape[3:]
    quarter = rows // 2
    b_load = ends([pltpu.make_async_copy(b_all.at[:, :, :, :, 1], b_ref, b_sem)])
    width = cols - rank
    chunk = fit(width, 1024)

    def unit(part, ds):
        def columns(n):
            at = pl.ds(pl.multiple_of(n * chunk, chunk), chunk)
            stage[part, ds, :, :, at] = dot(act[part, ds], w[:, at]).reshape(len(RING), rows, chunk).astype(BF)

        loop(width // chunk, columns)
        chosen = rows_of_adapter(place, ids_ref, part, ds, (len(RING) * rows, rank))
        stage[part, ds, :, :, width:] = pick_columns(dot(act[part, ds], w[:, width:]), chosen).reshape(len(RING), rows, rank).astype(BF)

    blocks = ((FAR, LAST), (OWN, NEXT))

    def slow(part, kind, d, i):
        df = blocks[1 - d][i] if kind == FREE else blocks[d][i]
        sems = (part, kind, d, i)
        src = stage.at[part, FAR if kind == PASS else TOWARD[d], df]
        dst = near.at[part, d, i] if kind == PASS else landed.at[part, d, df]
        return remote(src, dst, slow_send.at[sems], slow_recv.at[sems], place.neighbour(part, SLOW, STEP[d]))

    fast = FastScatter(place, lambda part, df: stage.at[part, OWN, df], fast_near, fast_landed, fast_send, fast_recv)
    for part in BOTH:
        unit(part, FAR)
        if part == 0:
            place.meet()
        for i in BOTH:
            for d in BOTH:
                slow(part, PASS, d, i).start()
    loop(len(RING), lambda i: unit(lax.rem(i, 2), NEXT + 2 * (i // 2)))
    for i in BOTH:
        for d in BOTH:
            for part in BOTH:
                slow(part, FREE, d, i).start()
    loop(2, lambda part: unit(part, OWN))
    for i in BOTH:
        for d in BOTH:
            for part in BOTH:
                slow(part, PASS, d, i).wait_recv()
                add(stage.at[part, TOWARD[d], blocks[d][i]], near.at[part, d, i])
                slow(part, SUM, d, i).start()
    for i in BOTH:
        for d in BOTH:
            df = blocks[d][i]
            for part in BOTH:
                slow(part, SUM, d, i).wait_recv()
                slow(part, FREE, 1 - d, i).wait_recv()
                add(stage.at[part, OWN, df], landed.at[part, UP, df], landed.at[part, DOWN, df])
                fast.ready(part, df)
    fast.sum()
    fast.finish()
    fast.store(out_ref)
    fast.sent()
    wait(b_load)
    for part in BOTH:
        for kind in range(3):
            for d in BOTH:
                for i in BOTH:
                    slow(part, kind, d, i).wait_send()


def row_proj(ids, act, w, b_all, adapters, rank, side, collective_id):
    rows = act.shape[2] // side
    cols = w.shape[1] - (adapters - 1) * rank
    blocks = (rows, cols)
    return pl.pallas_call(
        functools.partial(row_proj_kernel, side, adapters, rank),
        out_shape=[pltpu.VMEM((2 * rows, cols), BF), pltpu.VMEM(b_all.shape[:4] + b_all.shape[5:], BF)],
        in_specs=[SMEM, VMEM, VMEM, HBM],
        out_specs=[VMEM, VMEM],
        scratch_shapes=[
            DMA,
            pltpu.VMEM((2, side, side) + blocks, BF),
            pltpu.VMEM((2, 2, 2) + blocks, BF),
            pltpu.VMEM((2, 2, side) + blocks, BF),
        ] + fast_scratch(rows, cols) + [DMA((2, 3, 2, 2))] * 2 + FAST_SEMS,
        compiler_params=comm_params(collective_id, VMEM_MOST * 9 // 16),
        name='row_proj',
    )(ids, act, w, b_all)


def finish(sums_ref, resid, b_ref, chosen, scale, adapters):
    _, _, side, _, rank, part = b_ref.shape
    width = sums_ref.shape[1] - rank
    low = spread(sums_ref[:, width:].astype(F32), chosen, adapters)
    delta = [dot(low, b_ref[core, :, y, x].reshape(adapters * rank, part)) for y in range(side) for x in range(side) for core in BOTH]
    return resid.astype(F32) + (sums_ref[:, :width].astype(F32) + scale * jnp.concatenate(delta, axis=1))


def own_rows(place, ids_ref, shape):
    return jnp.full(shape, ids_ref[place.device(0, 0)], jnp.int32)


def gate_up_kernel(side, adapters, scale, ids_ref, sums_in, gain_in, x_all, a_all, b_all, wg_ref, wu_ref, bg_ref, bu_ref, wd_ref, ad_ref,
                   hid, mid_ref, wd, gbuf, raw, w, b, bx, gain_ref, sums_ref, a_ref, a_cols, b_ref, raw_sem, load_sem, a_sem, b_sem, credit, pair_send, pair_recv, send_sem, recv_sem):
    place = Place(side)
    share, width = wg_ref.shape
    half = raw.shape[1]
    rank = bg_ref.shape[2]
    seq_len = sums_ref.shape[0]
    edge = share // TILE * TILE
    for i in BOTH:
        raw[i, edge:] = jnp.zeros((half - edge, width), BF)
        for kind in BOTH:
            b[kind, i * half + edge:(i + 1) * half] = jnp.zeros((half - edge, adapters * rank), BF)
        wd[i * half + edge:(i + 1) * half] = jnp.zeros((half - edge, wd.shape[1]), BF)
    place.announce(place.partner)
    b_load = ends([pltpu.make_async_copy(b_all.at[:, :, :, :, 0], b_ref, b_sem), pltpu.make_async_copy(x_all.at[place.device(0, 0)], mid_ref, b_sem),
                   pltpu.make_async_copy(gain_in, gain_ref, b_sem), pltpu.make_async_copy(sums_in, sums_ref, b_sem)])
    a_load = ends([pltpu.make_async_copy(a_all, a_ref, a_sem)])
    mine = first(share)

    def raw_load(kind):
        return pltpu.make_async_copy((wg_ref, wu_ref)[kind], raw.at[0, mine], raw_sem)

    raw_load(0).start()
    loads = [pltpu.make_async_copy(wd_ref, wd.at[mine, first(width)], load_sem)]
    for a in range(adapters):
        loads.append(pltpu.make_async_copy(ad_ref.at[a], wd.at[mine, pl.ds(width + a * rank, rank)], load_sem))
        for kind, ref in enumerate((bg_ref, bu_ref)):
            loads.append(pltpu.make_async_copy(ref.at[a], b.at[kind, mine, pl.ds(a * rank, rank)], load_sem))
    ends(loads)
    other = pl.ds(half, share)
    moves = [(raw.at[0, mine], raw.at[1, mine])] * 2 + [(wd.at[mine], wd.at[other])] + [(b.at[kind, mine], b.at[kind, other]) for kind in BOTH]
    pair = [remote(src, dst, pair_send.at[i], pair_recv.at[i], place.partner) for i, (src, dst) in enumerate(moves)]
    rows = seq_len // 4
    chosen = own_rows(place, ids_ref, (seq_len, rank))
    wait(b_load)
    mid = finish(sums_ref, mid_ref[...], b_ref, chosen, scale, adapters).astype(BF)
    mid_ref[...] = mid
    h2 = normed(mid.astype(F32), gain_ref[...])
    for part in BOTH:
        for piece in BOTH:
            at = (2 * part + piece) * rows
            gbuf[part, OWN, OWN, piece] = h2[at:at + rows]
    place.meet()
    chunk = fit(2 * half, 256)

    group, quarter = a_ref.shape[5:]
    n_low = 2 * side * side * group
    per = group // (2 * adapters)

    def unit(ds, blocks=RING):
        lo, hi = min(blocks), max(blocks) + 1
        unit_rows = (hi - lo) * 2 * rows
        act_of = lambda: gbuf[:, ds, lo:hi].reshape(2 * unit_rows, width)
        chosen = jnp.concatenate([rows_of_adapter(place, ids_ref, part, ds, (len(RING) * 2 * rows, n_low))[lo * 2 * rows:hi * 2 * rows] for part in BOTH], axis=0)
        adapter = lax.rem(lax.broadcasted_iota(jnp.int32, chosen.shape, 1) // per, adapters)
        lows = jnp.where(adapter == chosen, dot(act_of(), a_cols[...]), 0.0).astype(BF)

        def columns(n):
            at = pl.ds(pl.multiple_of(n * chunk, chunk), chunk)
            act = act_of()
            gate, up = (dot(act, w[kind, :, at]) + scale * dot_rows(lows, bx[kind, at]) for kind in BOTH)
            hid[:, ds, lo * 2 * rows:hi * 2 * rows, at] = (gate * jax.nn.sigmoid(gate) * up).astype(BF).reshape(2, unit_rows, chunk)

        loop(2 * half // chunk, columns)

    gather = Gather(place, lambda part, ds, df: gbuf.at[part, ds, df], send_sem, recv_sem)
    gather.own(*BOTH)
    def turned(kind, i):
        def turn(n):
            at = pl.ds(pl.multiple_of(n * LANE, LANE), LANE)
            w[kind, at, i * half:(i + 1) * half] = raw[i, :, at].T

        loop(width // LANE, turn)

    for kind in BOTH:
        raw_load(kind).wait()
        if kind:
            pl.semaphore_wait(credit, 1)
        pair[kind].start()
        turned(kind, 0)
        if kind == 0:
            wait(loads)
            ends(pair[2:])
        else:
            gather.near()
        pair[kind].wait_recv()
        turned(kind, 1)
        pair[kind].wait_send()
        if kind == 0:
            pl.semaphore_signal(credit, inc=1, device_id={'tensor': place.partner}, device_id_type=MESH)
            raw_load(1).start()
    wait(a_load)
    for copy in pair[2:]:
        copy.wait_recv()
    row, col = (lax.broadcasted_iota(jnp.int32, (adapters * rank, n_low), axis) for axis in BOTH)
    core, chip = col // (n_low // 2), lax.rem(col, n_low // 2) // group
    kind_of, a_of = lax.rem(col, group) // (group // 2), lax.rem(col // per, adapters)
    to = a_of * rank + chip * 2 * per + core * per + lax.rem(col, per)
    for kind in BOTH:
        bx[kind] = dot(b[kind], jnp.where((row == to) & (kind_of == kind), 1.0, 0.0).astype(BF)).astype(BF)
    for core in BOTH:
        for i in RING:

            def turn_a(n):
                at = pl.ds(pl.multiple_of(n * LANE, LANE), LANE)
                to = pl.ds(pl.multiple_of(i * quarter + n * LANE, LANE), LANE)
                a_cols[to, core * n_low // 2:(core + 1) * n_low // 2] = a_ref[core, i // 2, :, :, i % 2, :, at].reshape(n_low // 2, LANE).T

            loop(quarter // LANE, turn_a)
    gather.row()
    unit(OWN)
    for blocks in PAIRS:
        gather.sides(*(j for j in blocks if j != OWN))
        loop(2, lambda i: unit(NEXT + 2 * i, blocks))
    for blocks in PAIRS:
        gather.far(*blocks)
        unit(FAR, blocks)
    gather.sent()
    for copy in pair[2:]:
        copy.wait_send()


def gate_up(ids, sums, gain, x_in, a_all, b_all, w, side, scale, collective_id):
    _, seq_len, depth = x_in.shape
    share = w[0].shape[0]
    adapters, _, rank = w[2].shape
    half = (share + LANE - 1) // LANE * LANE
    hidden = (2, side, side * seq_len // 2, 2 * half)
    n_low = 2 * adapters * rank
    return pl.pallas_call(
        functools.partial(gate_up_kernel, side, adapters, scale),
        out_shape=[pltpu.VMEM(hidden, BF), pltpu.VMEM((seq_len, depth), BF), pltpu.VMEM((2 * half, depth + adapters * rank), BF)],
        in_specs=[SMEM] + [HBM] * (5 + len(w)),
        out_specs=[VMEM] * 3,
        scratch_shapes=[
            pltpu.VMEM((2, side, side, 2, seq_len // 4, depth), BF),
            pltpu.VMEM((2, half, depth), BF),
            pltpu.VMEM((2, depth, 2 * half), BF),
            pltpu.VMEM((2, 2 * half, adapters * rank), BF),
            pltpu.VMEM((2, 2 * half, n_low), BF),
            pltpu.VMEM((1, depth), F32),
            pltpu.VMEM(sums.shape, BF),
            pltpu.VMEM(a_all.shape, BF),
            pltpu.VMEM((depth, n_low), BF),
            pltpu.VMEM(b_all.shape[:4] + b_all.shape[5:], BF),
            DMA, DMA, DMA, DMA, pltpu.SemaphoreType.REGULAR, DMA((5,)), DMA((5,)),
        ] + GATHER_SEMS,
        compiler_params=comm_params(collective_id, VMEM_MOST * 51 // 64),
        name='gate_up',
    )(ids, sums, gain.reshape(1, depth), x_in, a_all, b_all, *w)


def deliver_kernel(side, adapters, scale, ids_ref, sums_ref, x_ref, b_ref, out_ref, pair_send, pair_recv, send_sem, recv_sem):
    place = Place(side)
    place.announce(place.partner)
    seq_len = sums_ref.shape[0]
    rows = seq_len // 4
    chosen = own_rows(place, ids_ref, (seq_len, b_ref.shape[4]))
    y = finish(sums_ref, x_ref[...], b_ref, chosen, scale, adapters).astype(BF)
    for part in BOTH:
        for piece in BOTH:
            at = (2 * part + piece) * rows
            out_ref[place.device(0, 0), part, piece] = y[at:at + rows]
    place.meet()

    def block(part, ds, df):
        return out_ref.at[place.sequence(part, ds, df), part]

    def seen(part, ds, df, half):
        ref = block(part, ds, df) if half is None else block(part, ds, df).at[half]
        remote(ref, ref, pair_send, pair_recv, place.partner).start()

    for part in BOTH:
        seen(part, OWN, OWN, None)
    gather = Gather(place, block, send_sem, recv_sem, absolute=True, seen=seen)
    gather.own(*BOTH)
    gather.near()
    gather.row()
    gather.sides(*AWAY)
    gather.far(*RING)
    gather.sent()
    every = out_ref.at[first(side * side)]
    for sem in (pair_send, pair_recv):
        pltpu.make_async_copy(every, every, sem).wait()


def put_kernel(y_ref, out_ref, sem):
    wait(ends([pltpu.make_async_copy(y_ref.at[i], out_ref.at[i], sem) for i in range(y_ref.shape[0])]))


def deliver(ids, sums, x_mid, b_down, side, scale, collective_id):
    seq_len, depth = x_mid.shape
    rows = seq_len // 4
    y = pl.pallas_call(
        functools.partial(deliver_kernel, side, b_down.shape[1], scale),
        out_shape=pltpu.VMEM((2 * side * side, 2, 2, rows, depth), BF),
        in_specs=[SMEM] + [VMEM] * 3,
        scratch_shapes=[DMA, DMA] + GATHER_SEMS,
        compiler_params=comm_params(collective_id, VMEM_SMALL),
        name='deliver',
    )(ids, sums, x_mid, b_down)
    return pl.pallas_call(
        put_kernel,
        out_shape=jax.ShapeDtypeStruct(y.shape, BF),
        in_specs=[pl.BlockSpec(memory_space=pl.ANY)],
        out_specs=HBM,
        scratch_shapes=[DMA],
        compiler_params=pltpu.CompilerParams(vmem_limit_bytes=VMEM_LEAST),
        name='put',
    )(y)


def solution(mesh):
    tp_size = mesh.shape['tensor']
    side = math.isqrt(tp_size // 2)
    rows_only = P('tensor', None)
    head_split = P(None, 'tensor', None)
    last_split = P(None, None, 'tensor')
    b_head_split = P(None, None, 'tensor', None)
    in_specs = (P('data', None, None), P('data'), P(None), P(None),
                head_split, head_split, head_split, P('tensor', None, None),
                P(None, 'tensor'), P(None, 'tensor'), rows_only,
                last_split, b_head_split, last_split, b_head_split, last_split, b_head_split,
                P(None, 'tensor', None, None), last_split,
                last_split, last_split, last_split, last_split,
                head_split, last_split)

    def local_layer(x_in, adapter_ids, gain_attn, gain_mlp, w_q, w_k, w_v, w_o, w_gate, w_up, w_down, a_q, b_q, a_k, b_k, a_v, b_v, a_o, b_o, a_gate, b_gate, a_up, b_up, a_down, b_down):
        scale = ALPHA / b_q.shape[1]

        def across(a):
            return a.swapaxes(-1, -2)

        heads = [w[:, 0] for w in (w_q, w_k, w_v)] + [across(a) for a in (a_q, a_k, a_v)] + [b[:, :, 0] for b in (b_q, b_k, b_v)]
        sums, all_a, all_b = attend(adapter_ids, x_in, gain_attn, heads, w_o[0], a_o[:, 0], (across(a_gate), across(a_up)), (b_o, b_down), side, scale, 0)

        w = [across(w_gate), across(w_up), across(b_gate), across(b_up), w_down, a_down]
        hidden, x_mid, w_d = gate_up(adapter_ids, sums, gain_mlp, x_in, all_a, all_b, w, side, scale, 1)
        sums, b_d = row_proj(adapter_ids, hidden, w_d, pltpu.with_memory_space_constraint(all_b, pltpu.HBM), *a_o.shape[::3], side, 2)
        y = deliver(adapter_ids, sums, x_mid, b_d, side, scale, 3)
        return y.reshape(x_in.shape)

    return jax.shard_map(local_layer, mesh=mesh, in_specs=in_specs, out_specs=P('data', None, None), check_vma=False)
```

```python
import functools
import math

import jax
import jax.numpy as jnp
import numpy as np
from jax import lax
from jax.experimental import pallas as pl
from jax.experimental.pallas import tpu as pltpu
from jax.sharding import PartitionSpec as P

ALPHA = 16.0
ROPE_BASE = 10000.0
EPSILON = 1e-5
BF = jnp.bfloat16
F32 = jnp.float32
LANE = 128
TILE = 16
VMEM_MOST = 67043328
VMEM_SMALL = VMEM_MOST // 6
VMEM_LEAST = VMEM_MOST // 32
MESH = pl.DeviceIdType.MESH
HBM = pl.BlockSpec(memory_space=pltpu.HBM)
VMEM = pl.BlockSpec(memory_space=pltpu.VMEM)
SMEM = pl.BlockSpec(memory_space=pltpu.SMEM)
DMA = pltpu.SemaphoreType.DMA

OWN, NEXT, FAR, LAST = RING = range(4)
UP, DOWN = BOTH = range(2)
THREE = range(3)
STEP = (NEXT, -NEXT)
FROM = (LAST, NEXT)
AWAY = (NEXT, LAST, FAR)
PAIRS = ((OWN, NEXT), (LAST, FAR))
TOWARD = (NEXT, LAST)
FAST, SLOW = BOTH


def fit(size, most):
    return max(c for c in range(LANE, most + 1, LANE) if size % c == 0)


def first(size):
    return pl.ds(0, size)


def dot(a, b):
    return jnp.dot(a, b, preferred_element_type=F32)


def dot_rows(a, b):
    return lax.dot_general(a, b, (((1,), (1,)), ((), ())), preferred_element_type=F32)


def dot_columns(a, b):
    return lax.dot_general(a, b, (((0,), (0,)), ((), ())), preferred_element_type=F32)


def normed(act, gain):
    return (act * lax.rsqrt(jnp.mean(act * act, axis=-1, keepdims=True) + EPSILON) * gain).astype(BF)


def ends(copies):
    for copy in copies:
        copy.start()
    return copies


def wait(copies):
    for copy in copies:
        copy.wait()


def loop(count, body):
    lax.fori_loop(0, count, lambda i, carry: (body(i), carry)[1], 0)


class Place:
    def __init__(self, side):
        index = lax.axis_index('tensor')
        self.side = side
        self.core = lax.rem(index, 2)
        chip = index // 2
        self.y, self.x = chip // side, lax.rem(chip, side)
        self.partner = index + 1 - 2 * self.core

    def turn(self, at, steps):
        return lax.rem(at + steps + self.side, self.side)

    def device(self, dy, dx):
        return (self.turn(self.y, dy) * self.side + self.turn(self.x, dx)) * 2 + self.core

    def neighbour(self, part, ring, step):
        return self.device(0, step) if part == ring else self.device(step, 0)

    def sequence(self, part, ds, df):
        return self.device(jnp.where(part == 0, ds, df), jnp.where(part == 0, df, ds))

    def rows(self, ref):
        return lambda part, ds: ref.at[part, :, self.turn(self.x, ds)] if part else ref.at[part, self.turn(self.y, ds)]

    def spot(self, part):
        return self.y if part else self.x

    def announce(self, *more):
        to = [self.neighbour(0, ring, step) for ring in BOTH for step in STEP] + list(more)
        for device in to:
            pl.semaphore_signal(pltpu.get_barrier_semaphore(), inc=1, device_id={'tensor': device}, device_id_type=MESH)
        self.announced = len(to)

    def meet(self):
        pl.semaphore_wait(pltpu.get_barrier_semaphore(), self.announced)


def remote(src, dst, send_sem, recv_sem, to):
    return pltpu.make_async_remote_copy(src_ref=src, dst_ref=dst, send_sem=send_sem, recv_sem=recv_sem, device_id={'tensor': to}, device_id_type=MESH)


GATHER_SEMS = [DMA((2, 2, 2, 2, 4))] * 2


class Gather:
    def __init__(self, place, block, send_sem, recv_sem, absolute=False, seen=None):
        self.place, self.block, self.sems, self.absolute, self.seen = place, block, (send_sem, recv_sem), absolute, seen

    def message(self, part, ring, passed, d, j=OWN):
        spot = (lambda s: (s, j)) if ring == SLOW else (lambda s: (OWN, s))
        src, dst = (FROM[d], FAR) if passed else (OWN, FROM[d])
        a, b = self.block(part, *spot(src)), self.block(part, *spot(src if self.absolute else dst))
        if passed:
            a, b = a.at[d], b.at[d]
        return remote(a, b, *(sem.at[part, ring, passed, d, j] for sem in self.sems), self.place.neighbour(part, ring, STEP[d]))

    def arrived(self, part, ring, passed, d, j=OWN):
        self.message(part, ring, passed, d, j).wait_recv()
        if self.seen:
            at = FAR if passed else FROM[d]
            self.seen(part, *((at, j) if ring == SLOW else (OWN, at)), d if passed else None)

    def own(self, *rings):
        for ring in rings:
            for d in BOTH:
                for part in BOTH:
                    self.message(part, ring, 0, d).start()

    def near(self):
        for d in BOTH:
            for part in BOTH:
                self.arrived(part, FAST, 0, d)
                self.message(part, FAST, 1, d).start()
                for e in BOTH:
                    self.message(part, SLOW, 0, e, FROM[d]).start()

    def row(self):
        for part in BOTH:
            for d in BOTH:
                self.arrived(part, FAST, 1, d)
            for e in BOTH:
                self.message(part, SLOW, 0, e, FAR).start()
        self.sides(OWN)

    def sides(self, *blocks):
        for j in blocks:
            for part in BOTH:
                for d in BOTH:
                    self.arrived(part, SLOW, 0, d, j)
                    self.message(part, SLOW, 1, d, j).start()

    def far(self, *blocks):
        for j in blocks:
            for part in BOTH:
                for d in BOTH:
                    self.arrived(part, SLOW, 1, d, j)

    def sent(self):
        for part in BOTH:
            for d in BOTH:
                for passed in BOTH:
                    self.message(part, FAST, passed, d).wait_send()
                    for j in RING:
                        self.message(part, SLOW, passed, d, j).wait_send()


ROW_SEMS = [DMA((2, 2, 2, 2))] * 2


class RowGather:
    def __init__(self, place, row, mine, send_sem, recv_sem):
        self.place, self.row_at, self.mine, self.sems = place, row, mine, (send_sem, recv_sem)

    def message(self, part, ring, passed, d):
        if ring == SLOW:
            ref = self.row_at(part, FROM[d] if passed else OWN)
            ref = ref.at[:, d] if passed else ref
        else:
            ref = self.row_at(part, OWN).at[self.place.turn(self.mine(part), FROM[d] if passed else OWN)]
            ref = ref.at[d] if passed else ref
        return remote(ref, ref, *(sem.at[part, ring, passed, d] for sem in self.sems), self.place.neighbour(part, ring, STEP[d]))

    def pass_on(self, ring, passed):
        for part in BOTH:
            for d in BOTH:
                self.landing(part, ring, passed, d).wait_recv()
                if not passed:
                    self.message(part, ring, 1, d).start()
            if passed and ring == FAST:
                for d in BOTH:
                    self.message(part, SLOW, 0, d).start()

    def landing(self, part, ring, passed, d):
        at = FAR if passed else FROM[d]
        ref = self.row_at(part, at) if ring == SLOW else self.row_at(part, OWN).at[self.place.turn(self.mine(part), at)]
        if passed:
            ref = ref.at[:, d] if ring == SLOW else ref.at[d]
        return remote(ref, ref, *(sem.at[part, ring, passed, d] for sem in self.sems), self.place.neighbour(part, ring, STEP[d]))

    def own(self):
        for d in BOTH:
            for part in BOTH:
                self.message(part, FAST, 0, d).start()

    def near(self):
        self.pass_on(FAST, 0)

    def row(self):
        self.pass_on(FAST, 1)

    def sides(self):
        self.pass_on(SLOW, 0)

    def far(self):
        self.pass_on(SLOW, 1)

    def sent(self):
        for part in BOTH:
            for ring in BOTH:
                for passed in BOTH:
                    for d in BOTH:
                        self.message(part, ring, passed, d).wait_send()


def rows_of_adapter(place, ids_ref, part, ds, shape):
    block = lax.broadcasted_iota(jnp.int32, shape, 0) // (shape[0] // len(RING))
    chosen = jnp.zeros(shape, jnp.int32)
    for df in RING:
        chosen = jnp.where(block == df, ids_ref[place.sequence(part, ds, df)], chosen)
    return chosen


def pick_columns(low, chosen):
    rank = chosen.shape[1]
    kept = low[:, :rank]
    for a in range(1, low.shape[1] // rank):
        kept = jnp.where(chosen == a, low[:, a * rank:(a + 1) * rank], kept)
    return kept


def spread(low, chosen, adapters):
    return jnp.concatenate([jnp.where(chosen == a, low, 0.0) for a in range(adapters)], axis=1).astype(BF)


PASS, FREE, SUM = THREE
FAST_SEMS = [DMA((2, 3, 2))] * 2


def add(into, *others):
    def some(i):
        at = pl.ds(pl.multiple_of(i * TILE, TILE), TILE)
        total = into[at, :].astype(F32)
        for other in others:
            total += other[at, :].astype(F32)
        into[at, :] = total.astype(BF)

    loop(into.shape[0] // TILE, some)


class FastScatter:
    def __init__(self, place, stage, near, landed, send_sem, recv_sem):
        self.place, self.stage, self.near, self.landed, self.sems = place, stage, near, landed, (send_sem, recv_sem)
        quarter = near.shape[2]
        self.halves = (first(quarter), pl.ds(quarter, quarter))

    def message(self, part, kind, d):
        at = self.halves[1 - d] if kind == FREE else self.halves[d]
        src = self.stage(part, FAR if kind == PASS else TOWARD[d]).at[at]
        dst = self.near.at[part, d] if kind == PASS else self.landed.at[part, d, at]
        sems = [sem.at[part, kind, d] for sem in self.sems]
        return remote(src, dst, *sems, self.place.neighbour(part, FAST, STEP[d]))

    def ready(self, part, df):
        for d in BOTH:
            if df == FAR:
                self.message(part, PASS, d).start()
            elif df == TOWARD[d]:
                self.message(part, FREE, d).start()

    def sum(self):
        for d in BOTH:
            for part in BOTH:
                self.message(part, PASS, d).wait_recv()
                add(self.stage(part, TOWARD[d]).at[self.halves[d]], self.near.at[part, d])
                self.message(part, SUM, d).start()

    def finish(self):
        for part in BOTH:
            for d in BOTH:
                self.message(part, FREE, d).wait_recv()
                self.message(part, SUM, d).wait_recv()
            add(self.stage(part, OWN), self.landed.at[part, UP], self.landed.at[part, DOWN])

    def store(self, out_ref):
        rows = self.landed.shape[2]
        for part in BOTH:
            out_ref[part * rows:(part + 1) * rows] = self.stage(part, OWN)[...]

    def sent(self):
        for part in BOTH:
            for kind in THREE:
                for d in BOTH:
                    self.message(part, kind, d).wait_send()


def fast_scratch(rows, cols):
    return [pltpu.VMEM((2, 2, rows // 2, cols), BF), pltpu.VMEM((2, 2, rows, cols), BF)]


def comm_params(collective_id, limit=VMEM_MOST):
    return pltpu.CompilerParams(collective_id=collective_id, has_side_effects=True, vmem_limit_bytes=limit)


WO_CHUNKS = 8
X_SLOTS = 3


def attend_kernel(side, adapters, scale, ids_ref, x_ref, gain_in, cos_in, sin_in, *rest):
    w_heads, a_heads, b_heads, (wo_ref, ao_ref), a_mlp, b_rows, rest = rest[:3], rest[3:6], rest[6:9], rest[9:11], rest[11:13], rest[13:15], rest[15:]
    (out_ref, a_all, b_all), rest = rest[:3], rest[3:]
    (w, a_raw, b_raw, a_rows, bx, xbuf, h, z, lows, att, act, wo, stage, near, landed, am_raw, a_mine, b_mine, gain_ref, cos_ref, sin_ref, pair_send, pair_recv, table_sem, load_sem, x_sem, own_sem,
     kept_sem, hand_send, hand_recv, wo_load, wo_send, wo_recv, bulk_send, bulk_recv, swap_send, swap_recv,
     send_sem, recv_sem, a_send, a_recv, b_send, b_recv, fast_send, fast_recv) = rest
    place = Place(side)
    place.announce(place.partner, place.device(0, FAR), place.device(FAR, 0))
    head, seq_len, depth = cos_ref.shape[1], x_ref.shape[1], x_ref.shape[2]
    cols = len(w_heads) * head
    chips = side * side
    per = a_raw.shape[3]
    steps = chips // 2

    def x_loads(step):
        slot = lax.rem(step, X_SLOTS)
        return [pltpu.make_async_copy(x_ref.at[4 * lax.rem(step, steps) + 2 * i + place.core], xbuf.at[slot, i], x_sem.at[slot]) for i in BOTH]

    own_loads = ends([pltpu.make_async_copy(a_mlp[i], am_raw.at[i], own_sem) for i in BOTH] +
                     [pltpu.make_async_copy(b_rows[half].at[part], b_mine.at[part, place.y, place.x, half], own_sem) for part in BOTH for half in BOTH])
    width = wo_ref.shape[1]
    rank = ao_ref.shape[2]
    wo_loads = []
    for part in BOTH:
        wo_loads.append(pltpu.make_async_copy(wo_ref, wo.at[part, OWN, 0, :, first(width)], wo_load))
        for a in range(adapters):
            wo_loads.append(pltpu.make_async_copy(ao_ref.at[a], wo.at[part, OWN, 0, :, pl.ds(width + a * rank, rank)], wo_load))
    ends(wo_loads)
    loads = ends([pltpu.make_async_copy(src, dst, load_sem) for i in THREE for src, dst in
                  ((a_heads[i], a_raw.at[place.core, i]), (w_heads[i], w.at[:, pl.ds(i * head, head)]), (b_heads[i], b_raw.at[0, i]))])
    for step in range(X_SLOTS - 1):
        ends(x_loads(step))
    tables = ends([pltpu.make_async_copy(src, dst, table_sem) for src, dst in ((gain_in, gain_ref), (cos_in, cos_ref), (sin_in, sin_ref))])
    wait(own_loads)
    am_rows = jnp.concatenate([am_raw[i, a] for i in BOTH for a in range(adapters)], axis=0)
    for i in RING:
        a_mine[i // 2, place.y, place.x, i % 2] = am_rows[:, i * depth // 4:(i + 1) * depth // 4]
    place.meet()
    piece = head // WO_CHUNKS

    def wo_message(part, passed, d, i):
        src, dst = (wo.at[part, s, 0, pl.ds(i * piece, piece)] for s in ((FROM[d], FAR) if passed else (OWN, FROM[d])))
        sems = (part, passed, d, i)
        return remote(src, dst, wo_send.at[sems], wo_recv.at[sems], place.neighbour(part, SLOW, STEP[d]))

    def wo_to_partner(part, s):
        remote(wo.at[part, s, 0], wo.at[part, s, 1], bulk_send, bulk_recv, place.partner).start()

    passes = [range(d * WO_CHUNKS // 2, (d + 1) * WO_CHUNKS // 2) for d in BOTH]

    def wo_start(i):
        for d in BOTH:
            for part in BOTH:
                wo_message(part, 0, d, i).start()

    def wo_pass(k):
        for d in BOTH:
            for part in BOTH:
                wo_message(part, 0, d, passes[d][k]).wait_recv()
                wo_message(part, 1, d, passes[d][k]).start()

    def wo_arrived():
        for d in BOTH:
            for part in BOTH:
                for i in passes[1 - d]:
                    wo_message(part, 0, d, i).wait_recv()
                wo_to_partner(part, FROM[d])

    def wo_last():
        for part in BOTH:
            for d in BOTH:
                for i in passes[d]:
                    wo_message(part, 1, d, i).wait_recv()
            wo_to_partner(part, FAR)

    gathers = [RowGather(place, place.rows(a_mine), place.spot, a_send, a_recv), RowGather(place, place.rows(b_mine), place.spot, b_send, b_recv)]

    of_a, of_b = gathers

    def hand(i, *distances):
        dst = (a_all, b_all)[i]
        for ds in distances:
            for part in BOTH:
                here, there = gathers[i].row_at(part, ds), place.rows(dst.at[place.core])(part, ds)
                pltpu.make_async_copy(here, there, kept_sem.at[i]).start()
                remote(here, there, hand_send.at[i], hand_recv.at[i], place.partner).start()

    def happen(events, step):
        for at, what in events.items():
            pl.when(step == at)(lambda what=what: ([f(*args) for f, *args in what], None)[1])

    wait(wo_loads)
    for i in BOTH:
        wo_start(i)
    of_a.own()
    wait(loads)
    moves = [(a_raw.at[place.core], a_raw.at[place.core]), (w.at[:, first(cols)], w.at[:, pl.ds(cols, cols)]), (b_raw.at[0], b_raw.at[1])]
    pair = ends([remote(src, dst, pair_send.at[i], pair_recv.at[i], place.partner) for i, (src, dst) in enumerate(moves)])
    wait(tables)
    pair[0].wait_recv()
    for core in BOTH:
        pieces = [a_raw[core, i, a] if i < len(w_heads) else jnp.zeros((per, depth), BF) for a in range(adapters) for i in RING]
        a_rows[core * 2 * TILE:(core + 1) * 2 * TILE, :] = jnp.concatenate(pieces, axis=0)
    mine = [(place.y, place.x), (place.x, place.y)]

    low_gather = RowGather(place, lambda part, ds: lows.at[part, place.turn(mine[part][0], ds)], place.spot, send_sem, recv_sem)

    def norm(step, last):
        slot = lax.rem(step, X_SLOTS)

        @pl.when(step + X_SLOTS - 1 < last)
        def _():
            ends(x_loads(step + X_SLOTS - 1))

        wait(x_loads(step))
        for i in BOTH:
            h[i * seq_len:(i + 1) * seq_len, :] = normed(xbuf[slot, i].astype(F32), gain_ref[...])

    def products(step):
        happen({0: [(wo_start, 2)], 2: [(of_b.own,), (wo_start, 3)], 3: [(wo_start, 4)]}, step)
        norm(step, 2 * steps)
        low = dot_rows(a_rows[...], h[...])
        half, at = step // (steps // 2), lax.rem(step, steps // 2) * 2 * seq_len
        for part in BOTH:
            pieces = []
            for i in BOTH:
                options = [low[TILE * (2 * part + a):TILE * (2 * part + a + 1), i * seq_len:(i + 1) * seq_len] for a in range(adapters)]
                chosen = options[0]
                for a in range(1, adapters):
                    chosen = jnp.where(ids_ref[4 * step + 2 * i + place.core] == a, options[a], chosen)
                pieces.append(chosen)
            lows[part, mine[part][0], mine[part][1], half, :, pl.ds(pl.multiple_of(at, LANE), 2 * seq_len)] = jnp.concatenate(pieces, axis=1).astype(BF)

    loop(steps, products)
    low_gather.own()
    for copy in pair[1:]:
        copy.wait_recv()
    for part in BOTH:
        wo_to_partner(part, OWN)
    second = {1: [(wo_start, 5)], 2: [(low_gather.near,), (wo_start, 6)], 3: [(of_a.near,)], 4: [(low_gather.row,)], 5: [(of_b.near,)],
              6: [(wo_start, 7), (wo_pass, 0)], 9: [(low_gather.sides,), (of_b.row,), (hand, 1, OWN)], 13: [(wo_pass, 1)], 15: [(wo_pass, 2)]}

    def project(step):
        happen(second, 2 * step)
        norm(step + steps, 2 * steps)
        happen(second, 2 * step + 1)
        rows = pl.ds(pl.multiple_of(step * 2 * seq_len, LANE), 2 * seq_len)
        chunk = fit(2 * cols, 256)
        for n in range(2 * cols // chunk):
            z[rows, n * chunk:(n + 1) * chunk] = dot(h[...], w[:, n * chunk:(n + 1) * chunk])

    loop(steps, project)
    row, col = (lax.broadcasted_iota(jnp.int32, (2 * rank, rank), axis) for axis in BOTH)
    spot, kind = row // TILE, lax.rem(row, TILE) // per
    for part in BOTH:
        chip_of = spot if part == 0 else lax.rem(spot, side) * side + spot // side
        to = chip_of * 2 * per + part * per + lax.rem(row, per)
        for i in THREE:
            spread_rows = jnp.where((kind == i) & (col == to), 1.0, 0.0).astype(BF)
            for a in range(adapters):
                for o in BOTH:
                    bx[a, part, :, o * cols + i * head:o * cols + (i + 1) * head] = dot(spread_rows, b_raw[o, i, a]).astype(BF)
    low_gather.far()
    causal = lax.broadcasted_iota(jnp.int32, (seq_len, seq_len), 0) >= lax.broadcasted_iota(jnp.int32, (seq_len, seq_len), 1)

    def swap(part, ds):
        sems = (part, ds)
        to = place.neighbour(part, SLOW, ds)
        return remote(att.at[sems], act.at[part, lax.rem(len(RING) - ds, len(RING))], swap_send.at[sems], swap_recv.at[sems], to)

    def attention(i):
        dy, dx = side - 1 - i // side, side - 1 - lax.rem(i, side)
        chip = place.turn(place.y, dy) * side + place.turn(place.x, dx)
        adapter = ids_ref[2 * chip + place.core]
        half, at = chip // steps, pl.ds(pl.multiple_of(lax.rem(chip, steps) * seq_len, LANE), seq_len)
        zs = z[pl.ds(pl.multiple_of(chip * seq_len, LANE), seq_len), :]
        for part in BOTH:
            zs += scale * dot_columns(lows[part, :, :, half, :, at].reshape(-1, seq_len), bx[adapter, part])
        for i_head in BOTH:
            q, k, v = (zs[:, i_head * cols + i * head:i_head * cols + (i + 1) * head] for i in THREE)
            q, k = ((r * cos_ref[...] + pltpu.roll(r, head // 2, axis=1) * sin_ref[...]).astype(BF) for r in (q, k))
            scores = jnp.where(causal, dot_rows(q, k) * head ** -0.5, -1e30)
            e = jnp.exp(scores - jnp.max(scores, axis=-1, keepdims=True))
            prob = (e / jnp.sum(e, axis=-1, keepdims=True)).astype(BF)
            mixed = dot(prob, v.astype(BF)).astype(BF)
            for part, (ds, df) in enumerate(((dy, dx), (dx, dy))):
                att[part, ds, df, :, i_head * head:(i_head + 1) * head] = mixed[part * seq_len // 2:(part + 1) * seq_len // 2]

    def attention_pair(k):
        for i in BOTH:
            attention(2 * k + i)
        happen({0: [(wo_pass, 3)]}, k)
        row = side - 1 - 2 * k // side
        pl.when((lax.rem(2 * k + 2, side) == 0) & (row != OWN))(lambda: swap(0, row).start())

    loop(chips // 2, attention_pair)
    for ds in AWAY:
        swap(1, ds).start()
    of_a.row()
    hand(0, OWN)
    of_b.sides()
    hand(1, NEXT, LAST)
    wo_arrived()
    wo_last()
    for part in BOTH:
        act[part, OWN] = att[part, OWN]
    pltpu.make_async_copy(wo.at[:, :, 1], wo.at[:, :, 1], bulk_recv).wait()
    chunk = fit(width, 512)
    rows = seq_len // 2
    blocks = (len(RING), rows)
    fast = FastScatter(place, lambda part, df: stage.at[part, df], near, landed, fast_send, fast_recv)

    def sum_heads(part, at):
        return sum(dot(act[part, s].reshape(-1, 2 * head), wo[part, s, :, :, at].reshape(2 * head, -1)) for s in RING)

    for part in BOTH:
        for ds in AWAY:
            swap(part, ds).wait_recv()

        def columns(n):
            at = pl.ds(pl.multiple_of(n * chunk, chunk), chunk)
            stage[part, :, :, at] = sum_heads(part, at).reshape(blocks + (chunk,)).astype(BF)

        loop(width // chunk, columns)
        chosen = rows_of_adapter(place, ids_ref, part, OWN, (len(RING) * rows, rank))
        stage[part, :, :, width:] = pick_columns(sum_heads(part, pl.ds(width, adapters * rank)), chosen).reshape(blocks + (rank,)).astype(BF)
        for df in (FAR, NEXT, LAST):
            fast.ready(part, df)
    of_a.sides()
    hand(0, NEXT, LAST)
    fast.sum()
    for i in BOTH:
        gathers[1 - i].far()
        hand(1 - i, FAR)
    fast.finish()
    out = ends([pltpu.make_async_copy(stage.at[part, OWN], out_ref.at[pl.ds(part * rows, rows)], load_sem) for part in BOTH])
    fast.sent()
    for sem in (kept_sem, hand_send, hand_recv):
        for i, ref in enumerate((a_mine, b_mine)):
            pltpu.make_async_copy(ref, ref, sem.at[i]).wait()
    for copy in pair:
        copy.wait_send()
    for g in gathers + [low_gather]:
        g.sent()
    pltpu.make_async_copy(wo.at[:, :, 1], wo.at[:, :, 1], bulk_send).wait()
    for part in BOTH:
        for d in BOTH:
            for i in range(WO_CHUNKS):
                wo_message(part, 0, d, i).wait_send()
            for i in passes[d]:
                wo_message(part, 1, d, i).wait_send()
        for ds in AWAY:
            swap(part, ds).wait_send()
    wait(out)


def attend(ids, x_in, gain, heads, w_o, a_o, a_mlp, b_rows, side, scale, collective_id):
    _, seq_len, depth = x_in.shape
    head = heads[0].shape[1]
    cols = 3 * head
    adapters, _, rank = a_o.shape
    per = heads[3].shape[1]
    chips = side * side
    half_dim = head // 2
    inv_freq = ROPE_BASE ** (-2.0 * np.arange(half_dim) / head)
    angle = np.arange(seq_len)[:, None] * inv_freq[None, :]
    cos, sin = np.cos(angle), np.sin(angle)
    tables = [jnp.asarray(np.concatenate(pair, axis=1), F32) for pair in ((cos, cos), (-sin, sin))]
    n_pair = 3
    rows, out_cols = seq_len // 2, depth + rank
    every = (2, 2, side, side, 2)
    return pl.pallas_call(
        functools.partial(attend_kernel, side, adapters, scale),
        out_shape=[jax.ShapeDtypeStruct((seq_len, out_cols), BF), jax.ShapeDtypeStruct(every + (2 * adapters * per, depth // 4), BF),
                   jax.ShapeDtypeStruct(every + b_rows[0].shape[1:], BF)],
        in_specs=[SMEM] + [HBM] * (4 + len(heads) + 6),
        out_specs=[HBM] * 3,
        scratch_shapes=[
            pltpu.VMEM((depth, 2 * cols), BF),
            pltpu.VMEM((2, 3, adapters, per, depth), BF),
            pltpu.VMEM((2, 3, adapters, rank, head), BF),
            pltpu.VMEM((2 * 2 * TILE, depth), BF),
            pltpu.VMEM((adapters, 2, 2 * rank, 2 * cols), BF),
            pltpu.VMEM((X_SLOTS, 2, seq_len, depth), BF),
            pltpu.VMEM((2 * seq_len, depth), BF),
            pltpu.VMEM((chips * seq_len, 2 * cols), F32),
            pltpu.VMEM((2, side, side, 2, TILE, chips * seq_len // 2), BF),
            pltpu.VMEM((2, side, side, rows, 2 * head), BF),
            pltpu.VMEM((2, side, side, rows, 2 * head), BF),
            pltpu.VMEM((2, side, 2, head, depth + adapters * rank), BF),
            pltpu.VMEM((2, side, rows, out_cols), BF),
        ] + fast_scratch(rows, out_cols) + [
            pltpu.VMEM((2, adapters, per, depth), BF),
            pltpu.VMEM(every[1:] + (2 * adapters * per, depth // 4), BF),
            pltpu.VMEM(every[1:] + b_rows[0].shape[1:], BF),
            pltpu.VMEM((1, depth), F32),
            pltpu.VMEM(tables[0].shape, F32),
            pltpu.VMEM(tables[0].shape, F32),
            DMA((n_pair,)), DMA((n_pair,)), DMA, DMA, DMA((X_SLOTS,)), DMA, DMA((2,)), DMA((2,)), DMA((2,)), DMA, DMA((2, 2, 2, WO_CHUNKS)), DMA((2, 2, 2, WO_CHUNKS)), DMA, DMA, DMA((2, 4)), DMA((2, 4)),
        ] + ROW_SEMS * 3 + FAST_SEMS,
        compiler_params=comm_params(collective_id),
        name='attend',
    )(ids, x_in, gain.reshape(1, depth), *tables, *heads, w_o, a_o, *a_mlp, *b_rows)


def row_proj_kernel(side, adapters, rank, ids_ref, act, w, b_all, out_ref, b_ref, b_sem, stage, near, landed, fast_near, fast_landed, slow_send, slow_recv, fast_send, fast_recv):
    place = Place(side)
    place.announce()
    rows, cols = stage.shape[3:]
    quarter = rows // 2
    b_load = ends([pltpu.make_async_copy(b_all.at[:, :, :, :, 1], b_ref, b_sem)])
    width = cols - rank
    chunk = fit(width, 1024)

    def unit(part, ds):
        def columns(n):
            at = pl.ds(pl.multiple_of(n * chunk, chunk), chunk)
            stage[part, ds, :, :, at] = dot(act[part, ds], w[:, at]).reshape(len(RING), rows, chunk).astype(BF)

        loop(width // chunk, columns)
        chosen = rows_of_adapter(place, ids_ref, part, ds, (len(RING) * rows, rank))
        stage[part, ds, :, :, width:] = pick_columns(dot(act[part, ds], w[:, width:]), chosen).reshape(len(RING), rows, rank).astype(BF)

    blocks = ((FAR, LAST), (OWN, NEXT))

    def slow(part, kind, d, i):
        df = blocks[1 - d][i] if kind == FREE else blocks[d][i]
        sems = (part, kind, d, i)
        src = stage.at[part, FAR if kind == PASS else TOWARD[d], df]
        dst = near.at[part, d, i] if kind == PASS else landed.at[part, d, df]
        return remote(src, dst, slow_send.at[sems], slow_recv.at[sems], place.neighbour(part, SLOW, STEP[d]))

    fast = FastScatter(place, lambda part, df: stage.at[part, OWN, df], fast_near, fast_landed, fast_send, fast_recv)
    for part in BOTH:
        unit(part, FAR)
        if part == 0:
            place.meet()
        for i in BOTH:
            for d in BOTH:
                slow(part, PASS, d, i).start()
    loop(len(RING), lambda i: unit(lax.rem(i, 2), NEXT + 2 * (i // 2)))
    for i in BOTH:
        for d in BOTH:
            for part in BOTH:
                slow(part, FREE, d, i).start()
    loop(2, lambda part: unit(part, OWN))
    for i in BOTH:
        for d in BOTH:
            for part in BOTH:
                slow(part, PASS, d, i).wait_recv()
                add(stage.at[part, TOWARD[d], blocks[d][i]], near.at[part, d, i])
                slow(part, SUM, d, i).start()
    for i in BOTH:
        for d in BOTH:
            df = blocks[d][i]
            for part in BOTH:
                slow(part, SUM, d, i).wait_recv()
                slow(part, FREE, 1 - d, i).wait_recv()
                add(stage.at[part, OWN, df], landed.at[part, UP, df], landed.at[part, DOWN, df])
                fast.ready(part, df)
    fast.sum()
    fast.finish()
    fast.store(out_ref)
    fast.sent()
    wait(b_load)
    for part in BOTH:
        for kind in THREE:
            for d in BOTH:
                for i in BOTH:
                    slow(part, kind, d, i).wait_send()


def row_proj(ids, act, w, b_all, adapters, rank, side, collective_id):
    rows = act.shape[2] // side
    cols = w.shape[1] - (adapters - 1) * rank
    blocks = (rows, cols)
    return pl.pallas_call(
        functools.partial(row_proj_kernel, side, adapters, rank),
        out_shape=[pltpu.VMEM((2 * rows, cols), BF), pltpu.VMEM(b_all.shape[:4] + b_all.shape[5:], BF)],
        in_specs=[SMEM, VMEM, VMEM, HBM],
        out_specs=[VMEM, VMEM],
        scratch_shapes=[
            DMA,
            pltpu.VMEM((2, side, side) + blocks, BF),
            pltpu.VMEM((2, 2, 2) + blocks, BF),
            pltpu.VMEM((2, 2, side) + blocks, BF),
        ] + fast_scratch(rows, cols) + [DMA((2, 3, 2, 2))] * 2 + FAST_SEMS,
        compiler_params=comm_params(collective_id, VMEM_MOST * 9 // 16),
        name='row_proj',
    )(ids, act, w, b_all)


def finish(sums_ref, resid, b_ref, chosen, scale, adapters):
    _, _, side, _, rank, part = b_ref.shape
    width = sums_ref.shape[1] - rank
    low = spread(sums_ref[:, width:].astype(F32), chosen, adapters)
    delta = [dot(low, b_ref[core, :, y, x].reshape(adapters * rank, part)) for y in range(side) for x in range(side) for core in BOTH]
    return resid.astype(F32) + (sums_ref[:, :width].astype(F32) + scale * jnp.concatenate(delta, axis=1))


def own_rows(place, ids_ref, shape):
    return jnp.full(shape, ids_ref[place.device(0, 0)], jnp.int32)


def gate_up_kernel(side, adapters, scale, ids_ref, sums_in, gain_in, x_all, a_all, b_all, wg_ref, wu_ref, bg_ref, bu_ref, wd_ref, ad_ref,
                   hid, mid_ref, wd, gbuf, raw, w, b, bx, gain_ref, sums_ref, a_ref, a_cols, b_ref, raw_sem, load_sem, a_sem, b_sem, credit, pair_send, pair_recv, send_sem, recv_sem):
    place = Place(side)
    share, width = wg_ref.shape
    half = raw.shape[1]
    rank = bg_ref.shape[2]
    seq_len = sums_ref.shape[0]
    edge = share // TILE * TILE
    for i in BOTH:
        raw[i, edge:] = jnp.zeros((half - edge, width), BF)
        for kind in BOTH:
            b[kind, i * half + edge:(i + 1) * half] = jnp.zeros((half - edge, adapters * rank), BF)
        wd[i * half + edge:(i + 1) * half] = jnp.zeros((half - edge, wd.shape[1]), BF)
    place.announce(place.partner)
    b_load = ends([pltpu.make_async_copy(b_all.at[:, :, :, :, 0], b_ref, b_sem), pltpu.make_async_copy(x_all.at[place.device(0, 0)], mid_ref, b_sem),
                   pltpu.make_async_copy(gain_in, gain_ref, b_sem), pltpu.make_async_copy(sums_in, sums_ref, b_sem)])
    a_load = ends([pltpu.make_async_copy(a_all, a_ref, a_sem)])
    mine = first(share)

    def raw_load(kind):
        return pltpu.make_async_copy((wg_ref, wu_ref)[kind], raw.at[0, mine], raw_sem)

    raw_load(0).start()
    loads = [pltpu.make_async_copy(wd_ref, wd.at[mine, first(width)], load_sem)]
    for a in range(adapters):
        loads.append(pltpu.make_async_copy(ad_ref.at[a], wd.at[mine, pl.ds(width + a * rank, rank)], load_sem))
        for kind, ref in enumerate((bg_ref, bu_ref)):
            loads.append(pltpu.make_async_copy(ref.at[a], b.at[kind, mine, pl.ds(a * rank, rank)], load_sem))
    ends(loads)
    other = pl.ds(half, share)
    moves = [(raw.at[0, mine], raw.at[1, mine])] * 2 + [(wd.at[mine], wd.at[other])] + [(b.at[kind, mine], b.at[kind, other]) for kind in BOTH]
    pair = [remote(src, dst, pair_send.at[i], pair_recv.at[i], place.partner) for i, (src, dst) in enumerate(moves)]
    rows = seq_len // 4
    chosen = own_rows(place, ids_ref, (seq_len, rank))
    wait(b_load)
    mid = finish(sums_ref, mid_ref[...], b_ref, chosen, scale, adapters).astype(BF)
    mid_ref[...] = mid
    h2 = normed(mid.astype(F32), gain_ref[...])
    for part in BOTH:
        for piece in BOTH:
            at = (2 * part + piece) * rows
            gbuf[part, OWN, OWN, piece] = h2[at:at + rows]
    place.meet()
    chunk = fit(2 * half, 256)

    group, quarter = a_ref.shape[5:]
    n_low = 2 * side * side * group
    per = group // (2 * adapters)

    def unit(ds, blocks=RING):
        lo, hi = min(blocks), max(blocks) + 1
        unit_rows = (hi - lo) * 2 * rows
        act_of = lambda: gbuf[:, ds, lo:hi].reshape(2 * unit_rows, width)
        chosen = jnp.concatenate([rows_of_adapter(place, ids_ref, part, ds, (len(RING) * 2 * rows, n_low))[lo * 2 * rows:hi * 2 * rows] for part in BOTH], axis=0)
        adapter = lax.rem(lax.broadcasted_iota(jnp.int32, chosen.shape, 1) // per, adapters)
        lows = jnp.where(adapter == chosen, dot(act_of(), a_cols[...]), 0.0).astype(BF)

        def columns(n):
            at = pl.ds(pl.multiple_of(n * chunk, chunk), chunk)
            act = act_of()
            gate, up = (dot(act, w[kind, :, at]) + scale * dot_rows(lows, bx[kind, at]) for kind in BOTH)
            hid[:, ds, lo * 2 * rows:hi * 2 * rows, at] = (gate * jax.nn.sigmoid(gate) * up).astype(BF).reshape(2, unit_rows, chunk)

        loop(2 * half // chunk, columns)

    gather = Gather(place, lambda part, ds, df: gbuf.at[part, ds, df], send_sem, recv_sem)
    gather.own(*BOTH)
    def turned(kind, i):
        def turn(n):
            at = pl.ds(pl.multiple_of(n * LANE, LANE), LANE)
            w[kind, at, i * half:(i + 1) * half] = raw[i, :, at].T

        loop(width // LANE, turn)

    for kind in BOTH:
        raw_load(kind).wait()
        if kind:
            pl.semaphore_wait(credit, 1)
        pair[kind].start()
        turned(kind, 0)
        if kind == 0:
            wait(loads)
            ends(pair[2:])
        else:
            gather.near()
        pair[kind].wait_recv()
        turned(kind, 1)
        pair[kind].wait_send()
        if kind == 0:
            pl.semaphore_signal(credit, inc=1, device_id={'tensor': place.partner}, device_id_type=MESH)
            raw_load(1).start()
    wait(a_load)
    for copy in pair[2:]:
        copy.wait_recv()
    row, col = (lax.broadcasted_iota(jnp.int32, (adapters * rank, n_low), axis) for axis in BOTH)
    core, chip = col // (n_low // 2), lax.rem(col, n_low // 2) // group
    kind_of, a_of = lax.rem(col, group) // (group // 2), lax.rem(col // per, adapters)
    to = a_of * rank + chip * 2 * per + core * per + lax.rem(col, per)
    for kind in BOTH:
        bx[kind] = dot(b[kind], jnp.where((row == to) & (kind_of == kind), 1.0, 0.0).astype(BF)).astype(BF)
    for core in BOTH:
        for i in RING:

            def turn_a(n):
                at = pl.ds(pl.multiple_of(n * LANE, LANE), LANE)
                to = pl.ds(pl.multiple_of(i * quarter + n * LANE, LANE), LANE)
                a_cols[to, core * n_low // 2:(core + 1) * n_low // 2] = a_ref[core, i // 2, :, :, i % 2, :, at].reshape(n_low // 2, LANE).T

            loop(quarter // LANE, turn_a)
    gather.row()
    unit(OWN)
    for blocks in PAIRS:
        gather.sides(*(j for j in blocks if j != OWN))
        loop(2, lambda i: unit(NEXT + 2 * i, blocks))
    for blocks in PAIRS:
        gather.far(*blocks)
        unit(FAR, blocks)
    gather.sent()
    for copy in pair[2:]:
        copy.wait_send()


def gate_up(ids, sums, gain, x_in, a_all, b_all, w, side, scale, collective_id):
    _, seq_len, depth = x_in.shape
    share = w[0].shape[0]
    adapters, _, rank = w[2].shape
    half = (share + LANE - 1) // LANE * LANE
    hidden = (2, side, side * seq_len // 2, 2 * half)
    n_low = 2 * adapters * rank
    return pl.pallas_call(
        functools.partial(gate_up_kernel, side, adapters, scale),
        out_shape=[pltpu.VMEM(hidden, BF), pltpu.VMEM((seq_len, depth), BF), pltpu.VMEM((2 * half, depth + adapters * rank), BF)],
        in_specs=[SMEM] + [HBM] * (5 + len(w)),
        out_specs=[VMEM] * 3,
        scratch_shapes=[
            pltpu.VMEM((2, side, side, 2, seq_len // 4, depth), BF),
            pltpu.VMEM((2, half, depth), BF),
            pltpu.VMEM((2, depth, 2 * half), BF),
            pltpu.VMEM((2, 2 * half, adapters * rank), BF),
            pltpu.VMEM((2, 2 * half, n_low), BF),
            pltpu.VMEM((1, depth), F32),
            pltpu.VMEM(sums.shape, BF),
            pltpu.VMEM(a_all.shape, BF),
            pltpu.VMEM((depth, n_low), BF),
            pltpu.VMEM(b_all.shape[:4] + b_all.shape[5:], BF),
            DMA, DMA, DMA, DMA, pltpu.SemaphoreType.REGULAR, DMA((5,)), DMA((5,)),
        ] + GATHER_SEMS,
        compiler_params=comm_params(collective_id, VMEM_MOST * 51 // 64),
        name='gate_up',
    )(ids, sums, gain.reshape(1, depth), x_in, a_all, b_all, *w)


def deliver_kernel(side, adapters, scale, ids_ref, sums_ref, x_ref, b_ref, out_ref, pair_send, pair_recv, send_sem, recv_sem):
    place = Place(side)
    place.announce(place.partner)
    seq_len = sums_ref.shape[0]
    rows = seq_len // 4
    chosen = own_rows(place, ids_ref, (seq_len, b_ref.shape[4]))
    y = finish(sums_ref, x_ref[...], b_ref, chosen, scale, adapters).astype(BF)
    for part in BOTH:
        for piece in BOTH:
            at = (2 * part + piece) * rows
            out_ref[place.device(0, 0), part, piece] = y[at:at + rows]
    place.meet()

    def block(part, ds, df):
        return out_ref.at[place.sequence(part, ds, df), part]

    def seen(part, ds, df, half):
        ref = block(part, ds, df) if half is None else block(part, ds, df).at[half]
        remote(ref, ref, pair_send, pair_recv, place.partner).start()

    for part in BOTH:
        seen(part, OWN, OWN, None)
    gather = Gather(place, block, send_sem, recv_sem, absolute=True, seen=seen)
    gather.own(*BOTH)
    gather.near()
    gather.row()
    gather.sides(*AWAY)
    gather.far(*RING)
    gather.sent()
    every = out_ref.at[first(side * side)]
    for sem in (pair_send, pair_recv):
        pltpu.make_async_copy(every, every, sem).wait()


def put_kernel(y_ref, out_ref, sem):
    wait(ends([pltpu.make_async_copy(y_ref.at[i], out_ref.at[i], sem) for i in range(y_ref.shape[0])]))


def deliver(ids, sums, x_mid, b_down, side, scale, collective_id):
    seq_len, depth = x_mid.shape
    rows = seq_len // 4
    y = pl.pallas_call(
        functools.partial(deliver_kernel, side, b_down.shape[1], scale),
        out_shape=pltpu.VMEM((2 * side * side, 2, 2, rows, depth), BF),
        in_specs=[SMEM] + [VMEM] * 3,
        scratch_shapes=[DMA, DMA] + GATHER_SEMS,
        compiler_params=comm_params(collective_id, VMEM_SMALL),
        name='deliver',
    )(ids, sums, x_mid, b_down)
    return pl.pallas_call(
        put_kernel,
        out_shape=jax.ShapeDtypeStruct(y.shape, BF),
        in_specs=[pl.BlockSpec(memory_space=pl.ANY)],
        out_specs=HBM,
        scratch_shapes=[DMA],
        compiler_params=pltpu.CompilerParams(vmem_limit_bytes=VMEM_LEAST),
        name='put',
    )(y)


def solution(mesh):
    tp_size = mesh.shape['tensor']
    side = math.isqrt(tp_size // 2)
    rows_only = P('tensor', None)
    head_split = P(None, 'tensor', None)
    last_split = P(None, None, 'tensor')
    b_head_split = P(None, None, 'tensor', None)
    in_specs = (P('data', None, None), P('data'), P(None), P(None),
                head_split, head_split, head_split, P('tensor', None, None),
                P(None, 'tensor'), P(None, 'tensor'), rows_only,
                last_split, b_head_split, last_split, b_head_split, last_split, b_head_split,
                P(None, 'tensor', None, None), last_split,
                last_split, last_split, last_split, last_split,
                head_split, last_split)

    def local_layer(x_in, adapter_ids, gain_attn, gain_mlp, w_q, w_k, w_v, w_o, w_gate, w_up, w_down, a_q, b_q, a_k, b_k, a_v, b_v, a_o, b_o, a_gate, b_gate, a_up, b_up, a_down, b_down):
        scale = ALPHA / b_q.shape[1]

        def across(a):
            return a.swapaxes(-1, -2)

        heads = [w[:, 0] for w in (w_q, w_k, w_v)] + [across(a) for a in (a_q, a_k, a_v)] + [b[:, :, 0] for b in (b_q, b_k, b_v)]
        sums, all_a, all_b = attend(adapter_ids, x_in, gain_attn, heads, w_o[0], a_o[:, 0], (across(a_gate), across(a_up)), (b_o, b_down), side, scale, 0)

        w = [across(w_gate), across(w_up), across(b_gate), across(b_up), w_down, a_down]
        hidden, x_mid, w_d = gate_up(adapter_ids, sums, gain_mlp, x_in, all_a, all_b, w, side, scale, 1)
        sums, b_d = row_proj(adapter_ids, hidden, w_d, pltpu.with_memory_space_constraint(all_b, pltpu.HBM), *a_o.shape[::3], side, 2)
        y = deliver(adapter_ids, sums, x_mid, b_d, side, scale, 3)
        return y.reshape(x_in.shape)

    return jax.shard_map(local_layer, mesh=mesh, in_specs=in_specs, out_specs=P('data', None, None), check_vma=False)
```
